32 devices in a mesh: dp: 4 (over y, x), expert: 4 (over z), tensor: 2 (over core).
Axes of the slice: x: 2, y: 2, z: 4, core: 2. Of those that a mesh axis runs over, the one named last changes fastest.
Arguments:
- tokens_in: bfloat16 [12608, 512], P(('dp', 'expert')), may hold values from -6 to 6
- expert_ids: int32 [12608, 2], P(('dp', 'expert')), may hold values from 0 to 7, all different within a row; in each aligned block of 788 rows (0 to 787, 788 to 1575, ...) at most 248 rows name the same one
- combine: float32 [12608, 2], P(('dp', 'expert')), may hold values from 0.2 to 1
- out_cot: float32 [12608, 512], P(('dp', 'expert')), may hold values from -6 to 6
- inward_master: float32 [512, 1536], P('dp', 'tensor'), may hold values from -0.25 to 0.25
- outward_master: float32 [512, 512], P('dp', 'tensor'), may hold values from -1 to 1
- up_master: float32 [512, 8, 2048], P('dp', 'expert', 'tensor'), may hold values from -0.25 to 0.25
- down_master: float32 [512, 8, 2048], P('dp', 'expert', 'tensor'), may hold values from -0.125 to 0.125
- norm_gains: float32 [2, 512], replicated, may hold values from 0.5 to 1.5
- norm_biases: float32 [2, 512], replicated, may hold values from -2 to 2
- inward_moment: float32 [512, 1536], P('dp', 'tensor'), may hold values from -32 to 32
- outward_moment: float32 [512, 512], P('dp', 'tensor'), may hold values from -64 to 64
- up_moment: float32 [512, 8, 2048], P('dp', 'expert', 'tensor'), may hold values from -64 to 64
- down_moment: float32 [512, 8, 2048], P('dp', 'expert', 'tensor'), may hold values from -64 to 64
- first_moment: float32 [4, 512], replicated, may hold values from -64 to 64
- second_moment: float32 [4, 512], replicated, may hold values from 2.5216 to 25.216
- step_count: int32 [1], replicated, may hold values from 1 to 20
Outputs:
- block_out: bfloat16 [12608, 512], P(('dp', 'expert'))
- input_gradient: float32 [12608, 512], P(('dp', 'expert'))
- inward_gradient: float32 [512, 1536], P('dp', 'tensor')
- outward_gradient: float32 [512, 512], P('dp', 'tensor')
- up_gradient: float32 [512, 8, 2048], P('dp', 'expert', 'tensor')
- down_gradient: float32 [512, 8, 2048], P('dp', 'expert', 'tensor')
- gain_gradient: float32 [2, 512], replicated
- bias_gradient: float32 [2, 512], replicated
- inward_moment_new: float32 [512, 1536], P('dp', 'tensor')
- outward_moment_new: float32 [512, 512], P('dp', 'tensor')
- up_moment_new: float32 [512, 8, 2048], P('dp', 'expert', 'tensor')
- down_moment_new: float32 [512, 8, 2048], P('dp', 'expert', 'tensor')
- inward_new: float32 [512, 1536], P('dp', 'tensor')
- outward_new: float32 [512, 512], P('dp', 'tensor')
- up_new: float32 [512, 8, 2048], P('dp', 'expert', 'tensor')
- down_new: float32 [512, 8, 2048], P('dp', 'expert', 'tensor')
- inward_copy: bfloat16 [512, 1536], P('dp', 'tensor')
- outward_copy: bfloat16 [512, 512], P('dp', 'tensor')
- up_copy: bfloat16 [512, 8, 2048], P('dp', 'expert', 'tensor')
- down_copy: bfloat16 [512, 8, 2048], P('dp', 'expert', 'tensor')
- gains_new: float32 [2, 512], replicated
- biases_new: float32 [2, 512], replicated
- first_new: float32 [4, 512], replicated
- second_new: float32 [4, 512], replicated
The draws below stay inside these ranges and needn't reach their ends.
Inputs may be any that keep to these rules, and one draw needn't show every extreme that they name: `expert_ids`: the two ids of a row differ. Within the 788 rows of one device, no expert is named by more than 248 rows, a bound that some block reaches.
All inputs are finite; a program needn't handle non-finite values.
Results may differ from the reference program's by a relative error of at most 0.0095.
The reference program's roundings to bfloat16 on the way count: a program that leaves them out, or rounds other values in their place, can miss the bound.
Values may be sent and summed in bfloat16 or wider, within the bound.
A program may use at most 192 MiB of HBM per device.

```python
import math
import jax
import jax.numpy as jnp
import numpy as np
from jax import lax

D = 512
HEADS = 8
HD = 64
F = 2048
SEQ = 197
TOP = 2
IMG_DEV = 4
EXPERTS = 8
TOK_DEV = 788
TOKENS = 12608
CAP = 248
N_DP = 4
N_EXPERT = 4
N_TENSOR = 2


def shard_levels(stream_key, dims, cuts, smallest, top_value):
    def one(dim, blocks):
        draws = jax.random.uniform(jax.random.fold_in(jax.random.fold_in(stream_key, 6), dim), (blocks,), jnp.float32, smallest / len(cuts), top_value / len(cuts))
        return jnp.repeat(jnp.exp(draws), dims[dim] // blocks).reshape((-1,) + (1,) * (len(dims) - dim - 1))

    level = one(*cuts[0])
    for cut in cuts[1:]:
        level = level * one(*cut)
    return level


def assign_block(stream_key, own, number, rows, count, top, most, lean):
    ranking = jax.random.permutation(stream_key, count)
    packed, usual = shares(count, rows * top, most, lean, True), shares(count, rows * top, most, lean, False)
    places = jnp.arange(count)

    def named(sizes, turn):
        used = int((sizes > 0).sum())
        fixed = max(1, used // 4)
        passed = fixed + (places - fixed + turn * (used - fixed)) % max(1, count - fixed)
        return jnp.zeros((count,), jnp.int32).at[ranking[jnp.where(places < fixed, places, passed)]].set(jnp.asarray(sizes, jnp.int32))

    sizes = jnp.where(number % 4 == 0, named(packed, number // 4), named(usual, number - number // 4 - 1))
    mixed = jax.random.permutation(jax.random.fold_in(own, 3), count)
    donor, taker = mixed[0:count // 2 * 2:2], mixed[1:count // 2 * 2:2]
    margin = jnp.minimum(sizes[donor] - 1, most - sizes[taker]) // 2
    margin = jnp.where((donor == ranking[0]) | (taker == ranking[0]) | (sizes[taker] == 0), 0, jnp.maximum(margin, 0))
    passed = jax.random.randint(jax.random.fold_in(own, 4), (count // 2,), 0, 1 << 20) % (margin + 1)
    sizes = sizes.at[donor].add(-passed).at[taker].add(passed)
    members = jnp.searchsorted(jnp.cumsum(sizes), jnp.arange(rows * top), side="right").astype(jnp.int32)
    listing = members.reshape(top, rows).T
    listing = listing[jax.random.permutation(jax.random.fold_in(own, 1), rows)]
    turn = jax.random.randint(jax.random.fold_in(own, 2), (rows, 1), 0, top)
    return jnp.take_along_axis(listing, (jnp.arange(top)[None, :] + turn) % top, axis=1)


def shares(number_of, total, limit, lean, full):
    weights = [(1 << 20) // math.isqrt(grade ** lean) + 1 for grade in range(1, number_of + 1)]
    largest = limit if full else min(limit, max(-(-total // number_of), total * weights[0] // sum(weights)))
    least = 1 if total - largest >= number_of - 1 else 0
    given, rest = [largest] + [least] * (number_of - 1), total - largest - least * (number_of - 1)
    while rest > 0:
        free = [i for i in range(1, number_of) if given[i] < largest] or [i for i in range(1, number_of) if given[i] < limit]
        mass, left = sum([weights[i] for i in free]), rest
        for i in free:
            addition = min(limit - given[i], max(1, left * weights[i] // mass), rest)
            given[i] = given[i] + addition
            rest = rest - addition
    return np.array(given)


def gaussian(rng, shape, deviation, reach, shards=(), held_as=jnp.bfloat16):
    drawn = jax.random.normal(rng, shape, jnp.float32) * deviation
    if len(shards) > 0:
        drawn = shard_levels(rng, shape, shards, -0.22, 0.18) * drawn
    return jnp.clip(drawn, min=-reach, max=reach).astype(held_as)


def setup_inputs(seed: int = 0) -> dict:
    seeds = jax.random.split(jax.random.key(seed), 18)
    tokens_in = gaussian(seeds[0], (TOKENS, D), 1.0, 6.0, ((0, 16),))
    expert_ids_keys = jax.random.split(jax.random.fold_in(seeds[1], 1), TOKENS // TOK_DEV)
    expert_ids_turns = jax.random.permutation(jax.random.fold_in(seeds[1], 3), TOKENS // TOK_DEV)
    expert_ids = jax.vmap(lambda own, number: assign_block(jax.random.fold_in(seeds[1], 2), own, number, TOK_DEV, EXPERTS, TOP, CAP, 1))(expert_ids_keys, expert_ids_turns).reshape((TOKENS, TOP))
    combine = jnp.clip(0.2 + 0.8 * jax.random.uniform(seeds[2], (TOKENS, TOP), jnp.float32) ** shard_levels(seeds[2], (TOKENS, TOP), ((0, 16),), -0.2, 0.2), 0.2, 1.0)
    out_cot = gaussian(seeds[3], (TOKENS, D), 1.0, 6.0, ((0, 16),), jnp.float32)
    inward_master = gaussian(seeds[4], (D, 3 * D), D ** -0.5, 0.25, ((0, 4), (1, 2)), jnp.float32)
    outward_master = gaussian(seeds[5], (D, D), (D // 16) ** -0.5, 1.0, ((0, 4), (1, 2)), jnp.float32)
    up_master = gaussian(seeds[6], (D, EXPERTS, F), D ** -0.5, 0.25, ((0, 4), (1, 4), (2, 2)), jnp.float32)
    down_master = gaussian(seeds[7], (D, EXPERTS, F), F ** -0.5, 0.125, ((0, 4), (1, 4), (2, 2)), jnp.float32)
    norm_gains = jnp.clip(1.0 + 0.1 * jax.random.normal(seeds[8], (2, D), jnp.float32), 0.5, 1.5)
    norm_biases = gaussian(seeds[9], (2, D), 0.3, 2.0, (), jnp.float32)
    inward_moment = gaussian(seeds[10], (D, 3 * D), (0.05 * TOKENS ** 0.5), 32.0, ((0, 4), (1, 2)), jnp.float32)
    outward_moment = gaussian(seeds[11], (D, D), (0.1 * TOKENS ** 0.5), 64.0, ((0, 4), (1, 2)), jnp.float32)
    up_moment = gaussian(seeds[12], (D, EXPERTS, F), (0.2 * (TOK_DEV * N_DP) ** 0.5), 64.0, ((0, 4), (1, 4), (2, 2)), jnp.float32)
    down_moment = gaussian(seeds[13], (D, EXPERTS, F), (0.2 * (TOK_DEV * N_DP) ** 0.5), 64.0, ((0, 4), (1, 4), (2, 2)), jnp.float32)
    first_moment = gaussian(seeds[14], (4, D), (0.1 * TOKENS ** 0.5), 64.0, (), jnp.float32)
    second_moment = jnp.clip(jnp.exp(jax.random.uniform(seeds[15], (4, D), jnp.float32, math.log(2.5216), math.log(25.216))), 2.5216, 25.216)
    step_count = jax.random.randint(seeds[16], (1,), 1, 21).astype(jnp.int32)
    return {"tokens_in": tokens_in, "expert_ids": expert_ids, "combine": combine, "out_cot": out_cot, "inward_master": inward_master, "outward_master": outward_master, "up_master": up_master, "down_master": down_master, "norm_gains": norm_gains, "norm_biases": norm_biases, "inward_moment": inward_moment, "outward_moment": outward_moment, "up_moment": up_moment, "down_moment": down_moment, "first_moment": first_moment, "second_moment": second_moment, "step_count": step_count}


@jax.custom_vjp
def low(v):
    return lax.optimization_barrier(v.astype(jnp.bfloat16)).astype(jnp.float32)

@jax.custom_vjp
def low_back(v):
    return v

def low_keep(v):
    return (low(v), None)

def low_pass(kept, grad):
    return (grad,)

def back_keep(v):
    return (v, None)

def back_low(kept, grad):
    return (low(grad),)
low.defvjp(low_keep, low_pass)
low_back.defvjp(back_keep, back_low)

def layer_norm(values, gain_row, bias_row):
    center = values - lax.optimization_barrier(jnp.mean(values, axis=-1, keepdims=True))
    spread = lax.optimization_barrier(jnp.mean(center * center, axis=-1, keepdims=True))
    return center * lax.rsqrt(spread + 1e-06) * gain_row + bias_row

def newton_schulz(matrix):
    current = matrix / (jnp.sqrt(jnp.sum(matrix * matrix)) + 1e-07)
    for sweep_index in range(5):
        gram_matrix = jnp.dot(current, current.T, precision=lax.Precision.HIGHEST)
        polynom = -4.775 * gram_matrix + 2.0315 * jnp.dot(gram_matrix, gram_matrix, precision=lax.Precision.HIGHEST)
        current = 3.4445 * current + jnp.dot(polynom, current, precision=lax.Precision.HIGHEST)
    return current

def routing(expert_ids):
    groups = N_DP * N_EXPERT
    chosen = expert_ids.reshape(groups, TOK_DEV, TOP)
    expert_lanes = jnp.arange(EXPERTS, dtype=jnp.int32)
    route_hits = (chosen[:, :, :, None] == expert_lanes).astype(jnp.int32)
    per_token = lax.optimization_barrier(jnp.sum(route_hits, axis=2)).astype(jnp.int32)
    earlier = (jnp.cumsum(per_token, axis=1) - per_token).astype(jnp.int32)
    position = lax.optimization_barrier(jnp.sum(route_hits * earlier[:, :, None, :], axis=3)).astype(jnp.int32)
    group_ids = jnp.broadcast_to(jnp.arange(groups, dtype=jnp.int32)[:, None, None], position.shape)
    return (group_ids, chosen, position)

def make_forward(expert_ids, combine):
    group_ids, chosen, position = routing(expert_ids)
    groups = N_DP * N_EXPERT
    block_width = F // N_TENSOR

    def attend(block):
        query_part, key_part, value_part = block
        scores = low_back(jnp.einsum('bihd,bjhd->bhij', query_part, key_part, precision=lax.Precision.HIGHEST) * HD ** (-0.5))
        softmax_out = low(jax.nn.softmax(scores, axis=-1))
        return jnp.einsum('bhij,bjhd->bihd', softmax_out, value_part, precision=lax.Precision.HIGHEST)

    def forward(inputs, inward_w, outward_w, up_w, down_w, gains, biases):
        normed1 = low(layer_norm(inputs, gains[0], biases[0]))
        qkv_all = low_back(low(jnp.dot(normed1, low(inward_w), precision=lax.Precision.HIGHEST)))
        split_heads = qkv_all.reshape(groups, IMG_DEV, SEQ, HEADS, 3, HD)
        heads = lax.map(jax.checkpoint(attend), (split_heads[..., 0, :], split_heads[..., 1, :], split_heads[..., 2, :]))
        heads = low_back(low(heads.reshape(TOKENS, D)))
        attended = low_back(jnp.dot(heads, low(outward_w).T, precision=lax.Precision.HIGHEST))
        state = inputs + attended
        normed2 = low(layer_norm(state, gains[1], biases[1]))
        spread_rows = jnp.broadcast_to(normed2.reshape(groups, TOK_DEV, 1, D), (groups, TOK_DEV, TOP, D))
        buffer = jnp.zeros((groups, EXPERTS, CAP, D), jnp.float32).at[group_ids, chosen, position].add(spread_rows)
        entries = buffer.transpose(1, 0, 2, 3).reshape(EXPERTS, groups * CAP, D)
        up_parts = low(up_w).reshape(D, EXPERTS, N_TENSOR, block_width).transpose(2, 1, 0, 3)
        down_parts = low(down_w).reshape(D, EXPERTS, N_TENSOR, block_width).transpose(2, 1, 0, 3)

        def expert_part(weights):
            up_part, down_part = weights
            entry = low_back(entries)
            pre_act = low_back(jnp.einsum('erd,edf->erf', entry, up_part, precision=lax.Precision.HIGHEST))
            hidden = low(jax.nn.gelu(pre_act, approximate=False))
            return low_back(low(jnp.einsum('erf,edf->erd', hidden, down_part, precision=lax.Precision.HIGHEST)))

        def accumulate(running, weights):
            return (running + jax.checkpoint(expert_part)(weights), None)
        outputs, unused = lax.scan(accumulate, jnp.zeros((EXPERTS, groups * CAP, D), jnp.float32), (up_parts, down_parts))
        slots = outputs.reshape(EXPERTS, groups, CAP, D).transpose(1, 0, 2, 3)
        routed = slots[group_ids, chosen, position]
        mixed = lax.optimization_barrier(jnp.sum(routed * combine.reshape(groups, TOK_DEV, TOP, 1), axis=2)).reshape(TOKENS, D)
        return state + mixed
    return forward

def reference(tokens_in, expert_ids, combine, out_cot, inward_master, outward_master, up_master, down_master, norm_gains, norm_biases, inward_moment, outward_moment, up_moment, down_moment, first_moment, second_moment, step_count):
    forward = make_forward(expert_ids, combine)
    inputs = tokens_in.astype(jnp.float32)
    output, pullback = jax.vjp(forward, inputs, inward_master, outward_master, up_master, down_master, norm_gains, norm_biases)
    input_gradient, inward_gradient, outward_gradient, up_gradient, down_gradient, gain_gradient, bias_gradient = pullback(out_cot)
    inward_next = 0.95 * inward_moment + inward_gradient
    outward_next = 0.95 * outward_moment + outward_gradient
    up_next = 0.95 * up_moment + up_gradient
    down_next = 0.95 * down_moment + down_gradient
    inward_step = newton_schulz(inward_next) * (0.2 * math.sqrt(3 * D))
    outward_step = newton_schulz(outward_next) * (0.2 * math.sqrt(D))
    up_step = lax.map(newton_schulz, up_next.transpose(1, 0, 2)).transpose(1, 0, 2) * (0.2 * math.sqrt(F))
    down_step = lax.map(newton_schulz, down_next.transpose(1, 0, 2)).transpose(1, 0, 2) * (0.2 * math.sqrt(F))
    inward_new = inward_master - 0.1 * (inward_step + 0.1 * inward_master)
    outward_new = outward_master - 0.1 * (outward_step + 0.1 * outward_master)
    up_new = up_master - 0.1 * (up_step + 0.1 * up_master)
    down_new = down_master - 0.1 * (down_step + 0.1 * down_master)
    vector_grad = jnp.concatenate([gain_gradient, bias_gradient], axis=0)
    first_new = 0.9 * first_moment + 0.1 * vector_grad
    second_new = 0.999 * second_moment + 0.001 * vector_grad * vector_grad
    steps_done = step_count[0].astype(jnp.float32)
    direction = first_new / (1.0 - jnp.power(0.9, steps_done)) / (jnp.sqrt(second_new / (1.0 - jnp.power(0.999, steps_done))) + 1e-08)
    params_new = jnp.concatenate([norm_gains, norm_biases], axis=0) - 0.1 * direction
    return (output.astype(jnp.bfloat16), input_gradient, inward_gradient, outward_gradient, up_gradient, down_gradient, gain_gradient, bias_gradient, inward_next, outward_next, up_next, down_next, inward_new, outward_new, up_new, down_new, inward_new.astype(jnp.bfloat16), outward_new.astype(jnp.bfloat16), up_new.astype(jnp.bfloat16), down_new.astype(jnp.bfloat16), params_new[0:2], params_new[2:4], first_new, second_new)
```

```python
import math

import jax
import jax.numpy as jnp
import numpy as np
from jax import lax
from jax.sharding import PartitionSpec as P

D = 512
HD = 64
F = 2048
SEQ = 197
EXP_DEV = 2


def layer_norm(values, gain_row, bias_row):
    center = values - jnp.mean(values, axis=-1, keepdims=True)
    invert = lax.rsqrt(jnp.mean(center * center, axis=-1, keepdims=True) + 1e-06)
    scaled = center * invert
    return (scaled * gain_row + bias_row, scaled, invert)


def norm_backward(upstream, scaled, invert, gain_row):
    weighted = upstream * gain_row
    return invert * (
        weighted
        - jnp.mean(weighted, axis=-1, keepdims=True)
        - scaled * jnp.mean(weighted * scaled, axis=-1, keepdims=True)
    )


def gelu_exact(values):
    return 0.5 * values * (1.0 + lax.erf(values * 0.7071067811865476))


def gelu_slope(values):
    return 0.5 * (
        1.0 + lax.erf(values * 0.7071067811865476)
    ) + values * 0.3989422804014327 * jnp.exp(-0.5 * values * values)


def newton_schulz(matrix):
    current = matrix / (jnp.sqrt(jnp.sum(matrix * matrix)) + 1e-07)
    for sweep_index in range(5):
        gram_matrix = jnp.dot(current, current.T, precision=lax.Precision.HIGHEST)
        polynom = -4.775 * gram_matrix + 2.0315 * jnp.dot(
            gram_matrix, gram_matrix, precision=lax.Precision.HIGHEST
        )
        current = 3.4445 * current + jnp.dot(polynom, current, precision=lax.Precision.HIGHEST)
    return current


def start_body(
    tokens_in,
    expert_ids,
    combine,
    out_cot,
    inward_master,
    outward_master,
    up_master,
    down_master,
    norm_gains,
    norm_biases,
    inward_moment,
    outward_moment,
    up_moment,
    down_moment,
    first_moment,
    second_moment,
    step_count,
):
    dp_count = lax.axis_size("dp")
    expert_count = lax.axis_size("expert")
    tensor_count = lax.axis_size("tensor")
    token_rows = tokens_in.shape[0]
    expert_total = EXP_DEV * expert_count
    capacity = (token_rows * 10 // (4 * expert_total) + 7) // 8 * 8
    slot_total = expert_total * capacity
    inputs = tokens_in.astype(jnp.float32)
    w_inward, w_outward, w_up, w_down = (
        lax.all_gather(inward_master.astype(jnp.bfloat16), "dp", axis=0, tiled=True),
        lax.all_gather(outward_master.astype(jnp.bfloat16), "dp", axis=0, tiled=True),
        lax.all_gather(up_master.astype(jnp.bfloat16), "dp", axis=0, tiled=True),
        lax.all_gather(down_master.astype(jnp.bfloat16), "dp", axis=0, tiled=True),
    )
    expert_lanes = jnp.arange(expert_total, dtype=jnp.int32)
    route_hits = (expert_ids[:, :, None] == expert_lanes).astype(jnp.int32)
    per_token = jnp.sum(route_hits, axis=1)
    earlier = jnp.cumsum(per_token, axis=0) - per_token
    position = jnp.sum(route_hits * earlier[:, None, :], axis=2)
    target = expert_ids * capacity + position
    select = (target[:, :, None] == jnp.arange(slot_total, dtype=jnp.int32)).astype(jnp.bfloat16)
    normed1, scaled1, invert1 = layer_norm(inputs, norm_gains[0], norm_biases[0])
    normed1_low = normed1.astype(jnp.bfloat16)
    qkv_low = jnp.dot(normed1_low, w_inward, preferred_element_type=jnp.float32).astype(
        jnp.bfloat16
    )
    heads_here = w_inward.shape[1] // (3 * HD)
    images = token_rows // SEQ
    split_heads = qkv_low.reshape(images, SEQ, heads_here, 3, HD)
    query_part = split_heads[:, :, :, 0]
    key_part = split_heads[:, :, :, 1]
    value_part = split_heads[:, :, :, 2]
    score_scale = HD ** (-0.5)
    scores = (
        jnp.einsum("bihd,bjhd->bhij", query_part, key_part, preferred_element_type=jnp.float32)
        * score_scale
    )
    row_max = jnp.max(scores, axis=-1, keepdims=True)
    exponent = jnp.exp(scores - row_max)
    row_total = jnp.sum(exponent, axis=-1, keepdims=True)
    softmax_out = exponent / row_total
    softmax_low = softmax_out.astype(jnp.bfloat16)
    heads_out = (
        jnp.einsum("bhij,bjhd->bihd", softmax_low, value_part, preferred_element_type=jnp.float32)
        .astype(jnp.bfloat16)
        .reshape(token_rows, heads_here * HD)
    )
    attend_part = jnp.einsum("tc,dc->td", heads_out, w_outward, preferred_element_type=jnp.float32)
    attended = lax.psum(attend_part, "tensor")
    state = inputs + attended
    normed2, scaled2, invert2 = layer_norm(state, norm_gains[1], norm_biases[1])
    normed2_low = normed2.astype(jnp.bfloat16)
    slots_out = jnp.einsum(
        "tks,td->sd", select, normed2_low, preferred_element_type=jnp.float32
    ).astype(jnp.bfloat16)
    arrived = lax.all_to_all(
        slots_out.reshape(expert_count, EXP_DEV, capacity, D),
        "expert",
        split_axis=0,
        concat_axis=0,
        tiled=True,
    )
    pre_act = jnp.einsum("secd,def->secf", arrived, w_up, preferred_element_type=jnp.float32)
    hidden_low = gelu_exact(pre_act).astype(jnp.bfloat16)
    expert_part = jnp.einsum(
        "secf,def->secd", hidden_low, w_down, preferred_element_type=jnp.float32
    ).astype(jnp.bfloat16)
    returned = lax.all_to_all(expert_part, "expert", split_axis=0, concat_axis=0, tiled=True)
    routed = jnp.einsum(
        "tks,sd->tkd", select, returned.reshape(slot_total, D), preferred_element_type=jnp.float32
    )
    mixed_part = jnp.sum(routed * combine[:, :, None], axis=1)
    mixed_sum = lax.psum(mixed_part, "tensor")
    block_out = (state + mixed_sum).astype(jnp.bfloat16)
    routed_grad = (combine[:, :, None] * out_cot[:, None, :]).astype(jnp.bfloat16)
    slot_grad = jnp.einsum(
        "tks,tkd->sd", select, routed_grad, preferred_element_type=jnp.float32
    ).astype(jnp.bfloat16)
    grad_arrived = lax.all_to_all(
        slot_grad.reshape(expert_count, EXP_DEV, capacity, D),
        "expert",
        split_axis=0,
        concat_axis=0,
        tiled=True,
    )
    hidden_grad = jnp.einsum(
        "secd,def->secf", grad_arrived, w_down, preferred_element_type=jnp.float32
    )
    pre_grad = (hidden_grad * gelu_slope(pre_act)).astype(jnp.bfloat16)
    down_local = jnp.einsum(
        "secd,secf->def", grad_arrived, hidden_low, preferred_element_type=jnp.float32
    )
    up_local = jnp.einsum("secd,secf->def", arrived, pre_grad, preferred_element_type=jnp.float32)
    entry_grad = jnp.einsum(
        "secf,def->secd", pre_grad, w_up, preferred_element_type=jnp.float32
    ).astype(jnp.bfloat16)
    entry_back = lax.all_to_all(entry_grad, "expert", split_axis=0, concat_axis=0, tiled=True)
    normed2_part = jnp.einsum(
        "tks,sd->td", select, entry_back.reshape(slot_total, D), preferred_element_type=jnp.float32
    )
    normed2_grad = lax.psum(normed2_part, "tensor")
    state_grad = out_cot + norm_backward(normed2_grad, scaled2, invert2, norm_gains[1])
    state_low = state_grad.astype(jnp.bfloat16)
    outward_local = jnp.einsum(
        "td,tc->dc", state_low, heads_out, preferred_element_type=jnp.float32
    )
    heads_grad = (
        jnp.dot(state_low, w_outward, preferred_element_type=jnp.float32)
        .astype(jnp.bfloat16)
        .reshape(images, SEQ, heads_here, HD)
    )
    prob_grad = jnp.einsum(
        "bihd,bjhd->bhij", heads_grad, value_part, preferred_element_type=jnp.float32
    )
    score_grad = (
        softmax_out * (prob_grad - jnp.sum(softmax_out * prob_grad, axis=-1, keepdims=True))
    ).astype(jnp.bfloat16)
    query_grad = (
        jnp.einsum("bhij,bjhd->bihd", score_grad, key_part, preferred_element_type=jnp.float32)
        * score_scale
    )
    key_grad = (
        jnp.einsum("bhij,bihd->bjhd", score_grad, query_part, preferred_element_type=jnp.float32)
        * score_scale
    )
    value_grad = jnp.einsum(
        "bhij,bihd->bjhd", softmax_low, heads_grad, preferred_element_type=jnp.float32
    )
    qkv_grad = (
        jnp.stack([query_grad, key_grad, value_grad], axis=3)
        .reshape(token_rows, heads_here * 3 * HD)
        .astype(jnp.bfloat16)
    )
    inward_local = jnp.einsum(
        "td,tc->dc", normed1_low, qkv_grad, preferred_element_type=jnp.float32
    )
    normed1_part = jnp.einsum("tc,dc->td", qkv_grad, w_inward, preferred_element_type=jnp.float32)
    normed1_grad = lax.psum(normed1_part, "tensor")
    input_gradient = state_grad + norm_backward(normed1_grad, scaled1, invert1, norm_gains[0])
    norm_terms = jnp.stack(
        [
            jnp.sum(normed1_grad * scaled1, axis=0),
            jnp.sum(normed2_grad * scaled2, axis=0),
            jnp.sum(normed1_grad, axis=0),
            jnp.sum(normed2_grad, axis=0),
        ]
    )
    inward_total, outward_total, norm_total = lax.psum(
        (inward_local, outward_local, norm_terms), ("dp", "expert")
    )
    up_gradient, down_gradient = (
        lax.psum_scatter(up_local, "dp", scatter_dimension=0, tiled=True),
        lax.psum_scatter(down_local, "dp", scatter_dimension=0, tiled=True),
    )
    shard_rows = D // dp_count
    dp_here = lax.axis_index("dp")
    inward_gradient = lax.dynamic_slice_in_dim(inward_total, dp_here * shard_rows, shard_rows, 0)
    outward_gradient = lax.dynamic_slice_in_dim(outward_total, dp_here * shard_rows, shard_rows, 0)
    inward_next = 0.95 * inward_moment + inward_gradient
    outward_next = 0.95 * outward_moment + outward_gradient
    up_next = 0.95 * up_moment + up_gradient
    down_next = 0.95 * down_moment + down_gradient
    matrices = [up_next[:, expert_slot] for expert_slot in range(EXP_DEV)]
    matrices = matrices + [down_next[:, expert_slot] for expert_slot in range(EXP_DEV)]
    matrices = matrices + [jnp.concatenate([inward_next, outward_next], axis=1)]
    stacked = jnp.stack(matrices)
    slot_count = len(matrices)
    group_size = dp_count * tensor_count
    shard_width = stacked.shape[2]
    query_cols = inward_next.shape[1]

    def orth_expert(pieces):
        whole_matrix = pieces.transpose(0, 2, 1, 3).reshape(D, tensor_count * shard_width)
        result = newton_schulz(whole_matrix) * (0.2 * math.sqrt(F))
        return result.reshape(dp_count, shard_rows, tensor_count, shard_width).transpose(0, 2, 1, 3)

    def orth_attention(pieces):
        inward_whole = (
            pieces[..., :query_cols].transpose(0, 2, 1, 3).reshape(D, tensor_count * query_cols)
        )
        outward_whole = (
            pieces[..., query_cols:]
            .transpose(0, 2, 1, 3)
            .reshape(D, tensor_count * (shard_width - query_cols))
        )
        inward_result = newton_schulz(inward_whole) * (0.2 * math.sqrt(3 * D))
        outward_result = newton_schulz(outward_whole) * (0.2 * math.sqrt(D))
        inward_blocks = inward_result.reshape(
            dp_count, shard_rows, tensor_count, query_cols
        ).transpose(0, 2, 1, 3)
        outward_blocks = outward_result.reshape(
            dp_count, shard_rows, tensor_count, shard_width - query_cols
        ).transpose(0, 2, 1, 3)
        return jnp.concatenate([inward_blocks, outward_blocks], axis=3)

    owner_index = lax.axis_index(("dp", "tensor"))
    outgoing = stacked[np.arange(group_size) % slot_count]
    received = lax.all_to_all(outgoing, ("dp", "tensor"), split_axis=0, concat_axis=0, tiled=True)
    blocks = received.reshape(dp_count, tensor_count, shard_rows, shard_width)
    slot_here = owner_index % slot_count
    result_blocks = lax.cond(slot_here == slot_count - 1, orth_attention, orth_expert, blocks)
    arrived_steps = lax.all_to_all(
        result_blocks.reshape(group_size, shard_rows, shard_width),
        ("dp", "tensor"),
        split_axis=0,
        concat_axis=0,
        tiled=True,
    )
    picked = []
    for owned_slot in range(slot_count):
        replicas = (group_size - owned_slot + slot_count - 1) // slot_count
        source = owned_slot + slot_count * (owner_index % replicas)
        picked.append(lax.dynamic_index_in_dim(arrived_steps, source, 0, keepdims=False))
    up_step = jnp.stack(picked[0:EXP_DEV], axis=1)
    down_step = jnp.stack(picked[EXP_DEV : 2 * EXP_DEV], axis=1)
    attend_step = picked[2 * EXP_DEV]
    inward_new = inward_master - 0.1 * (attend_step[:, :query_cols] + 0.1 * inward_master)
    outward_new = outward_master - 0.1 * (attend_step[:, query_cols:] + 0.1 * outward_master)
    up_new = up_master - 0.1 * (up_step + 0.1 * up_master)
    down_new = down_master - 0.1 * (down_step + 0.1 * down_master)
    moment_first = 0.9 * first_moment + 0.1 * norm_total
    moment_second = 0.999 * second_moment + 0.001 * norm_total * norm_total
    steps_done = step_count[0].astype(jnp.float32)
    direction = (
        moment_first
        / (1.0 - jnp.power(0.9, steps_done))
        / (jnp.sqrt(moment_second / (1.0 - jnp.power(0.999, steps_done))) + 1e-08)
    )
    params_new = jnp.concatenate([norm_gains, norm_biases], axis=0) - 0.1 * direction
    return (
        block_out,
        input_gradient,
        inward_gradient,
        outward_gradient,
        up_gradient,
        down_gradient,
        norm_total[0:2],
        norm_total[2:4],
        inward_next,
        outward_next,
        up_next,
        down_next,
        inward_new,
        outward_new,
        up_new,
        down_new,
        inward_new.astype(jnp.bfloat16),
        outward_new.astype(jnp.bfloat16),
        up_new.astype(jnp.bfloat16),
        down_new.astype(jnp.bfloat16),
        params_new[0:2],
        params_new[2:4],
        moment_first,
        moment_second,
    )


PAIRS = (1, 2, 3)


def by_peer(blocks, me):
    low, high = (me & 1) == 1, (me & 2) == 2
    half = [jnp.where(low, blocks[k ^ 1], blocks[k]) for k in range(4)]
    return [jnp.where(high, half[k ^ 2], half[k]) for k in range(4)]


def swap_dp(value, k):
    return lax.ppermute(value, "dp", [(i, i ^ k) for i in range(4)])


def swap_expert(value, k):
    return lax.ppermute(value, "expert", [(i, i ^ k) for i in range(4)])


def swap_core(value):
    return lax.ppermute(value, "tensor", [(0, 1), (1, 0)])


def from_peers(swap, blocks):
    return [blocks[0]] + [swap(blocks[k], k) for k in PAIRS]


def dot3(left, right):
    return jnp.dot(left, right, precision=lax.Precision.HIGH)


def orth_factor(gram):
    norm = jnp.sqrt(jnp.trace(gram)) + 1e-07
    current = gram / (norm * norm)
    factor = None
    for sweep_index in range(5):
        change = -4.775 * current + 2.0315 * dot3(current, current)
        if factor is None:
            factor = 3.4445 * jnp.eye(D, dtype=jnp.float32) + change
        else:
            factor = 3.4445 * factor + dot3(change, factor)
        if sweep_index < 4:
            scaled = 3.4445 * current + dot3(change, current)
            current = 3.4445 * scaled + dot3(scaled, change)
    return factor / norm


def pair_body(
    tokens_in,
    expert_ids,
    combine,
    out_cot,
    inward_master,
    outward_master,
    up_master,
    down_master,
    norm_gains,
    norm_biases,
    inward_moment,
    outward_moment,
    up_moment,
    down_moment,
    first_moment,
    second_moment,
    step_count,
):
    bf16, f32 = jnp.bfloat16, jnp.float32
    dp_here, expert_here, core = (lax.axis_index(a) for a in ("dp", "expert", "tensor"))
    first_core = core == 0
    token_rows = tokens_in.shape[0]
    expert_total = EXP_DEV * 4
    capacity = (token_rows * 10 // (4 * expert_total) + 7) // 8 * 8
    slot_total = expert_total * capacity
    shard_rows = D // 4
    qcols = inward_master.shape[1]
    width = up_master.shape[2]

    def matmul(spec, a, b):
        return jnp.einsum(spec, a, b, preferred_element_type=f32)

    attend_shard = jnp.concatenate([inward_master, outward_master], axis=1).astype(bf16)
    attend_w = jnp.concatenate(
        by_peer(from_peers(swap_dp, [attend_shard] * 4), dp_here), axis=0
    )
    w_inward, w_outward = attend_w[:, :qcols], attend_w[:, qcols:]
    w_outward_other = swap_core(w_outward)
    expert_shard = jnp.stack(
        [up_master[:, 0], up_master[:, 1], down_master[:, 0], down_master[:, 1]]
    ).astype(bf16)
    expert_w = jnp.concatenate(
        by_peer(from_peers(swap_dp, [expert_shard] * 4), dp_here), axis=1
    )
    w_up, w_down = expert_w[:2], expert_w[2:]
    moment_rows = [up_moment[:, 0], up_moment[:, 1], down_moment[:, 0], down_moment[:, 1]]
    moment_whole = jnp.concatenate(
        by_peer(from_peers(swap_dp, by_peer(moment_rows, dp_here)), dp_here), axis=0
    )

    expert_lanes = jnp.arange(expert_total, dtype=jnp.int32)
    route_hits = (expert_ids[:, :, None] == expert_lanes).astype(jnp.int32)
    per_token = jnp.sum(route_hits, axis=1)
    earlier = jnp.cumsum(per_token, axis=0) - per_token
    position = jnp.sum(route_hits * earlier[:, None, :], axis=2)
    target = expert_ids * capacity + position
    select = (target[:, :, None] == jnp.arange(slot_total, dtype=jnp.int32)).astype(bf16)
    own_slots = (
        (2 * jnp.arange(4, dtype=jnp.int32)[:, None] + core) * capacity
        + jnp.arange(capacity, dtype=jnp.int32)[None]
    ).reshape(-1)
    own_select = (target[:, :, None] == own_slots).astype(bf16)

    def to_experts(slots):
        chunks = by_peer([slots[j * capacity : (j + 1) * capacity] for j in range(4)], expert_here)
        mine = jnp.concatenate(from_peers(swap_expert, chunks), axis=0)
        other = swap_core(mine)
        return jnp.stack([jnp.where(first_core, mine, other), jnp.where(first_core, other, mine)])

    def to_tokens(parts):
        mine = jnp.where(first_core, parts[0], parts[1])
        gone = jnp.where(first_core, parts[1], parts[0])
        total = (mine.astype(f32) + swap_core(gone).astype(f32)).astype(bf16)
        chunks = from_peers(
            swap_expert, [total[k * capacity : (k + 1) * capacity] for k in range(4)]
        )
        mine = jnp.stack(by_peer(chunks, expert_here))
        other = swap_core(mine)
        return jnp.stack(
            [jnp.where(first_core, mine, other), jnp.where(first_core, other, mine)], axis=1
        ).reshape(slot_total, D)

    routed_grad = (combine[:, :, None] * out_cot[:, None, :]).astype(bf16)
    slot_grad = matmul("tks,tkd->sd", own_select, routed_grad).astype(bf16)
    grad_arrived = to_experts(slot_grad)

    inputs = tokens_in.astype(f32)
    normed1, scaled1, invert1 = layer_norm(inputs, norm_gains[0], norm_biases[0])
    normed1_low = normed1.astype(bf16)
    qkv_low = jnp.dot(normed1_low, w_inward, preferred_element_type=f32).astype(bf16)
    heads_here = qcols // (3 * HD)
    images = token_rows // SEQ
    split_heads = qkv_low.reshape(images, SEQ, heads_here, 3, HD)
    query_part = split_heads[:, :, :, 0]
    key_part = split_heads[:, :, :, 1]
    value_part = split_heads[:, :, :, 2]
    score_scale = HD ** (-0.5)
    scores = matmul("bihd,bjhd->bhij", query_part, key_part) * score_scale
    row_max = jnp.max(scores, axis=-1, keepdims=True)
    exponent = jnp.exp(scores - row_max)
    softmax_out = exponent / jnp.sum(exponent, axis=-1, keepdims=True)
    softmax_low = softmax_out.astype(bf16)
    heads_out = (
        matmul("bhij,bjhd->bihd", softmax_low, value_part)
        .astype(bf16)
        .reshape(token_rows, heads_here * HD)
    )
    heads_other = swap_core(heads_out)
    attended = matmul("tc,dc->td", heads_out, w_outward) + matmul(
        "tc,dc->td", heads_other, w_outward_other
    )
    state = inputs + attended
    normed2, scaled2, invert2 = layer_norm(state, norm_gains[1], norm_biases[1])
    normed2_low = normed2.astype(bf16)
    slots_out = matmul("tks,td->sd", own_select, normed2_low).astype(bf16)
    arrived = to_experts(slots_out)

    pre_act = matmul("erd,edf->erf", arrived, w_up)
    hidden_low = gelu_exact(pre_act).astype(bf16)
    hidden_grad = matmul("erd,edf->erf", grad_arrived, w_down)
    pre_grad = (hidden_grad * gelu_slope(pre_act)).astype(bf16)
    entry_grad = matmul("erf,edf->erd", pre_grad, w_up).astype(bf16)
    entry_back = to_tokens(entry_grad)
    expert_part = matmul("erf,edf->erd", hidden_low, w_down).astype(bf16)
    up_local = matmul("erd,erf->edf", arrived, pre_grad)
    down_local = matmul("erd,erf->edf", grad_arrived, hidden_low)
    returned = to_tokens(expert_part)

    normed2_grad = matmul("tks,sd->td", select, entry_back)
    state_grad = out_cot + norm_backward(normed2_grad, scaled2, invert2, norm_gains[1])
    state_low = state_grad.astype(bf16)
    outward_local = matmul("td,tc->dc", state_low, heads_out)
    heads_grad = (
        jnp.dot(state_low, w_outward, preferred_element_type=f32)
        .astype(bf16)
        .reshape(images, SEQ, heads_here, HD)
    )
    prob_grad = matmul("bihd,bjhd->bhij", heads_grad, value_part)
    score_grad = (
        softmax_out * (prob_grad - jnp.sum(softmax_out * prob_grad, axis=-1, keepdims=True))
    ).astype(bf16)
    query_grad = matmul("bhij,bjhd->bihd", score_grad, key_part) * score_scale
    key_grad = matmul("bhij,bihd->bjhd", score_grad, query_part) * score_scale
    value_grad = matmul("bhij,bihd->bjhd", softmax_low, heads_grad)
    qkv_grad = (
        jnp.stack([query_grad, key_grad, value_grad], axis=3)
        .reshape(token_rows, heads_here * 3 * HD)
        .astype(bf16)
    )
    inward_local = matmul("td,tc->dc", normed1_low, qkv_grad)
    normed1_part = matmul("tc,dc->td", qkv_grad, w_inward)

    attend_local = jnp.concatenate([inward_local, outward_local], axis=1)
    attend_rows = by_peer(
        [attend_local[j * shard_rows : (j + 1) * shard_rows] for j in range(4)], dp_here
    )
    attend_got = from_peers(swap_dp, [r.astype(bf16) for r in attend_rows])
    attend_sum = attend_rows[0] + sum(g.astype(f32) for g in attend_got[1:])
    attend_low = attend_sum.astype(bf16)
    attend_grad = sum(
        g.astype(f32) for g in by_peer(from_peers(swap_expert, [attend_low] * 4), expert_here)
    )
    inward_gradient, outward_gradient = attend_grad[:, :qcols], attend_grad[:, qcols:]
    inward_next = 0.95 * inward_moment + inward_gradient
    outward_next = 0.95 * outward_moment + outward_gradient

    normed1_grad = normed1_part + swap_core(normed1_part)
    input_gradient = state_grad + norm_backward(normed1_grad, scaled1, invert1, norm_gains[0])
    norm_terms = jnp.stack(
        [
            jnp.sum(normed1_grad * scaled1, axis=0),
            jnp.sum(normed2_grad * scaled2, axis=0),
            jnp.sum(normed1_grad, axis=0),
            jnp.sum(normed2_grad, axis=0),
        ]
    )
    norm_plane = sum(by_peer(from_peers(swap_dp, [norm_terms] * 4), dp_here))
    norm_total = sum(by_peer(from_peers(swap_expert, [norm_plane] * 4), expert_here))

    routed = matmul("tks,sd->tkd", select, returned)
    block_out = (state + jnp.sum(routed * combine[:, :, None], axis=1)).astype(bf16)

    local = by_peer([up_local[0], up_local[1], down_local[0], down_local[1]], dp_here)
    got = from_peers(swap_dp, [m.astype(bf16) for m in local])
    owned_grad = local[0] + sum(g.astype(f32) for g in got[1:])

    def rows_home(value):
        rows = [value[j * shard_rows : (j + 1) * shard_rows] for j in range(4)]
        return by_peer(from_peers(swap_dp, by_peer(rows, dp_here)), dp_here)

    grads = [g.astype(f32) for g in rows_home(owned_grad.astype(bf16))]
    up_gradient, down_gradient = jnp.stack(grads[:2], axis=1), jnp.stack(grads[2:], axis=1)
    up_next = 0.95 * up_moment + up_gradient
    down_next = 0.95 * down_moment + down_gradient
    owned_next = 0.95 * moment_whole + owned_grad
    owned_gram = dot3(owned_next, owned_next.T)
    owned_factor = orth_factor(owned_gram + swap_core(owned_gram))
    owned_step = dot3(owned_factor, owned_next) * (0.2 * math.sqrt(F))
    steps = [s.astype(f32) for s in rows_home(owned_step.astype(bf16))]
    up_step, down_step = jnp.stack(steps[:2], axis=1), jnp.stack(steps[2:], axis=1)

    attend_next = jnp.concatenate([inward_next, outward_next], axis=1)
    attend_whole = jnp.concatenate(
        by_peer(
            [attend_next] + from_peers(swap_dp, [attend_next.astype(bf16)] * 4)[1:], dp_here
        ),
        axis=0,
    ).astype(f32)
    inward_gram = dot3(attend_whole[:, :qcols], attend_whole[:, :qcols].T)
    outward_gram = dot3(attend_whole[:, qcols:], attend_whole[:, qcols:].T)
    kept = jnp.where(first_core, inward_gram, outward_gram)
    given = jnp.where(first_core, outward_gram, inward_gram)
    factor = orth_factor(kept + swap_core(given))
    factor_rows = lax.dynamic_slice_in_dim(factor, dp_here * shard_rows, shard_rows, 0)
    factor_other = swap_core(factor_rows)
    inward_factor = jnp.where(first_core, factor_rows, factor_other)
    outward_factor = jnp.where(first_core, factor_other, factor_rows)
    inward_step = dot3(inward_factor, attend_whole[:, :qcols]) * (0.2 * math.sqrt(3 * D))
    outward_step = dot3(outward_factor, attend_whole[:, qcols:]) * (0.2 * math.sqrt(D))

    inward_new = inward_master - 0.1 * (inward_step + 0.1 * inward_master)
    outward_new = outward_master - 0.1 * (outward_step + 0.1 * outward_master)
    up_new = up_master - 0.1 * (up_step + 0.1 * up_master)
    down_new = down_master - 0.1 * (down_step + 0.1 * down_master)
    moment_first = 0.9 * first_moment + 0.1 * norm_total
    moment_second = 0.999 * second_moment + 0.001 * norm_total * norm_total
    steps_done = step_count[0].astype(f32)
    direction = (
        moment_first
        / (1.0 - jnp.power(0.9, steps_done))
        / (jnp.sqrt(moment_second / (1.0 - jnp.power(0.999, steps_done))) + 1e-08)
    )
    params_new = jnp.concatenate([norm_gains, norm_biases], axis=0) - 0.1 * direction
    return (
        block_out,
        input_gradient,
        inward_gradient,
        outward_gradient,
        up_gradient,
        down_gradient,
        norm_total[0:2],
        norm_total[2:4],
        inward_next,
        outward_next,
        up_next,
        down_next,
        inward_new,
        outward_new,
        up_new,
        down_new,
        inward_new.astype(bf16),
        outward_new.astype(bf16),
        up_new.astype(bf16),
        down_new.astype(bf16),
        params_new[0:2],
        params_new[2:4],
        moment_first,
        moment_second,
    )


def solution(mesh):
    sizes = tuple(mesh.shape[axis] for axis in ("dp", "expert", "tensor"))
    body = pair_body if sizes == (4, 4, 2) else start_body
    return jax.shard_map(
        body,
        mesh=mesh,
        in_specs=(
            P(("dp", "expert"), None),
            P(("dp", "expert"), None),
            P(("dp", "expert"), None),
            P(("dp", "expert"), None),
            P("dp", "tensor"),
            P("dp", "tensor"),
            P("dp", "expert", "tensor"),
            P("dp", "expert", "tensor"),
            P(),
            P(),
            P("dp", "tensor"),
            P("dp", "tensor"),
            P("dp", "expert", "tensor"),
            P("dp", "expert", "tensor"),
            P(),
            P(),
            P(),
        ),
        out_specs=(
            P(("dp", "expert"), None),
            P(("dp", "expert"), None),
            P("dp", "tensor"),
            P("dp", "tensor"),
            P("dp", "expert", "tensor"),
            P("dp", "expert", "tensor"),
            P(),
            P(),
            P("dp", "tensor"),
            P("dp", "tensor"),
            P("dp", "expert", "tensor"),
            P("dp", "expert", "tensor"),
            P("dp", "tensor"),
            P("dp", "tensor"),
            P("dp", "expert", "tensor"),
            P("dp", "expert", "tensor"),
            P("dp", "tensor"),
            P("dp", "tensor"),
            P("dp", "expert", "tensor"),
            P("dp", "expert", "tensor"),
            P(),
            P(),
            P(),
            P(),
        ),
        check_vma=False,
    )
```

```python
import functools
import math

import jax
import jax.numpy as jnp
import numpy as np
from jax import lax
from jax.experimental import pallas as pl
from jax.experimental.pallas import tpu as pltpu
from jax.sharding import PartitionSpec as P

D = 512
HD = 64
F = 2048
SEQ = 197
EXP_DEV = 2


def layer_norm(values, gain_row, bias_row):
    center = values - jnp.mean(values, axis=-1, keepdims=True)
    invert = lax.rsqrt(jnp.mean(center * center, axis=-1, keepdims=True) + 1e-06)
    scaled = center * invert
    return (scaled * gain_row + bias_row, scaled, invert)


def norm_backward(upstream, scaled, invert, gain_row):
    weighted = upstream * gain_row
    return invert * (
        weighted
        - jnp.mean(weighted, axis=-1, keepdims=True)
        - scaled * jnp.mean(weighted * scaled, axis=-1, keepdims=True)
    )


def gelu_exact(values):
    return 0.5 * values * (1.0 + lax.erf(values * 0.7071067811865476))


def gelu_slope(values):
    return 0.5 * (
        1.0 + lax.erf(values * 0.7071067811865476)
    ) + values * 0.3989422804014327 * jnp.exp(-0.5 * values * values)


def newton_schulz(matrix):
    current = matrix / (jnp.sqrt(jnp.sum(matrix * matrix)) + 1e-07)
    for sweep_index in range(5):
        gram_matrix = jnp.dot(current, current.T, precision=lax.Precision.HIGHEST)
        polynom = -4.775 * gram_matrix + 2.0315 * jnp.dot(
            gram_matrix, gram_matrix, precision=lax.Precision.HIGHEST
        )
        current = 3.4445 * current + jnp.dot(polynom, current, precision=lax.Precision.HIGHEST)
    return current


def start_body(
    tokens_in,
    expert_ids,
    combine,
    out_cot,
    inward_master,
    outward_master,
    up_master,
    down_master,
    norm_gains,
    norm_biases,
    inward_moment,
    outward_moment,
    up_moment,
    down_moment,
    first_moment,
    second_moment,
    step_count,
):
    dp_count = lax.axis_size("dp")
    expert_count = lax.axis_size("expert")
    tensor_count = lax.axis_size("tensor")
    token_rows = tokens_in.shape[0]
    expert_total = EXP_DEV * expert_count
    capacity = (token_rows * 10 // (4 * expert_total) + 7) // 8 * 8
    slot_total = expert_total * capacity
    inputs = tokens_in.astype(jnp.float32)
    w_inward, w_outward, w_up, w_down = (
        lax.all_gather(inward_master.astype(jnp.bfloat16), "dp", axis=0, tiled=True),
        lax.all_gather(outward_master.astype(jnp.bfloat16), "dp", axis=0, tiled=True),
        lax.all_gather(up_master.astype(jnp.bfloat16), "dp", axis=0, tiled=True),
        lax.all_gather(down_master.astype(jnp.bfloat16), "dp", axis=0, tiled=True),
    )
    expert_lanes = jnp.arange(expert_total, dtype=jnp.int32)
    route_hits = (expert_ids[:, :, None] == expert_lanes).astype(jnp.int32)
    per_token = jnp.sum(route_hits, axis=1)
    earlier = jnp.cumsum(per_token, axis=0) - per_token
    position = jnp.sum(route_hits * earlier[:, None, :], axis=2)
    target = expert_ids * capacity + position
    select = (target[:, :, None] == jnp.arange(slot_total, dtype=jnp.int32)).astype(jnp.bfloat16)
    normed1, scaled1, invert1 = layer_norm(inputs, norm_gains[0], norm_biases[0])
    normed1_low = normed1.astype(jnp.bfloat16)
    qkv_low = jnp.dot(normed1_low, w_inward, preferred_element_type=jnp.float32).astype(
        jnp.bfloat16
    )
    heads_here = w_inward.shape[1] // (3 * HD)
    images = token_rows // SEQ
    split_heads = qkv_low.reshape(images, SEQ, heads_here, 3, HD)
    query_part = split_heads[:, :, :, 0]
    key_part = split_heads[:, :, :, 1]
    value_part = split_heads[:, :, :, 2]
    score_scale = HD ** (-0.5)
    scores = (
        jnp.einsum("bihd,bjhd->bhij", query_part, key_part, preferred_element_type=jnp.float32)
        * score_scale
    )
    row_max = jnp.max(scores, axis=-1, keepdims=True)
    exponent = jnp.exp(scores - row_max)
    row_total = jnp.sum(exponent, axis=-1, keepdims=True)
    softmax_out = exponent / row_total
    softmax_low = softmax_out.astype(jnp.bfloat16)
    heads_out = (
        jnp.einsum("bhij,bjhd->bihd", softmax_low, value_part, preferred_element_type=jnp.float32)
        .astype(jnp.bfloat16)
        .reshape(token_rows, heads_here * HD)
    )
    attend_part = jnp.einsum("tc,dc->td", heads_out, w_outward, preferred_element_type=jnp.float32)
    attended = lax.psum(attend_part, "tensor")
    state = inputs + attended
    normed2, scaled2, invert2 = layer_norm(state, norm_gains[1], norm_biases[1])
    normed2_low = normed2.astype(jnp.bfloat16)
    slots_out = jnp.einsum(
        "tks,td->sd", select, normed2_low, preferred_element_type=jnp.float32
    ).astype(jnp.bfloat16)
    arrived = lax.all_to_all(
        slots_out.reshape(expert_count, EXP_DEV, capacity, D),
        "expert",
        split_axis=0,
        concat_axis=0,
        tiled=True,
    )
    pre_act = jnp.einsum("secd,def->secf", arrived, w_up, preferred_element_type=jnp.float32)
    hidden_low = gelu_exact(pre_act).astype(jnp.bfloat16)
    expert_part = jnp.einsum(
        "secf,def->secd", hidden_low, w_down, preferred_element_type=jnp.float32
    ).astype(jnp.bfloat16)
    returned = lax.all_to_all(expert_part, "expert", split_axis=0, concat_axis=0, tiled=True)
    routed = jnp.einsum(
        "tks,sd->tkd", select, returned.reshape(slot_total, D), preferred_element_type=jnp.float32
    )
    mixed_part = jnp.sum(routed * combine[:, :, None], axis=1)
    mixed_sum = lax.psum(mixed_part, "tensor")
    block_out = (state + mixed_sum).astype(jnp.bfloat16)
    routed_grad = (combine[:, :, None] * out_cot[:, None, :]).astype(jnp.bfloat16)
    slot_grad = jnp.einsum(
        "tks,tkd->sd", select, routed_grad, preferred_element_type=jnp.float32
    ).astype(jnp.bfloat16)
    grad_arrived = lax.all_to_all(
        slot_grad.reshape(expert_count, EXP_DEV, capacity, D),
        "expert",
        split_axis=0,
        concat_axis=0,
        tiled=True,
    )
    hidden_grad = jnp.einsum(
        "secd,def->secf", grad_arrived, w_down, preferred_element_type=jnp.float32
    )
    pre_grad = (hidden_grad * gelu_slope(pre_act)).astype(jnp.bfloat16)
    down_local = jnp.einsum(
        "secd,secf->def", grad_arrived, hidden_low, preferred_element_type=jnp.float32
    )
    up_local = jnp.einsum("secd,secf->def", arrived, pre_grad, preferred_element_type=jnp.float32)
    entry_grad = jnp.einsum(
        "secf,def->secd", pre_grad, w_up, preferred_element_type=jnp.float32
    ).astype(jnp.bfloat16)
    entry_back = lax.all_to_all(entry_grad, "expert", split_axis=0, concat_axis=0, tiled=True)
    normed2_part = jnp.einsum(
        "tks,sd->td", select, entry_back.reshape(slot_total, D), preferred_element_type=jnp.float32
    )
    normed2_grad = lax.psum(normed2_part, "tensor")
    state_grad = out_cot + norm_backward(normed2_grad, scaled2, invert2, norm_gains[1])
    state_low = state_grad.astype(jnp.bfloat16)
    outward_local = jnp.einsum(
        "td,tc->dc", state_low, heads_out, preferred_element_type=jnp.float32
    )
    heads_grad = (
        jnp.dot(state_low, w_outward, preferred_element_type=jnp.float32)
        .astype(jnp.bfloat16)
        .reshape(images, SEQ, heads_here, HD)
    )
    prob_grad = jnp.einsum(
        "bihd,bjhd->bhij", heads_grad, value_part, preferred_element_type=jnp.float32
    )
    score_grad = (
        softmax_out * (prob_grad - jnp.sum(softmax_out * prob_grad, axis=-1, keepdims=True))
    ).astype(jnp.bfloat16)
    query_grad = (
        jnp.einsum("bhij,bjhd->bihd", score_grad, key_part, preferred_element_type=jnp.float32)
        * score_scale
    )
    key_grad = (
        jnp.einsum("bhij,bihd->bjhd", score_grad, query_part, preferred_element_type=jnp.float32)
        * score_scale
    )
    value_grad = jnp.einsum(
        "bhij,bihd->bjhd", softmax_low, heads_grad, preferred_element_type=jnp.float32
    )
    qkv_grad = (
        jnp.stack([query_grad, key_grad, value_grad], axis=3)
        .reshape(token_rows, heads_here * 3 * HD)
        .astype(jnp.bfloat16)
    )
    inward_local = jnp.einsum(
        "td,tc->dc", normed1_low, qkv_grad, preferred_element_type=jnp.float32
    )
    normed1_part = jnp.einsum("tc,dc->td", qkv_grad, w_inward, preferred_element_type=jnp.float32)
    normed1_grad = lax.psum(normed1_part, "tensor")
    input_gradient = state_grad + norm_backward(normed1_grad, scaled1, invert1, norm_gains[0])
    norm_terms = jnp.stack(
        [
            jnp.sum(normed1_grad * scaled1, axis=0),
            jnp.sum(normed2_grad * scaled2, axis=0),
            jnp.sum(normed1_grad, axis=0),
            jnp.sum(normed2_grad, axis=0),
        ]
    )
    inward_total, outward_total, norm_total = lax.psum(
        (inward_local, outward_local, norm_terms), ("dp", "expert")
    )
    up_gradient, down_gradient = (
        lax.psum_scatter(up_local, "dp", scatter_dimension=0, tiled=True),
        lax.psum_scatter(down_local, "dp", scatter_dimension=0, tiled=True),
    )
    shard_rows = D // dp_count
    dp_here = lax.axis_index("dp")
    inward_gradient = lax.dynamic_slice_in_dim(inward_total, dp_here * shard_rows, shard_rows, 0)
    outward_gradient = lax.dynamic_slice_in_dim(outward_total, dp_here * shard_rows, shard_rows, 0)
    inward_next = 0.95 * inward_moment + inward_gradient
    outward_next = 0.95 * outward_moment + outward_gradient
    up_next = 0.95 * up_moment + up_gradient
    down_next = 0.95 * down_moment + down_gradient
    matrices = [up_next[:, expert_slot] for expert_slot in range(EXP_DEV)]
    matrices = matrices + [down_next[:, expert_slot] for expert_slot in range(EXP_DEV)]
    matrices = matrices + [jnp.concatenate([inward_next, outward_next], axis=1)]
    stacked = jnp.stack(matrices)
    slot_count = len(matrices)
    group_size = dp_count * tensor_count
    shard_width = stacked.shape[2]
    query_cols = inward_next.shape[1]

    def orth_expert(pieces):
        whole_matrix = pieces.transpose(0, 2, 1, 3).reshape(D, tensor_count * shard_width)
        result = newton_schulz(whole_matrix) * (0.2 * math.sqrt(F))
        return result.reshape(dp_count, shard_rows, tensor_count, shard_width).transpose(0, 2, 1, 3)

    def orth_attention(pieces):
        inward_whole = (
            pieces[..., :query_cols].transpose(0, 2, 1, 3).reshape(D, tensor_count * query_cols)
        )
        outward_whole = (
            pieces[..., query_cols:]
            .transpose(0, 2, 1, 3)
            .reshape(D, tensor_count * (shard_width - query_cols))
        )
        inward_result = newton_schulz(inward_whole) * (0.2 * math.sqrt(3 * D))
        outward_result = newton_schulz(outward_whole) * (0.2 * math.sqrt(D))
        inward_blocks = inward_result.reshape(
            dp_count, shard_rows, tensor_count, query_cols
        ).transpose(0, 2, 1, 3)
        outward_blocks = outward_result.reshape(
            dp_count, shard_rows, tensor_count, shard_width - query_cols
        ).transpose(0, 2, 1, 3)
        return jnp.concatenate([inward_blocks, outward_blocks], axis=3)

    owner_index = lax.axis_index(("dp", "tensor"))
    outgoing = stacked[np.arange(group_size) % slot_count]
    received = lax.all_to_all(outgoing, ("dp", "tensor"), split_axis=0, concat_axis=0, tiled=True)
    blocks = received.reshape(dp_count, tensor_count, shard_rows, shard_width)
    slot_here = owner_index % slot_count
    result_blocks = lax.cond(slot_here == slot_count - 1, orth_attention, orth_expert, blocks)
    arrived_steps = lax.all_to_all(
        result_blocks.reshape(group_size, shard_rows, shard_width),
        ("dp", "tensor"),
        split_axis=0,
        concat_axis=0,
        tiled=True,
    )
    picked = []
    for owned_slot in range(slot_count):
        replicas = (group_size - owned_slot + slot_count - 1) // slot_count
        source = owned_slot + slot_count * (owner_index % replicas)
        picked.append(lax.dynamic_index_in_dim(arrived_steps, source, 0, keepdims=False))
    up_step = jnp.stack(picked[0:EXP_DEV], axis=1)
    down_step = jnp.stack(picked[EXP_DEV : 2 * EXP_DEV], axis=1)
    attend_step = picked[2 * EXP_DEV]
    inward_new = inward_master - 0.1 * (attend_step[:, :query_cols] + 0.1 * inward_master)
    outward_new = outward_master - 0.1 * (attend_step[:, query_cols:] + 0.1 * outward_master)
    up_new = up_master - 0.1 * (up_step + 0.1 * up_master)
    down_new = down_master - 0.1 * (down_step + 0.1 * down_master)
    moment_first = 0.9 * first_moment + 0.1 * norm_total
    moment_second = 0.999 * second_moment + 0.001 * norm_total * norm_total
    steps_done = step_count[0].astype(jnp.float32)
    direction = (
        moment_first
        / (1.0 - jnp.power(0.9, steps_done))
        / (jnp.sqrt(moment_second / (1.0 - jnp.power(0.999, steps_done))) + 1e-08)
    )
    params_new = jnp.concatenate([norm_gains, norm_biases], axis=0) - 0.1 * direction
    return (
        block_out,
        input_gradient,
        inward_gradient,
        outward_gradient,
        up_gradient,
        down_gradient,
        norm_total[0:2],
        norm_total[2:4],
        inward_next,
        outward_next,
        up_next,
        down_next,
        inward_new,
        outward_new,
        up_new,
        down_new,
        inward_new.astype(jnp.bfloat16),
        outward_new.astype(jnp.bfloat16),
        up_new.astype(jnp.bfloat16),
        down_new.astype(jnp.bfloat16),
        params_new[0:2],
        params_new[2:4],
        moment_first,
        moment_second,
    )


PAIRS = (1, 2, 3)
FAR_FIRST = (3, 2, 1, 0)
PAD = 208
NT = (((1,), (1,)), ((), ()))
TN = (((0,), (0,)), ((), ()))


def mxu(left, right, dims=(((1,), (0,)), ((), ()))):
    return lax.dot_general(left, right, dims, preferred_element_type=jnp.float32)


def spread_rows(value, padded_ref):
    padded_ref[...] = jnp.zeros_like(padded_ref)
    for image in range(value.shape[0] // SEQ):
        padded_ref[image * PAD : image * PAD + SEQ, :] = value[image * SEQ : (image + 1) * SEQ]


def gather_rows(padded, out_ref):
    for image in range(out_ref.shape[0] // SEQ):
        out_ref[image * SEQ : (image + 1) * SEQ, :] = padded[
            image * PAD : image * PAD + SEQ
        ].astype(out_ref.dtype)


def peer(me, k):
    return (me, me + 1 - 2 * (me % 2), me + 2 - 4 * (me // 2), 3 - me)[k]


def one_hot(cond):
    return jnp.where(cond, 1.0, 0.0).astype(jnp.bfloat16)


def route(ids, ids_t, capacity, target_ref, target_t_ref):
    rows = ids.shape[0]
    before = lax.broadcasted_iota(jnp.int32, (rows, rows), 0)
    after = lax.broadcasted_iota(jnp.int32, (rows, rows), 1)
    lane = lax.broadcasted_iota(jnp.int32, (rows, 128), 1)
    hits = one_hot((lane == ids[:, 0:1]) | (lane == ids[:, 1:2]))
    earlier = mxu(one_hot(before > after), hits)
    target = jnp.zeros((rows, 128), jnp.int32)
    for r in range(2):
        own = ids[:, r : r + 1]
        position = jnp.sum(jnp.where(lane == own, earlier, 0.0), axis=1, keepdims=True)
        value = jnp.where(own >= 0, own * capacity + position.astype(jnp.int32), -1)
        target = jnp.where(lane == r, value, target)
    target_ref[...] = target
    row = lax.broadcasted_iota(jnp.int32, (16, rows), 0)
    hits = one_hot((row == ids_t[0:1]) | (row == ids_t[1:2]))
    earlier = mxu(hits, one_hot(before < after))
    for r in range(2):
        own = ids_t[r : r + 1]
        position = jnp.sum(jnp.where(row == own, earlier, 0.0), axis=0, keepdims=True)
        target_t_ref[r : r + 1, :] = jnp.where(
            own >= 0, own * capacity + position.astype(jnp.int32), -1
        )


def attend(qkv_ref, probs_ref, gift_ref):
    heads_here = qkv_ref.shape[1] // (3 * HD)
    key_lane = lax.broadcasted_iota(jnp.int32, (PAD, PAD), 1)
    for image in range(qkv_ref.shape[0] // PAD):
        rows = slice(image * PAD, (image + 1) * PAD)
        for head in range(heads_here):
            base = head * 3 * HD
            query = qkv_ref[rows, base : base + HD]
            key = qkv_ref[rows, base + HD : base + 2 * HD]
            value = qkv_ref[rows, base + 2 * HD : base + 3 * HD]
            scores = jnp.where(key_lane < SEQ, mxu(query, key, NT) * HD ** (-0.5), -1e30)
            exponent = jnp.exp(scores - jnp.max(scores, axis=-1, keepdims=True))
            probs = exponent / jnp.sum(exponent, axis=-1, keepdims=True)
            probs_ref[image * heads_here + head] = probs
            gift_ref[D + image * PAD : D + (image + 1) * PAD, head * HD : (head + 1) * HD] = mxu(
                probs.astype(jnp.bfloat16), value
            ).astype(jnp.bfloat16)


def front_kernel(
    ids_ref,
    ids_t_ref,
    combine_ref,
    cot_ref,
    tokens_ref,
    gains_ref,
    biases_ref,
    attend_shard_ref,
    expert_shard_ref,
    state_ref,
    gift_ref,
    qkv_ref,
    probs_ref,
    weight_ref,
    target_ref,
    expert_w_ref,
    arrived_ref,
    grad_arrived_ref,
    padded,
    target_t_ref,
    gift_other_ref,
    grad_chunks,
    token_chunks,
    inner_send,
    inner_recv,
    expert_send,
    expert_recv,
    slot_send,
    slot_recv,
    share_send,
    share_recv,
    gift_sems,
    keep_sems,
):
    bf16 = jnp.bfloat16
    dp_here, expert_here, core = (lax.axis_index(a) for a in ("dp", "expert", "tensor"))
    partner = {"tensor": 1 - core}
    capacity = grad_chunks.shape[1]
    shard_rows = attend_shard_ref.shape[0]
    qcols = qkv_ref.shape[1]
    mesh_id = pl.DeviceIdType.MESH

    barrier = pltpu.get_barrier_semaphore()
    for k in PAIRS:
        pl.semaphore_signal(
            barrier, inc=1, device_id={"dp": peer(dp_here, k)}, device_id_type=mesh_id
        )
        pl.semaphore_signal(
            barrier, inc=1, device_id={"expert": peer(expert_here, k)}, device_id_type=mesh_id
        )
    pl.semaphore_signal(barrier, inc=1, device_id=partner, device_id_type=mesh_id)
    pl.semaphore_wait(barrier, 7)

    def remote(source, target, send, recv, device):
        copy = pltpu.make_async_remote_copy(
            src_ref=source,
            dst_ref=target,
            send_sem=send,
            recv_sem=recv,
            device_id=device,
            device_id_type=mesh_id,
        )
        copy.start()
        return copy

    def keep(source, target, sem):
        copy = pltpu.make_async_copy(source, target, sem)
        copy.start()
        return copy

    here = pl.ds(pl.multiple_of(dp_here * shard_rows, shard_rows), shard_rows)
    inner = [
        remote(
            attend_shard_ref,
            weight_ref.at[here, :],
            inner_send.at[k - 1],
            inner_recv.at[k - 1],
            {"dp": peer(dp_here, k)},
        )
        for k in PAIRS
    ]
    weights = [
        remote(
            expert_shard_ref,
            expert_w_ref.at[:, here, :],
            expert_send.at[k - 1],
            expert_recv.at[k - 1],
            {"dp": peer(dp_here, k)},
        )
        for k in (1, 2)
    ]
    kept = [
        keep(expert_shard_ref, expert_w_ref.at[:, here, :], keep_sems.at[0]),
        keep(attend_shard_ref, weight_ref.at[here, :], keep_sems.at[1]),
    ]

    route(ids_ref[...], ids_t_ref[...], capacity, target_ref, target_t_ref)
    spread_rows(cot_ref[...], padded)
    cot = padded[...]
    grads = [(combine_ref[:, r : r + 1] * cot).astype(bf16) for r in range(2)]
    slot = lax.broadcasted_iota(jnp.int32, (capacity, cot.shape[0]), 0)

    def first_slot(k):
        return (2 * peer(expert_here, k) + core) * capacity

    for k in FAR_FIRST:
        grad_chunks[k] = sum(
            mxu(one_hot(target_t_ref[r : r + 1] == slot + first_slot(k)), grads[r])
            for r in range(2)
        ).astype(bf16)

    def send_chunks(chunks, landing, which):
        copies = {}
        for k in FAR_FIRST[:3]:
            copies[k] = remote(
                chunks.at[k],
                landing.at[0, k],
                slot_send.at[which, k],
                slot_recv.at[which, k],
                {"expert": peer(expert_here, k)},
            )
        kept.append(keep(chunks.at[0], landing.at[0, 0], keep_sems.at[2 + which]))
        shared = remote(
            chunks.at[0], landing.at[1, 0], share_send.at[which, 0], share_recv.at[which, 0], partner
        )
        return copies, [shared]

    def share_arrivals(copies, landing, which, shared):
        for k in FAR_FIRST[:3]:
            copies[k].wait_recv()
            shared.append(
                remote(
                    landing.at[0, k],
                    landing.at[1, k],
                    share_send.at[which, k],
                    share_recv.at[which, k],
                    partner,
                )
            )

    spread_rows(tokens_ref[...].astype(jnp.float32), padded)
    normed, unused, unused = layer_norm(padded[...], gains_ref[0:1], biases_ref[0:1])
    grad_copies, grad_shared = send_chunks(grad_chunks, grad_arrived_ref, 0)
    kept[1].wait()
    for copy in inner:
        copy.wait_recv()
    qkv_ref[...] = mxu(normed.astype(bf16), weight_ref[:, :qcols]).astype(bf16)
    gift_ref[0:D, :] = weight_ref[:, qcols:]
    attend(qkv_ref, probs_ref, gift_ref)
    share_arrivals(grad_copies, grad_arrived_ref, 0, grad_shared)
    gift = remote(gift_ref, gift_other_ref, gift_sems.at[0], gift_sems.at[1], partner)
    half = padded[...] + mxu(gift_ref[D:, :], gift_ref[0:D, :], NT)
    gift.wait()
    state = half + mxu(gift_other_ref[D:, :], gift_other_ref[0:D, :], NT)
    state_ref[...] = state
    normed, unused, unused = layer_norm(state, gains_ref[1:2], biases_ref[1:2])
    normed_low = normed.astype(bf16)
    for k in FAR_FIRST:
        first = slot + first_slot(k)
        pick = (target_t_ref[0:1] == first) | (target_t_ref[1:2] == first)
        token_chunks[k] = mxu(one_hot(pick), normed_low).astype(bf16)
    token_copies, token_shared = send_chunks(token_chunks, arrived_ref, 1)
    for copy in weights:
        copy.wait_recv()
    for k, part in ((1, slice(0, EXP_DEV)), (2, slice(EXP_DEV, 2 * EXP_DEV))):
        start = pl.multiple_of(peer(dp_here, k) * shard_rows, shard_rows)
        block = expert_w_ref.at[part, pl.ds(start, shard_rows), :]
        weights.append(
            remote(
                block,
                block,
                expert_send.at[k + 1],
                expert_recv.at[k + 1],
                {"dp": peer(dp_here, 3 - k)},
            )
        )
    share_arrivals(token_copies, arrived_ref, 1, token_shared)
    for copy in grad_shared + token_shared + weights[2:]:
        copy.wait()
    for copy in weights[:2]:
        copy.wait_send()
    for copies in (grad_copies, token_copies):
        for k in PAIRS:
            copies[k].wait_send()
    for copy in inner:
        copy.wait_send()
    kept[0].wait()
    for copy in kept[2:]:
        copy.wait()


def back_kernel(
    place_ref,
    tokens_ref,
    cot_ref,
    gains_ref,
    biases_ref,
    state_ref,
    gift_ref,
    qkv_ref,
    probs_ref,
    weight_ref,
    target_ref,
    *rest,
):
    chunk_refs = rest[:8]
    grad_ref, part_ref, terms_ref, inner_refs = rest[8], rest[9], rest[10], rest[11:15]
    padded, qkv_grad_ref, local_ref = rest[15:18]
    dp_here, expert_here, core = place_ref[0], place_ref[1], place_ref[2]
    bf16 = jnp.bfloat16
    qcols = qkv_ref.shape[1]
    rows_all = state_ref.shape[0]
    capacity = chunk_refs[0].shape[0]
    slot = lax.broadcasted_iota(jnp.int32, (rows_all, capacity), 1)
    target0, target1 = target_ref[:, 0:1], target_ref[:, 1:2]
    normed2_grad = jnp.zeros((rows_all, D), jnp.float32)
    for k in range(4):
        for j in range(2):
            first = (2 * (expert_here ^ k) + (core ^ j)) * capacity
            pick = (target0 == slot + first) | (target1 == slot + first)
            normed2_grad += mxu(
                jnp.where(pick, 1.0, 0.0).astype(bf16), chunk_refs[k + 4 * j][...]
            )
    unused, scaled2, invert2 = layer_norm(state_ref[...], gains_ref[1:2], biases_ref[1:2])
    terms_ref[0:1, :] = jnp.sum(normed2_grad * scaled2, axis=0, keepdims=True)
    terms_ref[1:2, :] = jnp.sum(normed2_grad, axis=0, keepdims=True)
    spread_rows(cot_ref[...], padded)
    state_grad = padded[...] + norm_backward(normed2_grad, scaled2, invert2, gains_ref[1:2])
    grad_ref[...] = state_grad
    state_low = state_grad.astype(bf16)
    local_ref[:, qcols:] = mxu(state_low, gift_ref[D:, :], TN)
    heads_grad = mxu(state_low, weight_ref[:, qcols:]).astype(bf16)
    heads_here = qcols // (3 * HD)
    scale = HD ** (-0.5)
    for image in range(rows_all // PAD):
        rows = slice(image * PAD, (image + 1) * PAD)
        for head in range(heads_here):
            base = head * 3 * HD
            query = qkv_ref[rows, base : base + HD]
            key = qkv_ref[rows, base + HD : base + 2 * HD]
            value = qkv_ref[rows, base + 2 * HD : base + 3 * HD]
            out_grad = heads_grad[image * PAD : (image + 1) * PAD, head * HD : (head + 1) * HD]
            probs = probs_ref[image * heads_here + head]
            prob_grad = mxu(out_grad, value, NT)
            score_grad = (
                probs * (prob_grad - jnp.sum(probs * prob_grad, axis=-1, keepdims=True))
            ).astype(bf16)
            qkv_grad_ref[rows, base : base + HD] = (mxu(score_grad, key) * scale).astype(bf16)
            qkv_grad_ref[rows, base + HD : base + 2 * HD] = (
                mxu(score_grad, query, TN) * scale
            ).astype(bf16)
            qkv_grad_ref[rows, base + 2 * HD : base + 3 * HD] = mxu(
                probs.astype(bf16), out_grad, TN
            ).astype(bf16)
    spread_rows(tokens_ref[...].astype(jnp.float32), padded)
    normed1, unused, unused = layer_norm(padded[...], gains_ref[0:1], biases_ref[0:1])
    local_ref[:, :qcols] = mxu(normed1.astype(bf16), qkv_grad_ref[...], TN)
    shard_rows = inner_refs[0].shape[0]
    for k in range(4):
        start = pl.multiple_of((dp_here ^ k) * shard_rows, shard_rows)
        inner_refs[k][...] = local_ref[pl.ds(start, shard_rows), :].astype(bf16)
    part_ref[...] = mxu(qkv_grad_ref[...], weight_ref[:, :qcols], NT)


def input_kernel(
    tokens_ref, gains_ref, biases_ref, grad_ref, part_ref, other_ref, terms_ref, out_ref, sums_ref, padded
):
    spread_rows(tokens_ref[...].astype(jnp.float32), padded)
    unused, scaled, invert = layer_norm(padded[...], gains_ref[0:1], biases_ref[0:1])
    normed_grad = part_ref[...] + other_ref[...]
    sums_ref[0:1, :] = jnp.sum(normed_grad * scaled, axis=0, keepdims=True)
    sums_ref[1:2, :] = terms_ref[0:1, :]
    sums_ref[2:3, :] = jnp.sum(normed_grad, axis=0, keepdims=True)
    sums_ref[3:4, :] = terms_ref[1:2, :]
    gather_rows(
        grad_ref[...] + norm_backward(normed_grad, scaled, invert, gains_ref[0:1]), out_ref
    )


def output_kernel(place_ref, combine_ref, state_ref, target_ref, *rest):
    chunk_refs, out_ref = rest[:8], rest[8]
    expert_here, core = place_ref[1], place_ref[2]
    rows_all = state_ref.shape[0]
    capacity = chunk_refs[0].shape[0]
    slot = lax.broadcasted_iota(jnp.int32, (rows_all, capacity), 1)
    total = state_ref[...]
    for r in range(2):
        routed = jnp.zeros((rows_all, D), jnp.float32)
        for k in range(4):
            for j in range(2):
                first = (2 * (expert_here ^ k) + (core ^ j)) * capacity
                pick = target_ref[:, r : r + 1] == slot + first
                routed += mxu(
                    jnp.where(pick, 1.0, 0.0).astype(jnp.bfloat16), chunk_refs[k + 4 * j][...]
                )
        total += combine_ref[:, r : r + 1] * routed
    gather_rows(total, out_ref)


def halves(value):
    high = value.astype(jnp.bfloat16)
    return high, (value - high.astype(jnp.float32)).astype(jnp.bfloat16)


def mxu3(left, right, dims=(((1,), (0,)), ((), ()))):
    return (
        mxu(left[0], right[0], dims) + mxu(left[1], right[0], dims) + mxu(left[0], right[1], dims)
    )


def factor_kernel(own_ref, other_ref, factor_ref, current, change, scaled):
    gram = own_ref[...] + other_ref[...]
    diagonal = lax.broadcasted_iota(jnp.int32, gram.shape, 0) == lax.broadcasted_iota(
        jnp.int32, gram.shape, 1
    )
    squares = jnp.sum(jnp.sum(jnp.where(diagonal, gram, 0.0), axis=1, keepdims=True), axis=0, keepdims=True)
    norm = jnp.sqrt(squares) + 1e-07
    current[...] = gram / (norm * norm)
    factor_ref[...] = jnp.where(diagonal, 1.0 / norm, 0.0)

    def sweep(index, carry):
        low = halves(current[...])
        change[...] = -4.775 * current[...] + 2.0315 * mxu3(low, low)
        step = halves(change[...])
        factor_ref[...] = 3.4445 * factor_ref[...] + mxu3(step, halves(factor_ref[...]))
        scaled[...] = 3.4445 * current[...] + mxu3(step, low)
        current[...] = 3.4445 * scaled[...] + mxu3(halves(scaled[...]), step)
        return carry

    lax.fori_loop(0, 5, sweep, 0)


def local_call(kernel, out_shape, name, flops, moved, scratch=(), scalars=True):
    vmem = pl.BlockSpec(memory_space=pltpu.VMEM)

    def call(*operands):
        specs = [vmem] * len(operands)
        if scalars:
            specs[0] = pl.BlockSpec(memory_space=pltpu.SMEM)
        return pl.pallas_call(
            kernel,
            out_shape=out_shape,
            in_specs=specs,
            out_specs=jax.tree.map(lambda unused: vmem, out_shape),
            scratch_shapes=list(scratch),
            name=name,
            cost_estimate=pl.CostEstimate(flops=flops, bytes_accessed=moved, transcendentals=0),
        )(*operands)

    return call


def by_peer(blocks, me):
    low, high = (me & 1) == 1, (me & 2) == 2
    half = [jnp.where(low, blocks[k ^ 1], blocks[k]) for k in range(4)]
    return [jnp.where(high, half[k ^ 2], half[k]) for k in range(4)]


def swap_dp(value, k):
    return lax.ppermute(value, "dp", [(i, i ^ k) for i in range(4)])


def swap_expert(value, k):
    return lax.ppermute(value, "expert", [(i, i ^ k) for i in range(4)])


def swap_core(value):
    return lax.ppermute(value, "tensor", [(0, 1), (1, 0)])


def from_peers(swap, blocks):
    return [blocks[0]] + [swap(blocks[k], k) for k in PAIRS]


def dot3(left, right):
    return jnp.dot(left, right, precision=lax.Precision.HIGH)


def orth_factor(own, other):
    return local_call(
        factor_kernel,
        jax.ShapeDtypeStruct((D, D), jnp.float32),
        "orth_factor",
        16_000_000_000,
        4_000_000,
        [pltpu.VMEM((D, D), jnp.float32)] * 3,
        scalars=False,
    )(own, other)


def pair_body(
    tokens_in,
    expert_ids,
    combine,
    out_cot,
    inward_master,
    outward_master,
    up_master,
    down_master,
    norm_gains,
    norm_biases,
    inward_moment,
    outward_moment,
    up_moment,
    down_moment,
    first_moment,
    second_moment,
    step_count,
):
    bf16, f32 = jnp.bfloat16, jnp.float32
    dp_here, expert_here, core = (lax.axis_index(a) for a in ("dp", "expert", "tensor"))
    first_core = core == 0
    token_rows = tokens_in.shape[0]
    expert_total = EXP_DEV * 4
    capacity = (token_rows * 10 // (4 * expert_total) + 7) // 8 * 8
    slot_total = expert_total * capacity
    shard_rows = D // 4
    qcols = inward_master.shape[1]
    width = up_master.shape[2]

    def matmul(spec, a, b):
        return jnp.einsum(spec, a, b, preferred_element_type=f32)

    def paired(first, second):
        return jnp.where(first_core, first, second), jnp.where(first_core, second, first)

    attend_shard = jnp.concatenate([inward_master, outward_master], axis=1).astype(bf16)
    expert_shard = jnp.stack(
        paired(up_master[:, 0], up_master[:, 1]) + paired(down_master[:, 0], down_master[:, 1])
    ).astype(bf16)
    moment_rows = [up_moment[:, 0], up_moment[:, 1], down_moment[:, 0], down_moment[:, 1]]
    moment_whole = jnp.concatenate(
        by_peer(from_peers(swap_dp, by_peer(moment_rows, dp_here)), dp_here), axis=0
    )

    images = token_rows // SEQ
    padded_rows = images * PAD
    place = jnp.stack([dp_here, expert_here, core])
    shape = jax.ShapeDtypeStruct
    rows_f32 = pltpu.VMEM((padded_rows, D), f32)

    def pad_tokens(value, fill):
        padded = jnp.pad(
            value.reshape(images, SEQ, 2), ((0, 0), (0, PAD - SEQ), (0, 0)), constant_values=fill
        )
        return padded.reshape(padded_rows, 2)

    ids_padded, combine_padded = pad_tokens(expert_ids, -1), pad_tokens(combine, 0.0)
    heads_here = qcols // (3 * HD)
    slots = shape((EXP_DEV, 4, capacity, D), bf16)
    outs = {
        "state": shape((padded_rows, D), f32),
        "gift": shape((D + padded_rows, heads_here * HD), bf16),
        "qkv": shape((padded_rows, qcols), bf16),
        "probs": shape((images * heads_here, PAD, PAD), f32),
        "weight": shape((D, attend_shard.shape[1]), bf16),
        "target": shape((padded_rows, 128), jnp.int32),
        "expert_w": shape((2 * EXP_DEV, D, width), bf16),
        "arrived": slots,
        "grad_arrived": slots,
    }
    in_vmem, anywhere = pl.BlockSpec(memory_space=pltpu.VMEM), pl.BlockSpec(memory_space=pl.ANY)
    dma = pltpu.SemaphoreType.DMA
    state, gift, qkv_low, probs, weight, target, expert_w, arrived, grad_arrived = pl.pallas_call(
        front_kernel,
        out_shape=tuple(outs.values()),
        in_specs=[in_vmem] * 9,
        out_specs=tuple([in_vmem] * 6 + [anywhere] * 3),
        scratch_shapes=[
            rows_f32,
            pltpu.VMEM((2, padded_rows), jnp.int32),
            pltpu.VMEM((D + padded_rows, heads_here * HD), bf16),
            pltpu.VMEM((4, capacity, D), bf16),
            pltpu.VMEM((4, capacity, D), bf16),
            dma((3,)),
            dma((3,)),
            dma((4,)),
            dma((4,)),
            dma((2, 4)),
            dma((2, 4)),
            dma((2, 4)),
            dma((2, 4)),
            dma((2,)),
            dma((4,)),
        ],
        name="front",
        cost_estimate=pl.CostEstimate(
            flops=60_000_000_000, bytes_accessed=30_000_000, transcendentals=0
        ),
        compiler_params=pltpu.CompilerParams(collective_id=0, has_side_effects=True),
    )(
        ids_padded,
        ids_padded.T,
        combine_padded,
        out_cot,
        tokens_in,
        norm_gains,
        norm_biases,
        attend_shard,
        expert_shard,
    )
    arrived = arrived.reshape(EXP_DEV, 4 * capacity, D)
    grad_arrived = grad_arrived.reshape(EXP_DEV, 4 * capacity, D)
    w_up, w_down = expert_w[:2], expert_w[2:]

    def to_tokens(parts):
        total = (parts[0].astype(f32) + swap_core(parts[1]).astype(f32)).astype(bf16)
        chunks = from_peers(
            swap_expert, [total[k * capacity : (k + 1) * capacity] for k in range(4)]
        )
        return chunks + [swap_core(c) for c in chunks]

    pre_act = matmul("erd,edf->erf", arrived, w_up)
    hidden_low = gelu_exact(pre_act).astype(bf16)
    hidden_grad = matmul("erd,edf->erf", grad_arrived, w_down)
    pre_grad = (hidden_grad * gelu_slope(pre_act)).astype(bf16)
    entry_grad = matmul("erf,edf->erd", pre_grad, w_up).astype(bf16)
    entry_back = to_tokens(entry_grad)
    expert_part = matmul("erf,edf->erd", hidden_low, w_down).astype(bf16)
    up_local = matmul("erd,erf->edf", arrived, pre_grad)
    down_local = matmul("erd,erf->edf", grad_arrived, hidden_low)
    returned = to_tokens(expert_part)

    state_grad, normed1_part, norm2_terms, *attend_rows = local_call(
        back_kernel,
        (shape((padded_rows, D), f32), shape((padded_rows, D), f32), shape((2, D), f32))
        + (shape((shard_rows, width), bf16),) * 4,
        "back",
        8_000_000_000,
        16_000_000,
        [rows_f32, pltpu.VMEM((padded_rows, qcols), bf16), pltpu.VMEM((D, width), f32)],
    )(
        place,
        tokens_in,
        out_cot,
        norm_gains,
        norm_biases,
        state,
        gift,
        qkv_low,
        probs,
        weight,
        target,
        *entry_back,
    )

    attend_sum = sum(g.astype(f32) for g in from_peers(swap_dp, attend_rows))
    attend_low = attend_sum.astype(bf16)
    attend_grad = sum(
        g.astype(f32) for g in by_peer(from_peers(swap_expert, [attend_low] * 4), expert_here)
    )
    inward_gradient, outward_gradient = attend_grad[:, :qcols], attend_grad[:, qcols:]
    inward_next = 0.95 * inward_moment + inward_gradient
    outward_next = 0.95 * outward_moment + outward_gradient

    input_gradient, norm_terms = local_call(
        input_kernel,
        (shape((token_rows, D), f32), shape((4, D), f32)),
        "input_grad",
        100_000_000,
        10_000_000,
        [rows_f32],
        scalars=False,
    )(
        tokens_in,
        norm_gains,
        norm_biases,
        state_grad,
        normed1_part,
        swap_core(normed1_part),
        norm2_terms,
    )
    norm_plane = sum(by_peer(from_peers(swap_dp, [norm_terms] * 4), dp_here))
    norm_total = sum(by_peer(from_peers(swap_expert, [norm_plane] * 4), expert_here))

    block_out = local_call(
        output_kernel,
        shape((token_rows, D), bf16),
        "block_out",
        4_000_000_000,
        6_000_000,
    )(place, combine_padded, state, target, *returned)

    local = by_peer(
        [*paired(up_local[0], up_local[1]), *paired(down_local[0], down_local[1])], dp_here
    )
    got = from_peers(swap_dp, [m.astype(bf16) for m in local])
    owned_grad = local[0] + sum(g.astype(f32) for g in got[1:])

    def rows_home(value):
        rows = [value[j * shard_rows : (j + 1) * shard_rows] for j in range(4)]
        return by_peer(from_peers(swap_dp, by_peer(rows, dp_here)), dp_here)

    grads = [g.astype(f32) for g in rows_home(owned_grad.astype(bf16))]
    up_gradient, down_gradient = jnp.stack(grads[:2], axis=1), jnp.stack(grads[2:], axis=1)
    up_next = 0.95 * up_moment + up_gradient
    down_next = 0.95 * down_moment + down_gradient
    owned_next = 0.95 * moment_whole + owned_grad
    owned_gram = dot3(owned_next, owned_next.T)
    owned_factor = orth_factor(owned_gram, swap_core(owned_gram))
    owned_step = dot3(owned_factor, owned_next) * (0.2 * math.sqrt(F))
    steps = [s.astype(f32) for s in rows_home(owned_step.astype(bf16))]
    up_step, down_step = jnp.stack(steps[:2], axis=1), jnp.stack(steps[2:], axis=1)

    attend_next = jnp.concatenate([inward_next, outward_next], axis=1)
    attend_whole = jnp.concatenate(
        by_peer(
            [attend_next] + from_peers(swap_dp, [attend_next.astype(bf16)] * 4)[1:], dp_here
        ),
        axis=0,
    ).astype(f32)
    inward_gram = dot3(attend_whole[:, :qcols], attend_whole[:, :qcols].T)
    outward_gram = dot3(attend_whole[:, qcols:], attend_whole[:, qcols:].T)
    kept = jnp.where(first_core, inward_gram, outward_gram)
    given = jnp.where(first_core, outward_gram, inward_gram)
    factor = orth_factor(kept, swap_core(given))
    factor_rows = lax.dynamic_slice_in_dim(factor, dp_here * shard_rows, shard_rows, 0)
    factor_other = swap_core(factor_rows)
    inward_factor = jnp.where(first_core, factor_rows, factor_other)
    outward_factor = jnp.where(first_core, factor_other, factor_rows)
    inward_step = dot3(inward_factor, attend_whole[:, :qcols]) * (0.2 * math.sqrt(3 * D))
    outward_step = dot3(outward_factor, attend_whole[:, qcols:]) * (0.2 * math.sqrt(D))

    inward_new = inward_master - 0.1 * (inward_step + 0.1 * inward_master)
    outward_new = outward_master - 0.1 * (outward_step + 0.1 * outward_master)
    up_new = up_master - 0.1 * (up_step + 0.1 * up_master)
    down_new = down_master - 0.1 * (down_step + 0.1 * down_master)
    moment_first = 0.9 * first_moment + 0.1 * norm_total
    moment_second = 0.999 * second_moment + 0.001 * norm_total * norm_total
    steps_done = step_count[0].astype(f32)
    direction = (
        moment_first
        / (1.0 - jnp.power(0.9, steps_done))
        / (jnp.sqrt(moment_second / (1.0 - jnp.power(0.999, steps_done))) + 1e-08)
    )
    params_new = jnp.concatenate([norm_gains, norm_biases], axis=0) - 0.1 * direction
    return (
        block_out,
        input_gradient,
        inward_gradient,
        outward_gradient,
        up_gradient,
        down_gradient,
        norm_total[0:2],
        norm_total[2:4],
        inward_next,
        outward_next,
        up_next,
        down_next,
        inward_new,
        outward_new,
        up_new,
        down_new,
        inward_new.astype(bf16),
        outward_new.astype(bf16),
        up_new.astype(bf16),
        down_new.astype(bf16),
        params_new[0:2],
        params_new[2:4],
        moment_first,
        moment_second,
    )


def solution(mesh):
    sizes = tuple(mesh.shape[axis] for axis in ("dp", "expert", "tensor"))
    body = pair_body if sizes == (4, 4, 2) else start_body
    return jax.shard_map(
        body,
        mesh=mesh,
        in_specs=(
            P(("dp", "expert"), None),
            P(("dp", "expert"), None),
            P(("dp", "expert"), None),
            P(("dp", "expert"), None),
            P("dp", "tensor"),
            P("dp", "tensor"),
            P("dp", "expert", "tensor"),
            P("dp", "expert", "tensor"),
            P(),
            P(),
            P("dp", "tensor"),
            P("dp", "tensor"),
            P("dp", "expert", "tensor"),
            P("dp", "expert", "tensor"),
            P(),
            P(),
            P(),
        ),
        out_specs=(
            P(("dp", "expert"), None),
            P(("dp", "expert"), None),
            P("dp", "tensor"),
            P("dp", "tensor"),
            P("dp", "expert", "tensor"),
            P("dp", "expert", "tensor"),
            P(),
            P(),
            P("dp", "tensor"),
            P("dp", "tensor"),
            P("dp", "expert", "tensor"),
            P("dp", "expert", "tensor"),
            P("dp", "tensor"),
            P("dp", "tensor"),
            P("dp", "expert", "tensor"),
            P("dp", "expert", "tensor"),
            P("dp", "tensor"),
            P("dp", "tensor"),
            P("dp", "expert", "tensor"),
            P("dp", "expert", "tensor"),
            P(),
            P(),
            P(),
            P(),
        ),
        check_vma=False,
    )
```

```python
import functools
import math

import jax
import jax.numpy as jnp
import numpy as np
from jax import lax
from jax.experimental import pallas as pl
from jax.experimental.pallas import tpu as pltpu
from jax.sharding import PartitionSpec as P

D = 512
HD = 64
F = 2048
SEQ = 197
EXP_DEV = 2


def layer_norm(values, gain_row, bias_row):
    center = values - jnp.mean(values, axis=-1, keepdims=True)
    invert = lax.rsqrt(jnp.mean(center * center, axis=-1, keepdims=True) + 1e-06)
    scaled = center * invert
    return (scaled * gain_row + bias_row, scaled, invert)


def norm_backward(upstream, scaled, invert, gain_row):
    weighted = upstream * gain_row
    return invert * (
        weighted
        - jnp.mean(weighted, axis=-1, keepdims=True)
        - scaled * jnp.mean(weighted * scaled, axis=-1, keepdims=True)
    )


def gelu_exact(values):
    return 0.5 * values * (1.0 + lax.erf(values * 0.7071067811865476))


def gelu_slope(values):
    return 0.5 * (
        1.0 + lax.erf(values * 0.7071067811865476)
    ) + values * 0.3989422804014327 * jnp.exp(-0.5 * values * values)


def newton_schulz(matrix):
    current = matrix / (jnp.sqrt(jnp.sum(matrix * matrix)) + 1e-07)
    for sweep_index in range(5):
        gram_matrix = jnp.dot(current, current.T, precision=lax.Precision.HIGHEST)
        polynom = -4.775 * gram_matrix + 2.0315 * jnp.dot(
            gram_matrix, gram_matrix, precision=lax.Precision.HIGHEST
        )
        current = 3.4445 * current + jnp.dot(polynom, current, precision=lax.Precision.HIGHEST)
    return current


def start_body(
    tokens_in,
    expert_ids,
    combine,
    out_cot,
    inward_master,
    outward_master,
    up_master,
    down_master,
    norm_gains,
    norm_biases,
    inward_moment,
    outward_moment,
    up_moment,
    down_moment,
    first_moment,
    second_moment,
    step_count,
):
    dp_count = lax.axis_size("dp")
    expert_count = lax.axis_size("expert")
    tensor_count = lax.axis_size("tensor")
    token_rows = tokens_in.shape[0]
    expert_total = EXP_DEV * expert_count
    capacity = (token_rows * 10 // (4 * expert_total) + 7) // 8 * 8
    slot_total = expert_total * capacity
    inputs = tokens_in.astype(jnp.float32)
    w_inward, w_outward, w_up, w_down = (
        lax.all_gather(inward_master.astype(jnp.bfloat16), "dp", axis=0, tiled=True),
        lax.all_gather(outward_master.astype(jnp.bfloat16), "dp", axis=0, tiled=True),
        lax.all_gather(up_master.astype(jnp.bfloat16), "dp", axis=0, tiled=True),
        lax.all_gather(down_master.astype(jnp.bfloat16), "dp", axis=0, tiled=True),
    )
    expert_lanes = jnp.arange(expert_total, dtype=jnp.int32)
    route_hits = (expert_ids[:, :, None] == expert_lanes).astype(jnp.int32)
    per_token = jnp.sum(route_hits, axis=1)
    earlier = jnp.cumsum(per_token, axis=0) - per_token
    position = jnp.sum(route_hits * earlier[:, None, :], axis=2)
    target = expert_ids * capacity + position
    select = (target[:, :, None] == jnp.arange(slot_total, dtype=jnp.int32)).astype(jnp.bfloat16)
    normed1, scaled1, invert1 = layer_norm(inputs, norm_gains[0], norm_biases[0])
    normed1_low = normed1.astype(jnp.bfloat16)
    qkv_low = jnp.dot(normed1_low, w_inward, preferred_element_type=jnp.float32).astype(
        jnp.bfloat16
    )
    heads_here = w_inward.shape[1] // (3 * HD)
    images = token_rows // SEQ
    split_heads = qkv_low.reshape(images, SEQ, heads_here, 3, HD)
    query_part = split_heads[:, :, :, 0]
    key_part = split_heads[:, :, :, 1]
    value_part = split_heads[:, :, :, 2]
    score_scale = HD ** (-0.5)
    scores = (
        jnp.einsum("bihd,bjhd->bhij", query_part, key_part, preferred_element_type=jnp.float32)
        * score_scale
    )
    row_max = jnp.max(scores, axis=-1, keepdims=True)
    exponent = jnp.exp(scores - row_max)
    row_total = jnp.sum(exponent, axis=-1, keepdims=True)
    softmax_out = exponent / row_total
    softmax_low = softmax_out.astype(jnp.bfloat16)
    heads_out = (
        jnp.einsum("bhij,bjhd->bihd", softmax_low, value_part, preferred_element_type=jnp.float32)
        .astype(jnp.bfloat16)
        .reshape(token_rows, heads_here * HD)
    )
    attend_part = jnp.einsum("tc,dc->td", heads_out, w_outward, preferred_element_type=jnp.float32)
    attended = lax.psum(attend_part, "tensor")
    state = inputs + attended
    normed2, scaled2, invert2 = layer_norm(state, norm_gains[1], norm_biases[1])
    normed2_low = normed2.astype(jnp.bfloat16)
    slots_out = jnp.einsum(
        "tks,td->sd", select, normed2_low, preferred_element_type=jnp.float32
    ).astype(jnp.bfloat16)
    arrived = lax.all_to_all(
        slots_out.reshape(expert_count, EXP_DEV, capacity, D),
        "expert",
        split_axis=0,
        concat_axis=0,
        tiled=True,
    )
    pre_act = jnp.einsum("secd,def->secf", arrived, w_up, preferred_element_type=jnp.float32)
    hidden_low = gelu_exact(pre_act).astype(jnp.bfloat16)
    expert_part = jnp.einsum(
        "secf,def->secd", hidden_low, w_down, preferred_element_type=jnp.float32
    ).astype(jnp.bfloat16)
    returned = lax.all_to_all(expert_part, "expert", split_axis=0, concat_axis=0, tiled=True)
    routed = jnp.einsum(
        "tks,sd->tkd", select, returned.reshape(slot_total, D), preferred_element_type=jnp.float32
    )
    mixed_part = jnp.sum(routed * combine[:, :, None], axis=1)
    mixed_sum = lax.psum(mixed_part, "tensor")
    block_out = (state + mixed_sum).astype(jnp.bfloat16)
    routed_grad = (combine[:, :, None] * out_cot[:, None, :]).astype(jnp.bfloat16)
    slot_grad = jnp.einsum(
        "tks,tkd->sd", select, routed_grad, preferred_element_type=jnp.float32
    ).astype(jnp.bfloat16)
    grad_arrived = lax.all_to_all(
        slot_grad.reshape(expert_count, EXP_DEV, capacity, D),
        "expert",
        split_axis=0,
        concat_axis=0,
        tiled=True,
    )
    hidden_grad = jnp.einsum(
        "secd,def->secf", grad_arrived, w_down, preferred_element_type=jnp.float32
    )
    pre_grad = (hidden_grad * gelu_slope(pre_act)).astype(jnp.bfloat16)
    down_local = jnp.einsum(
        "secd,secf->def", grad_arrived, hidden_low, preferred_element_type=jnp.float32
    )
    up_local = jnp.einsum("secd,secf->def", arrived, pre_grad, preferred_element_type=jnp.float32)
    entry_grad = jnp.einsum(
        "secf,def->secd", pre_grad, w_up, preferred_element_type=jnp.float32
    ).astype(jnp.bfloat16)
    entry_back = lax.all_to_all(entry_grad, "expert", split_axis=0, concat_axis=0, tiled=True)
    normed2_part = jnp.einsum(
        "tks,sd->td", select, entry_back.reshape(slot_total, D), preferred_element_type=jnp.float32
    )
    normed2_grad = lax.psum(normed2_part, "tensor")
    state_grad = out_cot + norm_backward(normed2_grad, scaled2, invert2, norm_gains[1])
    state_low = state_grad.astype(jnp.bfloat16)
    outward_local = jnp.einsum(
        "td,tc->dc", state_low, heads_out, preferred_element_type=jnp.float32
    )
    heads_grad = (
        jnp.dot(state_low, w_outward, preferred_element_type=jnp.float32)
        .astype(jnp.bfloat16)
        .reshape(images, SEQ, heads_here, HD)
    )
    prob_grad = jnp.einsum(
        "bihd,bjhd->bhij", heads_grad, value_part, preferred_element_type=jnp.float32
    )
    score_grad = (
        softmax_out * (prob_grad - jnp.sum(softmax_out * prob_grad, axis=-1, keepdims=True))
    ).astype(jnp.bfloat16)
    query_grad = (
        jnp.einsum("bhij,bjhd->bihd", score_grad, key_part, preferred_element_type=jnp.float32)
        * score_scale
    )
    key_grad = (
        jnp.einsum("bhij,bihd->bjhd", score_grad, query_part, preferred_element_type=jnp.float32)
        * score_scale
    )
    value_grad = jnp.einsum(
        "bhij,bihd->bjhd", softmax_low, heads_grad, preferred_element_type=jnp.float32
    )
    qkv_grad = (
        jnp.stack([query_grad, key_grad, value_grad], axis=3)
        .reshape(token_rows, heads_here * 3 * HD)
        .astype(jnp.bfloat16)
    )
    inward_local = jnp.einsum(
        "td,tc->dc", normed1_low, qkv_grad, preferred_element_type=jnp.float32
    )
    normed1_part = jnp.einsum("tc,dc->td", qkv_grad, w_inward, preferred_element_type=jnp.float32)
    normed1_grad = lax.psum(normed1_part, "tensor")
    input_gradient = state_grad + norm_backward(normed1_grad, scaled1, invert1, norm_gains[0])
    norm_terms = jnp.stack(
        [
            jnp.sum(normed1_grad * scaled1, axis=0),
            jnp.sum(normed2_grad * scaled2, axis=0),
            jnp.sum(normed1_grad, axis=0),
            jnp.sum(normed2_grad, axis=0),
        ]
    )
    inward_total, outward_total, norm_total = lax.psum(
        (inward_local, outward_local, norm_terms), ("dp", "expert")
    )
    up_gradient, down_gradient = (
        lax.psum_scatter(up_local, "dp", scatter_dimension=0, tiled=True),
        lax.psum_scatter(down_local, "dp", scatter_dimension=0, tiled=True),
    )
    shard_rows = D // dp_count
    dp_here = lax.axis_index("dp")
    inward_gradient = lax.dynamic_slice_in_dim(inward_total, dp_here * shard_rows, shard_rows, 0)
    outward_gradient = lax.dynamic_slice_in_dim(outward_total, dp_here * shard_rows, shard_rows, 0)
    inward_next = 0.95 * inward_moment + inward_gradient
    outward_next = 0.95 * outward_moment + outward_gradient
    up_next = 0.95 * up_moment + up_gradient
    down_next = 0.95 * down_moment + down_gradient
    matrices = [up_next[:, expert_slot] for expert_slot in range(EXP_DEV)]
    matrices = matrices + [down_next[:, expert_slot] for expert_slot in range(EXP_DEV)]
    matrices = matrices + [jnp.concatenate([inward_next, outward_next], axis=1)]
    stacked = jnp.stack(matrices)
    slot_count = len(matrices)
    group_size = dp_count * tensor_count
    shard_width = stacked.shape[2]
    query_cols = inward_next.shape[1]

    def orth_expert(pieces):
        whole_matrix = pieces.transpose(0, 2, 1, 3).reshape(D, tensor_count * shard_width)
        result = newton_schulz(whole_matrix) * (0.2 * math.sqrt(F))
        return result.reshape(dp_count, shard_rows, tensor_count, shard_width).transpose(0, 2, 1, 3)

    def orth_attention(pieces):
        inward_whole = (
            pieces[..., :query_cols].transpose(0, 2, 1, 3).reshape(D, tensor_count * query_cols)
        )
        outward_whole = (
            pieces[..., query_cols:]
            .transpose(0, 2, 1, 3)
            .reshape(D, tensor_count * (shard_width - query_cols))
        )
        inward_result = newton_schulz(inward_whole) * (0.2 * math.sqrt(3 * D))
        outward_result = newton_schulz(outward_whole) * (0.2 * math.sqrt(D))
        inward_blocks = inward_result.reshape(
            dp_count, shard_rows, tensor_count, query_cols
        ).transpose(0, 2, 1, 3)
        outward_blocks = outward_result.reshape(
            dp_count, shard_rows, tensor_count, shard_width - query_cols
        ).transpose(0, 2, 1, 3)
        return jnp.concatenate([inward_blocks, outward_blocks], axis=3)

    owner_index = lax.axis_index(("dp", "tensor"))
    outgoing = stacked[np.arange(group_size) % slot_count]
    received = lax.all_to_all(outgoing, ("dp", "tensor"), split_axis=0, concat_axis=0, tiled=True)
    blocks = received.reshape(dp_count, tensor_count, shard_rows, shard_width)
    slot_here = owner_index % slot_count
    result_blocks = lax.cond(slot_here == slot_count - 1, orth_attention, orth_expert, blocks)
    arrived_steps = lax.all_to_all(
        result_blocks.reshape(group_size, shard_rows, shard_width),
        ("dp", "tensor"),
        split_axis=0,
        concat_axis=0,
        tiled=True,
    )
    picked = []
    for owned_slot in range(slot_count):
        replicas = (group_size - owned_slot + slot_count - 1) // slot_count
        source = owned_slot + slot_count * (owner_index % replicas)
        picked.append(lax.dynamic_index_in_dim(arrived_steps, source, 0, keepdims=False))
    up_step = jnp.stack(picked[0:EXP_DEV], axis=1)
    down_step = jnp.stack(picked[EXP_DEV : 2 * EXP_DEV], axis=1)
    attend_step = picked[2 * EXP_DEV]
    inward_new = inward_master - 0.1 * (attend_step[:, :query_cols] + 0.1 * inward_master)
    outward_new = outward_master - 0.1 * (attend_step[:, query_cols:] + 0.1 * outward_master)
    up_new = up_master - 0.1 * (up_step + 0.1 * up_master)
    down_new = down_master - 0.1 * (down_step + 0.1 * down_master)
    moment_first = 0.9 * first_moment + 0.1 * norm_total
    moment_second = 0.999 * second_moment + 0.001 * norm_total * norm_total
    steps_done = step_count[0].astype(jnp.float32)
    direction = (
        moment_first
        / (1.0 - jnp.power(0.9, steps_done))
        / (jnp.sqrt(moment_second / (1.0 - jnp.power(0.999, steps_done))) + 1e-08)
    )
    params_new = jnp.concatenate([norm_gains, norm_biases], axis=0) - 0.1 * direction
    return (
        block_out,
        input_gradient,
        inward_gradient,
        outward_gradient,
        up_gradient,
        down_gradient,
        norm_total[0:2],
        norm_total[2:4],
        inward_next,
        outward_next,
        up_next,
        down_next,
        inward_new,
        outward_new,
        up_new,
        down_new,
        inward_new.astype(jnp.bfloat16),
        outward_new.astype(jnp.bfloat16),
        up_new.astype(jnp.bfloat16),
        down_new.astype(jnp.bfloat16),
        params_new[0:2],
        params_new[2:4],
        moment_first,
        moment_second,
    )


PAIRS = (1, 2, 3)
FAR_FIRST = (3, 2, 1, 0)
NOWHERE = 128 * 128 - 1
PAD = 208
NT = (((1,), (1,)), ((), ()))
TN = (((0,), (0,)), ((), ()))


def mxu(left, right, dims=(((1,), (0,)), ((), ()))):
    return lax.dot_general(left, right, dims, preferred_element_type=jnp.float32)


def spread_rows(value, padded_ref):
    padded_ref[...] = jnp.zeros_like(padded_ref)
    for image in range(value.shape[0] // SEQ):
        padded_ref[image * PAD : image * PAD + SEQ, :] = value[image * SEQ : (image + 1) * SEQ]


def gather_rows(padded, out_ref):
    for image in range(out_ref.shape[0] // SEQ):
        out_ref[image * SEQ : (image + 1) * SEQ, :] = padded[
            image * PAD : image * PAD + SEQ
        ].astype(out_ref.dtype)


def peer(me, k):
    return (me, me + 1 - 2 * (me % 2), me + 2 - 4 * (me // 2), 3 - me)[k]


def remote(source, target, send, recv, device):
    copy = pltpu.make_async_remote_copy(
        src_ref=source,
        dst_ref=target,
        send_sem=send,
        recv_sem=recv,
        device_id=device,
        device_id_type=pl.DeviceIdType.MESH,
    )
    copy.start()
    return copy


def keep(source, target, sem):
    copy = pltpu.make_async_copy(source, target, sem)
    copy.start()
    return copy


def greet(dp_here, expert_here, core, over_expert=True):
    barrier = pltpu.get_barrier_semaphore()
    devices = [{"dp": peer(dp_here, k)} for k in PAIRS] + [{"tensor": 1 - core}]
    if over_expert:
        devices += [{"expert": peer(expert_here, k)} for k in PAIRS]
    for device in devices:
        pl.semaphore_signal(
            barrier, inc=1, device_id=device, device_id_type=pl.DeviceIdType.MESH
        )
    return lambda: pl.semaphore_wait(barrier, len(devices))


def block_rows(index, size):
    return pl.ds(pl.multiple_of(index * size, size), size)


def one_hot(cond):
    return jnp.where(cond, 1.0, 0.0).astype(jnp.bfloat16)


def route(ids, capacity, target_ref, target_t_ref):
    rows = ids.shape[0]
    before = lax.broadcasted_iota(jnp.int32, (rows, rows), 0)
    after = lax.broadcasted_iota(jnp.int32, (rows, rows), 1)
    lane = lax.broadcasted_iota(jnp.int32, (rows, 128), 1)
    hits = one_hot((lane == ids[:, 0:1]) | (lane == ids[:, 1:2]))
    earlier = mxu(one_hot(before > after), hits)
    target = jnp.zeros((rows, 128), jnp.int32)
    parts = jnp.zeros((rows, 128), jnp.int32)
    for r in range(2):
        own = ids[:, r : r + 1]
        position = jnp.sum(jnp.where(lane == own, earlier, 0.0), axis=1, keepdims=True)
        value = jnp.where(own >= 0, own * capacity + position.astype(jnp.int32), NOWHERE)
        target = jnp.where(lane == r, value, target)
        parts = jnp.where(lane == 2 * r, value // 128, jnp.where(lane == 2 * r + 1, value % 128, parts))
    target_ref[...] = target
    identity = one_hot(
        lax.broadcasted_iota(jnp.int32, (8, 128), 0) == lax.broadcasted_iota(jnp.int32, (8, 128), 1)
    )
    flipped = mxu(identity, parts.astype(jnp.float32).astype(jnp.bfloat16), NT).astype(jnp.int32)
    for r in range(2):
        target_t_ref[r : r + 1, :] = flipped[2 * r : 2 * r + 1] * 128 + flipped[2 * r + 1 : 2 * r + 2]


def attend(qkv_ref, probs_ref, gift_ref):
    heads_here = qkv_ref.shape[1] // (3 * HD)
    key_lane = lax.broadcasted_iota(jnp.int32, (PAD, PAD), 1)
    for image in range(qkv_ref.shape[0] // PAD):
        rows = slice(image * PAD, (image + 1) * PAD)
        for head in range(heads_here):
            base = head * 3 * HD
            query = qkv_ref[rows, base : base + HD]
            key = qkv_ref[rows, base + HD : base + 2 * HD]
            value = qkv_ref[rows, base + 2 * HD : base + 3 * HD]
            scores = jnp.where(key_lane < SEQ, mxu(query, key, NT) * HD ** (-0.5), -1e30)
            exponent = jnp.exp(scores - jnp.max(scores, axis=-1, keepdims=True))
            probs = exponent / jnp.sum(exponent, axis=-1, keepdims=True)
            probs_ref[image * heads_here + head] = probs
            gift_ref[D + image * PAD : D + (image + 1) * PAD, head * HD : (head + 1) * HD] = mxu(
                probs.astype(jnp.bfloat16), value
            ).astype(jnp.bfloat16)


def front_kernel(
    ids_ref,
    combine_ref,
    cot_ref,
    tokens_ref,
    gains_ref,
    biases_ref,
    inward_ref,
    outward_ref,
    up_ref,
    down_ref,
    up_moment_ref,
    down_moment_ref,
    state_ref,
    gift_ref,
    qkv_ref,
    probs_ref,
    weight_ref,
    target_ref,
    combine_out_ref,
    expert_w_ref,
    arrived_ref,
    grad_arrived_ref,
    moment_whole_ref,
    padded,
    ids_padded,
    target_t_ref,
    attend_shard,
    expert_shard,
    moment_shard,
    gift_other_ref,
    grad_chunks,
    token_chunks,
    inner_send,
    inner_recv,
    expert_send,
    expert_recv,
    slot_send,
    slot_recv,
    share_send,
    share_recv,
    gift_sems,
    keep_sems,
    moment_send,
    moment_recv,
):
    bf16 = jnp.bfloat16
    dp_here, expert_here, core = (lax.axis_index(a) for a in ("dp", "expert", "tensor"))
    partner = {"tensor": 1 - core}
    capacity = grad_chunks.shape[1]
    shard_rows = attend_shard.shape[0]
    qcols = qkv_ref.shape[1]
    here = block_rows(dp_here, shard_rows)
    ready = greet(dp_here, expert_here, core)

    attend_shard[:, :qcols] = inward_ref[...].astype(bf16)
    attend_shard[:, qcols:] = outward_ref[...].astype(bf16)
    weight_ref[here, :] = attend_shard[...]
    ready()
    inner = [
        remote(
            attend_shard,
            weight_ref.at[here, :],
            inner_send.at[k - 1],
            inner_recv.at[k - 1],
            {"dp": peer(dp_here, k)},
        )
        for k in PAIRS
    ]
    kept = []

    spread_rows(ids_ref[...] + 1, ids_padded)
    route(ids_padded[...] - 1, capacity, target_ref, target_t_ref)
    spread_rows(combine_ref[...], combine_out_ref)
    spread_rows(cot_ref[...], padded)
    slot = lax.broadcasted_iota(jnp.int32, (capacity, padded.shape[0]), 0)

    def first_slot(k):
        return (2 * peer(expert_here, k) + core) * capacity

    def send_chunks(fill, chunks, landing, which):
        copies, shared = {}, []
        for place, k in enumerate(FAR_FIRST):
            chunks[k] = fill(slot + first_slot(k)).astype(bf16)
            if place > 0:
                last = FAR_FIRST[place - 1]
                copies[last] = remote(
                    chunks.at[last],
                    landing.at[0, last],
                    slot_send.at[which, last],
                    slot_recv.at[which, last],
                    {"expert": peer(expert_here, last)},
                )
        kept.append(keep(chunks.at[0], landing.at[0, 0], keep_sems.at[1 + which]))
        shared.append(
            remote(
                chunks.at[0],
                landing.at[1, 0],
                share_send.at[which, 0],
                share_recv.at[which, 0],
                partner,
            )
        )
        return copies, shared

    def share_arrivals(copies, landing, which, shared):
        for k in FAR_FIRST[:3]:
            copies[k].wait_recv()
            shared.append(
                remote(
                    landing.at[0, k],
                    landing.at[1, k],
                    share_send.at[which, k],
                    share_recv.at[which, k],
                    partner,
                )
            )

    grads = [(combine_out_ref[:, r : r + 1] * padded[...]).astype(bf16) for r in range(2)]
    grad_copies, grad_shared = send_chunks(
        lambda slots: sum(mxu(one_hot(target_t_ref[r : r + 1] == slots), grads[r]) for r in range(2)),
        grad_chunks,
        grad_arrived_ref,
        0,
    )
    for which, ref in enumerate((up_ref, down_ref)):
        pair = [ref[:, e, :].astype(bf16) for e in range(EXP_DEV)]
        for j in range(EXP_DEV):
            expert_shard[EXP_DEV * which + j] = jnp.where(core == 0, pair[j], pair[1 - j])
    spread_rows(tokens_ref[...].astype(jnp.float32), padded)
    normed, unused, unused = layer_norm(padded[...], gains_ref[0:1], biases_ref[0:1])
    normed_low = normed.astype(bf16)
    weights = [
        remote(
            expert_shard,
            expert_w_ref.at[:, here, :],
            expert_send.at[k - 1],
            expert_recv.at[k - 1],
            {"dp": peer(dp_here, k)},
        )
        for k in (1, 2)
    ]
    kept.append(keep(expert_shard, expert_w_ref.at[:, here, :], keep_sems.at[0]))
    for which, ref in enumerate((up_moment_ref, down_moment_ref)):
        for e in range(EXP_DEV):
            moment_shard[EXP_DEV * which + e] = ref[:, e, :].astype(bf16)
    for copy in inner:
        copy.wait_recv()
    qkv_ref[...] = mxu(normed_low, weight_ref[:, :qcols]).astype(bf16)
    gift_ref[0:D, :] = weight_ref[:, qcols:]
    attend(qkv_ref, probs_ref, gift_ref)
    gift = remote(gift_ref, gift_other_ref, gift_sems.at[0], gift_sems.at[1], partner)
    half = padded[...] + mxu(gift_ref[D:, :], gift_ref[0:D, :], NT)
    gift.wait()
    state = half + mxu(gift_other_ref[D:, :], gift_other_ref[0:D, :], NT)
    state_ref[...] = state
    normed, unused, unused = layer_norm(state, gains_ref[1:2], biases_ref[1:2])
    normed_low = normed.astype(bf16)
    token_copies, token_shared = send_chunks(
        lambda slots: mxu(
            one_hot((target_t_ref[0:1] == slots) | (target_t_ref[1:2] == slots)), normed_low
        ),
        token_chunks,
        arrived_ref,
        1,
    )
    for copy in weights:
        copy.wait_recv()
    for k, part in ((1, slice(0, EXP_DEV)), (2, slice(EXP_DEV, 2 * EXP_DEV))):
        block = expert_w_ref.at[part, block_rows(peer(dp_here, k), shard_rows), :]
        weights.append(
            remote(
                block,
                block,
                expert_send.at[k + 1],
                expert_recv.at[k + 1],
                {"dp": peer(dp_here, 3 - k)},
            )
        )
    moments = [
        remote(
            moment_shard.at[peer(dp_here, k)],
            moment_whole_ref.at[here, :],
            moment_send.at[k - 1],
            moment_recv.at[k - 1],
            {"dp": peer(dp_here, k)},
        )
        for k in PAIRS
    ]
    kept.append(keep(moment_shard.at[dp_here], moment_whole_ref.at[here, :], keep_sems.at[3]))
    share_arrivals(grad_copies, grad_arrived_ref, 0, grad_shared)
    share_arrivals(token_copies, arrived_ref, 1, token_shared)
    for copy in grad_shared + token_shared + moments + weights[2:]:
        copy.wait()
    for copy in weights[:2] + inner:
        copy.wait_send()
    for copies in (grad_copies, token_copies):
        for k in PAIRS:
            copies[k].wait_send()
    for copy in kept:
        copy.wait()


def back_kernel(
    cot_ref,
    tokens_ref,
    gains_ref,
    biases_ref,
    combine_ref,
    state_ref,
    gift_ref,
    qkv_ref,
    probs_ref,
    weight_ref,
    target_ref,
    entry_ref,
    part_ref,
    matrices_ref,
    moment_whole_ref,
    attend_moment_ref,
    input_ref,
    block_ref,
    norm_ref,
    attend_grad_ref,
    attend_whole_ref,
    own_steps_ref,
    home_grads_ref,
    padded,
    qkv_grad_ref,
    local_ref,
    normed_part_ref,
    normed_other_ref,
    handed,
    summed,
    returned,
    inner,
    inner_in,
    plane,
    plane_in,
    whole_own,
    norm_own,
    norm_in,
    owned_in,
    owned_low,
    owned_next,
    gram,
    gram_other,
    factor,
    change,
    hand_send,
    hand_recv,
    slot_send,
    slot_recv,
    share_send,
    share_recv,
    pair_send,
    pair_recv,
    dp_send,
    dp_recv,
    expert_send,
    expert_recv,
    keep_sems,
):
    bf16, f32 = jnp.bfloat16, jnp.float32
    dp_here, expert_here, core = (lax.axis_index(a) for a in ("dp", "expert", "tensor"))
    partner = {"tensor": 1 - core}
    qcols = qkv_ref.shape[1]
    rows_all = state_ref.shape[0]
    capacity = entry_ref.shape[2]
    shard_rows = inner.shape[1]
    here = block_rows(dp_here, shard_rows)
    greet(dp_here, expert_here, core)()
    sent = []

    def held(index):
        return 2 * (index // 2) + (index % 2 + core) % 2

    def to_dp(stage, sources, targets):
        copies = [
            remote(
                sources(k),
                targets(k),
                dp_send.at[stage, k - 1],
                dp_recv.at[stage, k - 1],
                {"dp": peer(dp_here, k)},
            )
            for k in PAIRS
        ]
        sent.extend(copies)
        return copies

    def to_expert(stage, source, target):
        copies = [
            remote(
                source,
                target,
                expert_send.at[stage, k - 1],
                expert_recv.at[stage, k - 1],
                {"expert": peer(expert_here, k)},
            )
            for k in PAIRS
        ]
        sent.extend(copies)
        return copies

    def arrive(copies):
        for copy in copies:
            copy.wait_recv()

    hands = []
    for which, ref in enumerate((entry_ref, part_ref)):
        hands.append(
            [
                remote(
                    ref.at[1, k],
                    handed.at[which, k],
                    hand_send.at[which, k],
                    hand_recv.at[which, k],
                    partner,
                )
                for k in range(4)
            ]
        )
        sent.extend(hands[which])
    kept = [keep(matrices_ref.at[held(dp_here)], owned_in.at[0], keep_sems.at[0])]
    matrices = to_dp(0, lambda k: matrices_ref.at[held(peer(dp_here, k))], lambda k: owned_in.at[k])
    homes, shares = [], []
    for which, ref in enumerate((entry_ref, part_ref)):
        arrive(hands[which])
        for k in range(4):
            summed[which, k] = (ref[0, k].astype(f32) + handed[which, k].astype(f32)).astype(bf16)
        homes.append(
            {
                k: remote(
                    summed.at[which, k],
                    returned.at[which, 0, k],
                    slot_send.at[which, k],
                    slot_recv.at[which, k],
                    {"expert": peer(expert_here, k)},
                )
                for k in FAR_FIRST[:3]
            }
        )
        sent.extend(homes[which].values())
        shares.append(
            [
                remote(
                    summed.at[which, 0],
                    returned.at[which, 1, 0],
                    share_send.at[which, 0],
                    share_recv.at[which, 0],
                    partner,
                )
            ]
        )
        returned[which, 0, 0] = summed[which, 0]

    def share(which):
        for k in FAR_FIRST[:3]:
            homes[which][k].wait_recv()
            shares[which].append(
                remote(
                    returned.at[which, 0, k],
                    returned.at[which, 1, k],
                    share_send.at[which, k],
                    share_recv.at[which, k],
                    partner,
                )
            )
        sent.extend(shares[which])
        arrive(shares[which])

    unused, scaled2, invert2 = layer_norm(state_ref[...], gains_ref[1:2], biases_ref[1:2])
    spread_rows(cot_ref[...], padded)
    slot = lax.broadcasted_iota(jnp.int32, (rows_all, capacity), 1)

    def picks(k, j, columns):
        first = slot + (2 * peer(expert_here, k) + (core + j) % 2) * capacity
        hit = target_ref[:, columns[0] : columns[0] + 1] == first
        for column in columns[1:]:
            hit = hit | (target_ref[:, column : column + 1] == first)
        return one_hot(hit)

    def pick_all(which, columns):
        total = jnp.zeros((rows_all, D), f32)
        for j in range(2):
            for k in FAR_FIRST:
                total += mxu(picks(k, j, columns), returned[which, j, k])
        return total

    share(0)
    normed2_grad = pick_all(0, (0, 1))
    norm_own[0, 4:8] = jnp.zeros((4, D), f32)
    norm_own[0, 1:2] = jnp.sum(normed2_grad * scaled2, axis=0, keepdims=True)
    norm_own[0, 3:4] = jnp.sum(normed2_grad, axis=0, keepdims=True)
    state_grad = padded[...] + norm_backward(normed2_grad, scaled2, invert2, gains_ref[1:2])
    padded[...] = state_grad
    state_low = state_grad.astype(bf16)
    local_ref[:, qcols:] = mxu(state_low, gift_ref[D:, :], TN)
    heads_grad = mxu(state_low, weight_ref[:, qcols:]).astype(bf16)
    heads_here = qcols // (3 * HD)
    scale = HD ** (-0.5)
    for image in range(rows_all // PAD):
        rows = slice(image * PAD, (image + 1) * PAD)
        for head in range(heads_here):
            base = head * 3 * HD
            query = qkv_ref[rows, base : base + HD]
            key = qkv_ref[rows, base + HD : base + 2 * HD]
            value = qkv_ref[rows, base + 2 * HD : base + 3 * HD]
            out_grad = heads_grad[image * PAD : (image + 1) * PAD, head * HD : (head + 1) * HD]
            probs = probs_ref[image * heads_here + head]
            prob_grad = mxu(out_grad, value, NT)
            score_grad = (
                probs * (prob_grad - jnp.sum(probs * prob_grad, axis=-1, keepdims=True))
            ).astype(bf16)
            qkv_grad_ref[rows, base : base + HD] = (mxu(score_grad, key) * scale).astype(bf16)
            qkv_grad_ref[rows, base + HD : base + 2 * HD] = (
                mxu(score_grad, query, TN) * scale
            ).astype(bf16)
            qkv_grad_ref[rows, base + 2 * HD : base + 3 * HD] = mxu(
                probs.astype(bf16), out_grad, TN
            ).astype(bf16)
    spread_rows(tokens_ref[...].astype(f32), normed_part_ref)
    normed1, scaled1, invert1 = layer_norm(normed_part_ref[...], gains_ref[0:1], biases_ref[0:1])
    local_ref[:, :qcols] = mxu(normed1.astype(bf16), qkv_grad_ref[...], TN)
    for k in range(4):
        inner[k] = local_ref[block_rows(peer(dp_here, k), shard_rows), :].astype(bf16)
    normed_part_ref[...] = mxu(qkv_grad_ref[...], weight_ref[:, :qcols], NT)
    rows_sums = to_dp(1, lambda k: inner.at[k], lambda k: inner_in.at[k - 1])
    pair = remote(normed_part_ref, normed_other_ref, pair_send.at[0], pair_recv.at[0], partner)
    sent.append(pair)

    share(1)
    total = state_ref[...]
    for r in range(2):
        total += combine_ref[:, r : r + 1] * pick_all(1, (r,))
    gather_rows(total, block_ref)

    pair.wait_recv()
    normed1_grad = normed_part_ref[...] + normed_other_ref[...]
    norm_own[0, 0:1] = jnp.sum(normed1_grad * scaled1, axis=0, keepdims=True)
    norm_own[0, 2:3] = jnp.sum(normed1_grad, axis=0, keepdims=True)
    norm_in[0, dp_here] = norm_own[0]
    norms = to_dp(2, lambda k: norm_own.at[0], lambda k: norm_in.at[0, dp_here])
    gather_rows(
        padded[...] + norm_backward(normed1_grad, scaled1, invert1, gains_ref[0:1]), input_ref
    )

    arrive(rows_sums)
    plane[...] = (
        inner[0].astype(f32)
        + inner_in[0].astype(f32)
        + inner_in[1].astype(f32)
        + inner_in[2].astype(f32)
    ).astype(bf16)
    plane_in[expert_here] = plane[...]
    arrive(norms)
    norm_plane = norm_in[0, 0] + norm_in[0, 1] + norm_in[0, 2] + norm_in[0, 3]
    norm_own[1] = norm_plane
    norm_in[1, expert_here] = norm_plane
    planes = to_expert(0, plane, plane_in.at[expert_here])
    norm_sums = to_expert(1, norm_own.at[1], norm_in.at[1, expert_here])

    arrive(matrices)
    kept[0].wait()
    owned = (
        owned_in[0].astype(f32)
        + owned_in[1].astype(f32)
        + owned_in[2].astype(f32)
        + owned_in[3].astype(f32)
    )
    owned_low[...] = owned.astype(bf16)
    owned_next[...] = 0.95 * moment_whole_ref[...].astype(f32) + owned
    split = halves(owned_next[...])
    gram[...] = mxu3(split, split, NT)
    pair = remote(gram, gram_other, pair_send.at[1], pair_recv.at[1], partner)
    home = to_dp(
        3,
        lambda k: owned_low.at[block_rows(peer(dp_here, k), shard_rows), :],
        lambda k: home_grads_ref.at[dp_here],
    )
    kept.append(keep(owned_low.at[here, :], home_grads_ref.at[dp_here], keep_sems.at[1]))
    pair.wait()
    find_factor(gram[...] + gram_other[...], factor, gram, change, gram_other)

    arrive(planes)
    attend_grad = (
        plane_in[0].astype(f32)
        + plane_in[1].astype(f32)
        + plane_in[2].astype(f32)
        + plane_in[3].astype(f32)
    )
    attend_grad_ref[...] = attend_grad
    attend_next = 0.95 * attend_moment_ref[...] + attend_grad
    whole_own[...] = attend_next.astype(bf16)
    attend_whole_ref[here, :] = whole_own[...]
    wholes = to_dp(4, lambda k: whole_own, lambda k: attend_whole_ref.at[here, :])
    arrive(norm_sums)
    norm_ref[...] = (
        norm_in[1, 0, 0:4] + norm_in[1, 1, 0:4] + norm_in[1, 2, 0:4] + norm_in[1, 3, 0:4]
    )
    own_steps_ref[...] = (
        mxu3(halves(factor[...]), halves(owned_next[...])) * (0.2 * math.sqrt(F))
    ).astype(bf16)
    arrive(home)
    arrive(wholes)
    for copy in sent:
        copy.wait_send()
    for copy in kept[1:]:
        copy.wait()


def halves(value):
    high = value.astype(jnp.bfloat16)
    return high, (value - high.astype(jnp.float32)).astype(jnp.bfloat16)


def mxu3(left, right, dims=(((1,), (0,)), ((), ()))):
    return (
        mxu(left[0], right[0], dims) + mxu(left[1], right[0], dims) + mxu(left[0], right[1], dims)
    )


def find_factor(gram, factor, current, change, scaled):
    diagonal = lax.broadcasted_iota(jnp.int32, gram.shape, 0) == lax.broadcasted_iota(
        jnp.int32, gram.shape, 1
    )
    squares = jnp.sum(
        jnp.sum(jnp.where(diagonal, gram, 0.0), axis=1, keepdims=True), axis=0, keepdims=True
    )
    norm = jnp.sqrt(squares) + 1e-07
    current[...] = gram / (norm * norm)
    factor[...] = jnp.where(diagonal, 1.0 / norm, 0.0)

    def sweep(index, carry):
        low = halves(current[...])
        change[...] = -4.775 * current[...] + 2.0315 * mxu3(low, low)
        step = halves(change[...])
        factor[...] = 3.4445 * factor[...] + mxu3(step, halves(factor[...]))
        scaled[...] = 3.4445 * current[...] + mxu3(step, low)
        current[...] = 3.4445 * scaled[...] + mxu3(halves(scaled[...]), step)
        return carry

    lax.fori_loop(0, 5, sweep, 0)


def finish_kernel(
    whole_ref,
    own_steps_ref,
    home_steps_ref,
    attend_step_ref,
    kept,
    given,
    taken,
    factor,
    change,
    mine,
    other,
    step_send,
    step_recv,
    pair_send,
    pair_recv,
):
    dp_here, core = lax.axis_index("dp"), lax.axis_index("tensor")
    partner = {"tensor": 1 - core}
    shard_rows = mine.shape[0]
    qcols = 3 * whole_ref.shape[1] // 4
    here = block_rows(dp_here, shard_rows)
    ready = greet(dp_here, None, core, over_expert=False)
    inward_gram = mxu(whole_ref[:, :qcols], whole_ref[:, :qcols], NT)
    outward_gram = mxu(whole_ref[:, qcols:], whole_ref[:, qcols:], NT)
    kept[...] = jnp.where(core == 0, inward_gram, outward_gram)
    given[...] = jnp.where(core == 0, outward_gram, inward_gram)
    ready()
    pair = remote(given, taken, pair_send.at[0], pair_recv.at[0], partner)
    steps = [
        remote(
            own_steps_ref.at[block_rows(peer(dp_here, k), shard_rows), :],
            home_steps_ref.at[dp_here],
            step_send.at[k - 1],
            step_recv.at[k - 1],
            {"dp": peer(dp_here, k)},
        )
        for k in PAIRS
    ]
    home_steps_ref[dp_here] = own_steps_ref[here, :]
    pair.wait()
    find_factor(kept[...] + taken[...], factor, kept, change, taken)
    mine[...] = factor[here, :]
    pair = remote(mine, other, pair_send.at[1], pair_recv.at[1], partner)
    for copy in steps:
        copy.wait()
    pair.wait()
    for owner, columns, count in ((0, slice(0, qcols), 3 * D), (1, slice(qcols, None), D)):
        rows = halves(jnp.where(core == owner, mine[...], other[...]))
        step = mxu(rows[0], whole_ref[:, columns]) + mxu(rows[1], whole_ref[:, columns])
        attend_step_ref[:, columns] = step * (0.2 * math.sqrt(count))


def apply_kernel(
    steps_done_ref,
    home_steps_ref,
    attend_step_ref,
    home_grads_ref,
    attend_grad_ref,
    norm_ref,
    gains_ref,
    biases_ref,
    first_ref,
    second_ref,
    inward_ref,
    outward_ref,
    up_ref,
    down_ref,
    inward_moment_ref,
    outward_moment_ref,
    up_moment_ref,
    down_moment_ref,
    block_ref,
    input_ref,
    block_out_ref,
    input_out_ref,
    inward_gradient_ref,
    outward_gradient_ref,
    up_gradient_ref,
    down_gradient_ref,
    gain_gradient_ref,
    bias_gradient_ref,
    inward_next_ref,
    outward_next_ref,
    up_next_ref,
    down_next_ref,
    inward_new_ref,
    outward_new_ref,
    up_new_ref,
    down_new_ref,
    inward_copy_ref,
    outward_copy_ref,
    up_copy_ref,
    down_copy_ref,
    gains_new_ref,
    biases_new_ref,
    first_new_ref,
    second_new_ref,
):
    f32 = jnp.float32
    qcols = inward_ref.shape[1]
    block_out_ref[...] = block_ref[...]
    input_out_ref[...] = input_ref[...]

    def finish(place, gradient, step, refs):
        master_ref, moment_ref, gradient_ref, next_ref, new_ref, copy_ref = refs
        gradient_ref[place] = gradient
        next_ref[place] = 0.95 * moment_ref[place] + gradient
        master = master_ref[place]
        new = master - 0.1 * (step + 0.1 * master)
        new_ref[place] = new
        copy_ref[place] = new.astype(copy_ref.dtype)

    experts = (
        (up_ref, up_moment_ref, up_gradient_ref, up_next_ref, up_new_ref, up_copy_ref),
        (down_ref, down_moment_ref, down_gradient_ref, down_next_ref, down_new_ref, down_copy_ref),
    )
    for which, refs in enumerate(experts):
        for e in range(EXP_DEV):
            index = EXP_DEV * which + e
            finish(
                (slice(None), e, slice(None)),
                home_grads_ref[index].astype(f32),
                home_steps_ref[index].astype(f32),
                refs,
            )
    everything = (slice(None), slice(None))
    finish(
        everything,
        attend_grad_ref[:, :qcols],
        attend_step_ref[:, :qcols],
        (
            inward_ref,
            inward_moment_ref,
            inward_gradient_ref,
            inward_next_ref,
            inward_new_ref,
            inward_copy_ref,
        ),
    )
    finish(
        everything,
        attend_grad_ref[:, qcols:],
        attend_step_ref[:, qcols:],
        (
            outward_ref,
            outward_moment_ref,
            outward_gradient_ref,
            outward_next_ref,
            outward_new_ref,
            outward_copy_ref,
        ),
    )

    @pl.when(pl.program_id(0) == 0)
    def norms():
        total = norm_ref[...]
        gain_gradient_ref[...] = total[0:2]
        bias_gradient_ref[...] = total[2:4]
        moment_first = 0.9 * first_ref[...] + 0.1 * total
        moment_second = 0.999 * second_ref[...] + 0.001 * total * total
        first_new_ref[...] = moment_first
        second_new_ref[...] = moment_second
        done = jnp.full((4, D), steps_done_ref[0], jnp.int32).astype(f32)
        direction = (
            moment_first
            / (1.0 - jnp.power(0.9, done))
            / (jnp.sqrt(moment_second / (1.0 - jnp.power(0.999, done))) + 1e-08)
        )
        gains_new_ref[...] = gains_ref[...] - 0.1 * direction[0:2]
        biases_new_ref[...] = biases_ref[...] - 0.1 * direction[2:4]


def pair_body(
    tokens_in,
    expert_ids,
    combine,
    out_cot,
    inward_master,
    outward_master,
    up_master,
    down_master,
    norm_gains,
    norm_biases,
    inward_moment,
    outward_moment,
    up_moment,
    down_moment,
    first_moment,
    second_moment,
    step_count,
):
    bf16, f32 = jnp.bfloat16, jnp.float32
    token_rows = tokens_in.shape[0]
    expert_total = EXP_DEV * 4
    capacity = (token_rows * 10 // (4 * expert_total) + 7) // 8 * 8
    shard_rows, qcols = inward_master.shape
    width = up_master.shape[2]
    images = token_rows // SEQ
    padded_rows = images * PAD
    heads_here = qcols // (3 * HD)
    shape = jax.ShapeDtypeStruct
    rows_f32 = pltpu.VMEM((padded_rows, D), f32)
    in_vmem, anywhere = pl.BlockSpec(memory_space=pltpu.VMEM), pl.BlockSpec(memory_space=pl.ANY)
    dma = pltpu.SemaphoreType.DMA

    def matmul(spec, a, b):
        return jnp.einsum(spec, a, b, preferred_element_type=f32)

    slots = shape((EXP_DEV, 4, capacity, D), bf16)
    (
        state,
        gift,
        qkv_low,
        probs,
        weight,
        target,
        combine_padded,
        expert_w,
        arrived,
        grad_arrived,
        moment_whole,
    ) = pl.pallas_call(
        front_kernel,
        out_shape=(
            shape((padded_rows, D), f32),
            shape((D + padded_rows, heads_here * HD), bf16),
            shape((padded_rows, qcols), bf16),
            shape((images * heads_here, PAD, PAD), f32),
            shape((D, width), bf16),
            shape((padded_rows, 128), jnp.int32),
            shape((padded_rows, 2), f32),
            shape((2 * EXP_DEV, D, width), bf16),
            slots,
            slots,
            shape((D, width), bf16),
        ),
        in_specs=[in_vmem] * 12,
        out_specs=tuple([in_vmem] * 7 + [anywhere] * 4),
        scratch_shapes=[
            rows_f32,
            pltpu.VMEM((padded_rows, 2), jnp.int32),
            pltpu.VMEM((2, padded_rows), jnp.int32),
            pltpu.VMEM((shard_rows, width), bf16),
            pltpu.VMEM((4, shard_rows, width), bf16),
            pltpu.VMEM((4, shard_rows, width), bf16),
            pltpu.VMEM((D + padded_rows, heads_here * HD), bf16),
            pltpu.VMEM((4, capacity, D), bf16),
            pltpu.VMEM((4, capacity, D), bf16),
            dma((3,)),
            dma((3,)),
            dma((4,)),
            dma((4,)),
            dma((2, 4)),
            dma((2, 4)),
            dma((2, 4)),
            dma((2, 4)),
            dma((2,)),
            dma((4,)),
            dma((3,)),
            dma((3,)),
        ],
        name="front",
        cost_estimate=pl.CostEstimate(
            flops=60_000_000_000, bytes_accessed=30_000_000, transcendentals=0
        ),
        compiler_params=pltpu.CompilerParams(collective_id=0, has_side_effects=True),
    )(
        expert_ids,
        combine,
        out_cot,
        tokens_in,
        norm_gains,
        norm_biases,
        inward_master,
        outward_master,
        up_master,
        down_master,
        up_moment,
        down_moment,
    )
    arrived = arrived.reshape(EXP_DEV, 4 * capacity, D)
    grad_arrived = grad_arrived.reshape(EXP_DEV, 4 * capacity, D)
    w_up, w_down = expert_w[:2], expert_w[2:]

    pre_act = matmul("erd,edf->erf", arrived, w_up)
    hidden_low = gelu_exact(pre_act).astype(bf16)
    hidden_grad = matmul("erd,edf->erf", grad_arrived, w_down)
    pre_grad = (hidden_grad * gelu_slope(pre_act)).astype(bf16)
    entry_grad = matmul("erf,edf->erd", pre_grad, w_up).astype(bf16)
    expert_part = matmul("erf,edf->erd", hidden_low, w_down).astype(bf16)
    up_local = matmul("erd,erf->edf", arrived, pre_grad)
    down_local = matmul("erd,erf->edf", grad_arrived, hidden_low)
    matrices = jnp.concatenate([up_local, down_local], axis=0).astype(bf16)

    chunks = (2, 4, capacity, D)
    square = pltpu.VMEM((D, D), f32)
    (
        input_gradient,
        block_out,
        norm_total,
        attend_grad,
        attend_whole,
        own_steps,
        home_grads,
    ) = pl.pallas_call(
        back_kernel,
        out_shape=(
            shape((token_rows, D), f32),
            shape((token_rows, D), bf16),
            shape((4, D), f32),
            shape((shard_rows, width), f32),
            shape((D, width), bf16),
            shape((D, width), bf16),
            shape((4, shard_rows, width), bf16),
        ),
        in_specs=[in_vmem] * 13 + [anywhere] + [in_vmem] * 2,
        out_specs=tuple([in_vmem] * 6 + [anywhere]),
        scratch_shapes=[
            rows_f32,
            pltpu.VMEM((padded_rows, qcols), bf16),
            pltpu.VMEM((D, width), f32),
            rows_f32,
            rows_f32,
            pltpu.VMEM(chunks, bf16),
            pltpu.VMEM(chunks, bf16),
            pltpu.VMEM((2,) + chunks, bf16),
            pltpu.VMEM((4, shard_rows, width), bf16),
            pltpu.VMEM((3, shard_rows, width), bf16),
            pltpu.VMEM((shard_rows, width), bf16),
            pltpu.VMEM((4, shard_rows, width), bf16),
            pltpu.VMEM((shard_rows, width), bf16),
            pltpu.VMEM((2, 8, D), f32),
            pltpu.VMEM((2, 4, 8, D), f32),
            pltpu.VMEM((4, D, width), bf16),
            pltpu.VMEM((D, width), bf16),
            pltpu.VMEM((D, width), f32),
        ]
        + [square] * 4
        + [dma((2, 4))] * 6
        + [dma((2,))] * 2
        + [dma((5, 3))] * 2
        + [dma((2, 3))] * 2
        + [dma((2,))],
        name="back",
        cost_estimate=pl.CostEstimate(
            flops=90_000_000_000, bytes_accessed=60_000_000, transcendentals=0
        ),
        compiler_params=pltpu.CompilerParams(
            collective_id=1, has_side_effects=True, vmem_limit_bytes=66_000_000
        ),
    )(
        out_cot,
        tokens_in,
        norm_gains,
        norm_biases,
        combine_padded,
        state,
        gift,
        qkv_low,
        probs,
        weight,
        target,
        entry_grad.reshape(chunks),
        expert_part.reshape(chunks),
        matrices,
        moment_whole,
        jnp.concatenate([inward_moment, outward_moment], axis=1),
    )
    factor_rows = pltpu.VMEM((shard_rows, D), f32)
    home_steps, attend_step = pl.pallas_call(
        finish_kernel,
        out_shape=(shape((4, shard_rows, width), bf16), shape((shard_rows, width), f32)),
        in_specs=[in_vmem] * 2,
        out_specs=(in_vmem, in_vmem),
        scratch_shapes=[square] * 5 + [factor_rows] * 2 + [dma((3,))] * 2 + [dma((2,))] * 2,
        name="finish",
        cost_estimate=pl.CostEstimate(
            flops=20_000_000_000, bytes_accessed=5_000_000, transcendentals=0
        ),
        compiler_params=pltpu.CompilerParams(collective_id=2, has_side_effects=True),
    )(attend_whole, own_steps)

    blocks = 4
    inward, outward, expert = (a.shape for a in (inward_master, outward_master, up_master))

    def split(whole, along=0):
        if along is None:
            return pl.BlockSpec(whole, lambda i: (0,) * len(whole))
        rows = pl.cdiv(pl.cdiv(whole[along], blocks), 8) * 8
        block = whole[:along] + (rows,) + whole[along + 1 :]
        return pl.BlockSpec(
            block, lambda i: (0,) * along + (i,) + (0,) * (len(whole) - along - 1)
        )

    two, four, attended = (2, D), (4, D), (shard_rows, width)
    matrix_shapes = (inward, outward, expert, expert)
    by_rows = [split(m) for m in matrix_shapes]
    tokens = split((token_rows, D))
    finished = pl.pallas_call(
        apply_kernel,
        grid=(blocks,),
        out_shape=tuple(
            [shape((token_rows, D), bf16), shape((token_rows, D), f32)]
            + [shape(m, f32) for m in matrix_shapes]
            + [shape(two, f32)] * 2
            + [shape(m, f32) for m in matrix_shapes * 2]
            + [shape(m, bf16) for m in matrix_shapes]
            + [shape(two, f32)] * 2
            + [shape(four, f32)] * 2
        ),
        in_specs=[pl.BlockSpec(memory_space=pltpu.SMEM)]
        + [split((4,) + attended, 1), split(attended), split((4,) + attended, 1), split(attended)]
        + [split(four, None), split(two, None), split(two, None), split(four, None), split(four, None)]
        + by_rows * 2
        + [tokens] * 2,
        out_specs=tuple(
            [tokens] * 2
            + by_rows
            + [split(two, None)] * 2
            + by_rows * 3
            + [split(two, None)] * 2
            + [split(four, None)] * 2
        ),
        name="apply",
        cost_estimate=pl.CostEstimate(
            flops=20_000_000, bytes_accessed=20_000_000, transcendentals=0
        ),
    )(
        step_count,
        home_steps,
        attend_step,
        home_grads,
        attend_grad,
        norm_total,
        norm_gains,
        norm_biases,
        first_moment,
        second_moment,
        inward_master,
        outward_master,
        up_master,
        down_master,
        inward_moment,
        outward_moment,
        up_moment,
        down_moment,
        block_out,
        input_gradient,
    )
    return tuple(finished)


def solution(mesh):
    sizes = tuple(mesh.shape[axis] for axis in ("dp", "expert", "tensor"))
    body = pair_body if sizes == (4, 4, 2) else start_body
    return jax.shard_map(
        body,
        mesh=mesh,
        in_specs=(
            P(("dp", "expert"), None),
            P(("dp", "expert"), None),
            P(("dp", "expert"), None),
            P(("dp", "expert"), None),
            P("dp", "tensor"),
            P("dp", "tensor"),
            P("dp", "expert", "tensor"),
            P("dp", "expert", "tensor"),
            P(),
            P(),
            P("dp", "tensor"),
            P("dp", "tensor"),
            P("dp", "expert", "tensor"),
            P("dp", "expert", "tensor"),
            P(),
            P(),
            P(),
        ),
        out_specs=(
            P(("dp", "expert"), None),
            P(("dp", "expert"), None),
            P("dp", "tensor"),
            P("dp", "tensor"),
            P("dp", "expert", "tensor"),
            P("dp", "expert", "tensor"),
            P(),
            P(),
            P("dp", "tensor"),
            P("dp", "tensor"),
            P("dp", "expert", "tensor"),
            P("dp", "expert", "tensor"),
            P("dp", "tensor"),
            P("dp", "tensor"),
            P("dp", "expert", "tensor"),
            P("dp", "expert", "tensor"),
            P("dp", "tensor"),
            P("dp", "tensor"),
            P("dp", "expert", "tensor"),
            P("dp", "expert", "tensor"),
            P(),
            P(),
            P(),
            P(),
        ),
        check_vma=False,
    )
```

```python
import functools
import math

import jax
import jax.numpy as jnp
import numpy as np
from jax import lax
from jax.experimental import pallas as pl
from jax.experimental.pallas import tpu as pltpu
from jax.sharding import PartitionSpec as P

D = 512
HD = 64
F = 2048
SEQ = 197
EXP_DEV = 2


def layer_norm(values, gain_row, bias_row):
    center = values - jnp.mean(values, axis=-1, keepdims=True)
    invert = lax.rsqrt(jnp.mean(center * center, axis=-1, keepdims=True) + 1e-06)
    scaled = center * invert
    return (scaled * gain_row + bias_row, scaled, invert)


def norm_backward(upstream, scaled, invert, gain_row):
    weighted = upstream * gain_row
    return invert * (
        weighted
        - jnp.mean(weighted, axis=-1, keepdims=True)
        - scaled * jnp.mean(weighted * scaled, axis=-1, keepdims=True)
    )


def gelu_exact(values):
    return 0.5 * values * (1.0 + lax.erf(values * 0.7071067811865476))


def gelu_slope(values):
    return 0.5 * (
        1.0 + lax.erf(values * 0.7071067811865476)
    ) + values * 0.3989422804014327 * jnp.exp(-0.5 * values * values)


def newton_schulz(matrix):
    current = matrix / (jnp.sqrt(jnp.sum(matrix * matrix)) + 1e-07)
    for sweep_index in range(5):
        gram_matrix = jnp.dot(current, current.T, precision=lax.Precision.HIGHEST)
        polynom = -4.775 * gram_matrix + 2.0315 * jnp.dot(
            gram_matrix, gram_matrix, precision=lax.Precision.HIGHEST
        )
        current = 3.4445 * current + jnp.dot(polynom, current, precision=lax.Precision.HIGHEST)
    return current


def start_body(
    tokens_in,
    expert_ids,
    combine,
    out_cot,
    inward_master,
    outward_master,
    up_master,
    down_master,
    norm_gains,
    norm_biases,
    inward_moment,
    outward_moment,
    up_moment,
    down_moment,
    first_moment,
    second_moment,
    step_count,
):
    dp_count = lax.axis_size("dp")
    expert_count = lax.axis_size("expert")
    tensor_count = lax.axis_size("tensor")
    token_rows = tokens_in.shape[0]
    expert_total = EXP_DEV * expert_count
    capacity = (token_rows * 10 // (4 * expert_total) + 7) // 8 * 8
    slot_total = expert_total * capacity
    inputs = tokens_in.astype(jnp.float32)
    w_inward, w_outward, w_up, w_down = (
        lax.all_gather(inward_master.astype(jnp.bfloat16), "dp", axis=0, tiled=True),
        lax.all_gather(outward_master.astype(jnp.bfloat16), "dp", axis=0, tiled=True),
        lax.all_gather(up_master.astype(jnp.bfloat16), "dp", axis=0, tiled=True),
        lax.all_gather(down_master.astype(jnp.bfloat16), "dp", axis=0, tiled=True),
    )
    expert_lanes = jnp.arange(expert_total, dtype=jnp.int32)
    route_hits = (expert_ids[:, :, None] == expert_lanes).astype(jnp.int32)
    per_token = jnp.sum(route_hits, axis=1)
    earlier = jnp.cumsum(per_token, axis=0) - per_token
    position = jnp.sum(route_hits * earlier[:, None, :], axis=2)
    target = expert_ids * capacity + position
    select = (target[:, :, None] == jnp.arange(slot_total, dtype=jnp.int32)).astype(jnp.bfloat16)
    normed1, scaled1, invert1 = layer_norm(inputs, norm_gains[0], norm_biases[0])
    normed1_low = normed1.astype(jnp.bfloat16)
    qkv_low = jnp.dot(normed1_low, w_inward, preferred_element_type=jnp.float32).astype(
        jnp.bfloat16
    )
    heads_here = w_inward.shape[1] // (3 * HD)
    images = token_rows // SEQ
    split_heads = qkv_low.reshape(images, SEQ, heads_here, 3, HD)
    query_part = split_heads[:, :, :, 0]
    key_part = split_heads[:, :, :, 1]
    value_part = split_heads[:, :, :, 2]
    score_scale = HD ** (-0.5)
    scores = (
        jnp.einsum("bihd,bjhd->bhij", query_part, key_part, preferred_element_type=jnp.float32)
        * score_scale
    )
    row_max = jnp.max(scores, axis=-1, keepdims=True)
    exponent = jnp.exp(scores - row_max)
    row_total = jnp.sum(exponent, axis=-1, keepdims=True)
    softmax_out = exponent / row_total
    softmax_low = softmax_out.astype(jnp.bfloat16)
    heads_out = (
        jnp.einsum("bhij,bjhd->bihd", softmax_low, value_part, preferred_element_type=jnp.float32)
        .astype(jnp.bfloat16)
        .reshape(token_rows, heads_here * HD)
    )
    attend_part = jnp.einsum("tc,dc->td", heads_out, w_outward, preferred_element_type=jnp.float32)
    attended = lax.psum(attend_part, "tensor")
    state = inputs + attended
    normed2, scaled2, invert2 = layer_norm(state, norm_gains[1], norm_biases[1])
    normed2_low = normed2.astype(jnp.bfloat16)
    slots_out = jnp.einsum(
        "tks,td->sd", select, normed2_low, preferred_element_type=jnp.float32
    ).astype(jnp.bfloat16)
    arrived = lax.all_to_all(
        slots_out.reshape(expert_count, EXP_DEV, capacity, D),
        "expert",
        split_axis=0,
        concat_axis=0,
        tiled=True,
    )
    pre_act = jnp.einsum("secd,def->secf", arrived, w_up, preferred_element_type=jnp.float32)
    hidden_low = gelu_exact(pre_act).astype(jnp.bfloat16)
    expert_part = jnp.einsum(
        "secf,def->secd", hidden_low, w_down, preferred_element_type=jnp.float32
    ).astype(jnp.bfloat16)
    returned = lax.all_to_all(expert_part, "expert", split_axis=0, concat_axis=0, tiled=True)
    routed = jnp.einsum(
        "tks,sd->tkd", select, returned.reshape(slot_total, D), preferred_element_type=jnp.float32
    )
    mixed_part = jnp.sum(routed * combine[:, :, None], axis=1)
    mixed_sum = lax.psum(mixed_part, "tensor")
    block_out = (state + mixed_sum).astype(jnp.bfloat16)
    routed_grad = (combine[:, :, None] * out_cot[:, None, :]).astype(jnp.bfloat16)
    slot_grad = jnp.einsum(
        "tks,tkd->sd", select, routed_grad, preferred_element_type=jnp.float32
    ).astype(jnp.bfloat16)
    grad_arrived = lax.all_to_all(
        slot_grad.reshape(expert_count, EXP_DEV, capacity, D),
        "expert",
        split_axis=0,
        concat_axis=0,
        tiled=True,
    )
    hidden_grad = jnp.einsum(
        "secd,def->secf", grad_arrived, w_down, preferred_element_type=jnp.float32
    )
    pre_grad = (hidden_grad * gelu_slope(pre_act)).astype(jnp.bfloat16)
    down_local = jnp.einsum(
        "secd,secf->def", grad_arrived, hidden_low, preferred_element_type=jnp.float32
    )
    up_local = jnp.einsum("secd,secf->def", arrived, pre_grad, preferred_element_type=jnp.float32)
    entry_grad = jnp.einsum(
        "secf,def->secd", pre_grad, w_up, preferred_element_type=jnp.float32
    ).astype(jnp.bfloat16)
    entry_back = lax.all_to_all(entry_grad, "expert", split_axis=0, concat_axis=0, tiled=True)
    normed2_part = jnp.einsum(
        "tks,sd->td", select, entry_back.reshape(slot_total, D), preferred_element_type=jnp.float32
    )
    normed2_grad = lax.psum(normed2_part, "tensor")
    state_grad = out_cot + norm_backward(normed2_grad, scaled2, invert2, norm_gains[1])
    state_low = state_grad.astype(jnp.bfloat16)
    outward_local = jnp.einsum(
        "td,tc->dc", state_low, heads_out, preferred_element_type=jnp.float32
    )
    heads_grad = (
        jnp.dot(state_low, w_outward, preferred_element_type=jnp.float32)
        .astype(jnp.bfloat16)
        .reshape(images, SEQ, heads_here, HD)
    )
    prob_grad = jnp.einsum(
        "bihd,bjhd->bhij", heads_grad, value_part, preferred_element_type=jnp.float32
    )
    score_grad = (
        softmax_out * (prob_grad - jnp.sum(softmax_out * prob_grad, axis=-1, keepdims=True))
    ).astype(jnp.bfloat16)
    query_grad = (
        jnp.einsum("bhij,bjhd->bihd", score_grad, key_part, preferred_element_type=jnp.float32)
        * score_scale
    )
    key_grad = (
        jnp.einsum("bhij,bihd->bjhd", score_grad, query_part, preferred_element_type=jnp.float32)
        * score_scale
    )
    value_grad = jnp.einsum(
        "bhij,bihd->bjhd", softmax_low, heads_grad, preferred_element_type=jnp.float32
    )
    qkv_grad = (
        jnp.stack([query_grad, key_grad, value_grad], axis=3)
        .reshape(token_rows, heads_here * 3 * HD)
        .astype(jnp.bfloat16)
    )
    inward_local = jnp.einsum(
        "td,tc->dc", normed1_low, qkv_grad, preferred_element_type=jnp.float32
    )
    normed1_part = jnp.einsum("tc,dc->td", qkv_grad, w_inward, preferred_element_type=jnp.float32)
    normed1_grad = lax.psum(normed1_part, "tensor")
    input_gradient = state_grad + norm_backward(normed1_grad, scaled1, invert1, norm_gains[0])
    norm_terms = jnp.stack(
        [
            jnp.sum(normed1_grad * scaled1, axis=0),
            jnp.sum(normed2_grad * scaled2, axis=0),
            jnp.sum(normed1_grad, axis=0),
            jnp.sum(normed2_grad, axis=0),
        ]
    )
    inward_total, outward_total, norm_total = lax.psum(
        (inward_local, outward_local, norm_terms), ("dp", "expert")
    )
    up_gradient, down_gradient = (
        lax.psum_scatter(up_local, "dp", scatter_dimension=0, tiled=True),
        lax.psum_scatter(down_local, "dp", scatter_dimension=0, tiled=True),
    )
    shard_rows = D // dp_count
    dp_here = lax.axis_index("dp")
    inward_gradient = lax.dynamic_slice_in_dim(inward_total, dp_here * shard_rows, shard_rows, 0)
    outward_gradient = lax.dynamic_slice_in_dim(outward_total, dp_here * shard_rows, shard_rows, 0)
    inward_next = 0.95 * inward_moment + inward_gradient
    outward_next = 0.95 * outward_moment + outward_gradient
    up_next = 0.95 * up_moment + up_gradient
    down_next = 0.95 * down_moment + down_gradient
    matrices = [up_next[:, expert_slot] for expert_slot in range(EXP_DEV)]
    matrices = matrices + [down_next[:, expert_slot] for expert_slot in range(EXP_DEV)]
    matrices = matrices + [jnp.concatenate([inward_next, outward_next], axis=1)]
    stacked = jnp.stack(matrices)
    slot_count = len(matrices)
    group_size = dp_count * tensor_count
    shard_width = stacked.shape[2]
    query_cols = inward_next.shape[1]

    def orth_expert(pieces):
        whole_matrix = pieces.transpose(0, 2, 1, 3).reshape(D, tensor_count * shard_width)
        result = newton_schulz(whole_matrix) * (0.2 * math.sqrt(F))
        return result.reshape(dp_count, shard_rows, tensor_count, shard_width).transpose(0, 2, 1, 3)

    def orth_attention(pieces):
        inward_whole = (
            pieces[..., :query_cols].transpose(0, 2, 1, 3).reshape(D, tensor_count * query_cols)
        )
        outward_whole = (
            pieces[..., query_cols:]
            .transpose(0, 2, 1, 3)
            .reshape(D, tensor_count * (shard_width - query_cols))
        )
        inward_result = newton_schulz(inward_whole) * (0.2 * math.sqrt(3 * D))
        outward_result = newton_schulz(outward_whole) * (0.2 * math.sqrt(D))
        inward_blocks = inward_result.reshape(
            dp_count, shard_rows, tensor_count, query_cols
        ).transpose(0, 2, 1, 3)
        outward_blocks = outward_result.reshape(
            dp_count, shard_rows, tensor_count, shard_width - query_cols
        ).transpose(0, 2, 1, 3)
        return jnp.concatenate([inward_blocks, outward_blocks], axis=3)

    owner_index = lax.axis_index(("dp", "tensor"))
    outgoing = stacked[np.arange(group_size) % slot_count]
    received = lax.all_to_all(outgoing, ("dp", "tensor"), split_axis=0, concat_axis=0, tiled=True)
    blocks = received.reshape(dp_count, tensor_count, shard_rows, shard_width)
    slot_here = owner_index % slot_count
    result_blocks = lax.cond(slot_here == slot_count - 1, orth_attention, orth_expert, blocks)
    arrived_steps = lax.all_to_all(
        result_blocks.reshape(group_size, shard_rows, shard_width),
        ("dp", "tensor"),
        split_axis=0,
        concat_axis=0,
        tiled=True,
    )
    picked = []
    for owned_slot in range(slot_count):
        replicas = (group_size - owned_slot + slot_count - 1) // slot_count
        source = owned_slot + slot_count * (owner_index % replicas)
        picked.append(lax.dynamic_index_in_dim(arrived_steps, source, 0, keepdims=False))
    up_step = jnp.stack(picked[0:EXP_DEV], axis=1)
    down_step = jnp.stack(picked[EXP_DEV : 2 * EXP_DEV], axis=1)
    attend_step = picked[2 * EXP_DEV]
    inward_new = inward_master - 0.1 * (attend_step[:, :query_cols] + 0.1 * inward_master)
    outward_new = outward_master - 0.1 * (attend_step[:, query_cols:] + 0.1 * outward_master)
    up_new = up_master - 0.1 * (up_step + 0.1 * up_master)
    down_new = down_master - 0.1 * (down_step + 0.1 * down_master)
    moment_first = 0.9 * first_moment + 0.1 * norm_total
    moment_second = 0.999 * second_moment + 0.001 * norm_total * norm_total
    steps_done = step_count[0].astype(jnp.float32)
    direction = (
        moment_first
        / (1.0 - jnp.power(0.9, steps_done))
        / (jnp.sqrt(moment_second / (1.0 - jnp.power(0.999, steps_done))) + 1e-08)
    )
    params_new = jnp.concatenate([norm_gains, norm_biases], axis=0) - 0.1 * direction
    return (
        block_out,
        input_gradient,
        inward_gradient,
        outward_gradient,
        up_gradient,
        down_gradient,
        norm_total[0:2],
        norm_total[2:4],
        inward_next,
        outward_next,
        up_next,
        down_next,
        inward_new,
        outward_new,
        up_new,
        down_new,
        inward_new.astype(jnp.bfloat16),
        outward_new.astype(jnp.bfloat16),
        up_new.astype(jnp.bfloat16),
        down_new.astype(jnp.bfloat16),
        params_new[0:2],
        params_new[2:4],
        moment_first,
        moment_second,
    )


PAIRS = (1, 2, 3)
FAR_FIRST = (3, 2, 1, 0)
MIDWAY = 1
LANES = 128
NOWHERE = 128 * 128 - 1
PAD = 208
NT = (((1,), (1,)), ((), ()))
TN = (((0,), (0,)), ((), ()))


def mxu(left, right, dims=(((1,), (0,)), ((), ()))):
    return lax.dot_general(left, right, dims, preferred_element_type=jnp.float32)


def spread_rows(value, padded_ref):
    padded_ref[...] = jnp.zeros_like(padded_ref)
    for image in range(value.shape[0] // SEQ):
        padded_ref[image * PAD : image * PAD + SEQ, :] = value[image * SEQ : (image + 1) * SEQ]


def gather_rows(padded, out_ref):
    for image in range(out_ref.shape[0] // SEQ):
        out_ref[image * SEQ : (image + 1) * SEQ, :] = padded[
            image * PAD : image * PAD + SEQ
        ].astype(out_ref.dtype)


def peer(me, k):
    return (me + k) % 2 + 2 * ((me // 2 + k // 2) % 2)


def remote(source, target, send, recv, device):
    copy = pltpu.make_async_remote_copy(
        src_ref=source,
        dst_ref=target,
        send_sem=send,
        recv_sem=recv,
        device_id=device,
        device_id_type=pl.DeviceIdType.MESH,
    )
    copy.start()
    return copy


class Copy:
    def __init__(self, parts):
        self.parts = parts
        self.make().start()

    def make(self):
        source, target, send, recv, device = self.parts()
        return pltpu.make_async_remote_copy(
            src_ref=source,
            dst_ref=target,
            send_sem=send,
            recv_sem=recv,
            device_id=device,
            device_id_type=pl.DeviceIdType.MESH,
        )

    def wait_recv(self):
        self.make().wait_recv()

    def wait_send(self):
        self.make().wait_send()


def keep(source, target, sem):
    copy = pltpu.make_async_copy(source, target, sem)
    copy.start()
    return copy


def greet(dp_here, expert_here, core, over_expert=True):
    barrier = pltpu.get_barrier_semaphore()
    devices = [{"dp": peer(dp_here, k)} for k in PAIRS] + [{"tensor": 1 - core}]
    if over_expert:
        devices += [{"expert": peer(expert_here, k)} for k in PAIRS]
    for device in devices:
        pl.semaphore_signal(
            barrier, inc=1, device_id=device, device_id_type=pl.DeviceIdType.MESH
        )
    return lambda: pl.semaphore_wait(barrier, len(devices))


def block_rows(index, size):
    return pl.ds(pl.multiple_of(index * size, size), size)


def one_hot(cond):
    return jnp.where(cond, 1.0, 0.0).astype(jnp.bfloat16)


def route(ids, capacity, target_ref, target_t_ref):
    rows = ids.shape[0]
    before = lax.broadcasted_iota(jnp.int32, (rows, rows), 0)
    after = lax.broadcasted_iota(jnp.int32, (rows, rows), 1)
    lane = lax.broadcasted_iota(jnp.int32, (rows, 128), 1)
    hits = one_hot((lane == ids[:, 0:1]) | (lane == ids[:, 1:2]))
    earlier = mxu(one_hot(before > after), hits)
    target = jnp.zeros((rows, 128), jnp.int32)
    parts = jnp.zeros((rows, 128), jnp.int32)
    for r in range(2):
        own = ids[:, r : r + 1]
        position = jnp.sum(jnp.where(lane == own, earlier, 0.0), axis=1, keepdims=True)
        value = jnp.where(own >= 0, own * capacity + position.astype(jnp.int32), NOWHERE)
        target = jnp.where(lane == r, value, target)
        parts = jnp.where(lane == 2 * r, value // 128, jnp.where(lane == 2 * r + 1, value % 128, parts))
    target_ref[...] = target
    identity = one_hot(
        lax.broadcasted_iota(jnp.int32, (8, 128), 0) == lax.broadcasted_iota(jnp.int32, (8, 128), 1)
    )
    flipped = mxu(identity, parts.astype(jnp.float32).astype(jnp.bfloat16), NT).astype(jnp.int32)
    for r in range(2):
        target_t_ref[r : r + 1, :] = flipped[2 * r : 2 * r + 1] * 128 + flipped[2 * r + 1 : 2 * r + 2]


def attend(qkv_ref, probs_ref, gift_ref):
    heads_here = qkv_ref.shape[1] // (3 * HD)
    key_lane = lax.broadcasted_iota(jnp.int32, (PAD, PAD), 1)

    def one_image(image, carry):
        rows = block_rows(image, PAD)
        out_rows = pl.ds(pl.multiple_of(D + image * PAD, 16), PAD)
        for head in range(heads_here):
            base = head * 3 * HD
            query = qkv_ref[rows, base : base + HD]
            key = qkv_ref[rows, base + HD : base + 2 * HD]
            value = qkv_ref[rows, base + 2 * HD : base + 3 * HD]
            scores = jnp.where(key_lane < SEQ, mxu(query, key, NT) * HD ** (-0.5), -1e30)
            exponent = jnp.exp(scores - jnp.max(scores, axis=-1, keepdims=True))
            probs = exponent / jnp.sum(exponent, axis=-1, keepdims=True)
            probs_ref[image * heads_here + head] = probs
            gift_ref[out_rows, head * HD : (head + 1) * HD] = mxu(
                probs.astype(jnp.bfloat16), value
            ).astype(jnp.bfloat16)
        return carry

    lax.fori_loop(0, qkv_ref.shape[0] // PAD, one_image, 0)


def woven(array):
    rows, count, width = array.shape
    tiles = array.reshape(rows, count, width // LANES, LANES)
    return tiles.transpose(0, 2, 1, 3).reshape(-1, LANES)


def unwoven(array, whole):
    rows, count, width = whole
    tiles = array.reshape(rows, width // LANES, count, LANES)
    return tiles.transpose(0, 2, 1, 3).reshape(whole)


def strand(tile, expert, rows, width):
    step = EXP_DEV * (width // LANES)
    return pl.ds(EXP_DEV * tile + expert, rows, stride=step)


def front_kernel(
    ids_ref,
    combine_ref,
    cot_ref,
    tokens_ref,
    gains_ref,
    biases_ref,
    inward_ref,
    outward_ref,
    up_ref,
    down_ref,
    up_moment_ref,
    down_moment_ref,
    state_ref,
    gift_ref,
    qkv_ref,
    probs_ref,
    weight_ref,
    target_ref,
    combine_out_ref,
    expert_w_ref,
    arrived_ref,
    grad_arrived_ref,
    moment_whole_ref,
    padded,
    columns,
    columns_padded,
    raw,
    target_t_ref,
    attend_shard,
    expert_shard,
    moment_shard,
    gift_other_ref,
    grad_chunks,
    token_chunks,
    inner_send,
    inner_recv,
    expert_send,
    expert_recv,
    slot_send,
    slot_recv,
    share_send,
    share_recv,
    gift_sems,
    keep_sems,
    moment_send,
    moment_recv,
    raw_sems,
):
    bf16 = jnp.bfloat16
    dp_here, expert_here, core = (lax.axis_index(a) for a in ("dp", "expert", "tensor"))
    partner = {"tensor": 1 - core}
    capacity = grad_chunks.shape[1]
    shard_rows = attend_shard.shape[0]
    qcols = qkv_ref.shape[1]
    width = attend_shard.shape[1]
    here = block_rows(dp_here, shard_rows)
    ready = greet(dp_here, expert_here, core)
    loads = [
        keep(ref, raw.at[place], raw_sems.at[place])
        for place, ref in enumerate((up_ref, down_ref, up_moment_ref, down_moment_ref))
    ]

    def unpick(place, tile, expert):
        return raw[place, strand(tile, expert, shard_rows, width), :].astype(bf16)

    attend_shard[:, :qcols] = inward_ref[...].astype(bf16)
    attend_shard[:, qcols:] = outward_ref[...].astype(bf16)
    weight_ref[here, :] = attend_shard[...]
    ready()
    inner = [
        remote(
            attend_shard,
            weight_ref.at[here, :],
            inner_send.at[k - 1],
            inner_recv.at[k - 1],
            {"dp": peer(dp_here, k)},
        )
        for k in PAIRS
    ]
    kept = []

    rest = combine_ref[...]
    for part in range(3):
        piece = rest.astype(bf16).astype(jnp.float32)
        columns[2 * part : 2 * part + 2, :] = piece
        rest = rest - piece
    columns[6:8, :] = (ids_ref[...] + 1).astype(jnp.float32)
    identity = one_hot(
        lax.broadcasted_iota(jnp.int32, (8, 128), 0) == lax.broadcasted_iota(jnp.int32, (8, 128), 1)
    )
    spread_rows(mxu(columns[...].astype(bf16), identity, TN), columns_padded)
    for r in range(2):
        combine_out_ref[:, r : r + 1] = (
            columns_padded[:, r : r + 1]
            + columns_padded[:, 2 + r : 3 + r]
            + columns_padded[:, 4 + r : 5 + r]
        )
    ids = columns_padded[...].astype(jnp.int32) - 1
    route(ids[:, 6:8], capacity, target_ref, target_t_ref)
    spread_rows(cot_ref[...], padded)
    slot = lax.broadcasted_iota(jnp.int32, (capacity, padded.shape[0]), 0)

    def first_slot(k):
        return (2 * peer(expert_here, k) + core) * capacity

    def send_chunks(fill, chunks, landing, which):
        copies, shared = {}, []
        for place, k in enumerate(FAR_FIRST):
            chunks[k] = fill(slot + first_slot(k)).astype(bf16)
            if place > 0:
                last = FAR_FIRST[place - 1]
                copies[last] = remote(
                    chunks.at[last],
                    landing.at[0, last],
                    slot_send.at[which, last],
                    slot_recv.at[which, last],
                    {"expert": peer(expert_here, last)},
                )
        kept.append(keep(chunks.at[0], landing.at[0, 0], keep_sems.at[1 + which]))
        shared.append(
            remote(
                chunks.at[0],
                landing.at[1, 0],
                share_send.at[which, 0],
                share_recv.at[which, 0],
                partner,
            )
        )
        return copies, shared

    def share_arrivals(copies, landing, which, shared):
        for k in FAR_FIRST[:3]:
            copies[k].wait_recv()
            shared.append(
                remote(
                    landing.at[0, k],
                    landing.at[1, k],
                    share_send.at[which, k],
                    share_recv.at[which, k],
                    partner,
                )
            )

    grads = [(combine_out_ref[:, r : r + 1] * padded[...]).astype(bf16) for r in range(2)]
    grad_copies, grad_shared = send_chunks(
        lambda slots: sum(mxu(one_hot(target_t_ref[r : r + 1] == slots), grads[r]) for r in range(2)),
        grad_chunks,
        grad_arrived_ref,
        0,
    )
    for which in range(2):
        loads[which].wait()
        for tile in range(width // LANES):
            pair = [unpick(which, tile, e) for e in range(EXP_DEV)]
            lanes = slice(tile * LANES, (tile + 1) * LANES)
            for j in range(EXP_DEV):
                expert_shard[EXP_DEV * which + j, :, lanes] = jnp.where(
                    core == 0, pair[j], pair[1 - j]
                )
    spread_rows(tokens_ref[...].astype(jnp.float32), padded)
    normed, unused, unused = layer_norm(padded[...], gains_ref[0:1], biases_ref[0:1])
    normed_low = normed.astype(bf16)
    weights = [
        remote(
            expert_shard,
            expert_w_ref.at[:, here, :],
            expert_send.at[k - 1],
            expert_recv.at[k - 1],
            {"dp": peer(dp_here, k)},
        )
        for k in (1, 2)
    ]
    kept.append(keep(expert_shard, expert_w_ref.at[:, here, :], keep_sems.at[0]))
    for which in range(2):
        loads[2 + which].wait()
        for tile in range(width // LANES):
            for e in range(EXP_DEV):
                moment_shard[EXP_DEV * which + e, :, tile * LANES : (tile + 1) * LANES] = unpick(
                    2 + which, tile, e
                )
    for copy in inner:
        copy.wait_recv()
    qkv_ref[...] = mxu(normed_low, weight_ref[:, :qcols]).astype(bf16)
    gift_ref[0:D, :] = weight_ref[:, qcols:]
    attend(qkv_ref, probs_ref, gift_ref)
    gift = remote(gift_ref, gift_other_ref, gift_sems.at[0], gift_sems.at[1], partner)
    half = padded[...] + mxu(gift_ref[D:, :], gift_ref[0:D, :], NT)
    gift.wait()
    state = half + mxu(gift_other_ref[D:, :], gift_other_ref[0:D, :], NT)
    state_ref[...] = state
    normed, unused, unused = layer_norm(state, gains_ref[1:2], biases_ref[1:2])
    normed_low = normed.astype(bf16)
    token_copies, token_shared = send_chunks(
        lambda slots: mxu(
            one_hot((target_t_ref[0:1] == slots) | (target_t_ref[1:2] == slots)), normed_low
        ),
        token_chunks,
        arrived_ref,
        1,
    )
    for copy in weights:
        copy.wait_recv()
    for k, part in ((1, slice(0, EXP_DEV)), (2, slice(EXP_DEV, 2 * EXP_DEV))):
        block = expert_w_ref.at[part, block_rows(peer(dp_here, k), shard_rows), :]
        weights.append(
            remote(
                block,
                block,
                expert_send.at[k + 1],
                expert_recv.at[k + 1],
                {"dp": peer(dp_here, 3 - k)},
            )
        )
    moments = [
        remote(
            moment_shard.at[peer(dp_here, k)],
            moment_whole_ref.at[here, :],
            moment_send.at[k - 1],
            moment_recv.at[k - 1],
            {"dp": peer(dp_here, k)},
        )
        for k in PAIRS
    ]
    kept.append(keep(moment_shard.at[dp_here], moment_whole_ref.at[here, :], keep_sems.at[3]))
    share_arrivals(grad_copies, grad_arrived_ref, 0, grad_shared)
    share_arrivals(token_copies, arrived_ref, 1, token_shared)
    for copy in grad_shared + token_shared + moments + weights[2:]:
        copy.wait()
    for copy in weights[:2] + inner:
        copy.wait_send()
    for copies in (grad_copies, token_copies):
        for k in PAIRS:
            copies[k].wait_send()
    for copy in kept:
        copy.wait()


def back_kernel(
    combine_ref,
    target_ref,
    gains_ref,
    biases_ref,
    inward_moment_ref,
    outward_moment_ref,
    cot_hbm,
    tokens_hbm,
    state_hbm,
    gift_hbm,
    qkv_hbm,
    probs_hbm,
    weight_hbm,
    expert_w_hbm,
    arrived_hbm,
    grad_arrived_hbm,
    moment_whole_hbm,
    input_ref,
    block_ref,
    norm_ref,
    attend_grad_ref,
    attend_whole_ref,
    own_steps_ref,
    home_grads_ref,
    give,
    handed,
    summed,
    returned,
    matrices,
    near_in,
    far_out,
    far_in,
    owned_low,
    normed_part,
    normed_other,
    inner,
    inner_in,
    plane,
    quarter_in,
    quarter,
    plane_total,
    whole_own,
    norm_own,
    norm_in,
    gram,
    gram_other,
    hand_send,
    hand_recv,
    slot_send,
    slot_recv,
    share_send,
    share_recv,
    pair_send,
    pair_recv,
    dp_send,
    dp_recv,
    expert_send,
    expert_recv,
    near_send,
    near_recv,
    far_send,
    far_recv,
    load_sems,
):
    bf16, f32 = jnp.bfloat16, jnp.float32
    dp_here, expert_here, core = (lax.axis_index(a) for a in ("dp", "expert", "tensor"))
    partner = {"tensor": 1 - core}
    capacity = give.shape[2]
    shard_rows = inner.shape[1]
    here = block_rows(dp_here, shard_rows)
    ready = greet(dp_here, expert_here, core)
    sent = []

    def to_dp(stage, sources, targets, peers=PAIRS):
        def copy(k):
            return Copy(
                lambda: (
                    sources(k),
                    targets(k),
                    dp_send.at[stage, k - 1],
                    dp_recv.at[stage, k - 1],
                    {"dp": peer(dp_here, k)},
                )
            )

        copies = [copy(k) for k in peers]
        sent.extend(copies)
        return copies

    def to_expert(stage, sources, targets):
        def copy(k):
            return Copy(
                lambda: (
                    sources(k),
                    targets(k),
                    expert_send.at[stage, k - 1],
                    expert_recv.at[stage, k - 1],
                    {"expert": peer(expert_here, k)},
                )
            )

        copies = [copy(k) for k in PAIRS]
        sent.extend(copies)
        return copies

    def arrive(copies):
        for copy in copies:
            copy.wait_recv()

    hands, homes, shares = ({}, {}), ({}, {}), ([], [])

    def hand(which, k):
        hands[which][k] = Copy(
            lambda: (
                give.at[which, k],
                handed.at[which, k],
                hand_send.at[which, k],
                hand_recv.at[which, k],
                partner,
            )
        )
        sent.append(hands[which][k])

    def add_up(which, k):
        hands[which][k].wait_recv()
        total = (summed[which, k].astype(f32) + handed[which, k].astype(f32)).astype(bf16)
        summed[which, k] = total
        if k == 0:
            returned[which, 0, 0] = total

    def send_home(which, k):
        if k == 0:
            shares[which].append(
                Copy(
                    lambda: (
                        summed.at[which, 0],
                        returned.at[which, 1, 0],
                        share_send.at[which, 0],
                        share_recv.at[which, 0],
                        partner,
                    )
                )
            )
        else:
            homes[which][k] = Copy(
                lambda: (
                    summed.at[which, k],
                    returned.at[which, 0, k],
                    slot_send.at[which, k],
                    slot_recv.at[which, k],
                    {"expert": peer(expert_here, k)},
                )
            )
            sent.append(homes[which][k])

    def share(which):
        def copy(k):
            return Copy(
                lambda: (
                    returned.at[which, 0, k],
                    returned.at[which, 1, k],
                    share_send.at[which, k],
                    share_recv.at[which, k],
                    partner,
                )
            )

        for k in FAR_FIRST[:3]:
            homes[which][k].wait_recv()
            shares[which].append(copy(k))
        sent.extend(shares[which])
        arrive(shares[which])

    def held(index):
        return 2 * (index // 2) + (index % 2 + core) % 2

    ways = ((slice(0, D // 2), 1, 2), (slice(D // 2, D), 2, 1))

    def near_copy(half, place):
        rows, first, second = ways[half]
        owner = (first, 3)[place]
        return Copy(
            lambda: (
                matrices.at[held(peer(dp_here, owner)), rows, :],
                near_in.at[half, place],
                near_send.at[half, place],
                near_recv.at[half, place],
                {"dp": peer(dp_here, first)},
            )
        )

    def far_copy(half):
        rows, first, second = ways[half]
        return Copy(
            lambda: (
                far_out.at[half],
                far_in.at[half],
                far_send.at[half],
                far_recv.at[half],
                {"dp": peer(dp_here, second)},
            )
        )

    def pass_on(near):
        arrive(near)
        for half, (rows, first, second) in enumerate(ways):
            far_out[half] = (
                matrices[held(peer(dp_here, second)), rows, :].astype(f32)
                + near_in[half, 1].astype(f32)
            ).astype(bf16)
        far = [far_copy(half) for half in range(2)]
        sent.extend(far)
        return far

    def experts(weights, rows, grads, hidden, pre_grad):
        loads = {}
        for j in (1, 0):
            for place, (source, target) in enumerate(
                (
                    (expert_w_hbm.at[j], weights.at[j]),
                    (arrived_hbm.at[j], rows.at[j]),
                    (expert_w_hbm.at[EXP_DEV + j], weights.at[EXP_DEV + j]),
                    (grad_arrived_hbm.at[j], grads.at[j]),
                )
            ):
                loads[j, place] = keep(source, target, load_sems.at[4 * j + place])
        ready()
        before = None
        for k in FAR_FIRST:
            for j in (1, 0):
                if before is None:
                    loads[j, 0].wait()
                    loads[j, 1].wait()
                pre = mxu(rows[j, k], weights[j])
                share_of_one = 0.5 * (1.0 + lax.erf(pre * 0.7071067811865476))
                hidden[j, k] = (pre * share_of_one).astype(bf16)
                slope = share_of_one + pre * 0.3989422804014327 * jnp.exp(-0.5 * pre * pre)
                if before is None:
                    loads[j, 2].wait()
                    loads[j, 3].wait()
                grad = (mxu(grads[j, k], weights[EXP_DEV + j]) * slope).astype(bf16)
                pre_grad[j, k] = grad
                entry = mxu(grad, weights[j], NT).astype(bf16)
                if j == 1:
                    give[0, k] = entry
                else:
                    summed[0, k] = entry
            if before is not None:
                add_up(0, before)
            hand(0, k)
            if before is not None:
                send_home(0, before)
            before = k
        for m in range(2 * EXP_DEV):
            left, right, j = (rows, pre_grad, m) if m < EXP_DEV else (grads, hidden, m - EXP_DEV)
            total = mxu(left[j, 0], right[j, 0], TN)
            for k in PAIRS:
                total += mxu(left[j, k], right[j, k], TN)
            matrices[m] = total.astype(bf16)
            if m == 0:
                add_up(0, before)
                send_home(0, before)
        near = [near_copy(half, place) for place in (1, 0) for half in range(2)]
        sent.extend(near)
        for k in FAR_FIRST:
            for j in (1, 0):
                part = mxu(hidden[j, k], weights[EXP_DEV + j], NT).astype(bf16)
                if j == 1:
                    give[1, k] = part
                else:
                    summed[1, k] = part
            if k != FAR_FIRST[0]:
                hand(1, k + 1)
        hand(1, 0)
        for k in FAR_FIRST:
            add_up(1, k)
        for k in FAR_FIRST:
            send_home(1, k)
        return near

    near = []
    slots = (EXP_DEV, 4, capacity)
    pl.run_scoped(
        lambda *refs: near.extend(experts(*refs)),
        pltpu.VMEM(expert_w_hbm.shape, bf16),
        pltpu.VMEM(slots + (D,), bf16),
        pltpu.VMEM(slots + (D,), bf16),
        pltpu.VMEM(slots + (expert_w_hbm.shape[2],), bf16),
        pltpu.VMEM(slots + (expert_w_hbm.shape[2],), bf16),
    )

    def backward(
        cot_ref,
        tokens_ref,
        state_ref,
        gift_ref,
        qkv_ref,
        probs_ref,
        weight_ref,
        padded,
        qkv_grad_ref,
        local_ref,
        out_grad_ref,
    ):
        loads = [
            keep(source, target, load_sems.at[place])
            for place, (source, target) in enumerate(
                (
                    (state_hbm, state_ref),
                    (cot_hbm, cot_ref),
                    (gift_hbm.at[D:, :], gift_ref),
                    (weight_hbm, weight_ref),
                    (qkv_hbm, qkv_ref),
                    (probs_hbm, probs_ref),
                    (tokens_hbm, tokens_ref),
                )
            )
        ]
        qcols = qkv_ref.shape[1]
        rows_all = state_ref.shape[0]
        loads[0].wait()
        unused, scaled2, invert2 = layer_norm(state_ref[...], gains_ref[1:2], biases_ref[1:2])
        loads[1].wait()
        spread_rows(cot_ref[...], padded)
        slot = lax.broadcasted_iota(jnp.int32, (rows_all, capacity), 1)

        def picks(k, j, columns):
            first = slot + (2 * peer(expert_here, k) + (core + j) % 2) * capacity
            hit = target_ref[:, columns[0] : columns[0] + 1] == first
            for column in columns[1:]:
                hit = hit | (target_ref[:, column : column + 1] == first)
            return one_hot(hit)

        def pick_all(which, columns):
            total = mxu(picks(0, 0, columns), returned[which, 0, 0])
            for j in range(2):
                for k in FAR_FIRST:
                    if k + j > 0:
                        total += mxu(picks(k, j, columns), returned[which, j, k])
            return total

        share(0)
        normed2_grad = pick_all(0, (0, 1))
        norm_own[0, 4:8] = jnp.zeros((4, D), f32)
        norm_own[0, 1:2] = jnp.sum(normed2_grad * scaled2, axis=0, keepdims=True)
        norm_own[0, 3:4] = jnp.sum(normed2_grad, axis=0, keepdims=True)
        state_grad = padded[...] + norm_backward(normed2_grad, scaled2, invert2, gains_ref[1:2])
        padded[...] = state_grad
        state_low = state_grad.astype(bf16)
        for copy in loads[2:]:
            copy.wait()

        local_ref[:, qcols:] = mxu(state_low, gift_ref[...], TN)
        out_grad_ref[...] = mxu(state_low, weight_ref[:, qcols:]).astype(bf16)
        heads_here = qcols // (3 * HD)
        scale = HD ** (-0.5)

        def one_image(image, carry):
            rows = block_rows(image, PAD)
            for head in range(heads_here):
                base = head * 3 * HD
                query = qkv_ref[rows, base : base + HD]
                key = qkv_ref[rows, base + HD : base + 2 * HD]
                value = qkv_ref[rows, base + 2 * HD : base + 3 * HD]
                out_grad = out_grad_ref[rows, head * HD : (head + 1) * HD]
                probs = probs_ref[image * heads_here + head]
                prob_grad = mxu(out_grad, value, NT)
                score_grad = (
                    probs * (prob_grad - jnp.sum(probs * prob_grad, axis=-1, keepdims=True))
                ).astype(bf16)
                qkv_grad_ref[rows, base : base + HD] = (mxu(score_grad, key) * scale).astype(bf16)
                qkv_grad_ref[rows, base + HD : base + 2 * HD] = (
                    mxu(score_grad, query, TN) * scale
                ).astype(bf16)
                qkv_grad_ref[rows, base + 2 * HD : base + 3 * HD] = mxu(
                    probs.astype(bf16), out_grad, TN
                ).astype(bf16)
            return carry

        lax.fori_loop(0, rows_all // PAD, one_image, 0)
        spread_rows(tokens_ref[...].astype(f32), normed_part)
        normed1, scaled1, invert1 = layer_norm(normed_part[...], gains_ref[0:1], biases_ref[0:1])
        local_ref[:, :qcols] = mxu(normed1.astype(bf16), qkv_grad_ref[...], TN)
        for k in range(4):
            inner[k] = local_ref[block_rows(peer(dp_here, k), shard_rows), :].astype(bf16)
        normed_part[...] = mxu(qkv_grad_ref[...], weight_ref[:, :qcols], NT)
        rows_sums = to_dp(1, lambda k: inner.at[k], lambda k: inner_in.at[k - 1])
        pair = Copy(
            lambda: (normed_part, normed_other, pair_send.at[0], pair_recv.at[0], partner)
        )
        sent.append(pair)
        far = pass_on(near)

        share(1)
        total = state_ref[...]
        for r in range(2):
            total += combine_ref[:, r : r + 1] * pick_all(1, (r,))
        gather_rows(total, block_ref)

        pair.wait_recv()
        normed1_grad = normed_part[...] + normed_other[...]
        norm_own[0, 0:1] = jnp.sum(normed1_grad * scaled1, axis=0, keepdims=True)
        norm_own[0, 2:3] = jnp.sum(normed1_grad, axis=0, keepdims=True)
        norm_in[0, dp_here] = norm_own[0]
        norms = to_dp(2, lambda k: norm_own.at[0], lambda k: norm_in.at[0, dp_here])
        gather_rows(
            padded[...] + norm_backward(normed1_grad, scaled1, invert1, gains_ref[0:1]), input_ref
        )
        return rows_sums, norms, far

    travelling = []
    rows_f32 = pltpu.VMEM(state_hbm.shape, f32)
    pl.run_scoped(
        lambda *refs: travelling.extend(backward(*refs)),
        pltpu.VMEM(cot_hbm.shape, f32),
        pltpu.VMEM(tokens_hbm.shape, bf16),
        rows_f32,
        pltpu.VMEM((gift_hbm.shape[0] - D, gift_hbm.shape[1]), bf16),
        pltpu.VMEM(qkv_hbm.shape, bf16),
        pltpu.VMEM(probs_hbm.shape, f32),
        pltpu.VMEM(weight_hbm.shape, bf16),
        rows_f32,
        pltpu.VMEM(qkv_hbm.shape, bf16),
        pltpu.VMEM(weight_hbm.shape, f32),
        pltpu.VMEM((state_hbm.shape[0], gift_hbm.shape[1]), bf16),
    )
    rows_sums, norms, far = travelling

    arrive(rows_sums)
    plane[...] = (
        inner[0].astype(f32)
        + inner_in[0].astype(f32)
        + inner_in[1].astype(f32)
        + inner_in[2].astype(f32)
    ).astype(bf16)
    quarter_rows = quarter.shape[0]
    my_quarter = block_rows(expert_here, quarter_rows)
    quarters = to_expert(
        0,
        lambda k: plane.at[block_rows(peer(expert_here, k), quarter_rows), :],
        lambda k: quarter_in.at[k - 1],
    )
    arrive(norms)
    norm_plane = norm_in[0, 0] + norm_in[0, 1] + norm_in[0, 2] + norm_in[0, 3]
    norm_own[1] = norm_plane
    norm_in[1, expert_here] = norm_plane
    norm_sums = to_expert(1, lambda k: norm_own.at[1], lambda k: norm_in.at[1, expert_here])

    def orthogonalize(owned_next, factor, change, moment_ref):
        load = keep(moment_whole_hbm, moment_ref, load_sems.at[0])
        arrive(quarters)
        quarter[...] = (
            plane[my_quarter, :].astype(f32)
            + quarter_in[0].astype(f32)
            + quarter_in[1].astype(f32)
            + quarter_in[2].astype(f32)
        ).astype(bf16)
        plane_total[my_quarter, :] = quarter[...]
        totals = to_expert(2, lambda k: quarter, lambda k: plane_total.at[my_quarter, :])
        arrive(far)
        load.wait()
        for half, (rows, first, second) in enumerate(ways):
            owned = (
                matrices[held(dp_here), rows, :].astype(f32)
                + near_in[half, 0].astype(f32)
                + far_in[half].astype(f32)
            )
            owned_low[rows, :] = owned.astype(bf16)
            owned_next[rows, :] = 0.95 * moment_ref[rows, :].astype(f32) + owned
        split = halves(owned_next[...])
        gram[...] = mxu3(split, split, NT)
        pair = remote(gram, gram_other, pair_send.at[1], pair_recv.at[1], partner)
        home = to_dp(
            3,
            lambda k: owned_low.at[block_rows(peer(dp_here, k), shard_rows), :],
            lambda k: home_grads_ref.at[dp_here],
        )
        own = keep(owned_low.at[here, :], home_grads_ref.at[dp_here], load_sems.at[1])
        pair.wait()

        def attention_next():
            arrive(totals)
            total = plane_total[...].astype(f32)
            attend_grad_ref[...] = total
            qcols = inward_moment_ref.shape[1]
            whole_own[:, :qcols] = (0.95 * inward_moment_ref[...] + total[:, :qcols]).astype(bf16)
            whole_own[:, qcols:] = (0.95 * outward_moment_ref[...] + total[:, qcols:]).astype(bf16)
            attend_whole_ref[here, :] = whole_own[...]
            return to_dp(4, lambda k: whole_own, lambda k: attend_whole_ref.at[here, :])

        wholes = find_factor(
            gram[...] + gram_other[...], factor, gram, change, gram_other, {MIDWAY: attention_next}
        )
        own_steps_ref[...] = (
            mxu3(halves(factor[...]), halves(owned_next[...])) * (0.2 * math.sqrt(F))
        ).astype(bf16)
        arrive(norm_sums)
        norm_ref[...] = (
            norm_in[1, 0, 0:4] + norm_in[1, 1, 0:4] + norm_in[1, 2, 0:4] + norm_in[1, 3, 0:4]
        )
        arrive(home)
        arrive(wholes)
        own.wait()

    square = pltpu.VMEM((D, D), f32)
    matrix = moment_whole_hbm.shape
    pl.run_scoped(
        orthogonalize, pltpu.VMEM(matrix, f32), square, square, pltpu.VMEM(matrix, bf16)
    )
    for copy in sent:
        copy.wait_send()


def halves(value):
    high = value.astype(jnp.bfloat16)
    return high, (value - high.astype(jnp.float32)).astype(jnp.bfloat16)


def mxu3(left, right, dims=(((1,), (0,)), ((), ()))):
    return (
        mxu(left[0], right[0], dims) + mxu(left[1], right[0], dims) + mxu(left[0], right[1], dims)
    )


def find_factor(gram, factor, current, change, scaled, between={}):
    diagonal = lax.broadcasted_iota(jnp.int32, gram.shape, 0) == lax.broadcasted_iota(
        jnp.int32, gram.shape, 1
    )
    squares = jnp.sum(
        jnp.sum(jnp.where(diagonal, gram, 0.0), axis=1, keepdims=True), axis=0, keepdims=True
    )
    norm = jnp.sqrt(squares) + 1e-07
    current[...] = gram / (norm * norm)
    factor[...] = jnp.where(diagonal, 1.0 / norm, 0.0)

    half = D // 2

    def product(out, left, right, by, added, added_by):
        upper = by * mxu3([x[:half] for x in left], right) + added_by * added[:half, :]
        corner = mxu3([x[half:] for x in left], [x[:, half:] for x in right])
        corner = by * corner + added_by * added[half:, half:]
        out[:half, :] = upper
        out[half:, :half] = upper[:, half:].T
        out[half:, half:] = corner

    def polynomial():
        low = halves(current[...])
        product(change, low, low, 2.0315, current, -4.775)
        step = halves(change[...])
        product(factor, step, halves(factor[...]), 1.0, factor, 3.4445)
        return low, step

    def sweep(index, carry):
        low, step = polynomial()
        product(scaled, step, low, 1.0, current, 3.4445)
        product(current, halves(scaled[...]), step, 1.0, scaled, 3.4445)
        return carry

    result, last = None, 0
    for index in (*sorted(between), 4):
        lax.fori_loop(last, index, sweep, 0)
        if index in between:
            result = between[index]()
        last = index
    polynomial()
    return result


def finish_kernel(
    whole_ref,
    own_steps_ref,
    home_steps_ref,
    attend_step_ref,
    kept,
    given,
    taken,
    factor,
    change,
    mine,
    other,
    step_send,
    step_recv,
    pair_send,
    pair_recv,
):
    dp_here, core = lax.axis_index("dp"), lax.axis_index("tensor")
    partner = {"tensor": 1 - core}
    shard_rows = mine.shape[0]
    qcols = 3 * whole_ref.shape[1] // 4
    here = block_rows(dp_here, shard_rows)
    ready = greet(dp_here, None, core, over_expert=False)
    inward_gram = mxu(whole_ref[:, :qcols], whole_ref[:, :qcols], NT)
    outward_gram = mxu(whole_ref[:, qcols:], whole_ref[:, qcols:], NT)
    kept[...] = jnp.where(core == 0, inward_gram, outward_gram)
    given[...] = jnp.where(core == 0, outward_gram, inward_gram)
    ready()
    pair = remote(given, taken, pair_send.at[0], pair_recv.at[0], partner)
    steps = [
        remote(
            own_steps_ref.at[block_rows(peer(dp_here, k), shard_rows), :],
            home_steps_ref.at[dp_here],
            step_send.at[k - 1],
            step_recv.at[k - 1],
            {"dp": peer(dp_here, k)},
        )
        for k in PAIRS
    ]
    home_steps_ref[dp_here] = own_steps_ref[here, :]
    pair.wait()
    find_factor(kept[...] + taken[...], factor, kept, change, taken)
    mine[...] = factor[here, :]
    pair = remote(mine, other, pair_send.at[1], pair_recv.at[1], partner)
    for copy in steps:
        copy.wait()
    pair.wait()
    for owner, columns, count in ((0, slice(0, qcols), 3 * D), (1, slice(qcols, None), D)):
        rows = halves(jnp.where(core == owner, mine[...], other[...]))
        step = mxu(rows[0], whole_ref[:, columns]) + mxu(rows[1], whole_ref[:, columns])
        attend_step_ref[:, columns] = step * (0.2 * math.sqrt(count))


def apply_kernel(
    steps_done_ref,
    home_steps_ref,
    attend_step_ref,
    home_grads_ref,
    attend_grad_ref,
    norm_ref,
    gains_ref,
    biases_ref,
    first_ref,
    second_ref,
    inward_ref,
    outward_ref,
    up_ref,
    down_ref,
    inward_moment_ref,
    outward_moment_ref,
    up_moment_ref,
    down_moment_ref,
    block_ref,
    input_ref,
    block_out_ref,
    input_out_ref,
    inward_gradient_ref,
    outward_gradient_ref,
    up_gradient_ref,
    down_gradient_ref,
    gain_gradient_ref,
    bias_gradient_ref,
    inward_next_ref,
    outward_next_ref,
    up_next_ref,
    down_next_ref,
    inward_new_ref,
    outward_new_ref,
    up_new_ref,
    down_new_ref,
    inward_copy_ref,
    outward_copy_ref,
    up_copy_ref,
    down_copy_ref,
    gains_new_ref,
    biases_new_ref,
    first_new_ref,
    second_new_ref,
    weave,
):
    f32 = jnp.float32
    qcols = inward_ref.shape[1]
    block_out_ref[...] = block_ref[...]
    input_out_ref[...] = input_ref[...]

    def finish(place, gradient, step, refs):
        master_ref, moment_ref, gradient_ref, next_ref, new_ref, copy_ref = refs
        gradient_ref[place] = gradient
        next_ref[place] = 0.95 * moment_ref[place] + gradient
        master = master_ref[place]
        new = master - 0.1 * (step + 0.1 * master)
        new_ref[place] = new
        copy_ref[place] = new.astype(copy_ref.dtype)

    experts = (
        (up_ref, up_moment_ref, up_gradient_ref, up_next_ref, up_new_ref, up_copy_ref),
        (down_ref, down_moment_ref, down_gradient_ref, down_next_ref, down_new_ref, down_copy_ref),
    )
    everything = (slice(None), slice(None))
    rows, width = attend_grad_ref.shape
    for which, refs in enumerate(experts):
        for place, home_ref in enumerate((home_grads_ref, home_steps_ref)):
            for e in range(EXP_DEV):
                for tile in range(width // LANES):
                    weave[place, strand(tile, e, rows, width), :] = home_ref[
                        EXP_DEV * which + e, :, tile * LANES : (tile + 1) * LANES
                    ].astype(f32)
        finish(everything, weave[0], weave[1], refs)
    finish(
        everything,
        attend_grad_ref[:, :qcols],
        attend_step_ref[:, :qcols],
        (
            inward_ref,
            inward_moment_ref,
            inward_gradient_ref,
            inward_next_ref,
            inward_new_ref,
            inward_copy_ref,
        ),
    )
    finish(
        everything,
        attend_grad_ref[:, qcols:],
        attend_step_ref[:, qcols:],
        (
            outward_ref,
            outward_moment_ref,
            outward_gradient_ref,
            outward_next_ref,
            outward_new_ref,
            outward_copy_ref,
        ),
    )

    @pl.when(pl.program_id(0) == 0)
    def norms():
        total = norm_ref[...]
        gain_gradient_ref[...] = total[0:2]
        bias_gradient_ref[...] = total[2:4]
        moment_first = 0.9 * first_ref[...] + 0.1 * total
        moment_second = 0.999 * second_ref[...] + 0.001 * total * total
        first_new_ref[...] = moment_first
        second_new_ref[...] = moment_second
        done = jnp.full((4, D), steps_done_ref[0], jnp.int32).astype(f32)
        direction = (
            moment_first
            / (1.0 - jnp.power(0.9, done))
            / (jnp.sqrt(moment_second / (1.0 - jnp.power(0.999, done))) + 1e-08)
        )
        gains_new_ref[...] = gains_ref[...] - 0.1 * direction[0:2]
        biases_new_ref[...] = biases_ref[...] - 0.1 * direction[2:4]


def pair_body(
    tokens_in,
    expert_ids,
    combine,
    out_cot,
    inward_master,
    outward_master,
    up_master,
    down_master,
    norm_gains,
    norm_biases,
    inward_moment,
    outward_moment,
    up_moment,
    down_moment,
    first_moment,
    second_moment,
    step_count,
):
    bf16, f32 = jnp.bfloat16, jnp.float32
    token_rows = tokens_in.shape[0]
    expert_total = EXP_DEV * 4
    capacity = (token_rows * 10 // (4 * expert_total) + 7) // 8 * 8
    shard_rows, qcols = inward_master.shape
    width = up_master.shape[2]
    images = token_rows // SEQ
    padded_rows = images * PAD
    heads_here = qcols // (3 * HD)
    shape = jax.ShapeDtypeStruct
    rows_f32 = pltpu.VMEM((padded_rows, D), f32)
    in_vmem, anywhere = pl.BlockSpec(memory_space=pltpu.VMEM), pl.BlockSpec(memory_space=pl.ANY)
    dma = pltpu.SemaphoreType.DMA

    slots = shape((EXP_DEV, 4, capacity, D), bf16)
    (
        state,
        gift,
        qkv_low,
        probs,
        weight,
        target,
        combine_padded,
        expert_w,
        arrived,
        grad_arrived,
        moment_whole,
    ) = pl.pallas_call(
        front_kernel,
        out_shape=(
            shape((padded_rows, D), f32),
            shape((D + padded_rows, heads_here * HD), bf16),
            shape((padded_rows, qcols), bf16),
            shape((images * heads_here, PAD, PAD), f32),
            shape((D, width), bf16),
            shape((padded_rows, 128), jnp.int32),
            shape((padded_rows, 2), f32),
            shape((2 * EXP_DEV, D, width), bf16),
            slots,
            slots,
            shape((D, width), bf16),
        ),
        in_specs=[in_vmem] * 8 + [anywhere] * 4,
        out_specs=tuple([in_vmem] * 7 + [anywhere] * 4),
        scratch_shapes=[
            rows_f32,
            pltpu.VMEM((8, token_rows), f32),
            pltpu.VMEM((padded_rows, 128), f32),
            pltpu.VMEM((4, EXP_DEV * shard_rows * width // LANES, LANES), f32),
            pltpu.VMEM((2, padded_rows), jnp.int32),
            pltpu.VMEM((shard_rows, width), bf16),
            pltpu.VMEM((4, shard_rows, width), bf16),
            pltpu.VMEM((4, shard_rows, width), bf16),
            pltpu.VMEM((D + padded_rows, heads_here * HD), bf16),
            pltpu.VMEM((4, capacity, D), bf16),
            pltpu.VMEM((4, capacity, D), bf16),
            dma((3,)),
            dma((3,)),
            dma((4,)),
            dma((4,)),
            dma((2, 4)),
            dma((2, 4)),
            dma((2, 4)),
            dma((2, 4)),
            dma((2,)),
            dma((4,)),
            dma((3,)),
            dma((3,)),
            dma((4,)),
        ],
        name="front",
        cost_estimate=pl.CostEstimate(
            flops=60_000_000_000, bytes_accessed=30_000_000, transcendentals=0
        ),
        compiler_params=pltpu.CompilerParams(collective_id=0, has_side_effects=True),
    )(
        expert_ids.T,
        combine.T,
        out_cot,
        tokens_in,
        norm_gains,
        norm_biases,
        inward_master,
        outward_master,
        *(woven(a) for a in (up_master, down_master, up_moment, down_moment)),
    )
    chunks = (2, 4, capacity, D)
    square = pltpu.VMEM((D, D), f32)
    rows_low = pltpu.VMEM((shard_rows, width), bf16)
    (
        input_gradient,
        block_out,
        norm_total,
        attend_grad,
        attend_whole,
        own_steps,
        home_grads,
    ) = pl.pallas_call(
        back_kernel,
        out_shape=(
            shape((token_rows, D), f32),
            shape((token_rows, D), bf16),
            shape((4, D), f32),
            shape((shard_rows, width), f32),
            shape((D, width), bf16),
            shape((D, width), bf16),
            shape((4, shard_rows, width), bf16),
        ),
        in_specs=[in_vmem] * 6 + [anywhere] * 11,
        out_specs=tuple([in_vmem] * 6 + [anywhere]),
        scratch_shapes=[
            pltpu.VMEM(chunks, bf16),
            pltpu.VMEM(chunks, bf16),
            pltpu.VMEM(chunks, bf16),
            pltpu.VMEM((2,) + chunks, bf16),
            pltpu.VMEM((4, D, width), bf16),
            pltpu.VMEM((2, 2, D // 2, width), bf16),
            pltpu.VMEM((2, D // 2, width), bf16),
            pltpu.VMEM((2, D // 2, width), bf16),
            pltpu.VMEM((D, width), bf16),
            rows_f32,
            rows_f32,
            pltpu.VMEM((4, shard_rows, width), bf16),
            pltpu.VMEM((3, shard_rows, width), bf16),
            rows_low,
            pltpu.VMEM((3, shard_rows // 4, width), bf16),
            pltpu.VMEM((shard_rows // 4, width), bf16),
            rows_low,
            rows_low,
            pltpu.VMEM((2, 8, D), f32),
            pltpu.VMEM((2, 4, 8, D), f32),
            square,
            square,
        ]
        + [dma((2, 4))] * 6
        + [dma((2,))] * 2
        + [dma((5, 3))] * 2
        + [dma((3, 3))] * 2
        + [dma((2, 2))] * 2
        + [dma((2,))] * 2
        + [dma((8,))],
        name="back",
        cost_estimate=pl.CostEstimate(
            flops=110_000_000_000, bytes_accessed=60_000_000, transcendentals=0
        ),
        compiler_params=pltpu.CompilerParams(
            collective_id=1, has_side_effects=True, vmem_limit_bytes=66_000_000
        ),
    )(
        combine_padded,
        target,
        norm_gains,
        norm_biases,
        inward_moment,
        outward_moment,
        out_cot,
        tokens_in,
        state,
        gift,
        qkv_low,
        probs,
        weight,
        expert_w,
        arrived,
        grad_arrived,
        moment_whole,
    )
    factor_rows = pltpu.VMEM((shard_rows, D), f32)
    home_steps, attend_step = pl.pallas_call(
        finish_kernel,
        out_shape=(shape((4, shard_rows, width), bf16), shape((shard_rows, width), f32)),
        in_specs=[in_vmem] * 2,
        out_specs=(in_vmem, in_vmem),
        scratch_shapes=[square] * 5 + [factor_rows] * 2 + [dma((3,))] * 2 + [dma((2,))] * 2,
        name="finish",
        cost_estimate=pl.CostEstimate(
            flops=20_000_000_000, bytes_accessed=5_000_000, transcendentals=0
        ),
        compiler_params=pltpu.CompilerParams(collective_id=2, has_side_effects=True),
    )(attend_whole, own_steps)

    blocks = 4
    inward, outward = inward_master.shape, outward_master.shape
    expert = (EXP_DEV * shard_rows * width // LANES, LANES)

    def split(whole, along=0):
        if along is None:
            return pl.BlockSpec(whole, lambda i: (0,) * len(whole))
        rows = pl.cdiv(pl.cdiv(whole[along], blocks), 8) * 8
        block = whole[:along] + (rows,) + whole[along + 1 :]
        return pl.BlockSpec(
            block, lambda i: (0,) * along + (i,) + (0,) * (len(whole) - along - 1)
        )

    two, four, attended = (2, D), (4, D), (shard_rows, width)
    matrix_shapes = (inward, outward, expert, expert)
    by_rows = [split(m) for m in matrix_shapes]
    tokens = split((token_rows, D))
    finished = pl.pallas_call(
        apply_kernel,
        grid=(blocks,),
        out_shape=tuple(
            [shape((token_rows, D), bf16), shape((token_rows, D), f32)]
            + [shape(m, f32) for m in matrix_shapes]
            + [shape(two, f32)] * 2
            + [shape(m, f32) for m in matrix_shapes * 2]
            + [shape(m, bf16) for m in matrix_shapes]
            + [shape(two, f32)] * 2
            + [shape(four, f32)] * 2
        ),
        in_specs=[pl.BlockSpec(memory_space=pltpu.SMEM)]
        + [split((4,) + attended, 1), split(attended), split((4,) + attended, 1), split(attended)]
        + [split(four, None), split(two, None), split(two, None), split(four, None), split(four, None)]
        + by_rows * 2
        + [tokens] * 2,
        out_specs=tuple(
            [tokens] * 2
            + by_rows
            + [split(two, None)] * 2
            + by_rows * 3
            + [split(two, None)] * 2
            + [split(four, None)] * 2
        ),
        scratch_shapes=[pltpu.VMEM((2, expert[0] // blocks, LANES), f32)],
        name="apply",
        cost_estimate=pl.CostEstimate(
            flops=20_000_000, bytes_accessed=20_000_000, transcendentals=0
        ),
    )(
        step_count,
        home_steps,
        attend_step,
        home_grads,
        attend_grad,
        norm_total,
        norm_gains,
        norm_biases,
        first_moment,
        second_moment,
        inward_master,
        outward_master,
        woven(up_master),
        woven(down_master),
        inward_moment,
        outward_moment,
        woven(up_moment),
        woven(down_moment),
        block_out,
        input_gradient,
    )
    return tuple(
        unwoven(a, up_master.shape) if a.shape == expert else a for a in finished
    )


def solution(mesh):
    sizes = tuple(mesh.shape[axis] for axis in ("dp", "expert", "tensor"))
    body = pair_body if sizes == (4, 4, 2) else start_body
    return jax.shard_map(
        body,
        mesh=mesh,
        in_specs=(
            P(("dp", "expert"), None),
            P(("dp", "expert"), None),
            P(("dp", "expert"), None),
            P(("dp", "expert"), None),
            P("dp", "tensor"),
            P("dp", "tensor"),
            P("dp", "expert", "tensor"),
            P("dp", "expert", "tensor"),
            P(),
            P(),
            P("dp", "tensor"),
            P("dp", "tensor"),
            P("dp", "expert", "tensor"),
            P("dp", "expert", "tensor"),
            P(),
            P(),
            P(),
        ),
        out_specs=(
            P(("dp", "expert"), None),
            P(("dp", "expert"), None),
            P("dp", "tensor"),
            P("dp", "tensor"),
            P("dp", "expert", "tensor"),
            P("dp", "expert", "tensor"),
            P(),
            P(),
            P("dp", "tensor"),
            P("dp", "tensor"),
            P("dp", "expert", "tensor"),
            P("dp", "expert", "tensor"),
            P("dp", "tensor"),
            P("dp", "tensor"),
            P("dp", "expert", "tensor"),
            P("dp", "expert", "tensor"),
            P("dp", "tensor"),
            P("dp", "tensor"),
            P("dp", "expert", "tensor"),
            P("dp", "expert", "tensor"),
            P(),
            P(),
            P(),
            P(),
        ),
        check_vma=False,
    )
```

```python
import functools
import math

import jax
import jax.numpy as jnp
import numpy as np
from jax import lax
from jax.experimental import pallas as pl
from jax.experimental.pallas import tpu as pltpu
from jax.sharding import PartitionSpec as P

D = 512
HD = 64
F = 2048
SEQ = 197
EXP_DEV = 2


def layer_norm(values, gain_row, bias_row):
    center = values - jnp.mean(values, axis=-1, keepdims=True)
    invert = lax.rsqrt(jnp.mean(center * center, axis=-1, keepdims=True) + 1e-06)
    scaled = center * invert
    return (scaled * gain_row + bias_row, scaled, invert)


def norm_backward(upstream, scaled, invert, gain_row):
    weighted = upstream * gain_row
    return invert * (
        weighted
        - jnp.mean(weighted, axis=-1, keepdims=True)
        - scaled * jnp.mean(weighted * scaled, axis=-1, keepdims=True)
    )


def gelu_exact(values):
    return 0.5 * values * (1.0 + lax.erf(values * 0.7071067811865476))


def gelu_slope(values):
    return 0.5 * (
        1.0 + lax.erf(values * 0.7071067811865476)
    ) + values * 0.3989422804014327 * jnp.exp(-0.5 * values * values)


def newton_schulz(matrix):
    current = matrix / (jnp.sqrt(jnp.sum(matrix * matrix)) + 1e-07)
    for sweep_index in range(5):
        gram_matrix = jnp.dot(current, current.T, precision=lax.Precision.HIGHEST)
        polynom = -4.775 * gram_matrix + 2.0315 * jnp.dot(
            gram_matrix, gram_matrix, precision=lax.Precision.HIGHEST
        )
        current = 3.4445 * current + jnp.dot(polynom, current, precision=lax.Precision.HIGHEST)
    return current


def start_body(
    tokens_in,
    expert_ids,
    combine,
    out_cot,
    inward_master,
    outward_master,
    up_master,
    down_master,
    norm_gains,
    norm_biases,
    inward_moment,
    outward_moment,
    up_moment,
    down_moment,
    first_moment,
    second_moment,
    step_count,
):
    dp_count = lax.axis_size("dp")
    expert_count = lax.axis_size("expert")
    tensor_count = lax.axis_size("tensor")
    token_rows = tokens_in.shape[0]
    expert_total = EXP_DEV * expert_count
    capacity = (token_rows * 10 // (4 * expert_total) + 7) // 8 * 8
    slot_total = expert_total * capacity
    inputs = tokens_in.astype(jnp.float32)
    w_inward, w_outward, w_up, w_down = (
        lax.all_gather(inward_master.astype(jnp.bfloat16), "dp", axis=0, tiled=True),
        lax.all_gather(outward_master.astype(jnp.bfloat16), "dp", axis=0, tiled=True),
        lax.all_gather(up_master.astype(jnp.bfloat16), "dp", axis=0, tiled=True),
        lax.all_gather(down_master.astype(jnp.bfloat16), "dp", axis=0, tiled=True),
    )
    expert_lanes = jnp.arange(expert_total, dtype=jnp.int32)
    route_hits = (expert_ids[:, :, None] == expert_lanes).astype(jnp.int32)
    per_token = jnp.sum(route_hits, axis=1)
    earlier = jnp.cumsum(per_token, axis=0) - per_token
    position = jnp.sum(route_hits * earlier[:, None, :], axis=2)
    target = expert_ids * capacity + position
    select = (target[:, :, None] == jnp.arange(slot_total, dtype=jnp.int32)).astype(jnp.bfloat16)
    normed1, scaled1, invert1 = layer_norm(inputs, norm_gains[0], norm_biases[0])
    normed1_low = normed1.astype(jnp.bfloat16)
    qkv_low = jnp.dot(normed1_low, w_inward, preferred_element_type=jnp.float32).astype(
        jnp.bfloat16
    )
    heads_here = w_inward.shape[1] // (3 * HD)
    images = token_rows // SEQ
    split_heads = qkv_low.reshape(images, SEQ, heads_here, 3, HD)
    query_part = split_heads[:, :, :, 0]
    key_part = split_heads[:, :, :, 1]
    value_part = split_heads[:, :, :, 2]
    score_scale = HD ** (-0.5)
    scores = (
        jnp.einsum("bihd,bjhd->bhij", query_part, key_part, preferred_element_type=jnp.float32)
        * score_scale
    )
    row_max = jnp.max(scores, axis=-1, keepdims=True)
    exponent = jnp.exp(scores - row_max)
    row_total = jnp.sum(exponent, axis=-1, keepdims=True)
    softmax_out = exponent / row_total
    softmax_low = softmax_out.astype(jnp.bfloat16)
    heads_out = (
        jnp.einsum("bhij,bjhd->bihd", softmax_low, value_part, preferred_element_type=jnp.float32)
        .astype(jnp.bfloat16)
        .reshape(token_rows, heads_here * HD)
    )
    attend_part = jnp.einsum("tc,dc->td", heads_out, w_outward, preferred_element_type=jnp.float32)
    attended = lax.psum(attend_part, "tensor")
    state = inputs + attended
    normed2, scaled2, invert2 = layer_norm(state, norm_gains[1], norm_biases[1])
    normed2_low = normed2.astype(jnp.bfloat16)
    slots_out = jnp.einsum(
        "tks,td->sd", select, normed2_low, preferred_element_type=jnp.float32
    ).astype(jnp.bfloat16)
    arrived = lax.all_to_all(
        slots_out.reshape(expert_count, EXP_DEV, capacity, D),
        "expert",
        split_axis=0,
        concat_axis=0,
        tiled=True,
    )
    pre_act = jnp.einsum("secd,def->secf", arrived, w_up, preferred_element_type=jnp.float32)
    hidden_low = gelu_exact(pre_act).astype(jnp.bfloat16)
    expert_part = jnp.einsum(
        "secf,def->secd", hidden_low, w_down, preferred_element_type=jnp.float32
    ).astype(jnp.bfloat16)
    returned = lax.all_to_all(expert_part, "expert", split_axis=0, concat_axis=0, tiled=True)
    routed = jnp.einsum(
        "tks,sd->tkd", select, returned.reshape(slot_total, D), preferred_element_type=jnp.float32
    )
    mixed_part = jnp.sum(routed * combine[:, :, None], axis=1)
    mixed_sum = lax.psum(mixed_part, "tensor")
    block_out = (state + mixed_sum).astype(jnp.bfloat16)
    routed_grad = (combine[:, :, None] * out_cot[:, None, :]).astype(jnp.bfloat16)
    slot_grad = jnp.einsum(
        "tks,tkd->sd", select, routed_grad, preferred_element_type=jnp.float32
    ).astype(jnp.bfloat16)
    grad_arrived = lax.all_to_all(
        slot_grad.reshape(expert_count, EXP_DEV, capacity, D),
        "expert",
        split_axis=0,
        concat_axis=0,
        tiled=True,
    )
    hidden_grad = jnp.einsum(
        "secd,def->secf", grad_arrived, w_down, preferred_element_type=jnp.float32
    )
    pre_grad = (hidden_grad * gelu_slope(pre_act)).astype(jnp.bfloat16)
    down_local = jnp.einsum(
        "secd,secf->def", grad_arrived, hidden_low, preferred_element_type=jnp.float32
    )
    up_local = jnp.einsum("secd,secf->def", arrived, pre_grad, preferred_element_type=jnp.float32)
    entry_grad = jnp.einsum(
        "secf,def->secd", pre_grad, w_up, preferred_element_type=jnp.float32
    ).astype(jnp.bfloat16)
    entry_back = lax.all_to_all(entry_grad, "expert", split_axis=0, concat_axis=0, tiled=True)
    normed2_part = jnp.einsum(
        "tks,sd->td", select, entry_back.reshape(slot_total, D), preferred_element_type=jnp.float32
    )
    normed2_grad = lax.psum(normed2_part, "tensor")
    state_grad = out_cot + norm_backward(normed2_grad, scaled2, invert2, norm_gains[1])
    state_low = state_grad.astype(jnp.bfloat16)
    outward_local = jnp.einsum(
        "td,tc->dc", state_low, heads_out, preferred_element_type=jnp.float32
    )
    heads_grad = (
        jnp.dot(state_low, w_outward, preferred_element_type=jnp.float32)
        .astype(jnp.bfloat16)
        .reshape(images, SEQ, heads_here, HD)
    )
    prob_grad = jnp.einsum(
        "bihd,bjhd->bhij", heads_grad, value_part, preferred_element_type=jnp.float32
    )
    score_grad = (
        softmax_out * (prob_grad - jnp.sum(softmax_out * prob_grad, axis=-1, keepdims=True))
    ).astype(jnp.bfloat16)
    query_grad = (
        jnp.einsum("bhij,bjhd->bihd", score_grad, key_part, preferred_element_type=jnp.float32)
        * score_scale
    )
    key_grad = (
        jnp.einsum("bhij,bihd->bjhd", score_grad, query_part, preferred_element_type=jnp.float32)
        * score_scale
    )
    value_grad = jnp.einsum(
        "bhij,bihd->bjhd", softmax_low, heads_grad, preferred_element_type=jnp.float32
    )
    qkv_grad = (
        jnp.stack([query_grad, key_grad, value_grad], axis=3)
        .reshape(token_rows, heads_here * 3 * HD)
        .astype(jnp.bfloat16)
    )
    inward_local = jnp.einsum(
        "td,tc->dc", normed1_low, qkv_grad, preferred_element_type=jnp.float32
    )
    normed1_part = jnp.einsum("tc,dc->td", qkv_grad, w_inward, preferred_element_type=jnp.float32)
    normed1_grad = lax.psum(normed1_part, "tensor")
    input_gradient = state_grad + norm_backward(normed1_grad, scaled1, invert1, norm_gains[0])
    norm_terms = jnp.stack(
        [
            jnp.sum(normed1_grad * scaled1, axis=0),
            jnp.sum(normed2_grad * scaled2, axis=0),
            jnp.sum(normed1_grad, axis=0),
            jnp.sum(normed2_grad, axis=0),
        ]
    )
    inward_total, outward_total, norm_total = lax.psum(
        (inward_local, outward_local, norm_terms), ("dp", "expert")
    )
    up_gradient, down_gradient = (
        lax.psum_scatter(up_local, "dp", scatter_dimension=0, tiled=True),
        lax.psum_scatter(down_local, "dp", scatter_dimension=0, tiled=True),
    )
    shard_rows = D // dp_count
    dp_here = lax.axis_index("dp")
    inward_gradient = lax.dynamic_slice_in_dim(inward_total, dp_here * shard_rows, shard_rows, 0)
    outward_gradient = lax.dynamic_slice_in_dim(outward_total, dp_here * shard_rows, shard_rows, 0)
    inward_next = 0.95 * inward_moment + inward_gradient
    outward_next = 0.95 * outward_moment + outward_gradient
    up_next = 0.95 * up_moment + up_gradient
    down_next = 0.95 * down_moment + down_gradient
    matrices = [up_next[:, expert_slot] for expert_slot in range(EXP_DEV)]
    matrices = matrices + [down_next[:, expert_slot] for expert_slot in range(EXP_DEV)]
    matrices = matrices + [jnp.concatenate([inward_next, outward_next], axis=1)]
    stacked = jnp.stack(matrices)
    slot_count = len(matrices)
    group_size = dp_count * tensor_count
    shard_width = stacked.shape[2]
    query_cols = inward_next.shape[1]

    def orth_expert(pieces):
        whole_matrix = pieces.transpose(0, 2, 1, 3).reshape(D, tensor_count * shard_width)
        result = newton_schulz(whole_matrix) * (0.2 * math.sqrt(F))
        return result.reshape(dp_count, shard_rows, tensor_count, shard_width).transpose(0, 2, 1, 3)

    def orth_attention(pieces):
        inward_whole = (
            pieces[..., :query_cols].transpose(0, 2, 1, 3).reshape(D, tensor_count * query_cols)
        )
        outward_whole = (
            pieces[..., query_cols:]
            .transpose(0, 2, 1, 3)
            .reshape(D, tensor_count * (shard_width - query_cols))
        )
        inward_result = newton_schulz(inward_whole) * (0.2 * math.sqrt(3 * D))
        outward_result = newton_schulz(outward_whole) * (0.2 * math.sqrt(D))
        inward_blocks = inward_result.reshape(
            dp_count, shard_rows, tensor_count, query_cols
        ).transpose(0, 2, 1, 3)
        outward_blocks = outward_result.reshape(
            dp_count, shard_rows, tensor_count, shard_width - query_cols
        ).transpose(0, 2, 1, 3)
        return jnp.concatenate([inward_blocks, outward_blocks], axis=3)

    owner_index = lax.axis_index(("dp", "tensor"))
    outgoing = stacked[np.arange(group_size) % slot_count]
    received = lax.all_to_all(outgoing, ("dp", "tensor"), split_axis=0, concat_axis=0, tiled=True)
    blocks = received.reshape(dp_count, tensor_count, shard_rows, shard_width)
    slot_here = owner_index % slot_count
    result_blocks = lax.cond(slot_here == slot_count - 1, orth_attention, orth_expert, blocks)
    arrived_steps = lax.all_to_all(
        result_blocks.reshape(group_size, shard_rows, shard_width),
        ("dp", "tensor"),
        split_axis=0,
        concat_axis=0,
        tiled=True,
    )
    picked = []
    for owned_slot in range(slot_count):
        replicas = (group_size - owned_slot + slot_count - 1) // slot_count
        source = owned_slot + slot_count * (owner_index % replicas)
        picked.append(lax.dynamic_index_in_dim(arrived_steps, source, 0, keepdims=False))
    up_step = jnp.stack(picked[0:EXP_DEV], axis=1)
    down_step = jnp.stack(picked[EXP_DEV : 2 * EXP_DEV], axis=1)
    attend_step = picked[2 * EXP_DEV]
    inward_new = inward_master - 0.1 * (attend_step[:, :query_cols] + 0.1 * inward_master)
    outward_new = outward_master - 0.1 * (attend_step[:, query_cols:] + 0.1 * outward_master)
    up_new = up_master - 0.1 * (up_step + 0.1 * up_master)
    down_new = down_master - 0.1 * (down_step + 0.1 * down_master)
    moment_first = 0.9 * first_moment + 0.1 * norm_total
    moment_second = 0.999 * second_moment + 0.001 * norm_total * norm_total
    steps_done = step_count[0].astype(jnp.float32)
    direction = (
        moment_first
        / (1.0 - jnp.power(0.9, steps_done))
        / (jnp.sqrt(moment_second / (1.0 - jnp.power(0.999, steps_done))) + 1e-08)
    )
    params_new = jnp.concatenate([norm_gains, norm_biases], axis=0) - 0.1 * direction
    return (
        block_out,
        input_gradient,
        inward_gradient,
        outward_gradient,
        up_gradient,
        down_gradient,
        norm_total[0:2],
        norm_total[2:4],
        inward_next,
        outward_next,
        up_next,
        down_next,
        inward_new,
        outward_new,
        up_new,
        down_new,
        inward_new.astype(jnp.bfloat16),
        outward_new.astype(jnp.bfloat16),
        up_new.astype(jnp.bfloat16),
        down_new.astype(jnp.bfloat16),
        params_new[0:2],
        params_new[2:4],
        moment_first,
        moment_second,
    )


PAIRS = (1, 2, 3)
FAR_FIRST = (3, 2, 1, 0)
MIDWAY = 1
LANES = 128
NOWHERE = 128 * 128 - 1
PAD = 208
NT = (((1,), (1,)), ((), ()))
TN = (((0,), (0,)), ((), ()))


def mxu(left, right, dims=(((1,), (0,)), ((), ()))):
    return lax.dot_general(left, right, dims, preferred_element_type=jnp.float32)


def spread_rows(value, padded_ref):
    padded_ref[...] = jnp.zeros_like(padded_ref)
    for image in range(value.shape[0] // SEQ):
        padded_ref[image * PAD : image * PAD + SEQ, :] = value[image * SEQ : (image + 1) * SEQ]


def gather_rows(padded, out_ref):
    for image in range(out_ref.shape[0] // SEQ):
        out_ref[image * SEQ : (image + 1) * SEQ, :] = padded[
            image * PAD : image * PAD + SEQ
        ].astype(out_ref.dtype)


def peer(me, k):
    return (me + k) % 2 + 2 * ((me // 2 + k // 2) % 2)


def remote(source, target, send, recv, device):
    copy = pltpu.make_async_remote_copy(
        src_ref=source,
        dst_ref=target,
        send_sem=send,
        recv_sem=recv,
        device_id=device,
        device_id_type=pl.DeviceIdType.MESH,
    )
    copy.start()
    return copy


class Copy:
    def __init__(self, parts, start=True):
        self.parts = parts
        if start:
            self.make().start()

    def make(self):
        source, target, send, recv, device = self.parts()
        return pltpu.make_async_remote_copy(
            src_ref=source,
            dst_ref=target,
            send_sem=send,
            recv_sem=recv,
            device_id=device,
            device_id_type=pl.DeviceIdType.MESH,
        )

    def wait_recv(self):
        self.make().wait_recv()

    def wait_send(self):
        self.make().wait_send()


def keep(source, target, sem):
    copy = pltpu.make_async_copy(source, target, sem)
    copy.start()
    return copy


def greet(dp_here, expert_here, core, over_expert=True):
    barrier = pltpu.get_barrier_semaphore()
    devices = [{"dp": peer(dp_here, k)} for k in PAIRS] + [{"tensor": 1 - core}]
    if over_expert:
        devices += [{"expert": peer(expert_here, k)} for k in PAIRS]
    for device in devices:
        pl.semaphore_signal(
            barrier, inc=1, device_id=device, device_id_type=pl.DeviceIdType.MESH
        )
    return lambda: pl.semaphore_wait(barrier, len(devices))


def block_rows(index, size):
    return pl.ds(pl.multiple_of(index * size, size), size)


def one_hot(cond):
    return jnp.where(cond, 1.0, 0.0).astype(jnp.bfloat16)


def route(ids, capacity, target_ref, target_t_ref):
    rows = ids.shape[0]
    square = (PAD, PAD)
    below = one_hot(
        lax.broadcasted_iota(jnp.int32, square, 0) > lax.broadcasted_iota(jnp.int32, square, 1)
    )
    lane = lax.broadcasted_iota(jnp.int32, (rows, 128), 1)
    hits = one_hot((lane == ids[:, 0:1]) | (lane == ids[:, 1:2]))
    earlier, passed = [], jnp.zeros((1, 128), jnp.float32)
    for image in range(rows // PAD):
        own = hits[image * PAD : (image + 1) * PAD]
        earlier.append(mxu(below, own) + passed)
        passed += jnp.sum(own.astype(jnp.float32), axis=0, keepdims=True)
    earlier = jnp.concatenate(earlier, axis=0)
    target = jnp.zeros((rows, 128), jnp.int32)
    parts = jnp.zeros((rows, 128), jnp.int32)
    for r in range(2):
        own = ids[:, r : r + 1]
        position = jnp.sum(jnp.where(lane == own, earlier, 0.0), axis=1, keepdims=True)
        value = jnp.where(own >= 0, own * capacity + position.astype(jnp.int32), NOWHERE)
        target = jnp.where(lane == r, value, target)
        parts = jnp.where(lane == 2 * r, value // 128, jnp.where(lane == 2 * r + 1, value % 128, parts))
    target_ref[...] = target
    identity = one_hot(
        lax.broadcasted_iota(jnp.int32, (8, 128), 0) == lax.broadcasted_iota(jnp.int32, (8, 128), 1)
    )
    flipped = mxu(identity, parts.astype(jnp.float32).astype(jnp.bfloat16), NT).astype(jnp.int32)
    for r in range(2):
        target_t_ref[r : r + 1, :] = flipped[2 * r : 2 * r + 1] * 128 + flipped[2 * r + 1 : 2 * r + 2]


def attend(qkv_ref, probs_ref, gift_ref):
    heads_here = qkv_ref.shape[1] // (3 * HD)
    key_lane = lax.broadcasted_iota(jnp.int32, (PAD, PAD), 1)

    def one_image(image, carry):
        rows = block_rows(image, PAD)
        out_rows = pl.ds(pl.multiple_of(D + image * PAD, 16), PAD)
        for head in range(heads_here):
            base = head * 3 * HD
            query = qkv_ref[rows, base : base + HD]
            key = qkv_ref[rows, base + HD : base + 2 * HD]
            value = qkv_ref[rows, base + 2 * HD : base + 3 * HD]
            scores = jnp.where(key_lane < SEQ, mxu(query, key, NT) * HD ** (-0.5), -1e30)
            exponent = jnp.exp(scores - jnp.max(scores, axis=-1, keepdims=True))
            probs = exponent / jnp.sum(exponent, axis=-1, keepdims=True)
            probs_ref[image * heads_here + head] = probs
            gift_ref[out_rows, head * HD : (head + 1) * HD] = mxu(
                probs.astype(jnp.bfloat16), value
            ).astype(jnp.bfloat16)
        return carry

    lax.fori_loop(0, qkv_ref.shape[0] // PAD, one_image, 0)


def woven(array):
    rows, count, width = array.shape
    tiles = array.reshape(rows, count, width // LANES, LANES)
    return tiles.transpose(0, 2, 1, 3).reshape(-1, LANES)


def unwoven(array, whole):
    rows, count, width = whole
    tiles = array.reshape(rows, width // LANES, count, LANES)
    return tiles.transpose(0, 2, 1, 3).reshape(whole)


def strand(tile, expert, rows, width):
    step = EXP_DEV * (width // LANES)
    return pl.ds(EXP_DEV * tile + expert, rows, stride=step)


def front_kernel(
    ids_ref,
    combine_ref,
    cot_ref,
    tokens_ref,
    gains_ref,
    biases_ref,
    inward_ref,
    outward_ref,
    up_ref,
    down_ref,
    up_moment_ref,
    down_moment_ref,
    state_ref,
    gift_ref,
    qkv_ref,
    probs_ref,
    weight_ref,
    target_ref,
    combine_out_ref,
    moment_shard,
    expert_w_ref,
    arrived_ref,
    grad_arrived_ref,
    padded,
    columns,
    columns_padded,
    raw,
    target_t_ref,
    attend_shard,
    expert_shard,
    gift_other_ref,
    grad_chunks,
    token_chunks,
    inner_send,
    inner_recv,
    expert_send,
    expert_recv,
    slot_send,
    slot_recv,
    share_send,
    share_recv,
    gift_sems,
    keep_sems,
    raw_sems,
):
    bf16 = jnp.bfloat16
    dp_here, expert_here, core = (lax.axis_index(a) for a in ("dp", "expert", "tensor"))
    partner = {"tensor": 1 - core}
    capacity = grad_chunks.shape[1]
    shard_rows = attend_shard.shape[0]
    qcols = qkv_ref.shape[1]
    width = attend_shard.shape[1]
    here = block_rows(dp_here, shard_rows)
    ready = greet(dp_here, expert_here, core)
    loads = [
        keep(ref, raw.at[place], raw_sems.at[place])
        for place, ref in enumerate((up_ref, down_ref, up_moment_ref, down_moment_ref))
    ]

    def unpick(place, tile, expert):
        return raw[place, strand(tile, expert, shard_rows, width), :].astype(bf16)

    attend_shard[:, :qcols] = inward_ref[...].astype(bf16)
    attend_shard[:, qcols:] = outward_ref[...].astype(bf16)
    weight_ref[here, :] = attend_shard[...]
    ready()
    inner = [
        remote(
            attend_shard,
            weight_ref.at[here, :],
            inner_send.at[k - 1],
            inner_recv.at[k - 1],
            {"dp": peer(dp_here, k)},
        )
        for k in PAIRS
    ]
    kept = []

    rest = combine_ref[...]
    for part in range(3):
        piece = rest.astype(bf16).astype(jnp.float32)
        columns[2 * part : 2 * part + 2, :] = piece
        rest = rest - piece
    columns[6:8, :] = (ids_ref[...] + 1).astype(jnp.float32)
    identity = one_hot(
        lax.broadcasted_iota(jnp.int32, (8, 128), 0) == lax.broadcasted_iota(jnp.int32, (8, 128), 1)
    )
    spread_rows(mxu(columns[...].astype(bf16), identity, TN), columns_padded)
    for r in range(2):
        combine_out_ref[:, r : r + 1] = (
            columns_padded[:, r : r + 1]
            + columns_padded[:, 2 + r : 3 + r]
            + columns_padded[:, 4 + r : 5 + r]
        )
    ids = columns_padded[...].astype(jnp.int32) - 1
    route(ids[:, 6:8], capacity, target_ref, target_t_ref)
    spread_rows(cot_ref[...], padded)
    slot = lax.broadcasted_iota(jnp.int32, (capacity, padded.shape[0]), 0)

    def first_slot(k):
        return (2 * peer(expert_here, k) + core) * capacity

    def send_chunks(fill, chunks, landing, which):
        def going(k, start=True):
            return Copy(
                lambda: (
                    chunks.at[k],
                    landing.at[0, k],
                    slot_send.at[which, k],
                    slot_recv.at[which, k],
                    {"expert": peer(expert_here, k)},
                ),
                start,
            )

        def make(k):
            chunks[k] = fill(slot + first_slot(k)).astype(bf16)

        def make_and_send(step, carry):
            make(2 - step)
            going(3 - step)
            return carry

        make(3)
        lax.fori_loop(0, 3, make_and_send, 0)
        copies, shared = {k: going(k, start=False) for k in PAIRS}, []
        kept.append(keep(chunks.at[0], landing.at[0, 0], keep_sems.at[1 + which]))
        shared.append(
            remote(
                chunks.at[0],
                landing.at[1, 0],
                share_send.at[which, 0],
                share_recv.at[which, 0],
                partner,
            )
        )
        return copies, shared

    def share_arrivals(copies, landing, which, shared):
        for k in FAR_FIRST[:3]:
            copies[k].wait_recv()
            shared.append(
                remote(
                    landing.at[0, k],
                    landing.at[1, k],
                    share_send.at[which, k],
                    share_recv.at[which, k],
                    partner,
                )
            )

    grads = [(combine_out_ref[:, r : r + 1] * padded[...]).astype(bf16) for r in range(2)]
    grad_copies, grad_shared = send_chunks(
        lambda slots: sum(mxu(one_hot(target_t_ref[r : r + 1] == slots), grads[r]) for r in range(2)),
        grad_chunks,
        grad_arrived_ref,
        0,
    )
    for which in range(2):
        loads[which].wait()
        for tile in range(width // LANES):
            pair = [unpick(which, tile, e) for e in range(EXP_DEV)]
            lanes = slice(tile * LANES, (tile + 1) * LANES)
            for j in range(EXP_DEV):
                expert_shard[EXP_DEV * which + j, :, lanes] = jnp.where(
                    core == 0, pair[j], pair[1 - j]
                )
    spread_rows(tokens_ref[...].astype(jnp.float32), padded)
    normed, unused, unused = layer_norm(padded[...], gains_ref[0:1], biases_ref[0:1])
    normed_low = normed.astype(bf16)
    weights = [
        remote(
            expert_shard,
            expert_w_ref.at[:, here, :],
            expert_send.at[k - 1],
            expert_recv.at[k - 1],
            {"dp": peer(dp_here, k)},
        )
        for k in (1, 2)
    ]
    kept.append(keep(expert_shard, expert_w_ref.at[:, here, :], keep_sems.at[0]))
    for which in range(2):
        loads[2 + which].wait()
        for tile in range(width // LANES):
            for e in range(EXP_DEV):
                moment_shard[EXP_DEV * which + e, :, tile * LANES : (tile + 1) * LANES] = unpick(
                    2 + which, tile, e
                )
    for copy in inner:
        copy.wait_recv()
    qkv_ref[...] = mxu(normed_low, weight_ref[:, :qcols]).astype(bf16)
    gift_ref[0:D, :] = weight_ref[:, qcols:]
    attend(qkv_ref, probs_ref, gift_ref)
    gift = remote(gift_ref, gift_other_ref, gift_sems.at[0], gift_sems.at[1], partner)
    half = padded[...] + mxu(gift_ref[D:, :], gift_ref[0:D, :], NT)
    gift.wait()
    state = half + mxu(gift_other_ref[D:, :], gift_other_ref[0:D, :], NT)
    state_ref[...] = state
    normed, unused, unused = layer_norm(state, gains_ref[1:2], biases_ref[1:2])
    normed_low = normed.astype(bf16)
    token_copies, token_shared = send_chunks(
        lambda slots: mxu(
            one_hot((target_t_ref[0:1] == slots) | (target_t_ref[1:2] == slots)), normed_low
        ),
        token_chunks,
        arrived_ref,
        1,
    )
    for copy in weights:
        copy.wait_recv()
    for k, part in ((1, slice(0, EXP_DEV)), (2, slice(EXP_DEV, 2 * EXP_DEV))):
        block = expert_w_ref.at[part, block_rows(peer(dp_here, k), shard_rows), :]
        weights.append(
            remote(
                block,
                block,
                expert_send.at[k + 1],
                expert_recv.at[k + 1],
                {"dp": peer(dp_here, 3 - k)},
            )
        )
    share_arrivals(grad_copies, grad_arrived_ref, 0, grad_shared)
    share_arrivals(token_copies, arrived_ref, 1, token_shared)
    for copy in grad_shared + token_shared + weights[2:]:
        copy.wait()
    for copy in weights[:2] + inner:
        copy.wait_send()
    for copies in (grad_copies, token_copies):
        for k in PAIRS:
            copies[k].wait_send()
    for copy in kept:
        copy.wait()


def back_kernel(
    combine_ref,
    target_ref,
    gains_ref,
    biases_ref,
    inward_moment_ref,
    outward_moment_ref,
    cot_hbm,
    tokens_hbm,
    state_hbm,
    gift_hbm,
    qkv_hbm,
    probs_hbm,
    weight_hbm,
    expert_w_hbm,
    arrived_hbm,
    grad_arrived_hbm,
    moment_hbm,
    input_ref,
    block_ref,
    norm_ref,
    attend_grad_ref,
    attend_whole_ref,
    own_steps_ref,
    home_grads_ref,
    give,
    handed,
    summed,
    returned,
    matrices,
    near_in,
    far_out,
    far_in,
    moment_whole,
    owned_low,
    normed_part,
    normed_other,
    inner,
    inner_in,
    plane,
    quarter_in,
    quarter,
    plane_total,
    whole_own,
    norm_own,
    norm_in,
    gram,
    gram_other,
    hand_send,
    hand_recv,
    slot_send,
    slot_recv,
    share_send,
    share_recv,
    pair_send,
    pair_recv,
    dp_send,
    dp_recv,
    expert_send,
    expert_recv,
    near_send,
    near_recv,
    far_send,
    far_recv,
    own_sems,
    load_sems,
):
    bf16, f32 = jnp.bfloat16, jnp.float32
    dp_here, expert_here, core = (lax.axis_index(a) for a in ("dp", "expert", "tensor"))
    partner = {"tensor": 1 - core}
    capacity = give.shape[2]
    shard_rows = inner.shape[1]
    here = block_rows(dp_here, shard_rows)
    ready = greet(dp_here, expert_here, core)
    sent = []

    def to_dp(stage, sources, targets, peers=PAIRS):
        def copy(k):
            return Copy(
                lambda: (
                    sources(k),
                    targets(k),
                    dp_send.at[stage, k - 1],
                    dp_recv.at[stage, k - 1],
                    {"dp": peer(dp_here, k)},
                )
            )

        copies = [copy(k) for k in peers]
        sent.extend(copies)
        return copies

    def to_expert(stage, sources, targets):
        def copy(k):
            return Copy(
                lambda: (
                    sources(k),
                    targets(k),
                    expert_send.at[stage, k - 1],
                    expert_recv.at[stage, k - 1],
                    {"expert": peer(expert_here, k)},
                )
            )

        copies = [copy(k) for k in PAIRS]
        sent.extend(copies)
        return copies

    def arrive(copies):
        for copy in copies:
            copy.wait_recv()

    shares = ([], [])

    def hand(which, k, start=True):
        return Copy(
            lambda: (
                give.at[which, k],
                handed.at[which, k],
                hand_send.at[which, k],
                hand_recv.at[which, k],
                partner,
            ),
            start,
        )

    def add_up(which, k):
        hand(which, k, start=False).wait_recv()
        total = (summed[which, k].astype(f32) + handed[which, k].astype(f32)).astype(bf16)
        summed[which, k] = total

    def send_home(which, k, start=True):
        return Copy(
            lambda: (
                summed.at[which, k],
                returned.at[which, 0, k],
                slot_send.at[which, k],
                slot_recv.at[which, k],
                {"expert": peer(expert_here, k)},
            ),
            start,
        )

    def stay_home(which):
        returned[which, 0, 0] = summed[which, 0]
        shares[which].append(
            Copy(
                lambda: (
                    summed.at[which, 0],
                    returned.at[which, 1, 0],
                    share_send.at[which, 0],
                    share_recv.at[which, 0],
                    partner,
                )
            )
        )

    def share(which):
        def copy(k):
            return Copy(
                lambda: (
                    returned.at[which, 0, k],
                    returned.at[which, 1, k],
                    share_send.at[which, k],
                    share_recv.at[which, k],
                    partner,
                )
            )

        for k in FAR_FIRST[:3]:
            send_home(which, k, start=False).wait_recv()
            shares[which].append(copy(k))
        sent.extend(shares[which])
        arrive(shares[which])

    def held(index):
        return 2 * (index // 2) + (index % 2 + core) % 2

    ways = ((slice(0, D // 2), 1, 2), (slice(D // 2, D), 2, 1))

    def near_copy(half, place):
        rows, first, second = ways[half]
        owner = (first, 3)[place]
        return Copy(
            lambda: (
                matrices.at[held(peer(dp_here, owner)), rows, :],
                near_in.at[half, place],
                near_send.at[half, place],
                near_recv.at[half, place],
                {"dp": peer(dp_here, first)},
            )
        )

    def far_copy(half):
        rows, first, second = ways[half]
        return Copy(
            lambda: (
                far_out.at[half],
                far_in.at[half],
                far_send.at[half],
                far_recv.at[half],
                {"dp": peer(dp_here, second)},
            )
        )

    def pass_on(near):
        arrive(near)
        for half, (rows, first, second) in enumerate(ways):
            far_out[half] = (
                matrices[held(peer(dp_here, second)), rows, :].astype(f32)
                + near_in[half, 1].astype(f32)
            ).astype(bf16)
        far = [far_copy(half) for half in range(2)]
        sent.extend(far)
        return far

    def experts(weights, rows, grads, hidden, pre_grad):
        loads = {}
        for j in (1, 0):
            for place, (source, target) in enumerate(
                (
                    (expert_w_hbm.at[j], weights.at[j]),
                    (arrived_hbm.at[j], rows.at[j]),
                    (expert_w_hbm.at[EXP_DEV + j], weights.at[EXP_DEV + j]),
                    (grad_arrived_hbm.at[j], grads.at[j]),
                )
            ):
                loads[j, place] = keep(source, target, load_sems.at[4 * j + place])
        ready()
        moments.extend(
            to_dp(0, lambda k: moment_hbm.at[peer(dp_here, k)], lambda k: moment_whole.at[here, :])
        )

        def chunk(k, first=False):
            for j in (1, 0):
                if first:
                    loads[j, 0].wait()
                    loads[j, 1].wait()
                pre = mxu(rows[j, k], weights[j])
                share_of_one = 0.5 * (1.0 + lax.erf(pre * 0.7071067811865476))
                hidden[j, k] = (pre * share_of_one).astype(bf16)
                slope = share_of_one + pre * 0.3989422804014327 * jnp.exp(-0.5 * pre * pre)
                if first:
                    loads[j, 2].wait()
                    loads[j, 3].wait()
                grad = (mxu(grads[j, k], weights[EXP_DEV + j]) * slope).astype(bf16)
                pre_grad[j, k] = grad
                entry = mxu(grad, weights[j], NT).astype(bf16)
                if j == 1:
                    give[0, k] = entry
                else:
                    summed[0, k] = entry

        def next_chunk(step, carry):
            chunk(2 - step)
            add_up(0, 3 - step)
            hand(0, 2 - step)
            send_home(0, 3 - step)
            return carry

        chunk(3, first=True)
        hand(0, 3)
        lax.fori_loop(0, 3, next_chunk, 0)

        def matrix(left, right, j):
            total = mxu(left[j, 0], right[j, 0], TN)
            for k in PAIRS:
                total += mxu(left[j, k], right[j, k], TN)
            return total.astype(bf16)

        def expert_matrices(j, carry):
            matrices[j] = matrix(rows, pre_grad, j)
            matrices[EXP_DEV + j] = matrix(grads, hidden, j)
            return carry

        lax.fori_loop(0, EXP_DEV, expert_matrices, 0)
        near = [near_copy(half, place) for place in (1, 0) for half in range(2)]
        sent.extend(near)
        add_up(0, 0)
        stay_home(0)

        def part_chunk(step, carry):
            k = 3 - step
            give[1, k] = mxu(hidden[1, k], weights[EXP_DEV + 1], NT).astype(bf16)
            summed[1, k] = mxu(hidden[0, k], weights[EXP_DEV], NT).astype(bf16)
            hand(1, k)
            return carry

        lax.fori_loop(0, 4, part_chunk, 0)
        for k in FAR_FIRST:
            add_up(1, k)
        for k in FAR_FIRST[:3]:
            send_home(1, k)
        stay_home(1)
        for which in range(2):
            sent.extend(hand(which, k, start=False) for k in range(4))
            sent.extend(send_home(which, k, start=False) for k in PAIRS)
        return near

    own_moment = keep(moment_hbm.at[dp_here], moment_whole.at[here, :], own_sems.at[0])
    near, moments = [], []
    slots = (EXP_DEV, 4, capacity)
    pl.run_scoped(
        lambda *refs: near.extend(experts(*refs)),
        pltpu.VMEM(expert_w_hbm.shape, bf16),
        pltpu.VMEM(slots + (D,), bf16),
        pltpu.VMEM(slots + (D,), bf16),
        pltpu.VMEM(slots + (expert_w_hbm.shape[2],), bf16),
        pltpu.VMEM(slots + (expert_w_hbm.shape[2],), bf16),
    )

    def backward(
        cot_ref,
        tokens_ref,
        state_ref,
        gift_ref,
        qkv_ref,
        probs_ref,
        weight_ref,
        padded,
        qkv_grad_ref,
        local_ref,
        out_grad_ref,
    ):
        loads = [
            keep(source, target, load_sems.at[place])
            for place, (source, target) in enumerate(
                (
                    (state_hbm, state_ref),
                    (cot_hbm, cot_ref),
                    (gift_hbm.at[D:, :], gift_ref),
                    (weight_hbm, weight_ref),
                    (qkv_hbm, qkv_ref),
                    (probs_hbm, probs_ref),
                    (tokens_hbm, tokens_ref),
                )
            )
        ]
        qcols = qkv_ref.shape[1]
        rows_all = state_ref.shape[0]
        loads[0].wait()
        unused, scaled2, invert2 = layer_norm(state_ref[...], gains_ref[1:2], biases_ref[1:2])
        loads[1].wait()
        spread_rows(cot_ref[...], padded)
        def pick_all(which, columns, rows):
            slot = lax.broadcasted_iota(jnp.int32, (PAD, capacity), 1)

            def picks(k, j):
                first = slot + (2 * peer(expert_here, k) + (core + j) % 2) * capacity
                hit = target_ref[rows, columns[0] : columns[0] + 1] == first
                for column in columns[1:]:
                    hit = hit | (target_ref[rows, column : column + 1] == first)
                return one_hot(hit)

            total = mxu(picks(0, 0), returned[which, 0, 0])
            for j in range(2):
                for k in FAR_FIRST:
                    if k + j > 0:
                        total += mxu(picks(k, j), returned[which, j, k])
            return total

        share(0)

        def one_gradient(image, carry):
            rows = block_rows(image, PAD)
            normed_part[rows, :] = pick_all(0, (0, 1), rows)
            return carry

        lax.fori_loop(0, rows_all // PAD, one_gradient, 0)
        normed2_grad = normed_part[...]
        norm_own[0, 4:8] = jnp.zeros((4, D), f32)
        norm_own[0, 1:2] = jnp.sum(normed2_grad * scaled2, axis=0, keepdims=True)
        norm_own[0, 3:4] = jnp.sum(normed2_grad, axis=0, keepdims=True)
        state_grad = padded[...] + norm_backward(normed2_grad, scaled2, invert2, gains_ref[1:2])
        padded[...] = state_grad
        state_low = state_grad.astype(bf16)
        for copy in loads[2:]:
            copy.wait()

        local_ref[:, qcols:] = mxu(state_low, gift_ref[...], TN)
        out_grad_ref[...] = mxu(state_low, weight_ref[:, qcols:]).astype(bf16)
        heads_here = qcols // (3 * HD)
        scale = HD ** (-0.5)

        def one_image(image, carry):
            rows = block_rows(image, PAD)
            for head in range(heads_here):
                base = head * 3 * HD
                query = qkv_ref[rows, base : base + HD]
                key = qkv_ref[rows, base + HD : base + 2 * HD]
                value = qkv_ref[rows, base + 2 * HD : base + 3 * HD]
                out_grad = out_grad_ref[rows, head * HD : (head + 1) * HD]
                probs = probs_ref[image * heads_here + head]
                prob_grad = mxu(out_grad, value, NT)
                score_grad = (
                    probs * (prob_grad - jnp.sum(probs * prob_grad, axis=-1, keepdims=True))
                ).astype(bf16)
                qkv_grad_ref[rows, base : base + HD] = (mxu(score_grad, key) * scale).astype(bf16)
                qkv_grad_ref[rows, base + HD : base + 2 * HD] = (
                    mxu(score_grad, query, TN) * scale
                ).astype(bf16)
                qkv_grad_ref[rows, base + 2 * HD : base + 3 * HD] = mxu(
                    probs.astype(bf16), out_grad, TN
                ).astype(bf16)
            return carry

        lax.fori_loop(0, rows_all // PAD, one_image, 0)
        spread_rows(tokens_ref[...].astype(f32), normed_part)
        normed1, scaled1, invert1 = layer_norm(normed_part[...], gains_ref[0:1], biases_ref[0:1])
        local_ref[:, :qcols] = mxu(normed1.astype(bf16), qkv_grad_ref[...], TN)
        for k in range(4):
            inner[k] = local_ref[block_rows(peer(dp_here, k), shard_rows), :].astype(bf16)
        normed_part[...] = mxu(qkv_grad_ref[...], weight_ref[:, :qcols], NT)
        rows_sums = to_dp(1, lambda k: inner.at[k], lambda k: inner_in.at[k - 1])
        pair = Copy(
            lambda: (normed_part, normed_other, pair_send.at[0], pair_recv.at[0], partner)
        )
        sent.append(pair)
        far = pass_on(near)

        share(1)

        def one_output(image, carry):
            rows = block_rows(image, PAD)
            total = state_ref[rows, :]
            for r in range(2):
                total += combine_ref[rows, r : r + 1] * pick_all(1, (r,), rows)
            state_ref[rows, :] = total
            return carry

        lax.fori_loop(0, rows_all // PAD, one_output, 0)
        gather_rows(state_ref[...], block_ref)

        pair.wait_recv()
        normed1_grad = normed_part[...] + normed_other[...]
        norm_own[0, 0:1] = jnp.sum(normed1_grad * scaled1, axis=0, keepdims=True)
        norm_own[0, 2:3] = jnp.sum(normed1_grad, axis=0, keepdims=True)
        norm_in[0, dp_here] = norm_own[0]
        norms = to_dp(2, lambda k: norm_own.at[0], lambda k: norm_in.at[0, dp_here])
        gather_rows(
            padded[...] + norm_backward(normed1_grad, scaled1, invert1, gains_ref[0:1]), input_ref
        )
        return rows_sums, norms, far

    travelling = []
    rows_f32 = pltpu.VMEM(state_hbm.shape, f32)
    pl.run_scoped(
        lambda *refs: travelling.extend(backward(*refs)),
        pltpu.VMEM(cot_hbm.shape, f32),
        pltpu.VMEM(tokens_hbm.shape, bf16),
        rows_f32,
        pltpu.VMEM((gift_hbm.shape[0] - D, gift_hbm.shape[1]), bf16),
        pltpu.VMEM(qkv_hbm.shape, bf16),
        pltpu.VMEM(probs_hbm.shape, f32),
        pltpu.VMEM(weight_hbm.shape, bf16),
        rows_f32,
        pltpu.VMEM(qkv_hbm.shape, bf16),
        pltpu.VMEM(weight_hbm.shape, f32),
        pltpu.VMEM((state_hbm.shape[0], gift_hbm.shape[1]), bf16),
    )
    rows_sums, norms, far = travelling

    arrive(rows_sums)
    plane[...] = (
        inner[0].astype(f32)
        + inner_in[0].astype(f32)
        + inner_in[1].astype(f32)
        + inner_in[2].astype(f32)
    ).astype(bf16)
    quarter_rows = quarter.shape[0]
    my_quarter = block_rows(expert_here, quarter_rows)
    quarters = to_expert(
        0,
        lambda k: plane.at[block_rows(peer(expert_here, k), quarter_rows), :],
        lambda k: quarter_in.at[k - 1],
    )
    arrive(norms)
    norm_plane = norm_in[0, 0] + norm_in[0, 1] + norm_in[0, 2] + norm_in[0, 3]
    norm_own[1] = norm_plane
    norm_in[1, expert_here] = norm_plane
    norm_sums = to_expert(1, lambda k: norm_own.at[1], lambda k: norm_in.at[1, expert_here])

    def orthogonalize(owned_next, factor, change):
        arrive(quarters)
        quarter[...] = (
            plane[my_quarter, :].astype(f32)
            + quarter_in[0].astype(f32)
            + quarter_in[1].astype(f32)
            + quarter_in[2].astype(f32)
        ).astype(bf16)
        plane_total[my_quarter, :] = quarter[...]
        totals = to_expert(2, lambda k: quarter, lambda k: plane_total.at[my_quarter, :])
        arrive(far + moments)
        own_moment.wait()
        for half, (rows, first, second) in enumerate(ways):
            owned = (
                matrices[held(dp_here), rows, :].astype(f32)
                + near_in[half, 0].astype(f32)
                + far_in[half].astype(f32)
            )
            owned_low[rows, :] = owned.astype(bf16)
            owned_next[rows, :] = 0.95 * moment_whole[rows, :].astype(f32) + owned
        split = halves(owned_next[...])
        gram[...] = mxu3(split, split, NT)
        pair = remote(gram, gram_other, pair_send.at[1], pair_recv.at[1], partner)
        home = to_dp(
            3,
            lambda k: owned_low.at[block_rows(peer(dp_here, k), shard_rows), :],
            lambda k: home_grads_ref.at[dp_here],
        )
        own = keep(owned_low.at[here, :], home_grads_ref.at[dp_here], load_sems.at[1])
        pair.wait()

        def attention_next():
            arrive(totals)
            total = plane_total[...].astype(f32)
            attend_grad_ref[...] = total
            qcols = inward_moment_ref.shape[1]
            whole_own[:, :qcols] = (0.95 * inward_moment_ref[...] + total[:, :qcols]).astype(bf16)
            whole_own[:, qcols:] = (0.95 * outward_moment_ref[...] + total[:, qcols:]).astype(bf16)
            attend_whole_ref[here, :] = whole_own[...]
            wholes.extend(to_dp(4, lambda k: whole_own, lambda k: attend_whole_ref.at[here, :]))

        wholes = []
        find_factor(gram[...] + gram_other[...], factor, gram, change, gram_other, attention_next)
        own_steps_ref[...] = (
            mxu3(halves(factor[...]), halves(owned_next[...])) * (0.2 * math.sqrt(F))
        ).astype(bf16)
        arrive(norm_sums)
        norm_ref[...] = (
            norm_in[1, 0, 0:4] + norm_in[1, 1, 0:4] + norm_in[1, 2, 0:4] + norm_in[1, 3, 0:4]
        )
        arrive(home)
        arrive(wholes)
        own.wait()

    square = pltpu.VMEM((D, D), f32)
    pl.run_scoped(orthogonalize, pltpu.VMEM(moment_whole.shape, f32), square, square)
    for copy in sent:
        copy.wait_send()


def halves(value):
    high = value.astype(jnp.bfloat16)
    return high, (value - high.astype(jnp.float32)).astype(jnp.bfloat16)


def mxu3(left, right, dims=(((1,), (0,)), ((), ()))):
    return (
        mxu(left[0], right[0], dims) + mxu(left[1], right[0], dims) + mxu(left[0], right[1], dims)
    )


def find_factor(gram, factor, current, change, scaled, between=None):
    diagonal = lax.broadcasted_iota(jnp.int32, gram.shape, 0) == lax.broadcasted_iota(
        jnp.int32, gram.shape, 1
    )
    squares = jnp.sum(
        jnp.sum(jnp.where(diagonal, gram, 0.0), axis=1, keepdims=True), axis=0, keepdims=True
    )
    norm = jnp.sqrt(squares) + 1e-07
    current[...] = gram / (norm * norm)
    factor[...] = jnp.where(diagonal, 1.0 / norm, 0.0)
    half = D // 2

    def stacked(left, right):
        count = left[0].shape[0]
        both = mxu(jnp.concatenate(left, axis=0), right[0])
        return both[:count] + both[count:] + mxu(left[0], right[1])

    def product(out, left, right, by, added, added_by):
        first = stacked(left, [x[:, :half] for x in right])
        first = by * first + added_by * added[:, :half]
        corner = stacked([x[half:] for x in left], [x[:, half:] for x in right])
        corner = by * corner + added_by * added[half:, half:]
        out[:, :half] = first
        out[:half, half:] = first[half:].T
        out[half:, half:] = corner

    def sweep(index, carry):
        if between is not None:
            pl.when(index == MIDWAY)(between)
        low = halves(current[...])
        product(change, low, low, 2.0315, current, -4.775)
        step = halves(change[...])
        product(factor, step, halves(factor[...]), 1.0, factor, 3.4445)

        @pl.when(index < 4)
        def next_gram():
            product(scaled, step, low, 1.0, current, 3.4445)
            product(current, halves(scaled[...]), step, 1.0, scaled, 3.4445)

        return carry

    lax.fori_loop(0, 5, sweep, 0)


def finish_kernel(
    whole_ref,
    own_steps_ref,
    home_steps_ref,
    attend_step_ref,
    kept,
    given,
    taken,
    factor,
    change,
    mine,
    other,
    step_send,
    step_recv,
    pair_send,
    pair_recv,
):
    dp_here, core = lax.axis_index("dp"), lax.axis_index("tensor")
    partner = {"tensor": 1 - core}
    shard_rows = mine.shape[0]
    qcols = 3 * whole_ref.shape[1] // 4
    here = block_rows(dp_here, shard_rows)
    ready = greet(dp_here, None, core, over_expert=False)
    inward_gram = mxu(whole_ref[:, :qcols], whole_ref[:, :qcols], NT)
    outward_gram = mxu(whole_ref[:, qcols:], whole_ref[:, qcols:], NT)
    kept[...] = jnp.where(core == 0, inward_gram, outward_gram)
    given[...] = jnp.where(core == 0, outward_gram, inward_gram)
    ready()
    pair = remote(given, taken, pair_send.at[0], pair_recv.at[0], partner)
    steps = [
        remote(
            own_steps_ref.at[block_rows(peer(dp_here, k), shard_rows), :],
            home_steps_ref.at[dp_here],
            step_send.at[k - 1],
            step_recv.at[k - 1],
            {"dp": peer(dp_here, k)},
        )
        for k in PAIRS
    ]
    home_steps_ref[dp_here] = own_steps_ref[here, :]
    pair.wait()
    find_factor(kept[...] + taken[...], factor, kept, change, taken)
    mine[...] = factor[here, :]
    pair = remote(mine, other, pair_send.at[1], pair_recv.at[1], partner)
    for copy in steps:
        copy.wait()
    pair.wait()
    for owner, columns, count in ((0, slice(0, qcols), 3 * D), (1, slice(qcols, None), D)):
        rows = halves(jnp.where(core == owner, mine[...], other[...]))
        step = mxu(rows[0], whole_ref[:, columns]) + mxu(rows[1], whole_ref[:, columns])
        attend_step_ref[:, columns] = step * (0.2 * math.sqrt(count))


def apply_kernel(
    steps_done_ref,
    home_steps_ref,
    attend_step_ref,
    home_grads_ref,
    attend_grad_ref,
    norm_ref,
    gains_ref,
    biases_ref,
    first_ref,
    second_ref,
    inward_ref,
    outward_ref,
    up_ref,
    down_ref,
    inward_moment_ref,
    outward_moment_ref,
    up_moment_ref,
    down_moment_ref,
    block_ref,
    input_ref,
    block_out_ref,
    input_out_ref,
    inward_gradient_ref,
    outward_gradient_ref,
    up_gradient_ref,
    down_gradient_ref,
    gain_gradient_ref,
    bias_gradient_ref,
    inward_next_ref,
    outward_next_ref,
    up_next_ref,
    down_next_ref,
    inward_new_ref,
    outward_new_ref,
    up_new_ref,
    down_new_ref,
    inward_copy_ref,
    outward_copy_ref,
    up_copy_ref,
    down_copy_ref,
    gains_new_ref,
    biases_new_ref,
    first_new_ref,
    second_new_ref,
    weave,
):
    f32 = jnp.float32
    qcols = inward_ref.shape[1]
    block_out_ref[...] = block_ref[...]
    input_out_ref[...] = input_ref[...]

    def finish(place, gradient, step, refs):
        master_ref, moment_ref, gradient_ref, next_ref, new_ref, copy_ref = refs
        gradient_ref[place] = gradient
        next_ref[place] = 0.95 * moment_ref[place] + gradient
        master = master_ref[place]
        new = master - 0.1 * (step + 0.1 * master)
        new_ref[place] = new
        copy_ref[place] = new.astype(copy_ref.dtype)

    experts = (
        (up_ref, up_moment_ref, up_gradient_ref, up_next_ref, up_new_ref, up_copy_ref),
        (down_ref, down_moment_ref, down_gradient_ref, down_next_ref, down_new_ref, down_copy_ref),
    )
    everything = (slice(None), slice(None))
    rows, width = attend_grad_ref.shape
    for which, refs in enumerate(experts):
        for place, home_ref in enumerate((home_grads_ref, home_steps_ref)):
            for e in range(EXP_DEV):
                for tile in range(width // LANES):
                    weave[place, strand(tile, e, rows, width), :] = home_ref[
                        EXP_DEV * which + e, :, tile * LANES : (tile + 1) * LANES
                    ].astype(f32)
        finish(everything, weave[0], weave[1], refs)
    finish(
        everything,
        attend_grad_ref[:, :qcols],
        attend_step_ref[:, :qcols],
        (
            inward_ref,
            inward_moment_ref,
            inward_gradient_ref,
            inward_next_ref,
            inward_new_ref,
            inward_copy_ref,
        ),
    )
    finish(
        everything,
        attend_grad_ref[:, qcols:],
        attend_step_ref[:, qcols:],
        (
            outward_ref,
            outward_moment_ref,
            outward_gradient_ref,
            outward_next_ref,
            outward_new_ref,
            outward_copy_ref,
        ),
    )

    @pl.when(pl.program_id(0) == 0)
    def norms():
        total = norm_ref[...]
        gain_gradient_ref[...] = total[0:2]
        bias_gradient_ref[...] = total[2:4]
        moment_first = 0.9 * first_ref[...] + 0.1 * total
        moment_second = 0.999 * second_ref[...] + 0.001 * total * total
        first_new_ref[...] = moment_first
        second_new_ref[...] = moment_second
        done = jnp.full((4, D), steps_done_ref[0], jnp.int32).astype(f32)
        direction = (
            moment_first
            / (1.0 - jnp.power(0.9, done))
            / (jnp.sqrt(moment_second / (1.0 - jnp.power(0.999, done))) + 1e-08)
        )
        gains_new_ref[...] = gains_ref[...] - 0.1 * direction[0:2]
        biases_new_ref[...] = biases_ref[...] - 0.1 * direction[2:4]


def pair_body(
    tokens_in,
    expert_ids,
    combine,
    out_cot,
    inward_master,
    outward_master,
    up_master,
    down_master,
    norm_gains,
    norm_biases,
    inward_moment,
    outward_moment,
    up_moment,
    down_moment,
    first_moment,
    second_moment,
    step_count,
):
    bf16, f32 = jnp.bfloat16, jnp.float32
    token_rows = tokens_in.shape[0]
    expert_total = EXP_DEV * 4
    capacity = (token_rows * 10 // (4 * expert_total) + 7) // 8 * 8
    shard_rows, qcols = inward_master.shape
    width = up_master.shape[2]
    images = token_rows // SEQ
    padded_rows = images * PAD
    heads_here = qcols // (3 * HD)
    shape = jax.ShapeDtypeStruct
    rows_f32 = pltpu.VMEM((padded_rows, D), f32)
    in_vmem, anywhere = pl.BlockSpec(memory_space=pltpu.VMEM), pl.BlockSpec(memory_space=pl.ANY)
    dma = pltpu.SemaphoreType.DMA

    slots = shape((EXP_DEV, 4, capacity, D), bf16)
    (
        state,
        gift,
        qkv_low,
        probs,
        weight,
        target,
        combine_padded,
        moment_shard,
        expert_w,
        arrived,
        grad_arrived,
    ) = pl.pallas_call(
        front_kernel,
        out_shape=(
            shape((padded_rows, D), f32),
            shape((D + padded_rows, heads_here * HD), bf16),
            shape((padded_rows, qcols), bf16),
            shape((images * heads_here, PAD, PAD), f32),
            shape((D, width), bf16),
            shape((padded_rows, 128), jnp.int32),
            shape((padded_rows, 2), f32),
            shape((4, shard_rows, width), bf16),
            shape((2 * EXP_DEV, D, width), bf16),
            slots,
            slots,
        ),
        in_specs=[in_vmem] * 8 + [anywhere] * 4,
        out_specs=tuple([in_vmem] * 8 + [anywhere] * 3),
        scratch_shapes=[
            rows_f32,
            pltpu.VMEM((8, token_rows), f32),
            pltpu.VMEM((padded_rows, 128), f32),
            pltpu.VMEM((4, EXP_DEV * shard_rows * width // LANES, LANES), f32),
            pltpu.VMEM((2, padded_rows), jnp.int32),
            pltpu.VMEM((shard_rows, width), bf16),
            pltpu.VMEM((4, shard_rows, width), bf16),
            pltpu.VMEM((D + padded_rows, heads_here * HD), bf16),
            pltpu.VMEM((4, capacity, D), bf16),
            pltpu.VMEM((4, capacity, D), bf16),
            dma((3,)),
            dma((3,)),
            dma((4,)),
            dma((4,)),
            dma((2, 4)),
            dma((2, 4)),
            dma((2, 4)),
            dma((2, 4)),
            dma((2,)),
            dma((3,)),
            dma((4,)),
        ],
        name="front",
        cost_estimate=pl.CostEstimate(
            flops=60_000_000_000, bytes_accessed=30_000_000, transcendentals=0
        ),
        compiler_params=pltpu.CompilerParams(collective_id=0, has_side_effects=True),
    )(
        expert_ids.T,
        combine.T,
        out_cot,
        tokens_in,
        norm_gains,
        norm_biases,
        inward_master,
        outward_master,
        *(woven(a) for a in (up_master, down_master, up_moment, down_moment)),
    )
    chunks = (2, 4, capacity, D)
    square = pltpu.VMEM((D, D), f32)
    rows_low = pltpu.VMEM((shard_rows, width), bf16)
    (
        input_gradient,
        block_out,
        norm_total,
        attend_grad,
        attend_whole,
        own_steps,
        home_grads,
    ) = pl.pallas_call(
        back_kernel,
        out_shape=(
            shape((token_rows, D), f32),
            shape((token_rows, D), bf16),
            shape((4, D), f32),
            shape((shard_rows, width), f32),
            shape((D, width), bf16),
            shape((D, width), bf16),
            shape((4, shard_rows, width), bf16),
        ),
        in_specs=[in_vmem] * 6 + [anywhere] * 11,
        out_specs=tuple([in_vmem] * 6 + [anywhere]),
        scratch_shapes=[
            pltpu.VMEM(chunks, bf16),
            pltpu.VMEM(chunks, bf16),
            pltpu.VMEM(chunks, bf16),
            pltpu.VMEM((2,) + chunks, bf16),
            pltpu.VMEM((4, D, width), bf16),
            pltpu.VMEM((2, 2, D // 2, width), bf16),
            pltpu.VMEM((2, D // 2, width), bf16),
            pltpu.VMEM((2, D // 2, width), bf16),
            pltpu.VMEM((D, width), bf16),
            pltpu.VMEM((D, width), bf16),
            rows_f32,
            rows_f32,
            pltpu.VMEM((4, shard_rows, width), bf16),
            pltpu.VMEM((3, shard_rows, width), bf16),
            rows_low,
            pltpu.VMEM((3, shard_rows // 4, width), bf16),
            pltpu.VMEM((shard_rows // 4, width), bf16),
            rows_low,
            rows_low,
            pltpu.VMEM((2, 8, D), f32),
            pltpu.VMEM((2, 4, 8, D), f32),
            square,
            square,
        ]
        + [dma((2, 4))] * 6
        + [dma((2,))] * 2
        + [dma((5, 3))] * 2
        + [dma((3, 3))] * 2
        + [dma((2, 2))] * 2
        + [dma((2,))] * 2
        + [dma((1,))]
        + [dma((8,))],
        name="back",
        cost_estimate=pl.CostEstimate(
            flops=110_000_000_000, bytes_accessed=60_000_000, transcendentals=0
        ),
        compiler_params=pltpu.CompilerParams(
            collective_id=1, has_side_effects=True, vmem_limit_bytes=66_000_000
        ),
    )(
        combine_padded,
        target,
        norm_gains,
        norm_biases,
        inward_moment,
        outward_moment,
        out_cot,
        tokens_in,
        state,
        gift,
        qkv_low,
        probs,
        weight,
        expert_w,
        arrived,
        grad_arrived,
        moment_shard,
    )
    factor_rows = pltpu.VMEM((shard_rows, D), f32)
    home_steps, attend_step = pl.pallas_call(
        finish_kernel,
        out_shape=(shape((4, shard_rows, width), bf16), shape((shard_rows, width), f32)),
        in_specs=[in_vmem] * 2,
        out_specs=(in_vmem, in_vmem),
        scratch_shapes=[square] * 5 + [factor_rows] * 2 + [dma((3,))] * 2 + [dma((2,))] * 2,
        name="finish",
        cost_estimate=pl.CostEstimate(
            flops=20_000_000_000, bytes_accessed=5_000_000, transcendentals=0
        ),
        compiler_params=pltpu.CompilerParams(collective_id=2, has_side_effects=True),
    )(attend_whole, own_steps)

    blocks = 4
    inward, outward = inward_master.shape, outward_master.shape
    expert = (EXP_DEV * shard_rows * width // LANES, LANES)

    def split(whole, along=0):
        if along is None:
            return pl.BlockSpec(whole, lambda i: (0,) * len(whole))
        rows = pl.cdiv(pl.cdiv(whole[along], blocks), 8) * 8
        block = whole[:along] + (rows,) + whole[along + 1 :]
        return pl.BlockSpec(
            block, lambda i: (0,) * along + (i,) + (0,) * (len(whole) - along - 1)
        )

    two, four, attended = (2, D), (4, D), (shard_rows, width)
    matrix_shapes = (inward, outward, expert, expert)
    by_rows = [split(m) for m in matrix_shapes]
    tokens = split((token_rows, D))
    finished = pl.pallas_call(
        apply_kernel,
        grid=(blocks,),
        out_shape=tuple(
            [shape((token_rows, D), bf16), shape((token_rows, D), f32)]
            + [shape(m, f32) for m in matrix_shapes]
            + [shape(two, f32)] * 2
            + [shape(m, f32) for m in matrix_shapes * 2]
            + [shape(m, bf16) for m in matrix_shapes]
            + [shape(two, f32)] * 2
            + [shape(four, f32)] * 2
        ),
        in_specs=[pl.BlockSpec(memory_space=pltpu.SMEM)]
        + [split((4,) + attended, 1), split(attended), split((4,) + attended, 1), split(attended)]
        + [split(four, None), split(two, None), split(two, None), split(four, None), split(four, None)]
        + by_rows * 2
        + [tokens] * 2,
        out_specs=tuple(
            [tokens] * 2
            + by_rows
            + [split(two, None)] * 2
            + by_rows * 3
            + [split(two, None)] * 2
            + [split(four, None)] * 2
        ),
        scratch_shapes=[pltpu.VMEM((2, expert[0] // blocks, LANES), f32)],
        name="apply",
        cost_estimate=pl.CostEstimate(
            flops=20_000_000, bytes_accessed=20_000_000, transcendentals=0
        ),
    )(
        step_count,
        home_steps,
        attend_step,
        home_grads,
        attend_grad,
        norm_total,
        norm_gains,
        norm_biases,
        first_moment,
        second_moment,
        inward_master,
        outward_master,
        woven(up_master),
        woven(down_master),
        inward_moment,
        outward_moment,
        woven(up_moment),
        woven(down_moment),
        block_out,
        input_gradient,
    )
    return tuple(
        unwoven(a, up_master.shape) if a.shape == expert else a for a in finished
    )


def solution(mesh):
    sizes = tuple(mesh.shape[axis] for axis in ("dp", "expert", "tensor"))
    body = pair_body if sizes == (4, 4, 2) else start_body
    return jax.shard_map(
        body,
        mesh=mesh,
        in_specs=(
            P(("dp", "expert"), None),
            P(("dp", "expert"), None),
            P(("dp", "expert"), None),
            P(("dp", "expert"), None),
            P("dp", "tensor"),
            P("dp", "tensor"),
            P("dp", "expert", "tensor"),
            P("dp", "expert", "tensor"),
            P(),
            P(),
            P("dp", "tensor"),
            P("dp", "tensor"),
            P("dp", "expert", "tensor"),
            P("dp", "expert", "tensor"),
            P(),
            P(),
            P(),
        ),
        out_specs=(
            P(("dp", "expert"), None),
            P(("dp", "expert"), None),
            P("dp", "tensor"),
            P("dp", "tensor"),
            P("dp", "expert", "tensor"),
            P("dp", "expert", "tensor"),
            P(),
            P(),
            P("dp", "tensor"),
            P("dp", "tensor"),
            P("dp", "expert", "tensor"),
            P("dp", "expert", "tensor"),
            P("dp", "tensor"),
            P("dp", "tensor"),
            P("dp", "expert", "tensor"),
            P("dp", "expert", "tensor"),
            P("dp", "tensor"),
            P("dp", "tensor"),
            P("dp", "expert", "tensor"),
            P("dp", "expert", "tensor"),
            P(),
            P(),
            P(),
            P(),
        ),
        check_vma=False,
    )
```

```python
import functools
import math

import jax
import jax.numpy as jnp
import numpy as np
from jax import lax
from jax.experimental import pallas as pl
from jax.experimental.pallas import tpu as pltpu
from jax.sharding import PartitionSpec as P

D = 512
HD = 64
F = 2048
SEQ = 197
EXP_DEV = 2


def layer_norm(values, gain_row, bias_row):
    center = values - jnp.mean(values, axis=-1, keepdims=True)
    invert = lax.rsqrt(jnp.mean(center * center, axis=-1, keepdims=True) + 1e-06)
    scaled = center * invert
    return (scaled * gain_row + bias_row, scaled, invert)


def norm_backward(upstream, scaled, invert, gain_row):
    weighted = upstream * gain_row
    return invert * (
        weighted
        - jnp.mean(weighted, axis=-1, keepdims=True)
        - scaled * jnp.mean(weighted * scaled, axis=-1, keepdims=True)
    )


def gelu_exact(values):
    return 0.5 * values * (1.0 + lax.erf(values * 0.7071067811865476))


def gelu_slope(values):
    return 0.5 * (
        1.0 + lax.erf(values * 0.7071067811865476)
    ) + values * 0.3989422804014327 * jnp.exp(-0.5 * values * values)


def newton_schulz(matrix):
    current = matrix / (jnp.sqrt(jnp.sum(matrix * matrix)) + 1e-07)
    for sweep_index in range(5):
        gram_matrix = jnp.dot(current, current.T, precision=lax.Precision.HIGHEST)
        polynom = -4.775 * gram_matrix + 2.0315 * jnp.dot(
            gram_matrix, gram_matrix, precision=lax.Precision.HIGHEST
        )
        current = 3.4445 * current + jnp.dot(polynom, current, precision=lax.Precision.HIGHEST)
    return current


def start_body(
    tokens_in,
    expert_ids,
    combine,
    out_cot,
    inward_master,
    outward_master,
    up_master,
    down_master,
    norm_gains,
    norm_biases,
    inward_moment,
    outward_moment,
    up_moment,
    down_moment,
    first_moment,
    second_moment,
    step_count,
):
    dp_count = lax.axis_size("dp")
    expert_count = lax.axis_size("expert")
    tensor_count = lax.axis_size("tensor")
    token_rows = tokens_in.shape[0]
    expert_total = EXP_DEV * expert_count
    capacity = (token_rows * 10 // (4 * expert_total) + 7) // 8 * 8
    slot_total = expert_total * capacity
    inputs = tokens_in.astype(jnp.float32)
    w_inward, w_outward, w_up, w_down = (
        lax.all_gather(inward_master.astype(jnp.bfloat16), "dp", axis=0, tiled=True),
        lax.all_gather(outward_master.astype(jnp.bfloat16), "dp", axis=0, tiled=True),
        lax.all_gather(up_master.astype(jnp.bfloat16), "dp", axis=0, tiled=True),
        lax.all_gather(down_master.astype(jnp.bfloat16), "dp", axis=0, tiled=True),
    )
    expert_lanes = jnp.arange(expert_total, dtype=jnp.int32)
    route_hits = (expert_ids[:, :, None] == expert_lanes).astype(jnp.int32)
    per_token = jnp.sum(route_hits, axis=1)
    earlier = jnp.cumsum(per_token, axis=0) - per_token
    position = jnp.sum(route_hits * earlier[:, None, :], axis=2)
    target = expert_ids * capacity + position
    select = (target[:, :, None] == jnp.arange(slot_total, dtype=jnp.int32)).astype(jnp.bfloat16)
    normed1, scaled1, invert1 = layer_norm(inputs, norm_gains[0], norm_biases[0])
    normed1_low = normed1.astype(jnp.bfloat16)
    qkv_low = jnp.dot(normed1_low, w_inward, preferred_element_type=jnp.float32).astype(
        jnp.bfloat16
    )
    heads_here = w_inward.shape[1] // (3 * HD)
    images = token_rows // SEQ
    split_heads = qkv_low.reshape(images, SEQ, heads_here, 3, HD)
    query_part = split_heads[:, :, :, 0]
    key_part = split_heads[:, :, :, 1]
    value_part = split_heads[:, :, :, 2]
    score_scale = HD ** (-0.5)
    scores = (
        jnp.einsum("bihd,bjhd->bhij", query_part, key_part, preferred_element_type=jnp.float32)
        * score_scale
    )
    row_max = jnp.max(scores, axis=-1, keepdims=True)
    exponent = jnp.exp(scores - row_max)
    row_total = jnp.sum(exponent, axis=-1, keepdims=True)
    softmax_out = exponent / row_total
    softmax_low = softmax_out.astype(jnp.bfloat16)
    heads_out = (
        jnp.einsum("bhij,bjhd->bihd", softmax_low, value_part, preferred_element_type=jnp.float32)
        .astype(jnp.bfloat16)
        .reshape(token_rows, heads_here * HD)
    )
    attend_part = jnp.einsum("tc,dc->td", heads_out, w_outward, preferred_element_type=jnp.float32)
    attended = lax.psum(attend_part, "tensor")
    state = inputs + attended
    normed2, scaled2, invert2 = layer_norm(state, norm_gains[1], norm_biases[1])
    normed2_low = normed2.astype(jnp.bfloat16)
    slots_out = jnp.einsum(
        "tks,td->sd", select, normed2_low, preferred_element_type=jnp.float32
    ).astype(jnp.bfloat16)
    arrived = lax.all_to_all(
        slots_out.reshape(expert_count, EXP_DEV, capacity, D),
        "expert",
        split_axis=0,
        concat_axis=0,
        tiled=True,
    )
    pre_act = jnp.einsum("secd,def->secf", arrived, w_up, preferred_element_type=jnp.float32)
    hidden_low = gelu_exact(pre_act).astype(jnp.bfloat16)
    expert_part = jnp.einsum(
        "secf,def->secd", hidden_low, w_down, preferred_element_type=jnp.float32
    ).astype(jnp.bfloat16)
    returned = lax.all_to_all(expert_part, "expert", split_axis=0, concat_axis=0, tiled=True)
    routed = jnp.einsum(
        "tks,sd->tkd", select, returned.reshape(slot_total, D), preferred_element_type=jnp.float32
    )
    mixed_part = jnp.sum(routed * combine[:, :, None], axis=1)
    mixed_sum = lax.psum(mixed_part, "tensor")
    block_out = (state + mixed_sum).astype(jnp.bfloat16)
    routed_grad = (combine[:, :, None] * out_cot[:, None, :]).astype(jnp.bfloat16)
    slot_grad = jnp.einsum(
        "tks,tkd->sd", select, routed_grad, preferred_element_type=jnp.float32
    ).astype(jnp.bfloat16)
    grad_arrived = lax.all_to_all(
        slot_grad.reshape(expert_count, EXP_DEV, capacity, D),
        "expert",
        split_axis=0,
        concat_axis=0,
        tiled=True,
    )
    hidden_grad = jnp.einsum(
        "secd,def->secf", grad_arrived, w_down, preferred_element_type=jnp.float32
    )
    pre_grad = (hidden_grad * gelu_slope(pre_act)).astype(jnp.bfloat16)
    down_local = jnp.einsum(
        "secd,secf->def", grad_arrived, hidden_low, preferred_element_type=jnp.float32
    )
    up_local = jnp.einsum("secd,secf->def", arrived, pre_grad, preferred_element_type=jnp.float32)
    entry_grad = jnp.einsum(
        "secf,def->secd", pre_grad, w_up, preferred_element_type=jnp.float32
    ).astype(jnp.bfloat16)
    entry_back = lax.all_to_all(entry_grad, "expert", split_axis=0, concat_axis=0, tiled=True)
    normed2_part = jnp.einsum(
        "tks,sd->td", select, entry_back.reshape(slot_total, D), preferred_element_type=jnp.float32
    )
    normed2_grad = lax.psum(normed2_part, "tensor")
    state_grad = out_cot + norm_backward(normed2_grad, scaled2, invert2, norm_gains[1])
    state_low = state_grad.astype(jnp.bfloat16)
    outward_local = jnp.einsum(
        "td,tc->dc", state_low, heads_out, preferred_element_type=jnp.float32
    )
    heads_grad = (
        jnp.dot(state_low, w_outward, preferred_element_type=jnp.float32)
        .astype(jnp.bfloat16)
        .reshape(images, SEQ, heads_here, HD)
    )
    prob_grad = jnp.einsum(
        "bihd,bjhd->bhij", heads_grad, value_part, preferred_element_type=jnp.float32
    )
    score_grad = (
        softmax_out * (prob_grad - jnp.sum(softmax_out * prob_grad, axis=-1, keepdims=True))
    ).astype(jnp.bfloat16)
    query_grad = (
        jnp.einsum("bhij,bjhd->bihd", score_grad, key_part, preferred_element_type=jnp.float32)
        * score_scale
    )
    key_grad = (
        jnp.einsum("bhij,bihd->bjhd", score_grad, query_part, preferred_element_type=jnp.float32)
        * score_scale
    )
    value_grad = jnp.einsum(
        "bhij,bihd->bjhd", softmax_low, heads_grad, preferred_element_type=jnp.float32
    )
    qkv_grad = (
        jnp.stack([query_grad, key_grad, value_grad], axis=3)
        .reshape(token_rows, heads_here * 3 * HD)
        .astype(jnp.bfloat16)
    )
    inward_local = jnp.einsum(
        "td,tc->dc", normed1_low, qkv_grad, preferred_element_type=jnp.float32
    )
    normed1_part = jnp.einsum("tc,dc->td", qkv_grad, w_inward, preferred_element_type=jnp.float32)
    normed1_grad = lax.psum(normed1_part, "tensor")
    input_gradient = state_grad + norm_backward(normed1_grad, scaled1, invert1, norm_gains[0])
    norm_terms = jnp.stack(
        [
            jnp.sum(normed1_grad * scaled1, axis=0),
            jnp.sum(normed2_grad * scaled2, axis=0),
            jnp.sum(normed1_grad, axis=0),
            jnp.sum(normed2_grad, axis=0),
        ]
    )
    inward_total, outward_total, norm_total = lax.psum(
        (inward_local, outward_local, norm_terms), ("dp", "expert")
    )
    up_gradient, down_gradient = (
        lax.psum_scatter(up_local, "dp", scatter_dimension=0, tiled=True),
        lax.psum_scatter(down_local, "dp", scatter_dimension=0, tiled=True),
    )
    shard_rows = D // dp_count
    dp_here = lax.axis_index("dp")
    inward_gradient = lax.dynamic_slice_in_dim(inward_total, dp_here * shard_rows, shard_rows, 0)
    outward_gradient = lax.dynamic_slice_in_dim(outward_total, dp_here * shard_rows, shard_rows, 0)
    inward_next = 0.95 * inward_moment + inward_gradient
    outward_next = 0.95 * outward_moment + outward_gradient
    up_next = 0.95 * up_moment + up_gradient
    down_next = 0.95 * down_moment + down_gradient
    matrices = [up_next[:, expert_slot] for expert_slot in range(EXP_DEV)]
    matrices = matrices + [down_next[:, expert_slot] for expert_slot in range(EXP_DEV)]
    matrices = matrices + [jnp.concatenate([inward_next, outward_next], axis=1)]
    stacked = jnp.stack(matrices)
    slot_count = len(matrices)
    group_size = dp_count * tensor_count
    shard_width = stacked.shape[2]
    query_cols = inward_next.shape[1]

    def orth_expert(pieces):
        whole_matrix = pieces.transpose(0, 2, 1, 3).reshape(D, tensor_count * shard_width)
        result = newton_schulz(whole_matrix) * (0.2 * math.sqrt(F))
        return result.reshape(dp_count, shard_rows, tensor_count, shard_width).transpose(0, 2, 1, 3)

    def orth_attention(pieces):
        inward_whole = (
            pieces[..., :query_cols].transpose(0, 2, 1, 3).reshape(D, tensor_count * query_cols)
        )
        outward_whole = (
            pieces[..., query_cols:]
            .transpose(0, 2, 1, 3)
            .reshape(D, tensor_count * (shard_width - query_cols))
        )
        inward_result = newton_schulz(inward_whole) * (0.2 * math.sqrt(3 * D))
        outward_result = newton_schulz(outward_whole) * (0.2 * math.sqrt(D))
        inward_blocks = inward_result.reshape(
            dp_count, shard_rows, tensor_count, query_cols
        ).transpose(0, 2, 1, 3)
        outward_blocks = outward_result.reshape(
            dp_count, shard_rows, tensor_count, shard_width - query_cols
        ).transpose(0, 2, 1, 3)
        return jnp.concatenate([inward_blocks, outward_blocks], axis=3)

    owner_index = lax.axis_index(("dp", "tensor"))
    outgoing = stacked[np.arange(group_size) % slot_count]
    received = lax.all_to_all(outgoing, ("dp", "tensor"), split_axis=0, concat_axis=0, tiled=True)
    blocks = received.reshape(dp_count, tensor_count, shard_rows, shard_width)
    slot_here = owner_index % slot_count
    result_blocks = lax.cond(slot_here == slot_count - 1, orth_attention, orth_expert, blocks)
    arrived_steps = lax.all_to_all(
        result_blocks.reshape(group_size, shard_rows, shard_width),
        ("dp", "tensor"),
        split_axis=0,
        concat_axis=0,
        tiled=True,
    )
    picked = []
    for owned_slot in range(slot_count):
        replicas = (group_size - owned_slot + slot_count - 1) // slot_count
        source = owned_slot + slot_count * (owner_index % replicas)
        picked.append(lax.dynamic_index_in_dim(arrived_steps, source, 0, keepdims=False))
    up_step = jnp.stack(picked[0:EXP_DEV], axis=1)
    down_step = jnp.stack(picked[EXP_DEV : 2 * EXP_DEV], axis=1)
    attend_step = picked[2 * EXP_DEV]
    inward_new = inward_master - 0.1 * (attend_step[:, :query_cols] + 0.1 * inward_master)
    outward_new = outward_master - 0.1 * (attend_step[:, query_cols:] + 0.1 * outward_master)
    up_new = up_master - 0.1 * (up_step + 0.1 * up_master)
    down_new = down_master - 0.1 * (down_step + 0.1 * down_master)
    moment_first = 0.9 * first_moment + 0.1 * norm_total
    moment_second = 0.999 * second_moment + 0.001 * norm_total * norm_total
    steps_done = step_count[0].astype(jnp.float32)
    direction = (
        moment_first
        / (1.0 - jnp.power(0.9, steps_done))
        / (jnp.sqrt(moment_second / (1.0 - jnp.power(0.999, steps_done))) + 1e-08)
    )
    params_new = jnp.concatenate([norm_gains, norm_biases], axis=0) - 0.1 * direction
    return (
        block_out,
        input_gradient,
        inward_gradient,
        outward_gradient,
        up_gradient,
        down_gradient,
        norm_total[0:2],
        norm_total[2:4],
        inward_next,
        outward_next,
        up_next,
        down_next,
        inward_new,
        outward_new,
        up_new,
        down_new,
        inward_new.astype(jnp.bfloat16),
        outward_new.astype(jnp.bfloat16),
        up_new.astype(jnp.bfloat16),
        down_new.astype(jnp.bfloat16),
        params_new[0:2],
        params_new[2:4],
        moment_first,
        moment_second,
    )


PAIRS = (1, 2, 3)
FAR_FIRST = (3, 2, 1, 0)
MIDWAY = 1
LANES = 128
NOWHERE = 128 * 128 - 1
PAD = 208
NT = (((1,), (1,)), ((), ()))
TN = (((0,), (0,)), ((), ()))


def mxu(left, right, dims=(((1,), (0,)), ((), ()))):
    return lax.dot_general(left, right, dims, preferred_element_type=jnp.float32)


def spread_rows(value, padded_ref):
    padded_ref[...] = jnp.zeros_like(padded_ref)
    for image in range(value.shape[0] // SEQ):
        padded_ref[image * PAD : image * PAD + SEQ, :] = value[image * SEQ : (image + 1) * SEQ]


def gather_rows(padded, out_ref):
    for image in range(out_ref.shape[0] // SEQ):
        out_ref[image * SEQ : (image + 1) * SEQ, :] = padded[
            image * PAD : image * PAD + SEQ
        ].astype(out_ref.dtype)


def peer(me, k):
    return (me + k) % 2 + 2 * ((me // 2 + k // 2) % 2)


def remote(source, target, send, recv, device):
    copy = pltpu.make_async_remote_copy(
        src_ref=source,
        dst_ref=target,
        send_sem=send,
        recv_sem=recv,
        device_id=device,
        device_id_type=pl.DeviceIdType.MESH,
    )
    copy.start()
    return copy


class Copy:
    def __init__(self, parts, start=True):
        self.parts = parts
        if start:
            self.make().start()

    def make(self):
        source, target, send, recv, device = self.parts()
        return pltpu.make_async_remote_copy(
            src_ref=source,
            dst_ref=target,
            send_sem=send,
            recv_sem=recv,
            device_id=device,
            device_id_type=pl.DeviceIdType.MESH,
        )

    def wait_recv(self):
        self.make().wait_recv()

    def wait_send(self):
        self.make().wait_send()


def keep(source, target, sem):
    copy = pltpu.make_async_copy(source, target, sem)
    copy.start()
    return copy


def greet(dp_here, expert_here, core, over_expert=True):
    barrier = pltpu.get_barrier_semaphore()
    devices = [{"dp": peer(dp_here, k)} for k in PAIRS] + [{"tensor": 1 - core}]
    if over_expert:
        devices += [{"expert": peer(expert_here, k)} for k in PAIRS]
    for device in devices:
        pl.semaphore_signal(
            barrier, inc=1, device_id=device, device_id_type=pl.DeviceIdType.MESH
        )
    return lambda: pl.semaphore_wait(barrier, len(devices))


def block_rows(index, size):
    return pl.ds(pl.multiple_of(index * size, size), size)


def one_hot(cond):
    return jnp.where(cond, 1.0, 0.0).astype(jnp.bfloat16)


def route(ids, capacity, target_ref, target_t_ref):
    rows = ids.shape[0]
    square = (PAD, PAD)
    below = one_hot(
        lax.broadcasted_iota(jnp.int32, square, 0) > lax.broadcasted_iota(jnp.int32, square, 1)
    )
    lane = lax.broadcasted_iota(jnp.int32, (rows, 128), 1)
    hits = one_hot((lane == ids[:, 0:1]) | (lane == ids[:, 1:2]))
    earlier, passed = [], jnp.zeros((1, 128), jnp.float32)
    for image in range(rows // PAD):
        own = hits[image * PAD : (image + 1) * PAD]
        earlier.append(mxu(below, own) + passed)
        passed += jnp.sum(own.astype(jnp.float32), axis=0, keepdims=True)
    earlier = jnp.concatenate(earlier, axis=0)
    target = jnp.zeros((rows, 128), jnp.int32)
    parts = jnp.zeros((rows, 128), jnp.int32)
    for r in range(2):
        own = ids[:, r : r + 1]
        position = jnp.sum(jnp.where(lane == own, earlier, 0.0), axis=1, keepdims=True)
        value = jnp.where(own >= 0, own * capacity + position.astype(jnp.int32), NOWHERE)
        target = jnp.where(lane == r, value, target)
        parts = jnp.where(lane == 2 * r, value // 128, jnp.where(lane == 2 * r + 1, value % 128, parts))
    target_ref[...] = target
    identity = one_hot(
        lax.broadcasted_iota(jnp.int32, (8, 128), 0) == lax.broadcasted_iota(jnp.int32, (8, 128), 1)
    )
    flipped = mxu(identity, parts.astype(jnp.float32).astype(jnp.bfloat16), NT).astype(jnp.int32)
    for r in range(2):
        target_t_ref[r : r + 1, :] = flipped[2 * r : 2 * r + 1] * 128 + flipped[2 * r + 1 : 2 * r + 2]


def attend(qkv_ref, probs_ref, gift_ref):
    heads_here = qkv_ref.shape[1] // (3 * HD)
    key_lane = lax.broadcasted_iota(jnp.int32, (PAD, PAD), 1)

    def one_image(image, carry):
        rows = block_rows(image, PAD)
        out_rows = pl.ds(pl.multiple_of(D + image * PAD, 16), PAD)
        for head in range(heads_here):
            base = head * 3 * HD
            query = qkv_ref[rows, base : base + HD]
            key = qkv_ref[rows, base + HD : base + 2 * HD]
            value = qkv_ref[rows, base + 2 * HD : base + 3 * HD]
            scores = jnp.where(key_lane < SEQ, mxu(query, key, NT) * HD ** (-0.5), -1e30)
            exponent = jnp.exp(scores - jnp.max(scores, axis=-1, keepdims=True))
            probs = exponent / jnp.sum(exponent, axis=-1, keepdims=True)
            probs_ref[image * heads_here + head] = probs
            gift_ref[out_rows, head * HD : (head + 1) * HD] = mxu(
                probs.astype(jnp.bfloat16), value
            ).astype(jnp.bfloat16)
        return carry

    lax.fori_loop(0, qkv_ref.shape[0] // PAD, one_image, 0)


def woven(array):
    rows, count, width = array.shape
    tiles = array.reshape(rows, count, width // LANES, LANES)
    return tiles.transpose(0, 2, 1, 3).reshape(-1, LANES)


def unwoven(array, whole):
    rows, count, width = whole
    tiles = array.reshape(rows, width // LANES, count, LANES)
    return tiles.transpose(0, 2, 1, 3).reshape(whole)


def strand(tile, expert, rows, width):
    step = EXP_DEV * (width // LANES)
    return pl.ds(EXP_DEV * tile + expert, rows, stride=step)


def front_kernel(
    ids_ref,
    combine_ref,
    cot_ref,
    tokens_ref,
    gains_ref,
    biases_ref,
    inward_ref,
    outward_ref,
    up_ref,
    down_ref,
    up_moment_ref,
    down_moment_ref,
    state_ref,
    gift_ref,
    qkv_ref,
    probs_ref,
    weight_ref,
    target_ref,
    combine_out_ref,
    moment_shard,
    expert_w_ref,
    arrived_ref,
    grad_arrived_ref,
    padded,
    columns,
    columns_padded,
    raw,
    target_t_ref,
    attend_shard,
    expert_shard,
    gift_other_ref,
    grad_chunks,
    token_chunks,
    inner_send,
    inner_recv,
    expert_send,
    expert_recv,
    slot_send,
    slot_recv,
    share_send,
    share_recv,
    gift_sems,
    keep_sems,
    raw_sems,
):
    bf16 = jnp.bfloat16
    dp_here, expert_here, core = (lax.axis_index(a) for a in ("dp", "expert", "tensor"))
    partner = {"tensor": 1 - core}
    capacity = grad_chunks.shape[1]
    shard_rows = attend_shard.shape[0]
    qcols = qkv_ref.shape[1]
    width = attend_shard.shape[1]
    here = block_rows(dp_here, shard_rows)
    ready = greet(dp_here, expert_here, core)
    loads = [
        keep(ref, raw.at[place], raw_sems.at[place])
        for place, ref in enumerate((up_ref, down_ref, up_moment_ref, down_moment_ref))
    ]

    def unpick(place, tile, expert):
        return raw[place, strand(tile, expert, shard_rows, width), :].astype(bf16)

    attend_shard[:, :qcols] = inward_ref[...].astype(bf16)
    attend_shard[:, qcols:] = outward_ref[...].astype(bf16)
    weight_ref[here, :] = attend_shard[...]
    ready()
    inner = [
        remote(
            attend_shard,
            weight_ref.at[here, :],
            inner_send.at[k - 1],
            inner_recv.at[k - 1],
            {"dp": peer(dp_here, k)},
        )
        for k in PAIRS
    ]
    kept = []

    rest = combine_ref[...]
    for part in range(3):
        piece = rest.astype(bf16).astype(jnp.float32)
        columns[2 * part : 2 * part + 2, :] = piece
        rest = rest - piece
    columns[6:8, :] = (ids_ref[...] + 1).astype(jnp.float32)
    identity = one_hot(
        lax.broadcasted_iota(jnp.int32, (8, 128), 0) == lax.broadcasted_iota(jnp.int32, (8, 128), 1)
    )
    spread_rows(mxu(columns[...].astype(bf16), identity, TN), columns_padded)
    for r in range(2):
        combine_out_ref[:, r : r + 1] = (
            columns_padded[:, r : r + 1]
            + columns_padded[:, 2 + r : 3 + r]
            + columns_padded[:, 4 + r : 5 + r]
        )
    ids = columns_padded[...].astype(jnp.int32) - 1
    route(ids[:, 6:8], capacity, target_ref, target_t_ref)
    spread_rows(cot_ref[...], padded)
    slot = lax.broadcasted_iota(jnp.int32, (capacity, padded.shape[0]), 0)

    def first_slot(k):
        return (2 * peer(expert_here, k) + core) * capacity

    def send_chunks(fill, chunks, landing, which):
        def going(k, start=True):
            return Copy(
                lambda: (
                    chunks.at[k],
                    landing.at[0, k],
                    slot_send.at[which, k],
                    slot_recv.at[which, k],
                    {"expert": peer(expert_here, k)},
                ),
                start,
            )

        def make(k):
            chunks[k] = fill(slot + first_slot(k)).astype(bf16)

        def make_and_send(step, carry):
            make(3 - step)

            @pl.when(step > 0)
            def send_last():
                going(4 - step)

            return carry

        lax.fori_loop(0, 4, make_and_send, 0)
        copies, shared = {k: going(k, start=False) for k in PAIRS}, []
        kept.append(keep(chunks.at[0], landing.at[0, 0], keep_sems.at[1 + which]))
        shared.append(
            remote(
                chunks.at[0],
                landing.at[1, 0],
                share_send.at[which, 0],
                share_recv.at[which, 0],
                partner,
            )
        )
        return copies, shared

    def share_arrivals(copies, landing, which, shared):
        for k in FAR_FIRST[:3]:
            copies[k].wait_recv()
            shared.append(
                remote(
                    landing.at[0, k],
                    landing.at[1, k],
                    share_send.at[which, k],
                    share_recv.at[which, k],
                    partner,
                )
            )

    grads = [(combine_out_ref[:, r : r + 1] * padded[...]).astype(bf16) for r in range(2)]
    grad_copies, grad_shared = send_chunks(
        lambda slots: sum(mxu(one_hot(target_t_ref[r : r + 1] == slots), grads[r]) for r in range(2)),
        grad_chunks,
        grad_arrived_ref,
        0,
    )
    for which in range(2):
        loads[which].wait()
        for tile in range(width // LANES):
            pair = [unpick(which, tile, e) for e in range(EXP_DEV)]
            lanes = slice(tile * LANES, (tile + 1) * LANES)
            for j in range(EXP_DEV):
                expert_shard[EXP_DEV * which + j, :, lanes] = jnp.where(
                    core == 0, pair[j], pair[1 - j]
                )
    spread_rows(tokens_ref[...].astype(jnp.float32), padded)
    normed, unused, unused = layer_norm(padded[...], gains_ref[0:1], biases_ref[0:1])
    normed_low = normed.astype(bf16)
    weights = [
        remote(
            expert_shard,
            expert_w_ref.at[:, here, :],
            expert_send.at[k - 1],
            expert_recv.at[k - 1],
            {"dp": peer(dp_here, k)},
        )
        for k in (1, 2)
    ]
    kept.append(keep(expert_shard, expert_w_ref.at[:, here, :], keep_sems.at[0]))
    for which in range(2):
        loads[2 + which].wait()
        for tile in range(width // LANES):
            for e in range(EXP_DEV):
                moment_shard[EXP_DEV * which + e, :, tile * LANES : (tile + 1) * LANES] = unpick(
                    2 + which, tile, e
                )
    for copy in inner:
        copy.wait_recv()
    qkv_ref[...] = mxu(normed_low, weight_ref[:, :qcols]).astype(bf16)
    gift_ref[0:D, :] = weight_ref[:, qcols:]
    attend(qkv_ref, probs_ref, gift_ref)
    gift = remote(gift_ref, gift_other_ref, gift_sems.at[0], gift_sems.at[1], partner)
    half = padded[...] + mxu(gift_ref[D:, :], gift_ref[0:D, :], NT)
    gift.wait()
    state = half + mxu(gift_other_ref[D:, :], gift_other_ref[0:D, :], NT)
    state_ref[...] = state
    normed, unused, unused = layer_norm(state, gains_ref[1:2], biases_ref[1:2])
    normed_low = normed.astype(bf16)
    token_copies, token_shared = send_chunks(
        lambda slots: mxu(
            one_hot((target_t_ref[0:1] == slots) | (target_t_ref[1:2] == slots)), normed_low
        ),
        token_chunks,
        arrived_ref,
        1,
    )
    for copy in weights:
        copy.wait_recv()
    for k, part in ((1, slice(0, EXP_DEV)), (2, slice(EXP_DEV, 2 * EXP_DEV))):
        block = expert_w_ref.at[part, block_rows(peer(dp_here, k), shard_rows), :]
        weights.append(
            remote(
                block,
                block,
                expert_send.at[k + 1],
                expert_recv.at[k + 1],
                {"dp": peer(dp_here, 3 - k)},
            )
        )
    share_arrivals(grad_copies, grad_arrived_ref, 0, grad_shared)
    share_arrivals(token_copies, arrived_ref, 1, token_shared)
    for copy in grad_shared + token_shared + weights[2:]:
        copy.wait()
    for copy in weights[:2] + inner:
        copy.wait_send()
    for copies in (grad_copies, token_copies):
        for k in PAIRS:
            copies[k].wait_send()
    for copy in kept:
        copy.wait()


def back_kernel(
    combine_ref,
    target_ref,
    gains_ref,
    biases_ref,
    inward_moment_ref,
    outward_moment_ref,
    cot_hbm,
    tokens_hbm,
    state_hbm,
    gift_hbm,
    qkv_hbm,
    probs_hbm,
    weight_hbm,
    expert_w_hbm,
    arrived_hbm,
    grad_arrived_hbm,
    moment_hbm,
    input_ref,
    block_ref,
    norm_ref,
    attend_grad_ref,
    attend_whole_ref,
    own_steps_ref,
    home_grads_ref,
    give,
    handed,
    summed,
    returned,
    matrices,
    near_in,
    far_out,
    far_in,
    moment_whole,
    owned_low,
    normed_part,
    normed_other,
    inner,
    inner_in,
    plane,
    quarter_in,
    quarter,
    plane_total,
    whole_own,
    norm_own,
    norm_in,
    gram,
    gram_other,
    hand_send,
    hand_recv,
    slot_send,
    slot_recv,
    share_send,
    share_recv,
    pair_send,
    pair_recv,
    dp_send,
    dp_recv,
    expert_send,
    expert_recv,
    near_send,
    near_recv,
    far_send,
    far_recv,
    own_sems,
    load_sems,
):
    bf16, f32 = jnp.bfloat16, jnp.float32
    dp_here, expert_here, core = (lax.axis_index(a) for a in ("dp", "expert", "tensor"))
    partner = {"tensor": 1 - core}
    capacity = give.shape[2]
    shard_rows = inner.shape[1]
    here = block_rows(dp_here, shard_rows)
    ready = greet(dp_here, expert_here, core)
    sent = []

    def to_dp(stage, sources, targets, peers=PAIRS):
        def copy(k):
            return Copy(
                lambda: (
                    sources(k),
                    targets(k),
                    dp_send.at[stage, k - 1],
                    dp_recv.at[stage, k - 1],
                    {"dp": peer(dp_here, k)},
                )
            )

        copies = [copy(k) for k in peers]
        sent.extend(copies)
        return copies

    def to_expert(stage, sources, targets):
        def copy(k):
            return Copy(
                lambda: (
                    sources(k),
                    targets(k),
                    expert_send.at[stage, k - 1],
                    expert_recv.at[stage, k - 1],
                    {"expert": peer(expert_here, k)},
                )
            )

        copies = [copy(k) for k in PAIRS]
        sent.extend(copies)
        return copies

    def arrive(copies):
        for copy in copies:
            copy.wait_recv()

    shares = ([], [])

    def hand(which, k, start=True):
        return Copy(
            lambda: (
                give.at[which, k],
                handed.at[which, k],
                hand_send.at[which, k],
                hand_recv.at[which, k],
                partner,
            ),
            start,
        )

    def add_up(which, k):
        hand(which, k, start=False).wait_recv()
        total = (summed[which, k].astype(f32) + handed[which, k].astype(f32)).astype(bf16)
        summed[which, k] = total

    def send_home(which, k, start=True):
        return Copy(
            lambda: (
                summed.at[which, k],
                returned.at[which, 0, k],
                slot_send.at[which, k],
                slot_recv.at[which, k],
                {"expert": peer(expert_here, k)},
            ),
            start,
        )

    def stay_home(which):
        returned[which, 0, 0] = summed[which, 0]
        shares[which].append(
            Copy(
                lambda: (
                    summed.at[which, 0],
                    returned.at[which, 1, 0],
                    share_send.at[which, 0],
                    share_recv.at[which, 0],
                    partner,
                )
            )
        )

    def share(which):
        def copy(k):
            return Copy(
                lambda: (
                    returned.at[which, 0, k],
                    returned.at[which, 1, k],
                    share_send.at[which, k],
                    share_recv.at[which, k],
                    partner,
                )
            )

        for k in FAR_FIRST[:3]:
            send_home(which, k, start=False).wait_recv()
            shares[which].append(copy(k))
        sent.extend(shares[which])
        arrive(shares[which])

    def held(index):
        return 2 * (index // 2) + (index % 2 + core) % 2

    ways = ((slice(0, D // 2), 1, 2), (slice(D // 2, D), 2, 1))

    def near_copy(half, place):
        rows, first, second = ways[half]
        owner = (first, 3)[place]
        return Copy(
            lambda: (
                matrices.at[held(peer(dp_here, owner)), rows, :],
                near_in.at[half, place],
                near_send.at[half, place],
                near_recv.at[half, place],
                {"dp": peer(dp_here, first)},
            )
        )

    def far_copy(half):
        rows, first, second = ways[half]
        return Copy(
            lambda: (
                far_out.at[half],
                far_in.at[half],
                far_send.at[half],
                far_recv.at[half],
                {"dp": peer(dp_here, second)},
            )
        )

    def pass_on(near):
        arrive(near)
        for half, (rows, first, second) in enumerate(ways):
            far_out[half] = (
                matrices[held(peer(dp_here, second)), rows, :].astype(f32)
                + near_in[half, 1].astype(f32)
            ).astype(bf16)
        far = [far_copy(half) for half in range(2)]
        sent.extend(far)
        return far

    def experts(weights, rows, grads, hidden, pre_grad):
        loads = {}
        for j in (1, 0):
            for place, (source, target) in enumerate(
                (
                    (expert_w_hbm.at[j], weights.at[j]),
                    (arrived_hbm.at[j], rows.at[j]),
                    (expert_w_hbm.at[EXP_DEV + j], weights.at[EXP_DEV + j]),
                    (grad_arrived_hbm.at[j], grads.at[j]),
                )
            ):
                loads[j, place] = keep(source, target, load_sems.at[4 * j + place])
        ready()
        for load in loads.values():
            load.wait()
        moments.extend(
            to_dp(0, lambda k: moment_hbm.at[peer(dp_here, k)], lambda k: moment_whole.at[here, :])
        )

        def chunk(k):
            for j in (1, 0):
                pre = mxu(rows[j, k], weights[j])
                share_of_one = 0.5 * (1.0 + lax.erf(pre * 0.7071067811865476))
                hidden[j, k] = (pre * share_of_one).astype(bf16)
                slope = share_of_one + pre * 0.3989422804014327 * jnp.exp(-0.5 * pre * pre)
                grad = (mxu(grads[j, k], weights[EXP_DEV + j]) * slope).astype(bf16)
                pre_grad[j, k] = grad
                entry = mxu(grad, weights[j], NT).astype(bf16)
                if j == 1:
                    give[0, k] = entry
                else:
                    summed[0, k] = entry

        def next_chunk(step, carry):
            chunk(3 - step)
            hand(0, 3 - step)

            @pl.when(step > 0)
            def last_chunk():
                add_up(0, 4 - step)
                send_home(0, 4 - step)

            return carry

        lax.fori_loop(0, 4, next_chunk, 0)

        def matrix(left, right, j):
            total = mxu(left[j, 0], right[j, 0], TN)
            for k in PAIRS:
                total += mxu(left[j, k], right[j, k], TN)
            return total.astype(bf16)

        def expert_matrices(j, carry):
            matrices[j] = matrix(rows, pre_grad, j)
            matrices[EXP_DEV + j] = matrix(grads, hidden, j)
            return carry

        lax.fori_loop(0, EXP_DEV, expert_matrices, 0)
        near = [near_copy(half, place) for place in (1, 0) for half in range(2)]
        sent.extend(near)
        add_up(0, 0)
        stay_home(0)

        def part_chunk(step, carry):
            k = 3 - step
            give[1, k] = mxu(hidden[1, k], weights[EXP_DEV + 1], NT).astype(bf16)
            summed[1, k] = mxu(hidden[0, k], weights[EXP_DEV], NT).astype(bf16)
            hand(1, k)
            return carry

        lax.fori_loop(0, 4, part_chunk, 0)
        for k in FAR_FIRST:
            add_up(1, k)
        for k in FAR_FIRST[:3]:
            send_home(1, k)
        stay_home(1)
        for which in range(2):
            sent.extend(hand(which, k, start=False) for k in range(4))
            sent.extend(send_home(which, k, start=False) for k in PAIRS)
        return near

    own_moment = keep(moment_hbm.at[dp_here], moment_whole.at[here, :], own_sems.at[0])
    near, moments = [], []
    slots = (EXP_DEV, 4, capacity)
    pl.run_scoped(
        lambda *refs: near.extend(experts(*refs)),
        pltpu.VMEM(expert_w_hbm.shape, bf16),
        pltpu.VMEM(slots + (D,), bf16),
        pltpu.VMEM(slots + (D,), bf16),
        pltpu.VMEM(slots + (expert_w_hbm.shape[2],), bf16),
        pltpu.VMEM(slots + (expert_w_hbm.shape[2],), bf16),
    )

    def backward(
        cot_ref,
        tokens_ref,
        state_ref,
        gift_ref,
        qkv_ref,
        probs_ref,
        weight_ref,
        padded,
        qkv_grad_ref,
        local_ref,
        out_grad_ref,
    ):
        loads = [
            keep(source, target, load_sems.at[place])
            for place, (source, target) in enumerate(
                (
                    (state_hbm, state_ref),
                    (cot_hbm, cot_ref),
                    (gift_hbm.at[D:, :], gift_ref),
                    (weight_hbm, weight_ref),
                    (qkv_hbm, qkv_ref),
                    (probs_hbm, probs_ref),
                    (tokens_hbm, tokens_ref),
                )
            )
        ]
        qcols = qkv_ref.shape[1]
        rows_all = state_ref.shape[0]
        loads[0].wait()
        unused, scaled2, invert2 = layer_norm(state_ref[...], gains_ref[1:2], biases_ref[1:2])
        loads[1].wait()
        spread_rows(cot_ref[...], padded)
        def pick_all(which, columns, rows):
            slot = lax.broadcasted_iota(jnp.int32, (PAD, capacity), 1)

            def picks(k, j):
                first = slot + (2 * peer(expert_here, k) + (core + j) % 2) * capacity
                hit = target_ref[rows, columns[0] : columns[0] + 1] == first
                for column in columns[1:]:
                    hit = hit | (target_ref[rows, column : column + 1] == first)
                return one_hot(hit)

            total = mxu(picks(0, 0), returned[which, 0, 0])
            for j in range(2):
                for k in FAR_FIRST:
                    if k + j > 0:
                        total += mxu(picks(k, j), returned[which, j, k])
            return total

        share(0)

        def one_gradient(image, carry):
            rows = block_rows(image, PAD)
            normed_part[rows, :] = pick_all(0, (0, 1), rows)
            return carry

        lax.fori_loop(0, rows_all // PAD, one_gradient, 0)
        normed2_grad = normed_part[...]
        norm_own[0, 4:8] = jnp.zeros((4, D), f32)
        norm_own[0, 1:2] = jnp.sum(normed2_grad * scaled2, axis=0, keepdims=True)
        norm_own[0, 3:4] = jnp.sum(normed2_grad, axis=0, keepdims=True)
        state_grad = padded[...] + norm_backward(normed2_grad, scaled2, invert2, gains_ref[1:2])
        padded[...] = state_grad
        state_low = state_grad.astype(bf16)
        for copy in loads[2:]:
            copy.wait()

        local_ref[:, qcols:] = mxu(state_low, gift_ref[...], TN)
        out_grad_ref[...] = mxu(state_low, weight_ref[:, qcols:]).astype(bf16)
        heads_here = qcols // (3 * HD)
        scale = HD ** (-0.5)

        def one_image(image, carry):
            rows = block_rows(image, PAD)
            for head in range(heads_here):
                base = head * 3 * HD
                query = qkv_ref[rows, base : base + HD]
                key = qkv_ref[rows, base + HD : base + 2 * HD]
                value = qkv_ref[rows, base + 2 * HD : base + 3 * HD]
                out_grad = out_grad_ref[rows, head * HD : (head + 1) * HD]
                probs = probs_ref[image * heads_here + head]
                prob_grad = mxu(out_grad, value, NT)
                score_grad = (
                    probs * (prob_grad - jnp.sum(probs * prob_grad, axis=-1, keepdims=True))
                ).astype(bf16)
                qkv_grad_ref[rows, base : base + HD] = (mxu(score_grad, key) * scale).astype(bf16)
                qkv_grad_ref[rows, base + HD : base + 2 * HD] = (
                    mxu(score_grad, query, TN) * scale
                ).astype(bf16)
                qkv_grad_ref[rows, base + 2 * HD : base + 3 * HD] = mxu(
                    probs.astype(bf16), out_grad, TN
                ).astype(bf16)
            return carry

        lax.fori_loop(0, rows_all // PAD, one_image, 0)
        spread_rows(tokens_ref[...].astype(f32), normed_part)
        normed1, scaled1, invert1 = layer_norm(normed_part[...], gains_ref[0:1], biases_ref[0:1])
        local_ref[:, :qcols] = mxu(normed1.astype(bf16), qkv_grad_ref[...], TN)
        for k in range(4):
            inner[k] = local_ref[block_rows(peer(dp_here, k), shard_rows), :].astype(bf16)
        normed_part[...] = mxu(qkv_grad_ref[...], weight_ref[:, :qcols], NT)
        rows_sums = to_dp(1, lambda k: inner.at[k], lambda k: inner_in.at[k - 1])
        pair = Copy(
            lambda: (normed_part, normed_other, pair_send.at[0], pair_recv.at[0], partner)
        )
        sent.append(pair)
        far = pass_on(near)

        share(1)

        def one_output(image, carry):
            rows = block_rows(image, PAD)
            total = state_ref[rows, :]
            for r in range(2):
                total += combine_ref[rows, r : r + 1] * pick_all(1, (r,), rows)
            state_ref[rows, :] = total
            return carry

        lax.fori_loop(0, rows_all // PAD, one_output, 0)
        gather_rows(state_ref[...], block_ref)

        pair.wait_recv()
        normed1_grad = normed_part[...] + normed_other[...]
        norm_own[0, 0:1] = jnp.sum(normed1_grad * scaled1, axis=0, keepdims=True)
        norm_own[0, 2:3] = jnp.sum(normed1_grad, axis=0, keepdims=True)
        norm_in[0, dp_here] = norm_own[0]
        norms = to_dp(2, lambda k: norm_own.at[0], lambda k: norm_in.at[0, dp_here])
        gather_rows(
            padded[...] + norm_backward(normed1_grad, scaled1, invert1, gains_ref[0:1]), input_ref
        )
        return rows_sums, norms, far

    travelling = []
    rows_f32 = pltpu.VMEM(state_hbm.shape, f32)
    pl.run_scoped(
        lambda *refs: travelling.extend(backward(*refs)),
        pltpu.VMEM(cot_hbm.shape, f32),
        pltpu.VMEM(tokens_hbm.shape, bf16),
        rows_f32,
        pltpu.VMEM((gift_hbm.shape[0] - D, gift_hbm.shape[1]), bf16),
        pltpu.VMEM(qkv_hbm.shape, bf16),
        pltpu.VMEM(probs_hbm.shape, f32),
        pltpu.VMEM(weight_hbm.shape, bf16),
        rows_f32,
        pltpu.VMEM(qkv_hbm.shape, bf16),
        pltpu.VMEM(weight_hbm.shape, f32),
        pltpu.VMEM((state_hbm.shape[0], gift_hbm.shape[1]), bf16),
    )
    rows_sums, norms, far = travelling

    arrive(rows_sums)
    plane[...] = (
        inner[0].astype(f32)
        + inner_in[0].astype(f32)
        + inner_in[1].astype(f32)
        + inner_in[2].astype(f32)
    ).astype(bf16)
    quarter_rows = quarter.shape[0]
    my_quarter = block_rows(expert_here, quarter_rows)
    quarters = to_expert(
        0,
        lambda k: plane.at[block_rows(peer(expert_here, k), quarter_rows), :],
        lambda k: quarter_in.at[k - 1],
    )
    arrive(norms)
    norm_plane = norm_in[0, 0] + norm_in[0, 1] + norm_in[0, 2] + norm_in[0, 3]
    norm_own[1] = norm_plane
    norm_in[1, expert_here] = norm_plane
    norm_sums = to_expert(1, lambda k: norm_own.at[1], lambda k: norm_in.at[1, expert_here])

    def orthogonalize(owned_next, factor, change):
        arrive(quarters)
        quarter[...] = (
            plane[my_quarter, :].astype(f32)
            + quarter_in[0].astype(f32)
            + quarter_in[1].astype(f32)
            + quarter_in[2].astype(f32)
        ).astype(bf16)
        plane_total[my_quarter, :] = quarter[...]
        totals = to_expert(2, lambda k: quarter, lambda k: plane_total.at[my_quarter, :])
        arrive(far + moments)
        own_moment.wait()
        for half, (rows, first, second) in enumerate(ways):
            owned = (
                matrices[held(dp_here), rows, :].astype(f32)
                + near_in[half, 0].astype(f32)
                + far_in[half].astype(f32)
            )
            owned_low[rows, :] = owned.astype(bf16)
            owned_next[rows, :] = 0.95 * moment_whole[rows, :].astype(f32) + owned
        split = halves(owned_next[...])
        gram[...] = mxu3(split, split, NT)
        pair = remote(gram, gram_other, pair_send.at[1], pair_recv.at[1], partner)

        def send_rows(peers):
            return to_dp(
                3,
                lambda k: owned_low.at[block_rows(peer(dp_here, k), shard_rows), :],
                lambda k: home_grads_ref.at[dp_here],
                peers,
            )

        home = send_rows((1, 2))
        own = keep(owned_low.at[here, :], home_grads_ref.at[dp_here], load_sems.at[1])
        pair.wait()

        def attention_next():
            arrive(totals)
            total = plane_total[...].astype(f32)
            attend_grad_ref[...] = total
            qcols = inward_moment_ref.shape[1]
            whole_own[:, :qcols] = (0.95 * inward_moment_ref[...] + total[:, :qcols]).astype(bf16)
            whole_own[:, qcols:] = (0.95 * outward_moment_ref[...] + total[:, qcols:]).astype(bf16)
            attend_whole_ref[here, :] = whole_own[...]
            wholes.extend(to_dp(4, lambda k: whole_own, lambda k: attend_whole_ref.at[here, :]))
            home.extend(send_rows((3,)))

        wholes = []
        find_factor(gram[...] + gram_other[...], factor, gram, change, gram_other, attention_next)
        own_steps_ref[...] = (
            mxu3(halves(factor[...]), halves(owned_next[...])) * (0.2 * math.sqrt(F))
        ).astype(bf16)
        arrive(norm_sums)
        norm_ref[...] = (
            norm_in[1, 0, 0:4] + norm_in[1, 1, 0:4] + norm_in[1, 2, 0:4] + norm_in[1, 3, 0:4]
        )
        arrive(home)
        arrive(wholes)
        own.wait()

    square = pltpu.VMEM((D, D), f32)
    pl.run_scoped(orthogonalize, pltpu.VMEM(moment_whole.shape, f32), square, square)
    for copy in sent:
        copy.wait_send()


def halves(value):
    high = value.astype(jnp.bfloat16)
    return high, (value - high.astype(jnp.float32)).astype(jnp.bfloat16)


def mxu3(left, right, dims=(((1,), (0,)), ((), ()))):
    return (
        mxu(left[0], right[0], dims) + mxu(left[1], right[0], dims) + mxu(left[0], right[1], dims)
    )


def find_factor(gram, factor, current, change, scaled, between=None):
    diagonal = lax.broadcasted_iota(jnp.int32, gram.shape, 0) == lax.broadcasted_iota(
        jnp.int32, gram.shape, 1
    )
    squares = jnp.sum(
        jnp.sum(jnp.where(diagonal, gram, 0.0), axis=1, keepdims=True), axis=0, keepdims=True
    )
    norm = jnp.sqrt(squares) + 1e-07
    current[...] = gram / (norm * norm)
    factor[...] = jnp.where(diagonal, 1.0 / norm, 0.0)
    half = D // 2

    def product(out, left, right, by, added, added_by):
        upper = by * mxu3([x[:half] for x in left], right) + added_by * added[:half, :]
        corner = mxu3([x[half:] for x in left], [x[:, half:] for x in right])
        corner = by * corner + added_by * added[half:, half:]
        out[:half, :] = upper
        out[half:, :half] = upper[:, half:].T
        out[half:, half:] = corner

    def polynomial():
        low = halves(current[...])
        product(change, low, low, 2.0315, current, -4.775)
        step = halves(change[...])
        product(factor, step, halves(factor[...]), 1.0, factor, 3.4445)
        return low, step

    def sweep(index, carry):
        if between is not None:
            pl.when(index == MIDWAY)(between)
        low, step = polynomial()
        product(scaled, step, low, 1.0, current, 3.4445)
        product(current, halves(scaled[...]), step, 1.0, scaled, 3.4445)
        return carry

    lax.fori_loop(0, 4, sweep, 0)
    polynomial()


def finish_kernel(
    whole_ref,
    own_steps_ref,
    home_steps_ref,
    attend_step_ref,
    kept,
    given,
    taken,
    factor,
    change,
    mine,
    other,
    step_send,
    step_recv,
    pair_send,
    pair_recv,
):
    dp_here, core = lax.axis_index("dp"), lax.axis_index("tensor")
    partner = {"tensor": 1 - core}
    shard_rows = mine.shape[0]
    qcols = 3 * whole_ref.shape[1] // 4
    here = block_rows(dp_here, shard_rows)
    ready = greet(dp_here, None, core, over_expert=False)
    inward_gram = mxu(whole_ref[:, :qcols], whole_ref[:, :qcols], NT)
    outward_gram = mxu(whole_ref[:, qcols:], whole_ref[:, qcols:], NT)
    kept[...] = jnp.where(core == 0, inward_gram, outward_gram)
    given[...] = jnp.where(core == 0, outward_gram, inward_gram)
    ready()
    pair = remote(given, taken, pair_send.at[0], pair_recv.at[0], partner)
    steps = [
        remote(
            own_steps_ref.at[block_rows(peer(dp_here, k), shard_rows), :],
            home_steps_ref.at[dp_here],
            step_send.at[k - 1],
            step_recv.at[k - 1],
            {"dp": peer(dp_here, k)},
        )
        for k in PAIRS
    ]
    home_steps_ref[dp_here] = own_steps_ref[here, :]
    pair.wait()
    find_factor(kept[...] + taken[...], factor, kept, change, taken)
    mine[...] = factor[here, :]
    pair = remote(mine, other, pair_send.at[1], pair_recv.at[1], partner)
    for copy in steps:
        copy.wait()
    pair.wait()
    for owner, columns, count in ((0, slice(0, qcols), 3 * D), (1, slice(qcols, None), D)):
        rows = halves(jnp.where(core == owner, mine[...], other[...]))
        step = mxu(rows[0], whole_ref[:, columns]) + mxu(rows[1], whole_ref[:, columns])
        attend_step_ref[:, columns] = step * (0.2 * math.sqrt(count))


def apply_kernel(
    steps_done_ref,
    home_steps_ref,
    attend_step_ref,
    home_grads_ref,
    attend_grad_ref,
    norm_ref,
    gains_ref,
    biases_ref,
    first_ref,
    second_ref,
    inward_ref,
    outward_ref,
    up_ref,
    down_ref,
    inward_moment_ref,
    outward_moment_ref,
    up_moment_ref,
    down_moment_ref,
    block_ref,
    input_ref,
    block_out_ref,
    input_out_ref,
    inward_gradient_ref,
    outward_gradient_ref,
    up_gradient_ref,
    down_gradient_ref,
    gain_gradient_ref,
    bias_gradient_ref,
    inward_next_ref,
    outward_next_ref,
    up_next_ref,
    down_next_ref,
    inward_new_ref,
    outward_new_ref,
    up_new_ref,
    down_new_ref,
    inward_copy_ref,
    outward_copy_ref,
    up_copy_ref,
    down_copy_ref,
    gains_new_ref,
    biases_new_ref,
    first_new_ref,
    second_new_ref,
    weave,
):
    f32 = jnp.float32
    qcols = inward_ref.shape[1]
    block_out_ref[...] = block_ref[...]
    input_out_ref[...] = input_ref[...]

    def finish(place, gradient, step, refs):
        master_ref, moment_ref, gradient_ref, next_ref, new_ref, copy_ref = refs
        gradient_ref[place] = gradient
        next_ref[place] = 0.95 * moment_ref[place] + gradient
        master = master_ref[place]
        new = master - 0.1 * (step + 0.1 * master)
        new_ref[place] = new
        copy_ref[place] = new.astype(copy_ref.dtype)

    experts = (
        (up_ref, up_moment_ref, up_gradient_ref, up_next_ref, up_new_ref, up_copy_ref),
        (down_ref, down_moment_ref, down_gradient_ref, down_next_ref, down_new_ref, down_copy_ref),
    )
    everything = (slice(None), slice(None))
    rows, width = attend_grad_ref.shape
    for which, refs in enumerate(experts):
        for place, home_ref in enumerate((home_grads_ref, home_steps_ref)):
            for e in range(EXP_DEV):
                for tile in range(width // LANES):
                    weave[place, strand(tile, e, rows, width), :] = home_ref[
                        EXP_DEV * which + e, :, tile * LANES : (tile + 1) * LANES
                    ].astype(f32)
        finish(everything, weave[0], weave[1], refs)
    finish(
        everything,
        attend_grad_ref[:, :qcols],
        attend_step_ref[:, :qcols],
        (
            inward_ref,
            inward_moment_ref,
            inward_gradient_ref,
            inward_next_ref,
            inward_new_ref,
            inward_copy_ref,
        ),
    )
    finish(
        everything,
        attend_grad_ref[:, qcols:],
        attend_step_ref[:, qcols:],
        (
            outward_ref,
            outward_moment_ref,
            outward_gradient_ref,
            outward_next_ref,
            outward_new_ref,
            outward_copy_ref,
        ),
    )

    @pl.when(pl.program_id(0) == 0)
    def norms():
        total = norm_ref[...]
        gain_gradient_ref[...] = total[0:2]
        bias_gradient_ref[...] = total[2:4]
        moment_first = 0.9 * first_ref[...] + 0.1 * total
        moment_second = 0.999 * second_ref[...] + 0.001 * total * total
        first_new_ref[...] = moment_first
        second_new_ref[...] = moment_second
        done = jnp.full((4, D), steps_done_ref[0], jnp.int32).astype(f32)
        direction = (
            moment_first
            / (1.0 - jnp.power(0.9, done))
            / (jnp.sqrt(moment_second / (1.0 - jnp.power(0.999, done))) + 1e-08)
        )
        gains_new_ref[...] = gains_ref[...] - 0.1 * direction[0:2]
        biases_new_ref[...] = biases_ref[...] - 0.1 * direction[2:4]


def pair_body(
    tokens_in,
    expert_ids,
    combine,
    out_cot,
    inward_master,
    outward_master,
    up_master,
    down_master,
    norm_gains,
    norm_biases,
    inward_moment,
    outward_moment,
    up_moment,
    down_moment,
    first_moment,
    second_moment,
    step_count,
):
    bf16, f32 = jnp.bfloat16, jnp.float32
    token_rows = tokens_in.shape[0]
    expert_total = EXP_DEV * 4
    capacity = (token_rows * 10 // (4 * expert_total) + 7) // 8 * 8
    shard_rows, qcols = inward_master.shape
    width = up_master.shape[2]
    images = token_rows // SEQ
    padded_rows = images * PAD
    heads_here = qcols // (3 * HD)
    shape = jax.ShapeDtypeStruct
    rows_f32 = pltpu.VMEM((padded_rows, D), f32)
    in_vmem, anywhere = pl.BlockSpec(memory_space=pltpu.VMEM), pl.BlockSpec(memory_space=pl.ANY)
    dma = pltpu.SemaphoreType.DMA

    slots = shape((EXP_DEV, 4, capacity, D), bf16)
    (
        state,
        gift,
        qkv_low,
        probs,
        weight,
        target,
        combine_padded,
        moment_shard,
        expert_w,
        arrived,
        grad_arrived,
    ) = pl.pallas_call(
        front_kernel,
        out_shape=(
            shape((padded_rows, D), f32),
            shape((D + padded_rows, heads_here * HD), bf16),
            shape((padded_rows, qcols), bf16),
            shape((images * heads_here, PAD, PAD), f32),
            shape((D, width), bf16),
            shape((padded_rows, 128), jnp.int32),
            shape((padded_rows, 2), f32),
            shape((4, shard_rows, width), bf16),
            shape((2 * EXP_DEV, D, width), bf16),
            slots,
            slots,
        ),
        in_specs=[in_vmem] * 8 + [anywhere] * 4,
        out_specs=tuple([in_vmem] * 8 + [anywhere] * 3),
        scratch_shapes=[
            rows_f32,
            pltpu.VMEM((8, token_rows), f32),
            pltpu.VMEM((padded_rows, 128), f32),
            pltpu.VMEM((4, EXP_DEV * shard_rows * width // LANES, LANES), f32),
            pltpu.VMEM((2, padded_rows), jnp.int32),
            pltpu.VMEM((shard_rows, width), bf16),
            pltpu.VMEM((4, shard_rows, width), bf16),
            pltpu.VMEM((D + padded_rows, heads_here * HD), bf16),
            pltpu.VMEM((4, capacity, D), bf16),
            pltpu.VMEM((4, capacity, D), bf16),
            dma((3,)),
            dma((3,)),
            dma((4,)),
            dma((4,)),
            dma((2, 4)),
            dma((2, 4)),
            dma((2, 4)),
            dma((2, 4)),
            dma((2,)),
            dma((3,)),
            dma((4,)),
        ],
        name="front",
        cost_estimate=pl.CostEstimate(
            flops=60_000_000_000, bytes_accessed=30_000_000, transcendentals=0
        ),
        compiler_params=pltpu.CompilerParams(collective_id=0, has_side_effects=True),
    )(
        expert_ids.T,
        combine.T,
        out_cot,
        tokens_in,
        norm_gains,
        norm_biases,
        inward_master,
        outward_master,
        *(woven(a) for a in (up_master, down_master, up_moment, down_moment)),
    )
    chunks = (2, 4, capacity, D)
    square = pltpu.VMEM((D, D), f32)
    rows_low = pltpu.VMEM((shard_rows, width), bf16)
    (
        input_gradient,
        block_out,
        norm_total,
        attend_grad,
        attend_whole,
        own_steps,
        home_grads,
    ) = pl.pallas_call(
        back_kernel,
        out_shape=(
            shape((token_rows, D), f32),
            shape((token_rows, D), bf16),
            shape((4, D), f32),
            shape((shard_rows, width), f32),
            shape((D, width), bf16),
            shape((D, width), bf16),
            shape((4, shard_rows, width), bf16),
        ),
        in_specs=[in_vmem] * 6 + [anywhere] * 11,
        out_specs=tuple([in_vmem] * 6 + [anywhere]),
        scratch_shapes=[
            pltpu.VMEM(chunks, bf16),
            pltpu.VMEM(chunks, bf16),
            pltpu.VMEM(chunks, bf16),
            pltpu.VMEM((2,) + chunks, bf16),
            pltpu.VMEM((4, D, width), bf16),
            pltpu.VMEM((2, 2, D // 2, width), bf16),
            pltpu.VMEM((2, D // 2, width), bf16),
            pltpu.VMEM((2, D // 2, width), bf16),
            pltpu.VMEM((D, width), bf16),
            pltpu.VMEM((D, width), bf16),
            rows_f32,
            rows_f32,
            pltpu.VMEM((4, shard_rows, width), bf16),
            pltpu.VMEM((3, shard_rows, width), bf16),
            rows_low,
            pltpu.VMEM((3, shard_rows // 4, width), bf16),
            pltpu.VMEM((shard_rows // 4, width), bf16),
            rows_low,
            rows_low,
            pltpu.VMEM((2, 8, D), f32),
            pltpu.VMEM((2, 4, 8, D), f32),
            square,
            square,
        ]
        + [dma((2, 4))] * 6
        + [dma((2,))] * 2
        + [dma((5, 3))] * 2
        + [dma((3, 3))] * 2
        + [dma((2, 2))] * 2
        + [dma((2,))] * 2
        + [dma((1,))]
        + [dma((8,))],
        name="back",
        cost_estimate=pl.CostEstimate(
            flops=110_000_000_000, bytes_accessed=60_000_000, transcendentals=0
        ),
        compiler_params=pltpu.CompilerParams(
            collective_id=1, has_side_effects=True, vmem_limit_bytes=66_000_000
        ),
    )(
        combine_padded,
        target,
        norm_gains,
        norm_biases,
        inward_moment,
        outward_moment,
        out_cot,
        tokens_in,
        state,
        gift,
        qkv_low,
        probs,
        weight,
        expert_w,
        arrived,
        grad_arrived,
        moment_shard,
    )
    factor_rows = pltpu.VMEM((shard_rows, D), f32)
    home_steps, attend_step = pl.pallas_call(
        finish_kernel,
        out_shape=(shape((4, shard_rows, width), bf16), shape((shard_rows, width), f32)),
        in_specs=[in_vmem] * 2,
        out_specs=(in_vmem, in_vmem),
        scratch_shapes=[square] * 5 + [factor_rows] * 2 + [dma((3,))] * 2 + [dma((2,))] * 2,
        name="finish",
        cost_estimate=pl.CostEstimate(
            flops=20_000_000_000, bytes_accessed=5_000_000, transcendentals=0
        ),
        compiler_params=pltpu.CompilerParams(collective_id=2, has_side_effects=True),
    )(attend_whole, own_steps)

    blocks = 4
    inward, outward = inward_master.shape, outward_master.shape
    expert = (EXP_DEV * shard_rows * width // LANES, LANES)

    def split(whole, along=0):
        if along is None:
            return pl.BlockSpec(whole, lambda i: (0,) * len(whole))
        rows = pl.cdiv(pl.cdiv(whole[along], blocks), 8) * 8
        block = whole[:along] + (rows,) + whole[along + 1 :]
        return pl.BlockSpec(
            block, lambda i: (0,) * along + (i,) + (0,) * (len(whole) - along - 1)
        )

    two, four, attended = (2, D), (4, D), (shard_rows, width)
    matrix_shapes = (inward, outward, expert, expert)
    by_rows = [split(m) for m in matrix_shapes]
    tokens = split((token_rows, D))
    finished = pl.pallas_call(
        apply_kernel,
        grid=(blocks,),
        out_shape=tuple(
            [shape((token_rows, D), bf16), shape((token_rows, D), f32)]
            + [shape(m, f32) for m in matrix_shapes]
            + [shape(two, f32)] * 2
            + [shape(m, f32) for m in matrix_shapes * 2]
            + [shape(m, bf16) for m in matrix_shapes]
            + [shape(two, f32)] * 2
            + [shape(four, f32)] * 2
        ),
        in_specs=[pl.BlockSpec(memory_space=pltpu.SMEM)]
        + [split((4,) + attended, 1), split(attended), split((4,) + attended, 1), split(attended)]
        + [split(four, None), split(two, None), split(two, None), split(four, None), split(four, None)]
        + by_rows * 2
        + [tokens] * 2,
        out_specs=tuple(
            [tokens] * 2
            + by_rows
            + [split(two, None)] * 2
            + by_rows * 3
            + [split(two, None)] * 2
            + [split(four, None)] * 2
        ),
        scratch_shapes=[pltpu.VMEM((2, expert[0] // blocks, LANES), f32)],
        name="apply",
        cost_estimate=pl.CostEstimate(
            flops=20_000_000, bytes_accessed=20_000_000, transcendentals=0
        ),
    )(
        step_count,
        home_steps,
        attend_step,
        home_grads,
        attend_grad,
        norm_total,
        norm_gains,
        norm_biases,
        first_moment,
        second_moment,
        inward_master,
        outward_master,
        woven(up_master),
        woven(down_master),
        inward_moment,
        outward_moment,
        woven(up_moment),
        woven(down_moment),
        block_out,
        input_gradient,
    )
    return tuple(
        unwoven(a, up_master.shape) if a.shape == expert else a for a in finished
    )


def solution(mesh):
    sizes = tuple(mesh.shape[axis] for axis in ("dp", "expert", "tensor"))
    body = pair_body if sizes == (4, 4, 2) else start_body
    return jax.shard_map(
        body,
        mesh=mesh,
        in_specs=(
            P(("dp", "expert"), None),
            P(("dp", "expert"), None),
            P(("dp", "expert"), None),
            P(("dp", "expert"), None),
            P("dp", "tensor"),
            P("dp", "tensor"),
            P("dp", "expert", "tensor"),
            P("dp", "expert", "tensor"),
            P(),
            P(),
            P("dp", "tensor"),
            P("dp", "tensor"),
            P("dp", "expert", "tensor"),
            P("dp", "expert", "tensor"),
            P(),
            P(),
            P(),
        ),
        out_specs=(
            P(("dp", "expert"), None),
            P(("dp", "expert"), None),
            P("dp", "tensor"),
            P("dp", "tensor"),
            P("dp", "expert", "tensor"),
            P("dp", "expert", "tensor"),
            P(),
            P(),
            P("dp", "tensor"),
            P("dp", "tensor"),
            P("dp", "expert", "tensor"),
            P("dp", "expert", "tensor"),
            P("dp", "tensor"),
            P("dp", "tensor"),
            P("dp", "expert", "tensor"),
            P("dp", "expert", "tensor"),
            P("dp", "tensor"),
            P("dp", "tensor"),
            P("dp", "expert", "tensor"),
            P("dp", "expert", "tensor"),
            P(),
            P(),
            P(),
            P(),
        ),
        check_vma=False,
    )
```

```python
import functools
import math

import jax
import jax.numpy as jnp
import numpy as np
from jax import lax
from jax.experimental import pallas as pl
from jax.experimental.pallas import tpu as pltpu
from jax.sharding import PartitionSpec as P

D = 512
HD = 64
F = 2048
SEQ = 197
EXP_DEV = 2


def layer_norm(values, gain_row, bias_row):
    center = values - jnp.mean(values, axis=-1, keepdims=True)
    invert = lax.rsqrt(jnp.mean(center * center, axis=-1, keepdims=True) + 1e-06)
    scaled = center * invert
    return (scaled * gain_row + bias_row, scaled, invert)


def norm_backward(upstream, scaled, invert, gain_row):
    weighted = upstream * gain_row
    return invert * (
        weighted
        - jnp.mean(weighted, axis=-1, keepdims=True)
        - scaled * jnp.mean(weighted * scaled, axis=-1, keepdims=True)
    )


def gelu_exact(values):
    return 0.5 * values * (1.0 + lax.erf(values * 0.7071067811865476))


def gelu_slope(values):
    return 0.5 * (
        1.0 + lax.erf(values * 0.7071067811865476)
    ) + values * 0.3989422804014327 * jnp.exp(-0.5 * values * values)


def newton_schulz(matrix):
    current = matrix / (jnp.sqrt(jnp.sum(matrix * matrix)) + 1e-07)
    for sweep_index in range(5):
        gram_matrix = jnp.dot(current, current.T, precision=lax.Precision.HIGHEST)
        polynom = -4.775 * gram_matrix + 2.0315 * jnp.dot(
            gram_matrix, gram_matrix, precision=lax.Precision.HIGHEST
        )
        current = 3.4445 * current + jnp.dot(polynom, current, precision=lax.Precision.HIGHEST)
    return current


def start_body(
    tokens_in,
    expert_ids,
    combine,
    out_cot,
    inward_master,
    outward_master,
    up_master,
    down_master,
    norm_gains,
    norm_biases,
    inward_moment,
    outward_moment,
    up_moment,
    down_moment,
    first_moment,
    second_moment,
    step_count,
):
    dp_count = lax.axis_size("dp")
    expert_count = lax.axis_size("expert")
    tensor_count = lax.axis_size("tensor")
    token_rows = tokens_in.shape[0]
    expert_total = EXP_DEV * expert_count
    capacity = (token_rows * 10 // (4 * expert_total) + 7) // 8 * 8
    slot_total = expert_total * capacity
    inputs = tokens_in.astype(jnp.float32)
    w_inward, w_outward, w_up, w_down = (
        lax.all_gather(inward_master.astype(jnp.bfloat16), "dp", axis=0, tiled=True),
        lax.all_gather(outward_master.astype(jnp.bfloat16), "dp", axis=0, tiled=True),
        lax.all_gather(up_master.astype(jnp.bfloat16), "dp", axis=0, tiled=True),
        lax.all_gather(down_master.astype(jnp.bfloat16), "dp", axis=0, tiled=True),
    )
    expert_lanes = jnp.arange(expert_total, dtype=jnp.int32)
    route_hits = (expert_ids[:, :, None] == expert_lanes).astype(jnp.int32)
    per_token = jnp.sum(route_hits, axis=1)
    earlier = jnp.cumsum(per_token, axis=0) - per_token
    position = jnp.sum(route_hits * earlier[:, None, :], axis=2)
    target = expert_ids * capacity + position
    select = (target[:, :, None] == jnp.arange(slot_total, dtype=jnp.int32)).astype(jnp.bfloat16)
    normed1, scaled1, invert1 = layer_norm(inputs, norm_gains[0], norm_biases[0])
    normed1_low = normed1.astype(jnp.bfloat16)
    qkv_low = jnp.dot(normed1_low, w_inward, preferred_element_type=jnp.float32).astype(
        jnp.bfloat16
    )
    heads_here = w_inward.shape[1] // (3 * HD)
    images = token_rows // SEQ
    split_heads = qkv_low.reshape(images, SEQ, heads_here, 3, HD)
    query_part = split_heads[:, :, :, 0]
    key_part = split_heads[:, :, :, 1]
    value_part = split_heads[:, :, :, 2]
    score_scale = HD ** (-0.5)
    scores = (
        jnp.einsum("bihd,bjhd->bhij", query_part, key_part, preferred_element_type=jnp.float32)
        * score_scale
    )
    row_max = jnp.max(scores, axis=-1, keepdims=True)
    exponent = jnp.exp(scores - row_max)
    row_total = jnp.sum(exponent, axis=-1, keepdims=True)
    softmax_out = exponent / row_total
    softmax_low = softmax_out.astype(jnp.bfloat16)
    heads_out = (
        jnp.einsum("bhij,bjhd->bihd", softmax_low, value_part, preferred_element_type=jnp.float32)
        .astype(jnp.bfloat16)
        .reshape(token_rows, heads_here * HD)
    )
    attend_part = jnp.einsum("tc,dc->td", heads_out, w_outward, preferred_element_type=jnp.float32)
    attended = lax.psum(attend_part, "tensor")
    state = inputs + attended
    normed2, scaled2, invert2 = layer_norm(state, norm_gains[1], norm_biases[1])
    normed2_low = normed2.astype(jnp.bfloat16)
    slots_out = jnp.einsum(
        "tks,td->sd", select, normed2_low, preferred_element_type=jnp.float32
    ).astype(jnp.bfloat16)
    arrived = lax.all_to_all(
        slots_out.reshape(expert_count, EXP_DEV, capacity, D),
        "expert",
        split_axis=0,
        concat_axis=0,
        tiled=True,
    )
    pre_act = jnp.einsum("secd,def->secf", arrived, w_up, preferred_element_type=jnp.float32)
    hidden_low = gelu_exact(pre_act).astype(jnp.bfloat16)
    expert_part = jnp.einsum(
        "secf,def->secd", hidden_low, w_down, preferred_element_type=jnp.float32
    ).astype(jnp.bfloat16)
    returned = lax.all_to_all(expert_part, "expert", split_axis=0, concat_axis=0, tiled=True)
    routed = jnp.einsum(
        "tks,sd->tkd", select, returned.reshape(slot_total, D), preferred_element_type=jnp.float32
    )
    mixed_part = jnp.sum(routed * combine[:, :, None], axis=1)
    mixed_sum = lax.psum(mixed_part, "tensor")
    block_out = (state + mixed_sum).astype(jnp.bfloat16)
    routed_grad = (combine[:, :, None] * out_cot[:, None, :]).astype(jnp.bfloat16)
    slot_grad = jnp.einsum(
        "tks,tkd->sd", select, routed_grad, preferred_element_type=jnp.float32
    ).astype(jnp.bfloat16)
    grad_arrived = lax.all_to_all(
        slot_grad.reshape(expert_count, EXP_DEV, capacity, D),
        "expert",
        split_axis=0,
        concat_axis=0,
        tiled=True,
    )
    hidden_grad = jnp.einsum(
        "secd,def->secf", grad_arrived, w_down, preferred_element_type=jnp.float32
    )
    pre_grad = (hidden_grad * gelu_slope(pre_act)).astype(jnp.bfloat16)
    down_local = jnp.einsum(
        "secd,secf->def", grad_arrived, hidden_low, preferred_element_type=jnp.float32
    )
    up_local = jnp.einsum("secd,secf->def", arrived, pre_grad, preferred_element_type=jnp.float32)
    entry_grad = jnp.einsum(
        "secf,def->secd", pre_grad, w_up, preferred_element_type=jnp.float32
    ).astype(jnp.bfloat16)
    entry_back = lax.all_to_all(entry_grad, "expert", split_axis=0, concat_axis=0, tiled=True)
    normed2_part = jnp.einsum(
        "tks,sd->td", select, entry_back.reshape(slot_total, D), preferred_element_type=jnp.float32
    )
    normed2_grad = lax.psum(normed2_part, "tensor")
    state_grad = out_cot + norm_backward(normed2_grad, scaled2, invert2, norm_gains[1])
    state_low = state_grad.astype(jnp.bfloat16)
    outward_local = jnp.einsum(
        "td,tc->dc", state_low, heads_out, preferred_element_type=jnp.float32
    )
    heads_grad = (
        jnp.dot(state_low, w_outward, preferred_element_type=jnp.float32)
        .astype(jnp.bfloat16)
        .reshape(images, SEQ, heads_here, HD)
    )
    prob_grad = jnp.einsum(
        "bihd,bjhd->bhij", heads_grad, value_part, preferred_element_type=jnp.float32
    )
    score_grad = (
        softmax_out * (prob_grad - jnp.sum(softmax_out * prob_grad, axis=-1, keepdims=True))
    ).astype(jnp.bfloat16)
    query_grad = (
        jnp.einsum("bhij,bjhd->bihd", score_grad, key_part, preferred_element_type=jnp.float32)
        * score_scale
    )
    key_grad = (
        jnp.einsum("bhij,bihd->bjhd", score_grad, query_part, preferred_element_type=jnp.float32)
        * score_scale
    )
    value_grad = jnp.einsum(
        "bhij,bihd->bjhd", softmax_low, heads_grad, preferred_element_type=jnp.float32
    )
    qkv_grad = (
        jnp.stack([query_grad, key_grad, value_grad], axis=3)
        .reshape(token_rows, heads_here * 3 * HD)
        .astype(jnp.bfloat16)
    )
    inward_local = jnp.einsum(
        "td,tc->dc", normed1_low, qkv_grad, preferred_element_type=jnp.float32
    )
    normed1_part = jnp.einsum("tc,dc->td", qkv_grad, w_inward, preferred_element_type=jnp.float32)
    normed1_grad = lax.psum(normed1_part, "tensor")
    input_gradient = state_grad + norm_backward(normed1_grad, scaled1, invert1, norm_gains[0])
    norm_terms = jnp.stack(
        [
            jnp.sum(normed1_grad * scaled1, axis=0),
            jnp.sum(normed2_grad * scaled2, axis=0),
            jnp.sum(normed1_grad, axis=0),
            jnp.sum(normed2_grad, axis=0),
        ]
    )
    inward_total, outward_total, norm_total = lax.psum(
        (inward_local, outward_local, norm_terms), ("dp", "expert")
    )
    up_gradient, down_gradient = (
        lax.psum_scatter(up_local, "dp", scatter_dimension=0, tiled=True),
        lax.psum_scatter(down_local, "dp", scatter_dimension=0, tiled=True),
    )
    shard_rows = D // dp_count
    dp_here = lax.axis_index("dp")
    inward_gradient = lax.dynamic_slice_in_dim(inward_total, dp_here * shard_rows, shard_rows, 0)
    outward_gradient = lax.dynamic_slice_in_dim(outward_total, dp_here * shard_rows, shard_rows, 0)
    inward_next = 0.95 * inward_moment + inward_gradient
    outward_next = 0.95 * outward_moment + outward_gradient
    up_next = 0.95 * up_moment + up_gradient
    down_next = 0.95 * down_moment + down_gradient
    matrices = [up_next[:, expert_slot] for expert_slot in range(EXP_DEV)]
    matrices = matrices + [down_next[:, expert_slot] for expert_slot in range(EXP_DEV)]
    matrices = matrices + [jnp.concatenate([inward_next, outward_next], axis=1)]
    stacked = jnp.stack(matrices)
    slot_count = len(matrices)
    group_size = dp_count * tensor_count
    shard_width = stacked.shape[2]
    query_cols = inward_next.shape[1]

    def orth_expert(pieces):
        whole_matrix = pieces.transpose(0, 2, 1, 3).reshape(D, tensor_count * shard_width)
        result = newton_schulz(whole_matrix) * (0.2 * math.sqrt(F))
        return result.reshape(dp_count, shard_rows, tensor_count, shard_width).transpose(0, 2, 1, 3)

    def orth_attention(pieces):
        inward_whole = (
            pieces[..., :query_cols].transpose(0, 2, 1, 3).reshape(D, tensor_count * query_cols)
        )
        outward_whole = (
            pieces[..., query_cols:]
            .transpose(0, 2, 1, 3)
            .reshape(D, tensor_count * (shard_width - query_cols))
        )
        inward_result = newton_schulz(inward_whole) * (0.2 * math.sqrt(3 * D))
        outward_result = newton_schulz(outward_whole) * (0.2 * math.sqrt(D))
        inward_blocks = inward_result.reshape(
            dp_count, shard_rows, tensor_count, query_cols
        ).transpose(0, 2, 1, 3)
        outward_blocks = outward_result.reshape(
            dp_count, shard_rows, tensor_count, shard_width - query_cols
        ).transpose(0, 2, 1, 3)
        return jnp.concatenate([inward_blocks, outward_blocks], axis=3)

    owner_index = lax.axis_index(("dp", "tensor"))
    outgoing = stacked[np.arange(group_size) % slot_count]
    received = lax.all_to_all(outgoing, ("dp", "tensor"), split_axis=0, concat_axis=0, tiled=True)
    blocks = received.reshape(dp_count, tensor_count, shard_rows, shard_width)
    slot_here = owner_index % slot_count
    result_blocks = lax.cond(slot_here == slot_count - 1, orth_attention, orth_expert, blocks)
    arrived_steps = lax.all_to_all(
        result_blocks.reshape(group_size, shard_rows, shard_width),
        ("dp", "tensor"),
        split_axis=0,
        concat_axis=0,
        tiled=True,
    )
    picked = []
    for owned_slot in range(slot_count):
        replicas = (group_size - owned_slot + slot_count - 1) // slot_count
        source = owned_slot + slot_count * (owner_index % replicas)
        picked.append(lax.dynamic_index_in_dim(arrived_steps, source, 0, keepdims=False))
    up_step = jnp.stack(picked[0:EXP_DEV], axis=1)
    down_step = jnp.stack(picked[EXP_DEV : 2 * EXP_DEV], axis=1)
    attend_step = picked[2 * EXP_DEV]
    inward_new = inward_master - 0.1 * (attend_step[:, :query_cols] + 0.1 * inward_master)
    outward_new = outward_master - 0.1 * (attend_step[:, query_cols:] + 0.1 * outward_master)
    up_new = up_master - 0.1 * (up_step + 0.1 * up_master)
    down_new = down_master - 0.1 * (down_step + 0.1 * down_master)
    moment_first = 0.9 * first_moment + 0.1 * norm_total
    moment_second = 0.999 * second_moment + 0.001 * norm_total * norm_total
    steps_done = step_count[0].astype(jnp.float32)
    direction = (
        moment_first
        / (1.0 - jnp.power(0.9, steps_done))
        / (jnp.sqrt(moment_second / (1.0 - jnp.power(0.999, steps_done))) + 1e-08)
    )
    params_new = jnp.concatenate([norm_gains, norm_biases], axis=0) - 0.1 * direction
    return (
        block_out,
        input_gradient,
        inward_gradient,
        outward_gradient,
        up_gradient,
        down_gradient,
        norm_total[0:2],
        norm_total[2:4],
        inward_next,
        outward_next,
        up_next,
        down_next,
        inward_new,
        outward_new,
        up_new,
        down_new,
        inward_new.astype(jnp.bfloat16),
        outward_new.astype(jnp.bfloat16),
        up_new.astype(jnp.bfloat16),
        down_new.astype(jnp.bfloat16),
        params_new[0:2],
        params_new[2:4],
        moment_first,
        moment_second,
    )


PAIRS = (1, 2, 3)
FAR_FIRST = (3, 2, 1, 0)
MIDWAY = 1
LANES = 128
NOWHERE = 128 * 128 - 1
PAD = 208
NT = (((1,), (1,)), ((), ()))
TN = (((0,), (0,)), ((), ()))


def mxu(left, right, dims=(((1,), (0,)), ((), ()))):
    return lax.dot_general(left, right, dims, preferred_element_type=jnp.float32)


def spread_rows(value, padded_ref):
    padded_ref[...] = jnp.zeros_like(padded_ref)
    for image in range(value.shape[0] // SEQ):
        padded_ref[image * PAD : image * PAD + SEQ, :] = value[image * SEQ : (image + 1) * SEQ]


def gather_rows(padded, out_ref):
    for image in range(out_ref.shape[0] // SEQ):
        out_ref[image * SEQ : (image + 1) * SEQ, :] = padded[
            image * PAD : image * PAD + SEQ
        ].astype(out_ref.dtype)


def peer(me, k):
    return (me + k) % 2 + 2 * ((me // 2 + k // 2) % 2)


def remote(source, target, send, recv, device):
    copy = pltpu.make_async_remote_copy(
        src_ref=source,
        dst_ref=target,
        send_sem=send,
        recv_sem=recv,
        device_id=device,
        device_id_type=pl.DeviceIdType.MESH,
    )
    copy.start()
    return copy


class Copy:
    def __init__(self, parts, start=True):
        self.parts = parts
        if start:
            self.make().start()

    def make(self):
        source, target, send, recv, device = self.parts()
        return pltpu.make_async_remote_copy(
            src_ref=source,
            dst_ref=target,
            send_sem=send,
            recv_sem=recv,
            device_id=device,
            device_id_type=pl.DeviceIdType.MESH,
        )

    def wait_recv(self):
        self.make().wait_recv()

    def wait_send(self):
        self.make().wait_send()


def keep(source, target, sem):
    copy = pltpu.make_async_copy(source, target, sem)
    copy.start()
    return copy


def greet(dp_here, expert_here, core, over_expert=True):
    barrier = pltpu.get_barrier_semaphore()
    devices = [{"dp": peer(dp_here, k)} for k in PAIRS] + [{"tensor": 1 - core}]
    if over_expert:
        devices += [{"expert": peer(expert_here, k)} for k in PAIRS]
    for device in devices:
        pl.semaphore_signal(
            barrier, inc=1, device_id=device, device_id_type=pl.DeviceIdType.MESH
        )
    return lambda: pl.semaphore_wait(barrier, len(devices))


def block_rows(index, size):
    return pl.ds(pl.multiple_of(index * size, size), size)


def one_hot(cond):
    return jnp.where(cond, 1.0, 0.0).astype(jnp.bfloat16)


def route(ids, capacity, target_ref, target_t_ref):
    rows = ids.shape[0]
    square = (PAD, PAD)
    below = one_hot(
        lax.broadcasted_iota(jnp.int32, square, 0) > lax.broadcasted_iota(jnp.int32, square, 1)
    )
    lane = lax.broadcasted_iota(jnp.int32, (rows, 128), 1)
    hits = one_hot((lane == ids[:, 0:1]) | (lane == ids[:, 1:2]))
    earlier, passed = [], jnp.zeros((1, 128), jnp.float32)
    for image in range(rows // PAD):
        own = hits[image * PAD : (image + 1) * PAD]
        earlier.append(mxu(below, own) + passed)
        passed += jnp.sum(own.astype(jnp.float32), axis=0, keepdims=True)
    earlier = jnp.concatenate(earlier, axis=0)
    target = jnp.zeros((rows, 128), jnp.int32)
    parts = jnp.zeros((rows, 128), jnp.int32)
    for r in range(2):
        own = ids[:, r : r + 1]
        position = jnp.sum(jnp.where(lane == own, earlier, 0.0), axis=1, keepdims=True)
        value = jnp.where(own >= 0, own * capacity + position.astype(jnp.int32), NOWHERE)
        target = jnp.where(lane == r, value, target)
        parts = jnp.where(lane == 2 * r, value // 128, jnp.where(lane == 2 * r + 1, value % 128, parts))
    target_ref[...] = target
    identity = one_hot(
        lax.broadcasted_iota(jnp.int32, (8, 128), 0) == lax.broadcasted_iota(jnp.int32, (8, 128), 1)
    )
    flipped = mxu(identity, parts.astype(jnp.float32).astype(jnp.bfloat16), NT).astype(jnp.int32)
    for r in range(2):
        target_t_ref[r : r + 1, :] = flipped[2 * r : 2 * r + 1] * 128 + flipped[2 * r + 1 : 2 * r + 2]


def attend(qkv_ref, probs_ref, gift_ref):
    heads_here = qkv_ref.shape[1] // (3 * HD)
    key_lane = lax.broadcasted_iota(jnp.int32, (PAD, PAD), 1)

    def one_image(image, carry):
        rows = block_rows(image, PAD)
        out_rows = pl.ds(pl.multiple_of(D + image * PAD, 16), PAD)
        for head in range(heads_here):
            base = head * 3 * HD
            query = qkv_ref[rows, base : base + HD]
            key = qkv_ref[rows, base + HD : base + 2 * HD]
            value = qkv_ref[rows, base + 2 * HD : base + 3 * HD]
            scores = jnp.where(key_lane < SEQ, mxu(query, key, NT) * HD ** (-0.5), -1e30)
            exponent = jnp.exp(scores - jnp.max(scores, axis=-1, keepdims=True))
            probs = exponent / jnp.sum(exponent, axis=-1, keepdims=True)
            probs_ref[image * heads_here + head] = probs
            gift_ref[out_rows, head * HD : (head + 1) * HD] = mxu(
                probs.astype(jnp.bfloat16), value
            ).astype(jnp.bfloat16)
        return carry

    lax.fori_loop(0, qkv_ref.shape[0] // PAD, one_image, 0)


def woven(array):
    rows, count, width = array.shape
    tiles = array.reshape(rows, count, width // LANES, LANES)
    return tiles.transpose(0, 2, 1, 3).reshape(-1, LANES)


def unwoven(array, whole):
    rows, count, width = whole
    tiles = array.reshape(rows, width // LANES, count, LANES)
    return tiles.transpose(0, 2, 1, 3).reshape(whole)


def strand(tile, expert, rows, width):
    step = EXP_DEV * (width // LANES)
    return pl.ds(EXP_DEV * tile + expert, rows, stride=step)


def front_kernel(
    ids_ref,
    combine_ref,
    cot_ref,
    tokens_ref,
    gains_ref,
    biases_ref,
    inward_ref,
    outward_ref,
    up_ref,
    down_ref,
    up_moment_ref,
    down_moment_ref,
    state_ref,
    gift_ref,
    qkv_ref,
    probs_ref,
    weight_ref,
    target_ref,
    combine_out_ref,
    moment_shard,
    expert_w_ref,
    arrived_ref,
    grad_arrived_ref,
    padded,
    columns,
    columns_padded,
    raw,
    target_t_ref,
    attend_shard,
    expert_shard,
    gift_other_ref,
    grad_chunks,
    token_chunks,
    inner_send,
    inner_recv,
    expert_send,
    expert_recv,
    slot_send,
    slot_recv,
    share_send,
    share_recv,
    gift_sems,
    keep_sems,
    raw_sems,
):
    bf16 = jnp.bfloat16
    dp_here, expert_here, core = (lax.axis_index(a) for a in ("dp", "expert", "tensor"))
    partner = {"tensor": 1 - core}
    capacity = grad_chunks.shape[1]
    shard_rows = attend_shard.shape[0]
    qcols = qkv_ref.shape[1]
    width = attend_shard.shape[1]
    here = block_rows(dp_here, shard_rows)
    ready = greet(dp_here, expert_here, core)
    loads = [
        keep(ref, raw.at[place], raw_sems.at[place])
        for place, ref in enumerate((up_ref, down_ref, up_moment_ref, down_moment_ref))
    ]

    def unpick(place, tile, expert):
        return raw[place, strand(tile, expert, shard_rows, width), :].astype(bf16)

    attend_shard[:, :qcols] = inward_ref[...].astype(bf16)
    attend_shard[:, qcols:] = outward_ref[...].astype(bf16)
    weight_ref[here, :] = attend_shard[...]
    ready()
    inner = [
        remote(
            attend_shard,
            weight_ref.at[here, :],
            inner_send.at[k - 1],
            inner_recv.at[k - 1],
            {"dp": peer(dp_here, k)},
        )
        for k in PAIRS
    ]
    kept = []

    rest = combine_ref[...]
    for part in range(3):
        piece = rest.astype(bf16).astype(jnp.float32)
        columns[2 * part : 2 * part + 2, :] = piece
        rest = rest - piece
    columns[6:8, :] = (ids_ref[...] + 1).astype(jnp.float32)
    identity = one_hot(
        lax.broadcasted_iota(jnp.int32, (8, 128), 0) == lax.broadcasted_iota(jnp.int32, (8, 128), 1)
    )
    spread_rows(mxu(columns[...].astype(bf16), identity, TN), columns_padded)
    for r in range(2):
        combine_out_ref[:, r : r + 1] = (
            columns_padded[:, r : r + 1]
            + columns_padded[:, 2 + r : 3 + r]
            + columns_padded[:, 4 + r : 5 + r]
        )
    ids = columns_padded[...].astype(jnp.int32) - 1
    route(ids[:, 6:8], capacity, target_ref, target_t_ref)
    spread_rows(cot_ref[...], padded)
    slot = lax.broadcasted_iota(jnp.int32, (capacity, padded.shape[0]), 0)

    def first_slot(k):
        return (2 * peer(expert_here, k) + core) * capacity

    def send_chunks(fill, chunks, landing, which):
        def going(k, start=True):
            return Copy(
                lambda: (
                    chunks.at[k],
                    landing.at[0, k],
                    slot_send.at[which, k],
                    slot_recv.at[which, k],
                    {"expert": peer(expert_here, k)},
                ),
                start,
            )

        def make(k):
            chunks[k] = fill(slot + first_slot(k)).astype(bf16)

        def make_and_send(step, carry):
            make(3 - step)

            @pl.when(step > 0)
            def send_last():
                going(4 - step)

            return carry

        lax.fori_loop(0, 4, make_and_send, 0)
        copies, shared = {k: going(k, start=False) for k in PAIRS}, []
        kept.append(keep(chunks.at[0], landing.at[0, 0], keep_sems.at[1 + which]))
        shared.append(
            remote(
                chunks.at[0],
                landing.at[1, 0],
                share_send.at[which, 0],
                share_recv.at[which, 0],
                partner,
            )
        )
        return copies, shared

    def share_arrivals(copies, landing, which, shared):
        for k in FAR_FIRST[:3]:
            copies[k].wait_recv()
            shared.append(
                remote(
                    landing.at[0, k],
                    landing.at[1, k],
                    share_send.at[which, k],
                    share_recv.at[which, k],
                    partner,
                )
            )

    grads = [(combine_out_ref[:, r : r + 1] * padded[...]).astype(bf16) for r in range(2)]
    grad_copies, grad_shared = send_chunks(
        lambda slots: sum(mxu(one_hot(target_t_ref[r : r + 1] == slots), grads[r]) for r in range(2)),
        grad_chunks,
        grad_arrived_ref,
        0,
    )
    for which in range(2):
        loads[which].wait()
        for tile in range(width // LANES):
            pair = [unpick(which, tile, e) for e in range(EXP_DEV)]
            lanes = slice(tile * LANES, (tile + 1) * LANES)
            for j in range(EXP_DEV):
                expert_shard[EXP_DEV * which + j, :, lanes] = jnp.where(
                    core == 0, pair[j], pair[1 - j]
                )
    spread_rows(tokens_ref[...].astype(jnp.float32), padded)
    normed, unused, unused = layer_norm(padded[...], gains_ref[0:1], biases_ref[0:1])
    normed_low = normed.astype(bf16)
    weights = [
        remote(
            expert_shard,
            expert_w_ref.at[:, here, :],
            expert_send.at[k - 1],
            expert_recv.at[k - 1],
            {"dp": peer(dp_here, k)},
        )
        for k in (1, 2)
    ]
    kept.append(keep(expert_shard, expert_w_ref.at[:, here, :], keep_sems.at[0]))
    for which in range(2):
        loads[2 + which].wait()
        for tile in range(width // LANES):
            for e in range(EXP_DEV):
                moment_shard[EXP_DEV * which + e, :, tile * LANES : (tile + 1) * LANES] = unpick(
                    2 + which, tile, e
                )
    for copy in inner:
        copy.wait_recv()
    qkv_ref[...] = mxu(normed_low, weight_ref[:, :qcols]).astype(bf16)
    gift_ref[0:D, :] = weight_ref[:, qcols:]
    attend(qkv_ref, probs_ref, gift_ref)
    gift = remote(gift_ref, gift_other_ref, gift_sems.at[0], gift_sems.at[1], partner)
    half = padded[...] + mxu(gift_ref[D:, :], gift_ref[0:D, :], NT)
    gift.wait()
    state = half + mxu(gift_other_ref[D:, :], gift_other_ref[0:D, :], NT)
    state_ref[...] = state
    normed, unused, unused = layer_norm(state, gains_ref[1:2], biases_ref[1:2])
    normed_low = normed.astype(bf16)
    token_copies, token_shared = send_chunks(
        lambda slots: mxu(
            one_hot((target_t_ref[0:1] == slots) | (target_t_ref[1:2] == slots)), normed_low
        ),
        token_chunks,
        arrived_ref,
        1,
    )
    for copy in weights:
        copy.wait_recv()
    for k, part in ((1, slice(0, EXP_DEV)), (2, slice(EXP_DEV, 2 * EXP_DEV))):
        block = expert_w_ref.at[part, block_rows(peer(dp_here, k), shard_rows), :]
        weights.append(
            remote(
                block,
                block,
                expert_send.at[k + 1],
                expert_recv.at[k + 1],
                {"dp": peer(dp_here, 3 - k)},
            )
        )
    share_arrivals(grad_copies, grad_arrived_ref, 0, grad_shared)
    share_arrivals(token_copies, arrived_ref, 1, token_shared)
    for copy in grad_shared + token_shared + weights[2:]:
        copy.wait()
    for copy in weights[:2] + inner:
        copy.wait_send()
    for copies in (grad_copies, token_copies):
        for k in PAIRS:
            copies[k].wait_send()
    for copy in kept:
        copy.wait()


def back_kernel(
    combine_ref,
    target_ref,
    gains_ref,
    biases_ref,
    inward_moment_ref,
    outward_moment_ref,
    cot_hbm,
    tokens_hbm,
    state_hbm,
    gift_hbm,
    qkv_hbm,
    probs_hbm,
    weight_hbm,
    expert_w_hbm,
    arrived_hbm,
    grad_arrived_hbm,
    moment_hbm,
    input_ref,
    block_ref,
    norm_ref,
    attend_grad_ref,
    attend_whole_ref,
    own_steps_ref,
    home_grads_ref,
    give,
    handed,
    summed,
    returned,
    matrices,
    near_in,
    far_out,
    far_in,
    moment_whole,
    owned_low,
    normed_part,
    normed_other,
    inner,
    inner_in,
    outer,
    outer_in,
    plane,
    quarter_in,
    quarter,
    plane_total,
    whole_own,
    norm_own,
    norm_in,
    gram,
    gram_other,
    hand_send,
    hand_recv,
    slot_send,
    slot_recv,
    share_send,
    share_recv,
    pair_send,
    pair_recv,
    dp_send,
    dp_recv,
    expert_send,
    expert_recv,
    near_send,
    near_recv,
    far_send,
    far_recv,
    own_sems,
    load_sems,
):
    bf16, f32 = jnp.bfloat16, jnp.float32
    dp_here, expert_here, core = (lax.axis_index(a) for a in ("dp", "expert", "tensor"))
    partner = {"tensor": 1 - core}
    capacity = give.shape[2]
    shard_rows = inner.shape[1]
    here = block_rows(dp_here, shard_rows)
    ready = greet(dp_here, expert_here, core)
    sent = []

    def to_dp(stage, sources, targets, peers=PAIRS):
        def copy(k):
            return Copy(
                lambda: (
                    sources(k),
                    targets(k),
                    dp_send.at[stage, k - 1],
                    dp_recv.at[stage, k - 1],
                    {"dp": peer(dp_here, k)},
                )
            )

        copies = [copy(k) for k in peers]
        sent.extend(copies)
        return copies

    def to_expert(stage, sources, targets):
        def copy(k):
            return Copy(
                lambda: (
                    sources(k),
                    targets(k),
                    expert_send.at[stage, k - 1],
                    expert_recv.at[stage, k - 1],
                    {"expert": peer(expert_here, k)},
                )
            )

        copies = [copy(k) for k in PAIRS]
        sent.extend(copies)
        return copies

    def arrive(copies):
        for copy in copies:
            copy.wait_recv()

    shares = ([], [])

    def hand(which, k, start=True):
        return Copy(
            lambda: (
                give.at[which, k],
                handed.at[which, k],
                hand_send.at[which, k],
                hand_recv.at[which, k],
                partner,
            ),
            start,
        )

    def add_up(which, k):
        hand(which, k, start=False).wait_recv()
        total = (summed[which, k].astype(f32) + handed[which, k].astype(f32)).astype(bf16)
        summed[which, k] = total

    def send_home(which, k, start=True):
        return Copy(
            lambda: (
                summed.at[which, k],
                returned.at[which, 0, k],
                slot_send.at[which, k],
                slot_recv.at[which, k],
                {"expert": peer(expert_here, k)},
            ),
            start,
        )

    def stay_home(which):
        returned[which, 0, 0] = summed[which, 0]
        shares[which].append(
            Copy(
                lambda: (
                    summed.at[which, 0],
                    returned.at[which, 1, 0],
                    share_send.at[which, 0],
                    share_recv.at[which, 0],
                    partner,
                )
            )
        )

    def share(which):
        def copy(k):
            return Copy(
                lambda: (
                    returned.at[which, 0, k],
                    returned.at[which, 1, k],
                    share_send.at[which, k],
                    share_recv.at[which, k],
                    partner,
                )
            )

        for k in FAR_FIRST[:3]:
            send_home(which, k, start=False).wait_recv()
            shares[which].append(copy(k))
        sent.extend(shares[which])

    def held(index):
        return 2 * (index // 2) + (index % 2 + core) % 2

    ways = ((slice(0, D // 2), 1, 2), (slice(D // 2, D), 2, 1))

    def near_copy(half, place):
        rows, first, second = ways[half]
        owner = (first, 3)[place]
        return Copy(
            lambda: (
                matrices.at[held(peer(dp_here, owner)), rows, :],
                near_in.at[half, place],
                near_send.at[half, place],
                near_recv.at[half, place],
                {"dp": peer(dp_here, first)},
            )
        )

    def far_copy(half):
        rows, first, second = ways[half]
        return Copy(
            lambda: (
                far_out.at[half],
                far_in.at[half],
                far_send.at[half],
                far_recv.at[half],
                {"dp": peer(dp_here, second)},
            )
        )

    def pass_on(near):
        arrive(near)
        for half, (rows, first, second) in enumerate(ways):
            far_out[half] = (
                matrices[held(peer(dp_here, second)), rows, :].astype(f32)
                + near_in[half, 1].astype(f32)
            ).astype(bf16)
        far = [far_copy(half) for half in range(2)]
        sent.extend(far)
        return far

    def experts(weights, rows, grads, hidden, pre_grad):
        loads = {}
        for j in (1, 0):
            for place, (source, target) in enumerate(
                (
                    (expert_w_hbm.at[j], weights.at[j]),
                    (arrived_hbm.at[j], rows.at[j]),
                    (expert_w_hbm.at[EXP_DEV + j], weights.at[EXP_DEV + j]),
                    (grad_arrived_hbm.at[j], grads.at[j]),
                )
            ):
                loads[j, place] = keep(source, target, load_sems.at[4 * j + place])
        ready()
        moments.extend(
            to_dp(0, lambda k: moment_hbm.at[peer(dp_here, k)], lambda k: moment_whole.at[here, :])
        )

        def chunk(k, step):
            def loaded(*places):
                @pl.when(step == 0)
                def wait():
                    for place in places:
                        loads[place].wait()

            for j in (1, 0):
                loaded((j, 0), (j, 1))
                pre = mxu(rows[j, k], weights[j])
                share_of_one = 0.5 * (1.0 + lax.erf(pre * 0.7071067811865476))
                hidden[j, k] = (pre * share_of_one).astype(bf16)
                slope = share_of_one + pre * 0.3989422804014327 * jnp.exp(-0.5 * pre * pre)
                loaded((j, 2), (j, 3))
                grad = (mxu(grads[j, k], weights[EXP_DEV + j]) * slope).astype(bf16)
                pre_grad[j, k] = grad
                entry = mxu(grad, weights[j], NT).astype(bf16)
                if j == 1:
                    give[0, k] = entry
                else:
                    summed[0, k] = entry

        def next_chunk(step, carry):
            chunk(3 - step, step)
            hand(0, 3 - step)

            @pl.when(step > 0)
            def last_chunk():
                add_up(0, 4 - step)
                send_home(0, 4 - step)

            return carry

        lax.fori_loop(0, 4, next_chunk, 0)

        def matrix(left, right, j):
            total = mxu(left[j, 0], right[j, 0], TN)
            for k in PAIRS:
                total += mxu(left[j, k], right[j, k], TN)
            return total.astype(bf16)

        def expert_matrices(j, carry):
            matrices[j] = matrix(rows, pre_grad, j)
            matrices[EXP_DEV + j] = matrix(grads, hidden, j)
            return carry

        lax.fori_loop(0, EXP_DEV, expert_matrices, 0)
        near = [near_copy(half, place) for place in (1, 0) for half in range(2)]
        sent.extend(near)
        add_up(0, 0)
        stay_home(0)

        def part_chunk(step, carry):
            k = 3 - step
            give[1, k] = mxu(hidden[1, k], weights[EXP_DEV + 1], NT).astype(bf16)
            summed[1, k] = mxu(hidden[0, k], weights[EXP_DEV], NT).astype(bf16)
            hand(1, k)
            return carry

        lax.fori_loop(0, 4, part_chunk, 0)
        for k in FAR_FIRST:
            add_up(1, k)
        for k in FAR_FIRST[:3]:
            send_home(1, k)
        stay_home(1)
        for which in range(2):
            sent.extend(hand(which, k, start=False) for k in range(4))
            sent.extend(send_home(which, k, start=False) for k in PAIRS)
        return near

    own_moment = keep(moment_hbm.at[dp_here], moment_whole.at[here, :], own_sems.at[0])
    near, moments = [], []
    slots = (EXP_DEV, 4, capacity)
    pl.run_scoped(
        lambda *refs: near.extend(experts(*refs)),
        pltpu.VMEM(expert_w_hbm.shape, bf16),
        pltpu.VMEM(slots + (D,), bf16),
        pltpu.VMEM(slots + (D,), bf16),
        pltpu.VMEM(slots + (expert_w_hbm.shape[2],), bf16),
        pltpu.VMEM(slots + (expert_w_hbm.shape[2],), bf16),
    )

    def backward(
        cot_ref,
        tokens_ref,
        state_ref,
        gift_ref,
        qkv_ref,
        probs_ref,
        weight_ref,
        padded,
        qkv_grad_ref,
        local_ref,
        out_grad_ref,
    ):
        loads = [
            keep(source, target, load_sems.at[place])
            for place, (source, target) in enumerate(
                (
                    (state_hbm, state_ref),
                    (cot_hbm, cot_ref),
                    (gift_hbm.at[D:, :], gift_ref),
                    (weight_hbm, weight_ref),
                    (qkv_hbm, qkv_ref),
                    (probs_hbm, probs_ref),
                    (tokens_hbm, tokens_ref),
                )
            )
        ]
        qcols = qkv_ref.shape[1]
        rows_all = state_ref.shape[0]
        loads[0].wait()
        unused, scaled2, invert2 = layer_norm(state_ref[...], gains_ref[1:2], biases_ref[1:2])
        loads[1].wait()
        spread_rows(cot_ref[...], padded)
        def pick_all(which, columns, rows, parts=(0, 1)):
            slot = lax.broadcasted_iota(jnp.int32, (PAD, capacity), 1)

            def picks(k, j):
                first = slot + (2 * peer(expert_here, k) + (core + j) % 2) * capacity
                hit = target_ref[rows, columns[0] : columns[0] + 1] == first
                for column in columns[1:]:
                    hit = hit | (target_ref[rows, column : column + 1] == first)
                return one_hot(hit)

            terms = [mxu(picks(k, j), returned[which, j, k]) for j in parts for k in FAR_FIRST]
            return sum(terms[1:], terms[0])

        share(0)

        def own_gradient(image, carry):
            rows = block_rows(image, PAD)
            normed_part[rows, :] = pick_all(0, (0, 1), rows, (0,))
            return carry

        def other_gradient(image, carry):
            rows = block_rows(image, PAD)
            normed_part[rows, :] += pick_all(0, (0, 1), rows, (1,))
            return carry

        lax.fori_loop(0, rows_all // PAD, own_gradient, 0)
        arrive(shares[0])
        lax.fori_loop(0, rows_all // PAD, other_gradient, 0)
        normed2_grad = normed_part[...]
        norm_own[0, 4:8] = jnp.zeros((4, D), f32)
        norm_own[0, 1:2] = jnp.sum(normed2_grad * scaled2, axis=0, keepdims=True)
        norm_own[0, 3:4] = jnp.sum(normed2_grad, axis=0, keepdims=True)
        state_grad = padded[...] + norm_backward(normed2_grad, scaled2, invert2, gains_ref[1:2])
        padded[...] = state_grad
        state_low = state_grad.astype(bf16)
        for copy in loads[2:]:
            copy.wait()

        local_ref[:, qcols:] = mxu(state_low, gift_ref[...], TN)
        for k in range(4):
            outer[k] = local_ref[block_rows(peer(dp_here, k), shard_rows), qcols:].astype(bf16)
        out_grad_ref[...] = mxu(state_low, weight_ref[:, qcols:]).astype(bf16)
        outward_sums = to_dp(5, lambda k: outer.at[k], lambda k: outer_in.at[k - 1])
        heads_here = qcols // (3 * HD)
        scale = HD ** (-0.5)

        def one_image(image, carry):
            rows = block_rows(image, PAD)
            for head in range(heads_here):
                base = head * 3 * HD
                query = qkv_ref[rows, base : base + HD]
                key = qkv_ref[rows, base + HD : base + 2 * HD]
                value = qkv_ref[rows, base + 2 * HD : base + 3 * HD]
                out_grad = out_grad_ref[rows, head * HD : (head + 1) * HD]
                probs = probs_ref[image * heads_here + head]
                prob_grad = mxu(out_grad, value, NT)
                score_grad = (
                    probs * (prob_grad - jnp.sum(probs * prob_grad, axis=-1, keepdims=True))
                ).astype(bf16)
                qkv_grad_ref[rows, base : base + HD] = (mxu(score_grad, key) * scale).astype(bf16)
                qkv_grad_ref[rows, base + HD : base + 2 * HD] = (
                    mxu(score_grad, query, TN) * scale
                ).astype(bf16)
                qkv_grad_ref[rows, base + 2 * HD : base + 3 * HD] = mxu(
                    probs.astype(bf16), out_grad, TN
                ).astype(bf16)
            return carry

        lax.fori_loop(0, rows_all // PAD, one_image, 0)
        spread_rows(tokens_ref[...].astype(f32), normed_part)
        normed1, scaled1, invert1 = layer_norm(normed_part[...], gains_ref[0:1], biases_ref[0:1])
        local_ref[:, :qcols] = mxu(normed1.astype(bf16), qkv_grad_ref[...], TN)
        for k in range(4):
            inner[k] = local_ref[block_rows(peer(dp_here, k), shard_rows), :qcols].astype(bf16)
        normed_part[...] = mxu(qkv_grad_ref[...], weight_ref[:, :qcols], NT)
        rows_sums = to_dp(1, lambda k: inner.at[k], lambda k: inner_in.at[k - 1]) + outward_sums
        pair = Copy(
            lambda: (normed_part, normed_other, pair_send.at[0], pair_recv.at[0], partner)
        )
        sent.append(pair)
        far = pass_on(near)

        share(1)
        arrive(shares[1])

        def one_output(image, carry):
            rows = block_rows(image, PAD)
            total = state_ref[rows, :]
            for r in range(2):
                total += combine_ref[rows, r : r + 1] * pick_all(1, (r,), rows)
            state_ref[rows, :] = total
            return carry

        lax.fori_loop(0, rows_all // PAD, one_output, 0)
        gather_rows(state_ref[...], block_ref)

        pair.wait_recv()
        normed1_grad = normed_part[...] + normed_other[...]
        norm_own[0, 0:1] = jnp.sum(normed1_grad * scaled1, axis=0, keepdims=True)
        norm_own[0, 2:3] = jnp.sum(normed1_grad, axis=0, keepdims=True)
        norm_in[0, dp_here] = norm_own[0]
        norms = to_dp(2, lambda k: norm_own.at[0], lambda k: norm_in.at[0, dp_here])
        gather_rows(
            padded[...] + norm_backward(normed1_grad, scaled1, invert1, gains_ref[0:1]), input_ref
        )
        return rows_sums, norms, far

    travelling = []
    rows_f32 = pltpu.VMEM(state_hbm.shape, f32)
    pl.run_scoped(
        lambda *refs: travelling.extend(backward(*refs)),
        pltpu.VMEM(cot_hbm.shape, f32),
        pltpu.VMEM(tokens_hbm.shape, bf16),
        rows_f32,
        pltpu.VMEM((gift_hbm.shape[0] - D, gift_hbm.shape[1]), bf16),
        pltpu.VMEM(qkv_hbm.shape, bf16),
        pltpu.VMEM(probs_hbm.shape, f32),
        pltpu.VMEM(weight_hbm.shape, bf16),
        rows_f32,
        pltpu.VMEM(qkv_hbm.shape, bf16),
        pltpu.VMEM(weight_hbm.shape, f32),
        pltpu.VMEM((state_hbm.shape[0], gift_hbm.shape[1]), bf16),
    )
    rows_sums, norms, far = travelling

    arrive(rows_sums)
    qcols = inner.shape[2]
    for columns, own, got in (
        (slice(0, qcols), inner, inner_in),
        (slice(qcols, None), outer, outer_in),
    ):
        plane[:, columns] = (
            own[0].astype(f32)
            + got[0].astype(f32)
            + got[1].astype(f32)
            + got[2].astype(f32)
        ).astype(bf16)
    quarter_rows = quarter.shape[0]
    my_quarter = block_rows(expert_here, quarter_rows)
    quarters = to_expert(
        0,
        lambda k: plane.at[block_rows(peer(expert_here, k), quarter_rows), :],
        lambda k: quarter_in.at[k - 1],
    )
    arrive(norms)
    norm_plane = norm_in[0, 0] + norm_in[0, 1] + norm_in[0, 2] + norm_in[0, 3]
    norm_own[1] = norm_plane
    norm_in[1, expert_here] = norm_plane
    norm_sums = to_expert(1, lambda k: norm_own.at[1], lambda k: norm_in.at[1, expert_here])

    def orthogonalize(owned_next, factor, change):
        arrive(quarters)
        quarter[...] = (
            plane[my_quarter, :].astype(f32)
            + quarter_in[0].astype(f32)
            + quarter_in[1].astype(f32)
            + quarter_in[2].astype(f32)
        ).astype(bf16)
        plane_total[my_quarter, :] = quarter[...]
        totals = to_expert(2, lambda k: quarter, lambda k: plane_total.at[my_quarter, :])
        arrive(far + moments)
        own_moment.wait()
        for half, (rows, first, second) in enumerate(ways):
            owned = (
                matrices[held(dp_here), rows, :].astype(f32)
                + near_in[half, 0].astype(f32)
                + far_in[half].astype(f32)
            )
            owned_low[rows, :] = owned.astype(bf16)
            owned_next[rows, :] = 0.95 * moment_whole[rows, :].astype(f32) + owned
        split = halves(owned_next[...])
        gram[...] = mxu3(split, split, NT)
        pair = remote(gram, gram_other, pair_send.at[1], pair_recv.at[1], partner)

        def send_rows(peers):
            return to_dp(
                3,
                lambda k: owned_low.at[block_rows(peer(dp_here, k), shard_rows), :],
                lambda k: home_grads_ref.at[dp_here],
                peers,
            )

        home = send_rows((1, 2))
        own = keep(owned_low.at[here, :], home_grads_ref.at[dp_here], load_sems.at[1])
        pair.wait()

        def attention_next():
            arrive(totals)
            total = plane_total[...].astype(f32)
            attend_grad_ref[...] = total
            whole_own[:, :qcols] = (0.95 * inward_moment_ref[...] + total[:, :qcols]).astype(bf16)
            whole_own[:, qcols:] = (0.95 * outward_moment_ref[...] + total[:, qcols:]).astype(bf16)
            attend_whole_ref[here, :] = whole_own[...]
            wholes.extend(to_dp(4, lambda k: whole_own, lambda k: attend_whole_ref.at[here, :]))
            home.extend(send_rows((3,)))

        wholes = []
        find_factor(gram[...] + gram_other[...], factor, gram, change, gram_other, attention_next)
        own_steps_ref[...] = (
            mxu3(halves(factor[...]), halves(owned_next[...])) * (0.2 * math.sqrt(F))
        ).astype(bf16)
        arrive(norm_sums)
        norm_ref[...] = (
            norm_in[1, 0, 0:4] + norm_in[1, 1, 0:4] + norm_in[1, 2, 0:4] + norm_in[1, 3, 0:4]
        )
        arrive(home)
        arrive(wholes)
        own.wait()

    square = pltpu.VMEM((D, D), f32)
    pl.run_scoped(orthogonalize, pltpu.VMEM(moment_whole.shape, f32), square, square)
    for copy in sent:
        copy.wait_send()


def halves(value):
    high = value.astype(jnp.bfloat16)
    return high, (value - high.astype(jnp.float32)).astype(jnp.bfloat16)


def mxu3(left, right, dims=(((1,), (0,)), ((), ()))):
    return (
        mxu(left[0], right[0], dims) + mxu(left[1], right[0], dims) + mxu(left[0], right[1], dims)
    )


def find_factor(gram, factor, current, change, scaled, between=None):
    diagonal = lax.broadcasted_iota(jnp.int32, gram.shape, 0) == lax.broadcasted_iota(
        jnp.int32, gram.shape, 1
    )
    squares = jnp.sum(
        jnp.sum(jnp.where(diagonal, gram, 0.0), axis=1, keepdims=True), axis=0, keepdims=True
    )
    norm = jnp.sqrt(squares) + 1e-07
    current[...] = gram / (norm * norm)
    factor[...] = jnp.where(diagonal, 1.0 / norm, 0.0)
    half = D // 2

    def product(out, left, right, by, added, added_by):
        upper = by * mxu3([x[:half] for x in left], right) + added_by * added[:half, :]
        corner = mxu3([x[half:] for x in left], [x[:, half:] for x in right])
        corner = by * corner + added_by * added[half:, half:]
        out[:half, :] = upper
        out[half:, :half] = upper[:, half:].T
        out[half:, half:] = corner

    def polynomial():
        low = halves(current[...])
        product(change, low, low, 2.0315, current, -4.775)
        step = halves(change[...])
        product(factor, step, halves(factor[...]), 1.0, factor, 3.4445)
        return low, step

    def sweep(index, carry):
        if between is not None:
            pl.when(index == MIDWAY)(between)
        low, step = polynomial()
        product(scaled, step, low, 1.0, current, 3.4445)
        product(current, halves(scaled[...]), step, 1.0, scaled, 3.4445)
        return carry

    lax.fori_loop(0, 4, sweep, 0)
    polynomial()


def finish_kernel(
    whole_ref,
    own_steps_ref,
    home_steps_ref,
    attend_step_ref,
    kept,
    given,
    taken,
    factor,
    change,
    mine,
    other,
    step_send,
    step_recv,
    pair_send,
    pair_recv,
):
    dp_here, core = lax.axis_index("dp"), lax.axis_index("tensor")
    partner = {"tensor": 1 - core}
    shard_rows = mine.shape[0]
    qcols = 3 * whole_ref.shape[1] // 4
    here = block_rows(dp_here, shard_rows)
    ready = greet(dp_here, None, core, over_expert=False)
    inward_gram = mxu(whole_ref[:, :qcols], whole_ref[:, :qcols], NT)
    outward_gram = mxu(whole_ref[:, qcols:], whole_ref[:, qcols:], NT)
    kept[...] = jnp.where(core == 0, inward_gram, outward_gram)
    given[...] = jnp.where(core == 0, outward_gram, inward_gram)
    ready()
    pair = remote(given, taken, pair_send.at[0], pair_recv.at[0], partner)
    steps = [
        remote(
            own_steps_ref.at[block_rows(peer(dp_here, k), shard_rows), :],
            home_steps_ref.at[dp_here],
            step_send.at[k - 1],
            step_recv.at[k - 1],
            {"dp": peer(dp_here, k)},
        )
        for k in PAIRS
    ]
    home_steps_ref[dp_here] = own_steps_ref[here, :]
    pair.wait()
    find_factor(kept[...] + taken[...], factor, kept, change, taken)
    mine[...] = factor[here, :]
    pair = remote(mine, other, pair_send.at[1], pair_recv.at[1], partner)
    for copy in steps:
        copy.wait()
    pair.wait()
    for owner, columns, count in ((0, slice(0, qcols), 3 * D), (1, slice(qcols, None), D)):
        rows = halves(jnp.where(core == owner, mine[...], other[...]))
        step = mxu(rows[0], whole_ref[:, columns]) + mxu(rows[1], whole_ref[:, columns])
        attend_step_ref[:, columns] = step * (0.2 * math.sqrt(count))


def apply_kernel(
    steps_done_ref,
    home_steps_ref,
    attend_step_ref,
    home_grads_ref,
    attend_grad_ref,
    norm_ref,
    gains_ref,
    biases_ref,
    first_ref,
    second_ref,
    inward_ref,
    outward_ref,
    up_ref,
    down_ref,
    inward_moment_ref,
    outward_moment_ref,
    up_moment_ref,
    down_moment_ref,
    block_ref,
    input_ref,
    block_out_ref,
    input_out_ref,
    inward_gradient_ref,
    outward_gradient_ref,
    up_gradient_ref,
    down_gradient_ref,
    gain_gradient_ref,
    bias_gradient_ref,
    inward_next_ref,
    outward_next_ref,
    up_next_ref,
    down_next_ref,
    inward_new_ref,
    outward_new_ref,
    up_new_ref,
    down_new_ref,
    inward_copy_ref,
    outward_copy_ref,
    up_copy_ref,
    down_copy_ref,
    gains_new_ref,
    biases_new_ref,
    first_new_ref,
    second_new_ref,
    weave,
):
    f32 = jnp.float32
    qcols = inward_ref.shape[1]
    block_out_ref[...] = block_ref[...]
    input_out_ref[...] = input_ref[...]

    def finish(place, gradient, step, refs):
        master_ref, moment_ref, gradient_ref, next_ref, new_ref, copy_ref = refs
        gradient_ref[place] = gradient
        next_ref[place] = 0.95 * moment_ref[place] + gradient
        master = master_ref[place]
        new = master - 0.1 * (step + 0.1 * master)
        new_ref[place] = new
        copy_ref[place] = new.astype(copy_ref.dtype)

    experts = (
        (up_ref, up_moment_ref, up_gradient_ref, up_next_ref, up_new_ref, up_copy_ref),
        (down_ref, down_moment_ref, down_gradient_ref, down_next_ref, down_new_ref, down_copy_ref),
    )
    everything = (slice(None), slice(None))
    rows, width = attend_grad_ref.shape
    for which, refs in enumerate(experts):
        for place, home_ref in enumerate((home_grads_ref, home_steps_ref)):
            for e in range(EXP_DEV):
                for tile in range(width // LANES):
                    weave[place, strand(tile, e, rows, width), :] = home_ref[
                        EXP_DEV * which + e, :, tile * LANES : (tile + 1) * LANES
                    ].astype(f32)
        finish(everything, weave[0], weave[1], refs)
    finish(
        everything,
        attend_grad_ref[:, :qcols],
        attend_step_ref[:, :qcols],
        (
            inward_ref,
            inward_moment_ref,
            inward_gradient_ref,
            inward_next_ref,
            inward_new_ref,
            inward_copy_ref,
        ),
    )
    finish(
        everything,
        attend_grad_ref[:, qcols:],
        attend_step_ref[:, qcols:],
        (
            outward_ref,
            outward_moment_ref,
            outward_gradient_ref,
            outward_next_ref,
            outward_new_ref,
            outward_copy_ref,
        ),
    )

    @pl.when(pl.program_id(0) == 0)
    def norms():
        total = norm_ref[...]
        gain_gradient_ref[...] = total[0:2]
        bias_gradient_ref[...] = total[2:4]
        moment_first = 0.9 * first_ref[...] + 0.1 * total
        moment_second = 0.999 * second_ref[...] + 0.001 * total * total
        first_new_ref[...] = moment_first
        second_new_ref[...] = moment_second
        done = jnp.full((4, D), steps_done_ref[0], jnp.int32).astype(f32)
        direction = (
            moment_first
            / (1.0 - jnp.power(0.9, done))
            / (jnp.sqrt(moment_second / (1.0 - jnp.power(0.999, done))) + 1e-08)
        )
        gains_new_ref[...] = gains_ref[...] - 0.1 * direction[0:2]
        biases_new_ref[...] = biases_ref[...] - 0.1 * direction[2:4]


def pair_body(
    tokens_in,
    expert_ids,
    combine,
    out_cot,
    inward_master,
    outward_master,
    up_master,
    down_master,
    norm_gains,
    norm_biases,
    inward_moment,
    outward_moment,
    up_moment,
    down_moment,
    first_moment,
    second_moment,
    step_count,
):
    bf16, f32 = jnp.bfloat16, jnp.float32
    token_rows = tokens_in.shape[0]
    expert_total = EXP_DEV * 4
    capacity = (token_rows * 10 // (4 * expert_total) + 7) // 8 * 8
    shard_rows, qcols = inward_master.shape
    width = up_master.shape[2]
    images = token_rows // SEQ
    padded_rows = images * PAD
    heads_here = qcols // (3 * HD)
    shape = jax.ShapeDtypeStruct
    rows_f32 = pltpu.VMEM((padded_rows, D), f32)
    in_vmem, anywhere = pl.BlockSpec(memory_space=pltpu.VMEM), pl.BlockSpec(memory_space=pl.ANY)
    dma = pltpu.SemaphoreType.DMA

    slots = shape((EXP_DEV, 4, capacity, D), bf16)
    (
        state,
        gift,
        qkv_low,
        probs,
        weight,
        target,
        combine_padded,
        moment_shard,
        expert_w,
        arrived,
        grad_arrived,
    ) = pl.pallas_call(
        front_kernel,
        out_shape=(
            shape((padded_rows, D), f32),
            shape((D + padded_rows, heads_here * HD), bf16),
            shape((padded_rows, qcols), bf16),
            shape((images * heads_here, PAD, PAD), f32),
            shape((D, width), bf16),
            shape((padded_rows, 128), jnp.int32),
            shape((padded_rows, 2), f32),
            shape((4, shard_rows, width), bf16),
            shape((2 * EXP_DEV, D, width), bf16),
            slots,
            slots,
        ),
        in_specs=[in_vmem] * 8 + [anywhere] * 4,
        out_specs=tuple([in_vmem] * 8 + [anywhere] * 3),
        scratch_shapes=[
            rows_f32,
            pltpu.VMEM((8, token_rows), f32),
            pltpu.VMEM((padded_rows, 128), f32),
            pltpu.VMEM((4, EXP_DEV * shard_rows * width // LANES, LANES), f32),
            pltpu.VMEM((2, padded_rows), jnp.int32),
            pltpu.VMEM((shard_rows, width), bf16),
            pltpu.VMEM((4, shard_rows, width), bf16),
            pltpu.VMEM((D + padded_rows, heads_here * HD), bf16),
            pltpu.VMEM((4, capacity, D), bf16),
            pltpu.VMEM((4, capacity, D), bf16),
            dma((3,)),
            dma((3,)),
            dma((4,)),
            dma((4,)),
            dma((2, 4)),
            dma((2, 4)),
            dma((2, 4)),
            dma((2, 4)),
            dma((2,)),
            dma((3,)),
            dma((4,)),
        ],
        name="front",
        cost_estimate=pl.CostEstimate(
            flops=60_000_000_000, bytes_accessed=30_000_000, transcendentals=0
        ),
        compiler_params=pltpu.CompilerParams(collective_id=0, has_side_effects=True),
    )(
        expert_ids.T,
        combine.T,
        out_cot,
        tokens_in,
        norm_gains,
        norm_biases,
        inward_master,
        outward_master,
        *(woven(a) for a in (up_master, down_master, up_moment, down_moment)),
    )
    chunks = (2, 4, capacity, D)
    square = pltpu.VMEM((D, D), f32)
    rows_low = pltpu.VMEM((shard_rows, width), bf16)
    (
        input_gradient,
        block_out,
        norm_total,
        attend_grad,
        attend_whole,
        own_steps,
        home_grads,
    ) = pl.pallas_call(
        back_kernel,
        out_shape=(
            shape((token_rows, D), f32),
            shape((token_rows, D), bf16),
            shape((4, D), f32),
            shape((shard_rows, width), f32),
            shape((D, width), bf16),
            shape((D, width), bf16),
            shape((4, shard_rows, width), bf16),
        ),
        in_specs=[in_vmem] * 6 + [anywhere] * 11,
        out_specs=tuple([in_vmem] * 6 + [anywhere]),
        scratch_shapes=[
            pltpu.VMEM(chunks, bf16),
            pltpu.VMEM(chunks, bf16),
            pltpu.VMEM(chunks, bf16),
            pltpu.VMEM((2,) + chunks, bf16),
            pltpu.VMEM((4, D, width), bf16),
            pltpu.VMEM((2, 2, D // 2, width), bf16),
            pltpu.VMEM((2, D // 2, width), bf16),
            pltpu.VMEM((2, D // 2, width), bf16),
            pltpu.VMEM((D, width), bf16),
            pltpu.VMEM((D, width), bf16),
            rows_f32,
            rows_f32,
            pltpu.VMEM((4, shard_rows, qcols), bf16),
            pltpu.VMEM((3, shard_rows, qcols), bf16),
            pltpu.VMEM((4, shard_rows, width - qcols), bf16),
            pltpu.VMEM((3, shard_rows, width - qcols), bf16),
            rows_low,
            pltpu.VMEM((3, shard_rows // 4, width), bf16),
            pltpu.VMEM((shard_rows // 4, width), bf16),
            rows_low,
            rows_low,
            pltpu.VMEM((2, 8, D), f32),
            pltpu.VMEM((2, 4, 8, D), f32),
            square,
            square,
        ]
        + [dma((2, 4))] * 6
        + [dma((2,))] * 2
        + [dma((6, 3))] * 2
        + [dma((3, 3))] * 2
        + [dma((2, 2))] * 2
        + [dma((2,))] * 2
        + [dma((1,))]
        + [dma((8,))],
        name="back",
        cost_estimate=pl.CostEstimate(
            flops=110_000_000_000, bytes_accessed=60_000_000, transcendentals=0
        ),
        compiler_params=pltpu.CompilerParams(
            collective_id=1, has_side_effects=True, vmem_limit_bytes=66_000_000
        ),
    )(
        combine_padded,
        target,
        norm_gains,
        norm_biases,
        inward_moment,
        outward_moment,
        out_cot,
        tokens_in,
        state,
        gift,
        qkv_low,
        probs,
        weight,
        expert_w,
        arrived,
        grad_arrived,
        moment_shard,
    )
    factor_rows = pltpu.VMEM((shard_rows, D), f32)
    home_steps, attend_step = pl.pallas_call(
        finish_kernel,
        out_shape=(shape((4, shard_rows, width), bf16), shape((shard_rows, width), f32)),
        in_specs=[in_vmem] * 2,
        out_specs=(in_vmem, in_vmem),
        scratch_shapes=[square] * 5 + [factor_rows] * 2 + [dma((3,))] * 2 + [dma((2,))] * 2,
        name="finish",
        cost_estimate=pl.CostEstimate(
            flops=20_000_000_000, bytes_accessed=5_000_000, transcendentals=0
        ),
        compiler_params=pltpu.CompilerParams(collective_id=2, has_side_effects=True),
    )(attend_whole, own_steps)

    blocks = 4
    inward, outward = inward_master.shape, outward_master.shape
    expert = (EXP_DEV * shard_rows * width // LANES, LANES)

    def split(whole, along=0):
        if along is None:
            return pl.BlockSpec(whole, lambda i: (0,) * len(whole))
        rows = pl.cdiv(pl.cdiv(whole[along], blocks), 8) * 8
        block = whole[:along] + (rows,) + whole[along + 1 :]
        return pl.BlockSpec(
            block, lambda i: (0,) * along + (i,) + (0,) * (len(whole) - along - 1)
        )

    two, four, attended = (2, D), (4, D), (shard_rows, width)
    matrix_shapes = (inward, outward, expert, expert)
    by_rows = [split(m) for m in matrix_shapes]
    tokens = split((token_rows, D))
    finished = pl.pallas_call(
        apply_kernel,
        grid=(blocks,),
        out_shape=tuple(
            [shape((token_rows, D), bf16), shape((token_rows, D), f32)]
            + [shape(m, f32) for m in matrix_shapes]
            + [shape(two, f32)] * 2
            + [shape(m, f32) for m in matrix_shapes * 2]
            + [shape(m, bf16) for m in matrix_shapes]
            + [shape(two, f32)] * 2
            + [shape(four, f32)] * 2
        ),
        in_specs=[pl.BlockSpec(memory_space=pltpu.SMEM)]
        + [split((4,) + attended, 1), split(attended), split((4,) + attended, 1), split(attended)]
        + [split(four, None), split(two, None), split(two, None), split(four, None), split(four, None)]
        + by_rows * 2
        + [tokens] * 2,
        out_specs=tuple(
            [tokens] * 2
            + by_rows
            + [split(two, None)] * 2
            + by_rows * 3
            + [split(two, None)] * 2
            + [split(four, None)] * 2
        ),
        scratch_shapes=[pltpu.VMEM((2, expert[0] // blocks, LANES), f32)],
        name="apply",
        cost_estimate=pl.CostEstimate(
            flops=20_000_000, bytes_accessed=20_000_000, transcendentals=0
        ),
    )(
        step_count,
        home_steps,
        attend_step,
        home_grads,
        attend_grad,
        norm_total,
        norm_gains,
        norm_biases,
        first_moment,
        second_moment,
        inward_master,
        outward_master,
        woven(up_master),
        woven(down_master),
        inward_moment,
        outward_moment,
        woven(up_moment),
        woven(down_moment),
        block_out,
        input_gradient,
    )
    return tuple(
        unwoven(a, up_master.shape) if a.shape == expert else a for a in finished
    )


def solution(mesh):
    sizes = tuple(mesh.shape[axis] for axis in ("dp", "expert", "tensor"))
    body = pair_body if sizes == (4, 4, 2) else start_body
    return jax.shard_map(
        body,
        mesh=mesh,
        in_specs=(
            P(("dp", "expert"), None),
            P(("dp", "expert"), None),
            P(("dp", "expert"), None),
            P(("dp", "expert"), None),
            P("dp", "tensor"),
            P("dp", "tensor"),
            P("dp", "expert", "tensor"),
            P("dp", "expert", "tensor"),
            P(),
            P(),
            P("dp", "tensor"),
            P("dp", "tensor"),
            P("dp", "expert", "tensor"),
            P("dp", "expert", "tensor"),
            P(),
            P(),
            P(),
        ),
        out_specs=(
            P(("dp", "expert"), None),
            P(("dp", "expert"), None),
            P("dp", "tensor"),
            P("dp", "tensor"),
            P("dp", "expert", "tensor"),
            P("dp", "expert", "tensor"),
            P(),
            P(),
            P("dp", "tensor"),
            P("dp", "tensor"),
            P("dp", "expert", "tensor"),
            P("dp", "expert", "tensor"),
            P("dp", "tensor"),
            P("dp", "tensor"),
            P("dp", "expert", "tensor"),
            P("dp", "expert", "tensor"),
            P("dp", "tensor"),
            P("dp", "tensor"),
            P("dp", "expert", "tensor"),
            P("dp", "expert", "tensor"),
            P(),
            P(),
            P(),
            P(),
        ),
        check_vma=False,
    )
```

```python
import functools
import math

import jax
import jax.numpy as jnp
import numpy as np
from jax import lax
from jax.experimental import pallas as pl
from jax.experimental.pallas import tpu as pltpu
from jax.sharding import PartitionSpec as P

D = 512
HD = 64
F = 2048
SEQ = 197
EXP_DEV = 2


def layer_norm(values, gain_row, bias_row):
    center = values - jnp.mean(values, axis=-1, keepdims=True)
    invert = lax.rsqrt(jnp.mean(center * center, axis=-1, keepdims=True) + 1e-06)
    scaled = center * invert
    return (scaled * gain_row + bias_row, scaled, invert)


def norm_backward(upstream, scaled, invert, gain_row):
    weighted = upstream * gain_row
    return invert * (
        weighted
        - jnp.mean(weighted, axis=-1, keepdims=True)
        - scaled * jnp.mean(weighted * scaled, axis=-1, keepdims=True)
    )


def gelu_exact(values):
    return 0.5 * values * (1.0 + lax.erf(values * 0.7071067811865476))


def gelu_slope(values):
    return 0.5 * (
        1.0 + lax.erf(values * 0.7071067811865476)
    ) + values * 0.3989422804014327 * jnp.exp(-0.5 * values * values)


def newton_schulz(matrix):
    current = matrix / (jnp.sqrt(jnp.sum(matrix * matrix)) + 1e-07)
    for sweep_index in range(5):
        gram_matrix = jnp.dot(current, current.T, precision=lax.Precision.HIGHEST)
        polynom = -4.775 * gram_matrix + 2.0315 * jnp.dot(
            gram_matrix, gram_matrix, precision=lax.Precision.HIGHEST
        )
        current = 3.4445 * current + jnp.dot(polynom, current, precision=lax.Precision.HIGHEST)
    return current


def start_body(
    tokens_in,
    expert_ids,
    combine,
    out_cot,
    inward_master,
    outward_master,
    up_master,
    down_master,
    norm_gains,
    norm_biases,
    inward_moment,
    outward_moment,
    up_moment,
    down_moment,
    first_moment,
    second_moment,
    step_count,
):
    dp_count = lax.axis_size("dp")
    expert_count = lax.axis_size("expert")
    tensor_count = lax.axis_size("tensor")
    token_rows = tokens_in.shape[0]
    expert_total = EXP_DEV * expert_count
    capacity = (token_rows * 10 // (4 * expert_total) + 7) // 8 * 8
    slot_total = expert_total * capacity
    inputs = tokens_in.astype(jnp.float32)
    w_inward, w_outward, w_up, w_down = (
        lax.all_gather(inward_master.astype(jnp.bfloat16), "dp", axis=0, tiled=True),
        lax.all_gather(outward_master.astype(jnp.bfloat16), "dp", axis=0, tiled=True),
        lax.all_gather(up_master.astype(jnp.bfloat16), "dp", axis=0, tiled=True),
        lax.all_gather(down_master.astype(jnp.bfloat16), "dp", axis=0, tiled=True),
    )
    expert_lanes = jnp.arange(expert_total, dtype=jnp.int32)
    route_hits = (expert_ids[:, :, None] == expert_lanes).astype(jnp.int32)
    per_token = jnp.sum(route_hits, axis=1)
    earlier = jnp.cumsum(per_token, axis=0) - per_token
    position = jnp.sum(route_hits * earlier[:, None, :], axis=2)
    target = expert_ids * capacity + position
    select = (target[:, :, None] == jnp.arange(slot_total, dtype=jnp.int32)).astype(jnp.bfloat16)
    normed1, scaled1, invert1 = layer_norm(inputs, norm_gains[0], norm_biases[0])
    normed1_low = normed1.astype(jnp.bfloat16)
    qkv_low = jnp.dot(normed1_low, w_inward, preferred_element_type=jnp.float32).astype(
        jnp.bfloat16
    )
    heads_here = w_inward.shape[1] // (3 * HD)
    images = token_rows // SEQ
    split_heads = qkv_low.reshape(images, SEQ, heads_here, 3, HD)
    query_part = split_heads[:, :, :, 0]
    key_part = split_heads[:, :, :, 1]
    value_part = split_heads[:, :, :, 2]
    score_scale = HD ** (-0.5)
    scores = (
        jnp.einsum("bihd,bjhd->bhij", query_part, key_part, preferred_element_type=jnp.float32)
        * score_scale
    )
    row_max = jnp.max(scores, axis=-1, keepdims=True)
    exponent = jnp.exp(scores - row_max)
    row_total = jnp.sum(exponent, axis=-1, keepdims=True)
    softmax_out = exponent / row_total
    softmax_low = softmax_out.astype(jnp.bfloat16)
    heads_out = (
        jnp.einsum("bhij,bjhd->bihd", softmax_low, value_part, preferred_element_type=jnp.float32)
        .astype(jnp.bfloat16)
        .reshape(token_rows, heads_here * HD)
    )
    attend_part = jnp.einsum("tc,dc->td", heads_out, w_outward, preferred_element_type=jnp.float32)
    attended = lax.psum(attend_part, "tensor")
    state = inputs + attended
    normed2, scaled2, invert2 = layer_norm(state, norm_gains[1], norm_biases[1])
    normed2_low = normed2.astype(jnp.bfloat16)
    slots_out = jnp.einsum(
        "tks,td->sd", select, normed2_low, preferred_element_type=jnp.float32
    ).astype(jnp.bfloat16)
    arrived = lax.all_to_all(
        slots_out.reshape(expert_count, EXP_DEV, capacity, D),
        "expert",
        split_axis=0,
        concat_axis=0,
        tiled=True,
    )
    pre_act = jnp.einsum("secd,def->secf", arrived, w_up, preferred_element_type=jnp.float32)
    hidden_low = gelu_exact(pre_act).astype(jnp.bfloat16)
    expert_part = jnp.einsum(
        "secf,def->secd", hidden_low, w_down, preferred_element_type=jnp.float32
    ).astype(jnp.bfloat16)
    returned = lax.all_to_all(expert_part, "expert", split_axis=0, concat_axis=0, tiled=True)
    routed = jnp.einsum(
        "tks,sd->tkd", select, returned.reshape(slot_total, D), preferred_element_type=jnp.float32
    )
    mixed_part = jnp.sum(routed * combine[:, :, None], axis=1)
    mixed_sum = lax.psum(mixed_part, "tensor")
    block_out = (state + mixed_sum).astype(jnp.bfloat16)
    routed_grad = (combine[:, :, None] * out_cot[:, None, :]).astype(jnp.bfloat16)
    slot_grad = jnp.einsum(
        "tks,tkd->sd", select, routed_grad, preferred_element_type=jnp.float32
    ).astype(jnp.bfloat16)
    grad_arrived = lax.all_to_all(
        slot_grad.reshape(expert_count, EXP_DEV, capacity, D),
        "expert",
        split_axis=0,
        concat_axis=0,
        tiled=True,
    )
    hidden_grad = jnp.einsum(
        "secd,def->secf", grad_arrived, w_down, preferred_element_type=jnp.float32
    )
    pre_grad = (hidden_grad * gelu_slope(pre_act)).astype(jnp.bfloat16)
    down_local = jnp.einsum(
        "secd,secf->def", grad_arrived, hidden_low, preferred_element_type=jnp.float32
    )
    up_local = jnp.einsum("secd,secf->def", arrived, pre_grad, preferred_element_type=jnp.float32)
    entry_grad = jnp.einsum(
        "secf,def->secd", pre_grad, w_up, preferred_element_type=jnp.float32
    ).astype(jnp.bfloat16)
    entry_back = lax.all_to_all(entry_grad, "expert", split_axis=0, concat_axis=0, tiled=True)
    normed2_part = jnp.einsum(
        "tks,sd->td", select, entry_back.reshape(slot_total, D), preferred_element_type=jnp.float32
    )
    normed2_grad = lax.psum(normed2_part, "tensor")
    state_grad = out_cot + norm_backward(normed2_grad, scaled2, invert2, norm_gains[1])
    state_low = state_grad.astype(jnp.bfloat16)
    outward_local = jnp.einsum(
        "td,tc->dc", state_low, heads_out, preferred_element_type=jnp.float32
    )
    heads_grad = (
        jnp.dot(state_low, w_outward, preferred_element_type=jnp.float32)
        .astype(jnp.bfloat16)
        .reshape(images, SEQ, heads_here, HD)
    )
    prob_grad = jnp.einsum(
        "bihd,bjhd->bhij", heads_grad, value_part, preferred_element_type=jnp.float32
    )
    score_grad = (
        softmax_out * (prob_grad - jnp.sum(softmax_out * prob_grad, axis=-1, keepdims=True))
    ).astype(jnp.bfloat16)
    query_grad = (
        jnp.einsum("bhij,bjhd->bihd", score_grad, key_part, preferred_element_type=jnp.float32)
        * score_scale
    )
    key_grad = (
        jnp.einsum("bhij,bihd->bjhd", score_grad, query_part, preferred_element_type=jnp.float32)
        * score_scale
    )
    value_grad = jnp.einsum(
        "bhij,bihd->bjhd", softmax_low, heads_grad, preferred_element_type=jnp.float32
    )
    qkv_grad = (
        jnp.stack([query_grad, key_grad, value_grad], axis=3)
        .reshape(token_rows, heads_here * 3 * HD)
        .astype(jnp.bfloat16)
    )
    inward_local = jnp.einsum(
        "td,tc->dc", normed1_low, qkv_grad, preferred_element_type=jnp.float32
    )
    normed1_part = jnp.einsum("tc,dc->td", qkv_grad, w_inward, preferred_element_type=jnp.float32)
    normed1_grad = lax.psum(normed1_part, "tensor")
    input_gradient = state_grad + norm_backward(normed1_grad, scaled1, invert1, norm_gains[0])
    norm_terms = jnp.stack(
        [
            jnp.sum(normed1_grad * scaled1, axis=0),
            jnp.sum(normed2_grad * scaled2, axis=0),
            jnp.sum(normed1_grad, axis=0),
            jnp.sum(normed2_grad, axis=0),
        ]
    )
    inward_total, outward_total, norm_total = lax.psum(
        (inward_local, outward_local, norm_terms), ("dp", "expert")
    )
    up_gradient, down_gradient = (
        lax.psum_scatter(up_local, "dp", scatter_dimension=0, tiled=True),
        lax.psum_scatter(down_local, "dp", scatter_dimension=0, tiled=True),
    )
    shard_rows = D // dp_count
    dp_here = lax.axis_index("dp")
    inward_gradient = lax.dynamic_slice_in_dim(inward_total, dp_here * shard_rows, shard_rows, 0)
    outward_gradient = lax.dynamic_slice_in_dim(outward_total, dp_here * shard_rows, shard_rows, 0)
    inward_next = 0.95 * inward_moment + inward_gradient
    outward_next = 0.95 * outward_moment + outward_gradient
    up_next = 0.95 * up_moment + up_gradient
    down_next = 0.95 * down_moment + down_gradient
    matrices = [up_next[:, expert_slot] for expert_slot in range(EXP_DEV)]
    matrices = matrices + [down_next[:, expert_slot] for expert_slot in range(EXP_DEV)]
    matrices = matrices + [jnp.concatenate([inward_next, outward_next], axis=1)]
    stacked = jnp.stack(matrices)
    slot_count = len(matrices)
    group_size = dp_count * tensor_count
    shard_width = stacked.shape[2]
    query_cols = inward_next.shape[1]

    def orth_expert(pieces):
        whole_matrix = pieces.transpose(0, 2, 1, 3).reshape(D, tensor_count * shard_width)
        result = newton_schulz(whole_matrix) * (0.2 * math.sqrt(F))
        return result.reshape(dp_count, shard_rows, tensor_count, shard_width).transpose(0, 2, 1, 3)

    def orth_attention(pieces):
        inward_whole = (
            pieces[..., :query_cols].transpose(0, 2, 1, 3).reshape(D, tensor_count * query_cols)
        )
        outward_whole = (
            pieces[..., query_cols:]
            .transpose(0, 2, 1, 3)
            .reshape(D, tensor_count * (shard_width - query_cols))
        )
        inward_result = newton_schulz(inward_whole) * (0.2 * math.sqrt(3 * D))
        outward_result = newton_schulz(outward_whole) * (0.2 * math.sqrt(D))
        inward_blocks = inward_result.reshape(
            dp_count, shard_rows, tensor_count, query_cols
        ).transpose(0, 2, 1, 3)
        outward_blocks = outward_result.reshape(
            dp_count, shard_rows, tensor_count, shard_width - query_cols
        ).transpose(0, 2, 1, 3)
        return jnp.concatenate([inward_blocks, outward_blocks], axis=3)

    owner_index = lax.axis_index(("dp", "tensor"))
    outgoing = stacked[np.arange(group_size) % slot_count]
    received = lax.all_to_all(outgoing, ("dp", "tensor"), split_axis=0, concat_axis=0, tiled=True)
    blocks = received.reshape(dp_count, tensor_count, shard_rows, shard_width)
    slot_here = owner_index % slot_count
    result_blocks = lax.cond(slot_here == slot_count - 1, orth_attention, orth_expert, blocks)
    arrived_steps = lax.all_to_all(
        result_blocks.reshape(group_size, shard_rows, shard_width),
        ("dp", "tensor"),
        split_axis=0,
        concat_axis=0,
        tiled=True,
    )
    picked = []
    for owned_slot in range(slot_count):
        replicas = (group_size - owned_slot + slot_count - 1) // slot_count
        source = owned_slot + slot_count * (owner_index % replicas)
        picked.append(lax.dynamic_index_in_dim(arrived_steps, source, 0, keepdims=False))
    up_step = jnp.stack(picked[0:EXP_DEV], axis=1)
    down_step = jnp.stack(picked[EXP_DEV : 2 * EXP_DEV], axis=1)
    attend_step = picked[2 * EXP_DEV]
    inward_new = inward_master - 0.1 * (attend_step[:, :query_cols] + 0.1 * inward_master)
    outward_new = outward_master - 0.1 * (attend_step[:, query_cols:] + 0.1 * outward_master)
    up_new = up_master - 0.1 * (up_step + 0.1 * up_master)
    down_new = down_master - 0.1 * (down_step + 0.1 * down_master)
    moment_first = 0.9 * first_moment + 0.1 * norm_total
    moment_second = 0.999 * second_moment + 0.001 * norm_total * norm_total
    steps_done = step_count[0].astype(jnp.float32)
    direction = (
        moment_first
        / (1.0 - jnp.power(0.9, steps_done))
        / (jnp.sqrt(moment_second / (1.0 - jnp.power(0.999, steps_done))) + 1e-08)
    )
    params_new = jnp.concatenate([norm_gains, norm_biases], axis=0) - 0.1 * direction
    return (
        block_out,
        input_gradient,
        inward_gradient,
        outward_gradient,
        up_gradient,
        down_gradient,
        norm_total[0:2],
        norm_total[2:4],
        inward_next,
        outward_next,
        up_next,
        down_next,
        inward_new,
        outward_new,
        up_new,
        down_new,
        inward_new.astype(jnp.bfloat16),
        outward_new.astype(jnp.bfloat16),
        up_new.astype(jnp.bfloat16),
        down_new.astype(jnp.bfloat16),
        params_new[0:2],
        params_new[2:4],
        moment_first,
        moment_second,
    )


PAIRS = (1, 2, 3)
FAR_FIRST = (3, 2, 1, 0)
MIDWAY = 1
LANES = 128
NOWHERE = 128 * 128 - 1
PAD = 208
NT = (((1,), (1,)), ((), ()))
TN = (((0,), (0,)), ((), ()))


def mxu(left, right, dims=(((1,), (0,)), ((), ()))):
    return lax.dot_general(left, right, dims, preferred_element_type=jnp.float32)


def spread_rows(value, padded_ref):
    tail = jnp.zeros((PAD - SEQ, value.shape[1]), value.dtype)
    for image in range(value.shape[0] // SEQ):
        padded_ref[image * PAD : image * PAD + SEQ, :] = value[image * SEQ : (image + 1) * SEQ]
        padded_ref[image * PAD + SEQ : (image + 1) * PAD, :] = tail


def gather_rows(padded, out_ref):
    for image in range(out_ref.shape[0] // SEQ):
        out_ref[image * SEQ : (image + 1) * SEQ, :] = padded[
            image * PAD : image * PAD + SEQ
        ].astype(out_ref.dtype)


def peer(me, k):
    return (me + k) % 2 + 2 * ((me // 2 + k // 2) % 2)


def remote(source, target, send, recv, device):
    copy = pltpu.make_async_remote_copy(
        src_ref=source,
        dst_ref=target,
        send_sem=send,
        recv_sem=recv,
        device_id=device,
        device_id_type=pl.DeviceIdType.MESH,
    )
    copy.start()
    return copy


class Copy:
    def __init__(self, parts, start=True):
        self.parts = parts
        if start:
            self.make().start()

    def make(self):
        source, target, send, recv, device = self.parts()
        return pltpu.make_async_remote_copy(
            src_ref=source,
            dst_ref=target,
            send_sem=send,
            recv_sem=recv,
            device_id=device,
            device_id_type=pl.DeviceIdType.MESH,
        )

    def wait_recv(self):
        self.make().wait_recv()

    def wait_send(self):
        self.make().wait_send()


def keep(source, target, sem):
    copy = pltpu.make_async_copy(source, target, sem)
    copy.start()
    return copy


def greet(dp_here, expert_here, core, over_expert=True):
    barrier = pltpu.get_barrier_semaphore()
    devices = [{"dp": peer(dp_here, k)} for k in PAIRS] + [{"tensor": 1 - core}]
    if over_expert:
        devices += [{"expert": peer(expert_here, k)} for k in PAIRS]
    for device in devices:
        pl.semaphore_signal(
            barrier, inc=1, device_id=device, device_id_type=pl.DeviceIdType.MESH
        )
    return lambda: pl.semaphore_wait(barrier, len(devices))


def block_rows(index, size):
    return pl.ds(pl.multiple_of(index * size, size), size)


def one_hot(cond):
    return jnp.where(cond, 1.0, 0.0).astype(jnp.bfloat16)


def route(ids, capacity, target_ref, target_t_ref):
    rows = ids.shape[0]
    square = (PAD, PAD)
    below = one_hot(
        lax.broadcasted_iota(jnp.int32, square, 0) > lax.broadcasted_iota(jnp.int32, square, 1)
    )
    lane = lax.broadcasted_iota(jnp.int32, (rows, 128), 1)
    hits = one_hot((lane == ids[:, 0:1]) | (lane == ids[:, 1:2]))
    earlier, passed = [], jnp.zeros((1, 128), jnp.float32)
    for image in range(rows // PAD):
        own = hits[image * PAD : (image + 1) * PAD]
        earlier.append(mxu(below, own) + passed)
        passed += jnp.sum(own.astype(jnp.float32), axis=0, keepdims=True)
    earlier = jnp.concatenate(earlier, axis=0)
    target = jnp.zeros((rows, 128), jnp.int32)
    parts = jnp.zeros((rows, 128), jnp.int32)
    for r in range(2):
        own = ids[:, r : r + 1]
        position = jnp.sum(jnp.where(lane == own, earlier, 0.0), axis=1, keepdims=True)
        value = jnp.where(own >= 0, own * capacity + position.astype(jnp.int32), NOWHERE)
        target = jnp.where(lane == r, value, target)
        parts = jnp.where(lane == 2 * r, value // 128, jnp.where(lane == 2 * r + 1, value % 128, parts))
    target_ref[...] = target
    identity = one_hot(
        lax.broadcasted_iota(jnp.int32, (8, 128), 0) == lax.broadcasted_iota(jnp.int32, (8, 128), 1)
    )
    flipped = mxu(identity, parts.astype(jnp.float32).astype(jnp.bfloat16), NT).astype(jnp.int32)
    for r in range(2):
        target_t_ref[r : r + 1, :] = flipped[2 * r : 2 * r + 1] * 128 + flipped[2 * r + 1 : 2 * r + 2]


def attend(qkv_ref, probs_ref, gift_ref):
    heads_here = qkv_ref.shape[1] // (3 * HD)
    key_lane = lax.broadcasted_iota(jnp.int32, (PAD, PAD), 1)

    def one_image(image, carry):
        rows = block_rows(image, PAD)
        out_rows = pl.ds(pl.multiple_of(D + image * PAD, 16), PAD)
        for head in range(heads_here):
            base = head * 3 * HD
            query = qkv_ref[rows, base : base + HD]
            key = qkv_ref[rows, base + HD : base + 2 * HD]
            value = qkv_ref[rows, base + 2 * HD : base + 3 * HD]
            scores = jnp.where(key_lane < SEQ, mxu(query, key, NT) * HD ** (-0.5), -1e30)
            exponent = jnp.exp(scores - jnp.max(scores, axis=-1, keepdims=True))
            probs = exponent / jnp.sum(exponent, axis=-1, keepdims=True)
            probs_ref[image * heads_here + head] = probs
            gift_ref[out_rows, head * HD : (head + 1) * HD] = mxu(
                probs.astype(jnp.bfloat16), value
            ).astype(jnp.bfloat16)
        return carry

    lax.fori_loop(0, qkv_ref.shape[0] // PAD, one_image, 0)


def woven(array):
    rows, count, width = array.shape
    tiles = array.reshape(rows, count, width // LANES, LANES)
    return tiles.transpose(0, 2, 1, 3).reshape(-1, LANES)


def unwoven(array, whole):
    rows, count, width = whole
    tiles = array.reshape(rows, width // LANES, count, LANES)
    return tiles.transpose(0, 2, 1, 3).reshape(whole)


def strand(tile, expert, rows, width):
    step = EXP_DEV * (width // LANES)
    return pl.ds(EXP_DEV * tile + expert, rows, stride=step)


def front_kernel(
    ids_ref,
    combine_ref,
    cot_ref,
    tokens_ref,
    gains_ref,
    biases_ref,
    inward_ref,
    outward_ref,
    up_ref,
    down_ref,
    up_moment_ref,
    down_moment_ref,
    state_ref,
    gift_ref,
    qkv_ref,
    probs_ref,
    weight_ref,
    target_ref,
    combine_out_ref,
    moment_shard,
    expert_w_ref,
    arrived_ref,
    grad_arrived_ref,
    padded,
    columns,
    columns_padded,
    raw,
    target_t_ref,
    attend_shard,
    expert_shard,
    gift_other_ref,
    grad_chunks,
    token_chunks,
    inner_send,
    inner_recv,
    expert_send,
    expert_recv,
    slot_send,
    slot_recv,
    share_send,
    share_recv,
    gift_sems,
    keep_sems,
    raw_sems,
):
    bf16 = jnp.bfloat16
    dp_here, expert_here, core = (lax.axis_index(a) for a in ("dp", "expert", "tensor"))
    partner = {"tensor": 1 - core}
    capacity = grad_chunks.shape[1]
    shard_rows = attend_shard.shape[0]
    qcols = qkv_ref.shape[1]
    width = attend_shard.shape[1]
    here = block_rows(dp_here, shard_rows)
    ready = greet(dp_here, expert_here, core)
    loads = [
        keep(ref, raw.at[place], raw_sems.at[place])
        for place, ref in enumerate((up_ref, down_ref, up_moment_ref, down_moment_ref))
    ]

    def unpick(place, tile, expert):
        return raw[place, strand(tile, expert, shard_rows, width), :].astype(bf16)

    attend_shard[:, :qcols] = inward_ref[...].astype(bf16)
    attend_shard[:, qcols:] = outward_ref[...].astype(bf16)
    weight_ref[here, :] = attend_shard[...]
    ready()
    inner = [
        remote(
            attend_shard,
            weight_ref.at[here, :],
            inner_send.at[k - 1],
            inner_recv.at[k - 1],
            {"dp": peer(dp_here, k)},
        )
        for k in PAIRS
    ]
    kept = []

    rest = combine_ref[...]
    for part in range(3):
        piece = rest.astype(bf16).astype(jnp.float32)
        columns[2 * part : 2 * part + 2, :] = piece
        rest = rest - piece
    columns[6:8, :] = (ids_ref[...] + 1).astype(jnp.float32)
    identity = one_hot(
        lax.broadcasted_iota(jnp.int32, (8, 128), 0) == lax.broadcasted_iota(jnp.int32, (8, 128), 1)
    )
    spread_rows(mxu(columns[...].astype(bf16), identity, TN), columns_padded)
    for r in range(2):
        combine_out_ref[:, r : r + 1] = (
            columns_padded[:, r : r + 1]
            + columns_padded[:, 2 + r : 3 + r]
            + columns_padded[:, 4 + r : 5 + r]
        )
    ids = columns_padded[...].astype(jnp.int32) - 1
    route(ids[:, 6:8], capacity, target_ref, target_t_ref)
    spread_rows(cot_ref[...], padded)
    slot = lax.broadcasted_iota(jnp.int32, (capacity, padded.shape[0]), 0)

    def first_slot(k):
        return (2 * peer(expert_here, k) + core) * capacity

    def send_chunks(fill, chunks, landing, which):
        def going(k, start=True):
            return Copy(
                lambda: (
                    chunks.at[k],
                    landing.at[0, k],
                    slot_send.at[which, k],
                    slot_recv.at[which, k],
                    {"expert": peer(expert_here, k)},
                ),
                start,
            )

        def make(k):
            chunks[k] = fill(slot + first_slot(k)).astype(bf16)

        def make_and_send(step, carry):
            make(3 - step)

            @pl.when(step > 0)
            def send_last():
                going(4 - step)

            return carry

        lax.fori_loop(0, 4, make_and_send, 0)
        copies, shared = {k: going(k, start=False) for k in PAIRS}, []
        kept.append(keep(chunks.at[0], landing.at[0, 0], keep_sems.at[1 + which]))
        shared.append(
            remote(
                chunks.at[0],
                landing.at[1, 0],
                share_send.at[which, 0],
                share_recv.at[which, 0],
                partner,
            )
        )
        return copies, shared

    def share_arrivals(copies, landing, which, shared):
        for k in FAR_FIRST[:3]:
            copies[k].wait_recv()
            shared.append(
                remote(
                    landing.at[0, k],
                    landing.at[1, k],
                    share_send.at[which, k],
                    share_recv.at[which, k],
                    partner,
                )
            )

    grads = [(combine_out_ref[:, r : r + 1] * padded[...]).astype(bf16) for r in range(2)]
    grad_copies, grad_shared = send_chunks(
        lambda slots: sum(mxu(one_hot(target_t_ref[r : r + 1] == slots), grads[r]) for r in range(2)),
        grad_chunks,
        grad_arrived_ref,
        0,
    )
    for which in range(2):
        loads[which].wait()
        for tile in range(width // LANES):
            pair = [unpick(which, tile, e) for e in range(EXP_DEV)]
            lanes = slice(tile * LANES, (tile + 1) * LANES)
            for j in range(EXP_DEV):
                expert_shard[EXP_DEV * which + j, :, lanes] = jnp.where(
                    core == 0, pair[j], pair[1 - j]
                )
    spread_rows(tokens_ref[...].astype(jnp.float32), padded)
    normed, unused, unused = layer_norm(padded[...], gains_ref[0:1], biases_ref[0:1])
    normed_low = normed.astype(bf16)
    weights = [
        remote(
            expert_shard,
            expert_w_ref.at[:, here, :],
            expert_send.at[k - 1],
            expert_recv.at[k - 1],
            {"dp": peer(dp_here, k)},
        )
        for k in (1, 2)
    ]
    kept.append(keep(expert_shard, expert_w_ref.at[:, here, :], keep_sems.at[0]))
    for which in range(2):
        loads[2 + which].wait()
        for tile in range(width // LANES):
            for e in range(EXP_DEV):
                moment_shard[EXP_DEV * which + e, :, tile * LANES : (tile + 1) * LANES] = unpick(
                    2 + which, tile, e
                )
    for copy in inner:
        copy.wait_recv()
    qkv_ref[...] = mxu(normed_low, weight_ref[:, :qcols]).astype(bf16)
    gift_ref[0:D, :] = weight_ref[:, qcols:]
    attend(qkv_ref, probs_ref, gift_ref)
    gift = remote(gift_ref, gift_other_ref, gift_sems.at[0], gift_sems.at[1], partner)
    half = padded[...] + mxu(gift_ref[D:, :], gift_ref[0:D, :], NT)
    gift.wait()
    state = half + mxu(gift_other_ref[D:, :], gift_other_ref[0:D, :], NT)
    state_ref[...] = state
    normed, unused, unused = layer_norm(state, gains_ref[1:2], biases_ref[1:2])
    normed_low = normed.astype(bf16)
    token_copies, token_shared = send_chunks(
        lambda slots: mxu(
            one_hot((target_t_ref[0:1] == slots) | (target_t_ref[1:2] == slots)), normed_low
        ),
        token_chunks,
        arrived_ref,
        1,
    )
    for copy in weights:
        copy.wait_recv()
    for k, part in ((1, slice(0, EXP_DEV)), (2, slice(EXP_DEV, 2 * EXP_DEV))):
        block = expert_w_ref.at[part, block_rows(peer(dp_here, k), shard_rows), :]
        weights.append(
            remote(
                block,
                block,
                expert_send.at[k + 1],
                expert_recv.at[k + 1],
                {"dp": peer(dp_here, 3 - k)},
            )
        )
    share_arrivals(grad_copies, grad_arrived_ref, 0, grad_shared)
    share_arrivals(token_copies, arrived_ref, 1, token_shared)
    for copy in grad_shared + token_shared + weights[2:]:
        copy.wait()
    for copy in weights[:2] + inner:
        copy.wait_send()
    for copies in (grad_copies, token_copies):
        for k in PAIRS:
            copies[k].wait_send()
    for copy in kept:
        copy.wait()


def back_kernel(
    combine_ref,
    target_ref,
    gains_ref,
    biases_ref,
    inward_moment_ref,
    outward_moment_ref,
    cot_hbm,
    tokens_hbm,
    state_hbm,
    gift_hbm,
    qkv_hbm,
    probs_hbm,
    weight_hbm,
    expert_w_hbm,
    arrived_hbm,
    grad_arrived_hbm,
    moment_hbm,
    input_ref,
    block_ref,
    norm_ref,
    attend_grad_ref,
    attend_whole_ref,
    own_steps_ref,
    home_grads_ref,
    give,
    handed,
    summed,
    returned,
    matrices,
    near_in,
    far_out,
    far_in,
    moment_whole,
    owned_low,
    normed_part,
    normed_other,
    inner,
    inner_in,
    outer,
    outer_in,
    plane,
    quarter_in,
    quarter,
    plane_total,
    whole_own,
    norm_own,
    norm_in,
    gram,
    gram_other,
    hand_send,
    hand_recv,
    slot_send,
    slot_recv,
    share_send,
    share_recv,
    pair_send,
    pair_recv,
    dp_send,
    dp_recv,
    expert_send,
    expert_recv,
    near_send,
    near_recv,
    far_send,
    far_recv,
    own_sems,
    load_sems,
):
    bf16, f32 = jnp.bfloat16, jnp.float32
    dp_here, expert_here, core = (lax.axis_index(a) for a in ("dp", "expert", "tensor"))
    partner = {"tensor": 1 - core}
    capacity = give.shape[2]
    shard_rows = inner.shape[1]
    here = block_rows(dp_here, shard_rows)
    ready = greet(dp_here, expert_here, core)
    sent = []

    def to_dp(stage, sources, targets, peers=PAIRS):
        def copy(k):
            return Copy(
                lambda: (
                    sources(k),
                    targets(k),
                    dp_send.at[stage, k - 1],
                    dp_recv.at[stage, k - 1],
                    {"dp": peer(dp_here, k)},
                )
            )

        copies = [copy(k) for k in peers]
        sent.extend(copies)
        return copies

    def to_expert(stage, sources, targets):
        def copy(k):
            return Copy(
                lambda: (
                    sources(k),
                    targets(k),
                    expert_send.at[stage, k - 1],
                    expert_recv.at[stage, k - 1],
                    {"expert": peer(expert_here, k)},
                )
            )

        copies = [copy(k) for k in PAIRS]
        sent.extend(copies)
        return copies

    def arrive(copies):
        for copy in copies:
            copy.wait_recv()

    shares = ([], [])

    def hand(which, k, start=True):
        return Copy(
            lambda: (
                give.at[which, k],
                handed.at[which, k],
                hand_send.at[which, k],
                hand_recv.at[which, k],
                partner,
            ),
            start,
        )

    def add_up(which, k):
        hand(which, k, start=False).wait_recv()
        total = (summed[which, k].astype(f32) + handed[which, k].astype(f32)).astype(bf16)
        summed[which, k] = total

    def send_home(which, k, start=True):
        return Copy(
            lambda: (
                summed.at[which, k],
                returned.at[which, 0, k],
                slot_send.at[which, k],
                slot_recv.at[which, k],
                {"expert": peer(expert_here, k)},
            ),
            start,
        )

    def stay_home(which):
        returned[which, 0, 0] = summed[which, 0]
        shares[which].append(
            Copy(
                lambda: (
                    summed.at[which, 0],
                    returned.at[which, 1, 0],
                    share_send.at[which, 0],
                    share_recv.at[which, 0],
                    partner,
                )
            )
        )

    def share(which):
        def copy(k):
            return Copy(
                lambda: (
                    returned.at[which, 0, k],
                    returned.at[which, 1, k],
                    share_send.at[which, k],
                    share_recv.at[which, k],
                    partner,
                )
            )

        for k in FAR_FIRST[:3]:
            send_home(which, k, start=False).wait_recv()
            shares[which].append(copy(k))
        sent.extend(shares[which])

    def held(index):
        return 2 * (index // 2) + (index % 2 + core) % 2

    ways = ((slice(0, D // 2), 1, 2), (slice(D // 2, D), 2, 1))

    def near_copy(half, place):
        rows, first, second = ways[half]
        owner = (first, 3)[place]
        return Copy(
            lambda: (
                matrices.at[held(peer(dp_here, owner)), rows, :],
                near_in.at[half, place],
                near_send.at[half, place],
                near_recv.at[half, place],
                {"dp": peer(dp_here, first)},
            )
        )

    def far_copy(half):
        rows, first, second = ways[half]
        return Copy(
            lambda: (
                far_out.at[half],
                far_in.at[half],
                far_send.at[half],
                far_recv.at[half],
                {"dp": peer(dp_here, second)},
            )
        )

    def pass_on(near):
        arrive(near)
        for half, (rows, first, second) in enumerate(ways):
            far_out[half] = (
                matrices[held(peer(dp_here, second)), rows, :].astype(f32)
                + near_in[half, 1].astype(f32)
            ).astype(bf16)
        far = [far_copy(half) for half in range(2)]
        sent.extend(far)
        return far

    def experts(weights, rows, grads, hidden, pre_grad):
        loads = {}
        for j in (1, 0):
            for place, (source, target) in enumerate(
                (
                    (expert_w_hbm.at[j], weights.at[j]),
                    (arrived_hbm.at[j], rows.at[j]),
                    (expert_w_hbm.at[EXP_DEV + j], weights.at[EXP_DEV + j]),
                    (grad_arrived_hbm.at[j], grads.at[j]),
                )
            ):
                loads[j, place] = keep(source, target, load_sems.at[4 * j + place])
        ready()
        moments.extend(
            to_dp(0, lambda k: moment_hbm.at[peer(dp_here, k)], lambda k: moment_whole.at[here, :])
        )

        def chunk(k, step):
            def loaded(*places):
                @pl.when(step == 0)
                def wait():
                    for place in places:
                        loads[place].wait()

            for j in (1, 0):
                loaded((j, 0), (j, 1))
                pre = mxu(rows[j, k], weights[j])
                share_of_one = 0.5 * (1.0 + lax.erf(pre * 0.7071067811865476))
                hidden[j, k] = (pre * share_of_one).astype(bf16)
                slope = share_of_one + pre * 0.3989422804014327 * jnp.exp(-0.5 * pre * pre)
                loaded((j, 2), (j, 3))
                grad = (mxu(grads[j, k], weights[EXP_DEV + j]) * slope).astype(bf16)
                pre_grad[j, k] = grad
                entry = mxu(grad, weights[j], NT).astype(bf16)
                if j == 1:
                    give[0, k] = entry
                else:
                    summed[0, k] = entry

        def next_chunk(step, carry):
            chunk(3 - step, step)
            hand(0, 3 - step)

            @pl.when(step > 0)
            def last_chunk():
                add_up(0, 4 - step)
                send_home(0, 4 - step)

            return carry

        lax.fori_loop(0, 4, next_chunk, 0)

        def matrix(left, right, j):
            total = mxu(left[j, 0], right[j, 0], TN)
            for k in PAIRS:
                total += mxu(left[j, k], right[j, k], TN)
            return total.astype(bf16)

        def expert_matrices(j, carry):
            matrices[j] = matrix(rows, pre_grad, j)
            matrices[EXP_DEV + j] = matrix(grads, hidden, j)
            return carry

        lax.fori_loop(0, EXP_DEV, expert_matrices, 0)
        near = [near_copy(half, place) for place in (1, 0) for half in range(2)]
        sent.extend(near)
        add_up(0, 0)
        stay_home(0)

        def part_chunk(step, carry):
            k = 3 - step
            give[1, k] = mxu(hidden[1, k], weights[EXP_DEV + 1], NT).astype(bf16)
            summed[1, k] = mxu(hidden[0, k], weights[EXP_DEV], NT).astype(bf16)
            hand(1, k)
            return carry

        lax.fori_loop(0, 4, part_chunk, 0)
        for k in FAR_FIRST:
            add_up(1, k)
        for k in FAR_FIRST[:3]:
            send_home(1, k)
        stay_home(1)
        for which in range(2):
            sent.extend(hand(which, k, start=False) for k in range(4))
            sent.extend(send_home(which, k, start=False) for k in PAIRS)
        return near

    own_moment = keep(moment_hbm.at[dp_here], moment_whole.at[here, :], own_sems.at[0])
    near, moments = [], []
    slots = (EXP_DEV, 4, capacity)
    pl.run_scoped(
        lambda *refs: near.extend(experts(*refs)),
        pltpu.VMEM(expert_w_hbm.shape, bf16),
        pltpu.VMEM(slots + (D,), bf16),
        pltpu.VMEM(slots + (D,), bf16),
        pltpu.VMEM(slots + (expert_w_hbm.shape[2],), bf16),
        pltpu.VMEM(slots + (expert_w_hbm.shape[2],), bf16),
    )

    def backward(
        cot_ref,
        tokens_ref,
        state_ref,
        gift_ref,
        qkv_ref,
        probs_ref,
        weight_ref,
        padded,
        qkv_grad_ref,
        local_ref,
        out_grad_ref,
    ):
        loads = [
            keep(source, target, load_sems.at[place])
            for place, (source, target) in enumerate(
                (
                    (state_hbm, state_ref),
                    (cot_hbm, cot_ref),
                    (gift_hbm.at[D:, :], gift_ref),
                    (weight_hbm, weight_ref),
                    (qkv_hbm, qkv_ref),
                    (probs_hbm, probs_ref),
                    (tokens_hbm, tokens_ref),
                )
            )
        ]
        qcols = qkv_ref.shape[1]
        rows_all = state_ref.shape[0]
        loads[0].wait()
        unused, scaled2, invert2 = layer_norm(state_ref[...], gains_ref[1:2], biases_ref[1:2])
        loads[1].wait()
        spread_rows(cot_ref[...], padded)
        def pick_all(which, columns, rows, parts=(0, 1)):
            slot = lax.broadcasted_iota(jnp.int32, (PAD, capacity), 1)

            def picks(k, j):
                first = slot + (2 * peer(expert_here, k) + (core + j) % 2) * capacity
                hit = target_ref[rows, columns[0] : columns[0] + 1] == first
                for column in columns[1:]:
                    hit = hit | (target_ref[rows, column : column + 1] == first)
                return one_hot(hit)

            terms = [mxu(picks(k, j), returned[which, j, k]) for j in parts for k in FAR_FIRST]
            return sum(terms[1:], terms[0])

        share(0)

        def own_gradient(image, carry):
            rows = block_rows(image, PAD)
            normed_part[rows, :] = pick_all(0, (0, 1), rows, (0,))
            return carry

        def other_gradient(image, carry):
            rows = block_rows(image, PAD)
            normed_part[rows, :] += pick_all(0, (0, 1), rows, (1,))
            return carry

        lax.fori_loop(0, rows_all // PAD, own_gradient, 0)
        arrive(shares[0])
        lax.fori_loop(0, rows_all // PAD, other_gradient, 0)
        normed2_grad = normed_part[...]
        norm_own[0, 4:8] = jnp.zeros((4, D), f32)
        norm_own[0, 1:2] = jnp.sum(normed2_grad * scaled2, axis=0, keepdims=True)
        norm_own[0, 3:4] = jnp.sum(normed2_grad, axis=0, keepdims=True)
        state_grad = padded[...] + norm_backward(normed2_grad, scaled2, invert2, gains_ref[1:2])
        padded[...] = state_grad
        state_low = state_grad.astype(bf16)
        for copy in loads[2:]:
            copy.wait()

        local_ref[:, qcols:] = mxu(state_low, gift_ref[...], TN)
        for k in range(4):
            outer[k] = local_ref[block_rows(peer(dp_here, k), shard_rows), qcols:].astype(bf16)
        out_grad_ref[...] = mxu(state_low, weight_ref[:, qcols:]).astype(bf16)
        outward_sums = to_dp(5, lambda k: outer.at[k], lambda k: outer_in.at[k - 1])
        heads_here = qcols // (3 * HD)
        scale = HD ** (-0.5)

        def one_image(image, carry):
            rows = block_rows(image, PAD)
            for head in range(heads_here):
                base = head * 3 * HD
                query = qkv_ref[rows, base : base + HD]
                key = qkv_ref[rows, base + HD : base + 2 * HD]
                value = qkv_ref[rows, base + 2 * HD : base + 3 * HD]
                out_grad = out_grad_ref[rows, head * HD : (head + 1) * HD]
                probs = probs_ref[image * heads_here + head]
                prob_grad = mxu(out_grad, value, NT)
                score_grad = (
                    probs * (prob_grad - jnp.sum(probs * prob_grad, axis=-1, keepdims=True))
                ).astype(bf16)
                qkv_grad_ref[rows, base : base + HD] = (mxu(score_grad, key) * scale).astype(bf16)
                qkv_grad_ref[rows, base + HD : base + 2 * HD] = (
                    mxu(score_grad, query, TN) * scale
                ).astype(bf16)
                qkv_grad_ref[rows, base + 2 * HD : base + 3 * HD] = mxu(
                    probs.astype(bf16), out_grad, TN
                ).astype(bf16)
            return carry

        lax.fori_loop(0, rows_all // PAD, one_image, 0)
        spread_rows(tokens_ref[...].astype(f32), normed_part)
        normed1, scaled1, invert1 = layer_norm(normed_part[...], gains_ref[0:1], biases_ref[0:1])
        local_ref[:, :qcols] = mxu(normed1.astype(bf16), qkv_grad_ref[...], TN)
        for k in range(4):
            inner[k] = local_ref[block_rows(peer(dp_here, k), shard_rows), :qcols].astype(bf16)
        normed_part[...] = mxu(qkv_grad_ref[...], weight_ref[:, :qcols], NT)
        rows_sums = to_dp(1, lambda k: inner.at[k], lambda k: inner_in.at[k - 1]) + outward_sums
        pair = Copy(
            lambda: (normed_part, normed_other, pair_send.at[0], pair_recv.at[0], partner)
        )
        sent.append(pair)
        far = pass_on(near)

        share(1)
        arrive(shares[1])

        def one_output(image, carry):
            rows = block_rows(image, PAD)
            total = state_ref[rows, :]
            for r in range(2):
                total += combine_ref[rows, r : r + 1] * pick_all(1, (r,), rows)
            state_ref[rows, :] = total
            return carry

        lax.fori_loop(0, rows_all // PAD, one_output, 0)
        gather_rows(state_ref[...], block_ref)

        pair.wait_recv()
        normed1_grad = normed_part[...] + normed_other[...]
        norm_own[0, 0:1] = jnp.sum(normed1_grad * scaled1, axis=0, keepdims=True)
        norm_own[0, 2:3] = jnp.sum(normed1_grad, axis=0, keepdims=True)
        norm_in[0, dp_here] = norm_own[0]
        norms = to_dp(2, lambda k: norm_own.at[0], lambda k: norm_in.at[0, dp_here])
        gather_rows(
            padded[...] + norm_backward(normed1_grad, scaled1, invert1, gains_ref[0:1]), input_ref
        )
        return rows_sums, norms, far

    travelling = []
    rows_f32 = pltpu.VMEM(state_hbm.shape, f32)
    pl.run_scoped(
        lambda *refs: travelling.extend(backward(*refs)),
        pltpu.VMEM(cot_hbm.shape, f32),
        pltpu.VMEM(tokens_hbm.shape, bf16),
        rows_f32,
        pltpu.VMEM((gift_hbm.shape[0] - D, gift_hbm.shape[1]), bf16),
        pltpu.VMEM(qkv_hbm.shape, bf16),
        pltpu.VMEM(probs_hbm.shape, f32),
        pltpu.VMEM(weight_hbm.shape, bf16),
        rows_f32,
        pltpu.VMEM(qkv_hbm.shape, bf16),
        pltpu.VMEM(weight_hbm.shape, f32),
        pltpu.VMEM((state_hbm.shape[0], gift_hbm.shape[1]), bf16),
    )
    rows_sums, norms, far = travelling

    arrive(rows_sums)
    qcols = inner.shape[2]
    for columns, own, got in (
        (slice(0, qcols), inner, inner_in),
        (slice(qcols, None), outer, outer_in),
    ):
        plane[:, columns] = (
            own[0].astype(f32)
            + got[0].astype(f32)
            + got[1].astype(f32)
            + got[2].astype(f32)
        ).astype(bf16)
    quarter_rows = quarter.shape[0]
    my_quarter = block_rows(expert_here, quarter_rows)
    quarters = to_expert(
        0,
        lambda k: plane.at[block_rows(peer(expert_here, k), quarter_rows), :],
        lambda k: quarter_in.at[k - 1],
    )
    arrive(norms)
    norm_plane = norm_in[0, 0] + norm_in[0, 1] + norm_in[0, 2] + norm_in[0, 3]
    norm_own[1] = norm_plane
    norm_in[1, expert_here] = norm_plane
    norm_sums = to_expert(1, lambda k: norm_own.at[1], lambda k: norm_in.at[1, expert_here])

    def orthogonalize(owned_next, factor, change):
        arrive(quarters)
        quarter[...] = (
            plane[my_quarter, :].astype(f32)
            + quarter_in[0].astype(f32)
            + quarter_in[1].astype(f32)
            + quarter_in[2].astype(f32)
        ).astype(bf16)
        plane_total[my_quarter, :] = quarter[...]
        totals = to_expert(2, lambda k: quarter, lambda k: plane_total.at[my_quarter, :])
        arrive(far + moments)
        own_moment.wait()
        for half, (rows, first, second) in enumerate(ways):
            owned = (
                matrices[held(dp_here), rows, :].astype(f32)
                + near_in[half, 0].astype(f32)
                + far_in[half].astype(f32)
            )
            owned_low[rows, :] = owned.astype(bf16)
            owned_next[rows, :] = 0.95 * moment_whole[rows, :].astype(f32) + owned
        split = halves(owned_next[...])
        gram[...] = mxu3(split, split, NT)
        pair = remote(gram, gram_other, pair_send.at[1], pair_recv.at[1], partner)

        def send_rows(peers):
            return to_dp(
                3,
                lambda k: owned_low.at[block_rows(peer(dp_here, k), shard_rows), :],
                lambda k: home_grads_ref.at[dp_here],
                peers,
            )

        home = send_rows((1, 2))
        own = keep(owned_low.at[here, :], home_grads_ref.at[dp_here], load_sems.at[1])
        pair.wait()

        def attention_next():
            arrive(totals)
            total = plane_total[...].astype(f32)
            attend_grad_ref[...] = total
            whole_own[:, :qcols] = (0.95 * inward_moment_ref[...] + total[:, :qcols]).astype(bf16)
            whole_own[:, qcols:] = (0.95 * outward_moment_ref[...] + total[:, qcols:]).astype(bf16)
            attend_whole_ref[here, :] = whole_own[...]
            wholes.extend(to_dp(4, lambda k: whole_own, lambda k: attend_whole_ref.at[here, :]))
            home.extend(send_rows((3,)))

        wholes = []
        find_factor(gram[...] + gram_other[...], factor, gram, change, gram_other, attention_next)
        own_steps_ref[...] = (
            mxu3(halves(factor[...]), halves(owned_next[...])) * (0.2 * math.sqrt(F))
        ).astype(bf16)
        arrive(norm_sums)
        norm_ref[...] = (
            norm_in[1, 0, 0:4] + norm_in[1, 1, 0:4] + norm_in[1, 2, 0:4] + norm_in[1, 3, 0:4]
        )
        arrive(home)
        arrive(wholes)
        own.wait()

    square = pltpu.VMEM((D, D), f32)
    pl.run_scoped(orthogonalize, pltpu.VMEM(moment_whole.shape, f32), square, square)
    for copy in sent:
        copy.wait_send()


def halves(value):
    high = value.astype(jnp.bfloat16)
    return high, (value - high.astype(jnp.float32)).astype(jnp.bfloat16)


def mxu3(left, right, dims=(((1,), (0,)), ((), ()))):
    return (
        mxu(left[0], right[0], dims) + mxu(left[1], right[0], dims) + mxu(left[0], right[1], dims)
    )


def find_factor(gram, factor, current, change, scaled, between=None):
    diagonal = lax.broadcasted_iota(jnp.int32, gram.shape, 0) == lax.broadcasted_iota(
        jnp.int32, gram.shape, 1
    )
    squares = jnp.sum(
        jnp.sum(jnp.where(diagonal, gram, 0.0), axis=1, keepdims=True), axis=0, keepdims=True
    )
    norm = jnp.sqrt(squares) + 1e-07
    current[...] = gram / (norm * norm)
    factor[...] = jnp.where(diagonal, 1.0 / norm, 0.0)
    half = D // 2

    def product(out, left, right, by, added, added_by):
        upper = by * mxu3([x[:half] for x in left], right) + added_by * added[:half, :]
        corner = mxu3([x[half:] for x in left], [x[:, half:] for x in right])
        corner = by * corner + added_by * added[half:, half:]
        out[:half, :] = upper
        out[half:, :half] = upper[:, half:].T
        out[half:, half:] = corner

    def polynomial():
        low = halves(current[...])
        product(change, low, low, 2.0315, current, -4.775)
        step = halves(change[...])
        product(factor, step, halves(factor[...]), 1.0, factor, 3.4445)
        return low, step

    def sweep(index, carry):
        if between is not None:
            pl.when(index == MIDWAY)(between)
        low, step = polynomial()
        product(scaled, step, low, 1.0, current, 3.4445)
        product(current, halves(scaled[...]), step, 1.0, scaled, 3.4445)
        return carry

    lax.fori_loop(0, 4, sweep, 0)
    polynomial()


def finish_kernel(
    whole_ref,
    own_steps_ref,
    home_steps_ref,
    attend_step_ref,
    kept,
    given,
    taken,
    factor,
    change,
    mine,
    other,
    step_send,
    step_recv,
    pair_send,
    pair_recv,
):
    dp_here, core = lax.axis_index("dp"), lax.axis_index("tensor")
    partner = {"tensor": 1 - core}
    shard_rows = mine.shape[0]
    qcols = 3 * whole_ref.shape[1] // 4
    here = block_rows(dp_here, shard_rows)
    ready = greet(dp_here, None, core, over_expert=False)
    inward_gram = mxu(whole_ref[:, :qcols], whole_ref[:, :qcols], NT)
    outward_gram = mxu(whole_ref[:, qcols:], whole_ref[:, qcols:], NT)
    kept[...] = jnp.where(core == 0, inward_gram, outward_gram)
    given[...] = jnp.where(core == 0, outward_gram, inward_gram)
    ready()
    pair = remote(given, taken, pair_send.at[0], pair_recv.at[0], partner)
    steps = [
        remote(
            own_steps_ref.at[block_rows(peer(dp_here, k), shard_rows), :],
            home_steps_ref.at[dp_here],
            step_send.at[k - 1],
            step_recv.at[k - 1],
            {"dp": peer(dp_here, k)},
        )
        for k in PAIRS
    ]
    home_steps_ref[dp_here] = own_steps_ref[here, :]
    pair.wait()
    find_factor(kept[...] + taken[...], factor, kept, change, taken)
    mine[...] = factor[here, :]
    pair = remote(mine, other, pair_send.at[1], pair_recv.at[1], partner)
    for copy in steps:
        copy.wait()
    pair.wait()
    for owner, columns, count in ((0, slice(0, qcols), 3 * D), (1, slice(qcols, None), D)):
        rows = halves(jnp.where(core == owner, mine[...], other[...]))
        step = mxu(rows[0], whole_ref[:, columns]) + mxu(rows[1], whole_ref[:, columns])
        attend_step_ref[:, columns] = step * (0.2 * math.sqrt(count))


def apply_kernel(
    steps_done_ref,
    home_steps_ref,
    attend_step_ref,
    home_grads_ref,
    attend_grad_ref,
    norm_ref,
    gains_ref,
    biases_ref,
    first_ref,
    second_ref,
    inward_ref,
    outward_ref,
    up_ref,
    down_ref,
    inward_moment_ref,
    outward_moment_ref,
    up_moment_ref,
    down_moment_ref,
    block_ref,
    input_ref,
    block_out_ref,
    input_out_ref,
    inward_gradient_ref,
    outward_gradient_ref,
    up_gradient_ref,
    down_gradient_ref,
    gain_gradient_ref,
    bias_gradient_ref,
    inward_next_ref,
    outward_next_ref,
    up_next_ref,
    down_next_ref,
    inward_new_ref,
    outward_new_ref,
    up_new_ref,
    down_new_ref,
    inward_copy_ref,
    outward_copy_ref,
    up_copy_ref,
    down_copy_ref,
    gains_new_ref,
    biases_new_ref,
    first_new_ref,
    second_new_ref,
    weave,
):
    f32 = jnp.float32
    qcols = inward_ref.shape[1]
    block_out_ref[...] = block_ref[...]
    input_out_ref[...] = input_ref[...]

    def finish(place, gradient, step, refs):
        master_ref, moment_ref, gradient_ref, next_ref, new_ref, copy_ref = refs
        gradient_ref[place] = gradient
        next_ref[place] = 0.95 * moment_ref[place] + gradient
        master = master_ref[place]
        new = master - 0.1 * (step + 0.1 * master)
        new_ref[place] = new
        copy_ref[place] = new.astype(copy_ref.dtype)

    experts = (
        (up_ref, up_moment_ref, up_gradient_ref, up_next_ref, up_new_ref, up_copy_ref),
        (down_ref, down_moment_ref, down_gradient_ref, down_next_ref, down_new_ref, down_copy_ref),
    )
    everything = (slice(None), slice(None))
    rows, width = attend_grad_ref.shape
    for which, refs in enumerate(experts):
        for place, home_ref in enumerate((home_grads_ref, home_steps_ref)):
            for e in range(EXP_DEV):
                for tile in range(width // LANES):
                    weave[place, strand(tile, e, rows, width), :] = home_ref[
                        EXP_DEV * which + e, :, tile * LANES : (tile + 1) * LANES
                    ].astype(f32)
        finish(everything, weave[0], weave[1], refs)
    finish(
        everything,
        attend_grad_ref[:, :qcols],
        attend_step_ref[:, :qcols],
        (
            inward_ref,
            inward_moment_ref,
            inward_gradient_ref,
            inward_next_ref,
            inward_new_ref,
            inward_copy_ref,
        ),
    )
    finish(
        everything,
        attend_grad_ref[:, qcols:],
        attend_step_ref[:, qcols:],
        (
            outward_ref,
            outward_moment_ref,
            outward_gradient_ref,
            outward_next_ref,
            outward_new_ref,
            outward_copy_ref,
        ),
    )

    @pl.when(pl.program_id(0) == 0)
    def norms():
        total = norm_ref[...]
        gain_gradient_ref[...] = total[0:2]
        bias_gradient_ref[...] = total[2:4]
        moment_first = 0.9 * first_ref[...] + 0.1 * total
        moment_second = 0.999 * second_ref[...] + 0.001 * total * total
        first_new_ref[...] = moment_first
        second_new_ref[...] = moment_second
        done = jnp.full((4, D), steps_done_ref[0], jnp.int32).astype(f32)
        direction = (
            moment_first
            / (1.0 - jnp.power(0.9, done))
            / (jnp.sqrt(moment_second / (1.0 - jnp.power(0.999, done))) + 1e-08)
        )
        gains_new_ref[...] = gains_ref[...] - 0.1 * direction[0:2]
        biases_new_ref[...] = biases_ref[...] - 0.1 * direction[2:4]


def pair_body(
    tokens_in,
    expert_ids,
    combine,
    out_cot,
    inward_master,
    outward_master,
    up_master,
    down_master,
    norm_gains,
    norm_biases,
    inward_moment,
    outward_moment,
    up_moment,
    down_moment,
    first_moment,
    second_moment,
    step_count,
):
    bf16, f32 = jnp.bfloat16, jnp.float32
    token_rows = tokens_in.shape[0]
    expert_total = EXP_DEV * 4
    capacity = (token_rows * 10 // (4 * expert_total) + 7) // 8 * 8
    shard_rows, qcols = inward_master.shape
    width = up_master.shape[2]
    images = token_rows // SEQ
    padded_rows = images * PAD
    heads_here = qcols // (3 * HD)
    shape = jax.ShapeDtypeStruct
    rows_f32 = pltpu.VMEM((padded_rows, D), f32)
    in_vmem, anywhere = pl.BlockSpec(memory_space=pltpu.VMEM), pl.BlockSpec(memory_space=pl.ANY)
    dma = pltpu.SemaphoreType.DMA

    slots = shape((EXP_DEV, 4, capacity, D), bf16)
    (
        state,
        gift,
        qkv_low,
        probs,
        weight,
        target,
        combine_padded,
        moment_shard,
        expert_w,
        arrived,
        grad_arrived,
    ) = pl.pallas_call(
        front_kernel,
        out_shape=(
            shape((padded_rows, D), f32),
            shape((D + padded_rows, heads_here * HD), bf16),
            shape((padded_rows, qcols), bf16),
            shape((images * heads_here, PAD, PAD), f32),
            shape((D, width), bf16),
            shape((padded_rows, 128), jnp.int32),
            shape((padded_rows, 2), f32),
            shape((4, shard_rows, width), bf16),
            shape((2 * EXP_DEV, D, width), bf16),
            slots,
            slots,
        ),
        in_specs=[in_vmem] * 8 + [anywhere] * 4,
        out_specs=tuple([in_vmem] * 8 + [anywhere] * 3),
        scratch_shapes=[
            rows_f32,
            pltpu.VMEM((8, token_rows), f32),
            pltpu.VMEM((padded_rows, 128), f32),
            pltpu.VMEM((4, EXP_DEV * shard_rows * width // LANES, LANES), f32),
            pltpu.VMEM((2, padded_rows), jnp.int32),
            pltpu.VMEM((shard_rows, width), bf16),
            pltpu.VMEM((4, shard_rows, width), bf16),
            pltpu.VMEM((D + padded_rows, heads_here * HD), bf16),
            pltpu.VMEM((4, capacity, D), bf16),
            pltpu.VMEM((4, capacity, D), bf16),
            dma((3,)),
            dma((3,)),
            dma((4,)),
            dma((4,)),
            dma((2, 4)),
            dma((2, 4)),
            dma((2, 4)),
            dma((2, 4)),
            dma((2,)),
            dma((3,)),
            dma((4,)),
        ],
        name="front",
        cost_estimate=pl.CostEstimate(
            flops=60_000_000_000, bytes_accessed=30_000_000, transcendentals=0
        ),
        compiler_params=pltpu.CompilerParams(collective_id=0, has_side_effects=True),
    )(
        expert_ids.T,
        combine.T,
        out_cot,
        tokens_in,
        norm_gains,
        norm_biases,
        inward_master,
        outward_master,
        *(woven(a) for a in (up_master, down_master, up_moment, down_moment)),
    )
    chunks = (2, 4, capacity, D)
    square = pltpu.VMEM((D, D), f32)
    rows_low = pltpu.VMEM((shard_rows, width), bf16)
    (
        input_gradient,
        block_out,
        norm_total,
        attend_grad,
        attend_whole,
        own_steps,
        home_grads,
    ) = pl.pallas_call(
        back_kernel,
        out_shape=(
            shape((token_rows, D), f32),
            shape((token_rows, D), bf16),
            shape((4, D), f32),
            shape((shard_rows, width), f32),
            shape((D, width), bf16),
            shape((D, width), bf16),
            shape((4, shard_rows, width), bf16),
        ),
        in_specs=[in_vmem] * 6 + [anywhere] * 11,
        out_specs=tuple([in_vmem] * 6 + [anywhere]),
        scratch_shapes=[
            pltpu.VMEM(chunks, bf16),
            pltpu.VMEM(chunks, bf16),
            pltpu.VMEM(chunks, bf16),
            pltpu.VMEM((2,) + chunks, bf16),
            pltpu.VMEM((4, D, width), bf16),
            pltpu.VMEM((2, 2, D // 2, width), bf16),
            pltpu.VMEM((2, D // 2, width), bf16),
            pltpu.VMEM((2, D // 2, width), bf16),
            pltpu.VMEM((D, width), bf16),
            pltpu.VMEM((D, width), bf16),
            rows_f32,
            rows_f32,
            pltpu.VMEM((4, shard_rows, qcols), bf16),
            pltpu.VMEM((3, shard_rows, qcols), bf16),
            pltpu.VMEM((4, shard_rows, width - qcols), bf16),
            pltpu.VMEM((3, shard_rows, width - qcols), bf16),
            rows_low,
            pltpu.VMEM((3, shard_rows // 4, width), bf16),
            pltpu.VMEM((shard_rows // 4, width), bf16),
            rows_low,
            rows_low,
            pltpu.VMEM((2, 8, D), f32),
            pltpu.VMEM((2, 4, 8, D), f32),
            square,
            square,
        ]
        + [dma((2, 4))] * 6
        + [dma((2,))] * 2
        + [dma((6, 3))] * 2
        + [dma((3, 3))] * 2
        + [dma((2, 2))] * 2
        + [dma((2,))] * 2
        + [dma((1,))]
        + [dma((8,))],
        name="back",
        cost_estimate=pl.CostEstimate(
            flops=110_000_000_000, bytes_accessed=60_000_000, transcendentals=0
        ),
        compiler_params=pltpu.CompilerParams(
            collective_id=1, has_side_effects=True, vmem_limit_bytes=66_000_000
        ),
    )(
        combine_padded,
        target,
        norm_gains,
        norm_biases,
        inward_moment,
        outward_moment,
        out_cot,
        tokens_in,
        state,
        gift,
        qkv_low,
        probs,
        weight,
        expert_w,
        arrived,
        grad_arrived,
        moment_shard,
    )
    factor_rows = pltpu.VMEM((shard_rows, D), f32)
    home_steps, attend_step = pl.pallas_call(
        finish_kernel,
        out_shape=(shape((4, shard_rows, width), bf16), shape((shard_rows, width), f32)),
        in_specs=[in_vmem] * 2,
        out_specs=(in_vmem, in_vmem),
        scratch_shapes=[square] * 5 + [factor_rows] * 2 + [dma((3,))] * 2 + [dma((2,))] * 2,
        name="finish",
        cost_estimate=pl.CostEstimate(
            flops=20_000_000_000, bytes_accessed=5_000_000, transcendentals=0
        ),
        compiler_params=pltpu.CompilerParams(collective_id=2, has_side_effects=True),
    )(attend_whole, own_steps)

    blocks = 4
    inward, outward = inward_master.shape, outward_master.shape
    expert = (EXP_DEV * shard_rows * width // LANES, LANES)

    def split(whole, along=0):
        if along is None:
            return pl.BlockSpec(whole, lambda i: (0,) * len(whole))
        rows = pl.cdiv(pl.cdiv(whole[along], blocks), 8) * 8
        block = whole[:along] + (rows,) + whole[along + 1 :]
        return pl.BlockSpec(
            block, lambda i: (0,) * along + (i,) + (0,) * (len(whole) - along - 1)
        )

    two, four, attended = (2, D), (4, D), (shard_rows, width)
    matrix_shapes = (inward, outward, expert, expert)
    by_rows = [split(m) for m in matrix_shapes]
    tokens = split((token_rows, D))
    finished = pl.pallas_call(
        apply_kernel,
        grid=(blocks,),
        out_shape=tuple(
            [shape((token_rows, D), bf16), shape((token_rows, D), f32)]
            + [shape(m, f32) for m in matrix_shapes]
            + [shape(two, f32)] * 2
            + [shape(m, f32) for m in matrix_shapes * 2]
            + [shape(m, bf16) for m in matrix_shapes]
            + [shape(two, f32)] * 2
            + [shape(four, f32)] * 2
        ),
        in_specs=[pl.BlockSpec(memory_space=pltpu.SMEM)]
        + [split((4,) + attended, 1), split(attended), split((4,) + attended, 1), split(attended)]
        + [split(four, None), split(two, None), split(two, None), split(four, None), split(four, None)]
        + by_rows * 2
        + [tokens] * 2,
        out_specs=tuple(
            [tokens] * 2
            + by_rows
            + [split(two, None)] * 2
            + by_rows * 3
            + [split(two, None)] * 2
            + [split(four, None)] * 2
        ),
        scratch_shapes=[pltpu.VMEM((2, expert[0] // blocks, LANES), f32)],
        name="apply",
        cost_estimate=pl.CostEstimate(
            flops=20_000_000, bytes_accessed=20_000_000, transcendentals=0
        ),
    )(
        step_count,
        home_steps,
        attend_step,
        home_grads,
        attend_grad,
        norm_total,
        norm_gains,
        norm_biases,
        first_moment,
        second_moment,
        inward_master,
        outward_master,
        woven(up_master),
        woven(down_master),
        inward_moment,
        outward_moment,
        woven(up_moment),
        woven(down_moment),
        block_out,
        input_gradient,
    )
    return tuple(
        unwoven(a, up_master.shape) if a.shape == expert else a for a in finished
    )


def solution(mesh):
    sizes = tuple(mesh.shape[axis] for axis in ("dp", "expert", "tensor"))
    body = pair_body if sizes == (4, 4, 2) else start_body
    return jax.shard_map(
        body,
        mesh=mesh,
        in_specs=(
            P(("dp", "expert"), None),
            P(("dp", "expert"), None),
            P(("dp", "expert"), None),
            P(("dp", "expert"), None),
            P("dp", "tensor"),
            P("dp", "tensor"),
            P("dp", "expert", "tensor"),
            P("dp", "expert", "tensor"),
            P(),
            P(),
            P("dp", "tensor"),
            P("dp", "tensor"),
            P("dp", "expert", "tensor"),
            P("dp", "expert", "tensor"),
            P(),
            P(),
            P(),
        ),
        out_specs=(
            P(("dp", "expert"), None),
            P(("dp", "expert"), None),
            P("dp", "tensor"),
            P("dp", "tensor"),
            P("dp", "expert", "tensor"),
            P("dp", "expert", "tensor"),
            P(),
            P(),
            P("dp", "tensor"),
            P("dp", "tensor"),
            P("dp", "expert", "tensor"),
            P("dp", "expert", "tensor"),
            P("dp", "tensor"),
            P("dp", "tensor"),
            P("dp", "expert", "tensor"),
            P("dp", "expert", "tensor"),
            P("dp", "tensor"),
            P("dp", "tensor"),
            P("dp", "expert", "tensor"),
            P("dp", "expert", "tensor"),
            P(),
            P(),
            P(),
            P(),
        ),
        check_vma=False,
    )
```
